32 devices in a mesh: dp: 8 (over y, x, core), tensor: 4 (over z).
Axes of the slice: x: 2, y: 2, z: 4, core: 2. Of those that a mesh axis runs over, the one named last changes fastest.
Arguments:
- tokens: bfloat16 [8192, 1536], P(('dp', 'tensor')), may hold values from -6 to 6
- segments: int32 [8, 1024], P('dp'), may hold values from 0 to 3, never falling along the last dimension, each value on 1 to 512 neighbouring positions
- gain_one: bfloat16 [1536], P('dp'), may hold values from 0.25 to 1.75
- query_w: bfloat16 [1536, 1536], P('dp', 'tensor'), may hold values from -0.15625 to 0.15625
- query_b: bfloat16 [1536], P('tensor'), may hold values from -3 to 3
- key_w: bfloat16 [1536, 256], P('dp'), may hold values from -0.15625 to 0.15625
- key_b: bfloat16 [256], replicated, may hold values from -3 to 3
- value_w: bfloat16 [1536, 256], P('dp'), may hold values from -0.15625 to 0.15625
- value_b: bfloat16 [256], replicated, may hold values from -3 to 3
- out_w: bfloat16 [1536, 1536], P('dp', 'tensor'), may hold values from -0.4375 to 0.4375
- gain_two: bfloat16 [1536], P('dp'), may hold values from 0.25 to 1.75
- gate_w: bfloat16 [1536, 8960], P('dp', 'tensor'), may hold values from -0.15625 to 0.15625
- up_w: bfloat16 [1536, 8960], P('dp', 'tensor'), may hold values from -0.15625 to 0.15625
- down_w: bfloat16 [1536, 8960], P('dp', 'tensor'), may hold values from -0.0625 to 0.0625
- cotangent: bfloat16 [8192, 1536], P(('dp', 'tensor')), may hold values from -6 to 6
Outputs:
- mixed: bfloat16 [8192, 1536], P(('dp', 'tensor'))
- input_grad: bfloat16 [8192, 1536], P(('dp', 'tensor'))
- grad_gain_one: float32 [1536], P(('dp', 'tensor'))
- grad_query_w: float32 [1536, 1536], P('dp', 'tensor')
- grad_query_b: float32 [1536], P(('dp', 'tensor'))
- grad_key_w: float32 [1536, 256], P(('dp', 'tensor'))
- grad_key_b: float32 [256], replicated
- grad_value_w: float32 [1536, 256], P(('dp', 'tensor'))
- grad_value_b: float32 [256], replicated
- grad_out_w: float32 [1536, 1536], P('dp', 'tensor')
- grad_gain_two: float32 [1536], P(('dp', 'tensor'))
- grad_gate_w: float32 [1536, 8960], P('dp', 'tensor')
- grad_up_w: float32 [1536, 8960], P('dp', 'tensor')
- grad_down_w: float32 [1536, 8960], P('dp', 'tensor')
The draws below stay inside these ranges and needn't reach their ends.
Inputs may be any that keep to these rules, and one draw needn't show every extreme that they name: `segments`: in each sequence of 1024 positions the document numbers never fall; each of the 4 documents covers 1 to 512 positions, and one covers exactly 512.
All inputs are finite; a program needn't handle non-finite values.
Results may differ from the reference program's by a relative error of at most 0.02.
Values may be sent and summed in bfloat16 or wider, within the bound.
A program may use at most 256 MiB of HBM per device.

```python
import math
import jax
import jax.numpy as jnp
import numpy as np
from jax import lax

D = 1536
HEADS = 12
KV_HEADS = 2
HEAD_DIM = 128
FF = 8960
DOCS = 4
LEN = 1024
DOC_MAX = 512
NSEQ = 8
TOKENS = 8192


def shard_levels(rng, shape, split, least, high):
    level = 1.0
    for axis_at, parts in split:
        draws = jax.random.uniform(jax.random.fold_in(jax.random.fold_in(rng, 6), axis_at), (parts,), jnp.float32, least / len(split), high / len(split))
        level = level * jnp.repeat(jnp.exp(draws), shape[axis_at] // parts).reshape((-1,) + (1,) * (len(shape) - 1 - axis_at))
    return level


def profile(count, total, limit, skew):
    weights = [(1 << 20) // math.isqrt(standing ** skew) + 1 for standing in range(2, count + 1)]
    rest, given = total - limit - (count - 1), [1] * (count - 1)
    while rest > 0:
        candidates = [i for i in range(count - 1) if given[i] < limit]
        mass, budget = sum([weights[i] for i in candidates]), rest
        for i in candidates:
            extra = min(limit - given[i], max(1, budget * weights[i] // mass), rest)
            given[i] = given[i] + extra
            rest = rest - extra
    return np.array([limit] + given)


def ragged(rng, count, total, reach, lean):
    if count == 2:
        one = jax.random.randint(rng, (), max(1, total - reach), min(reach, total - 1) + 1)
        return jnp.stack([one, total - one])
    lengths = jnp.asarray(profile(count, total, reach, lean), jnp.int32)
    couples = (count - 1) // 2
    donor, sink = lengths[1:1 + 2 * couples:2], lengths[2:2 + 2 * couples:2]
    margin = jnp.minimum(donor - 1, reach - sink)
    passed = jax.random.randint(jax.random.fold_in(rng, 1), (couples,), 0, 1 << 20) % (margin + 1)
    lengths = lengths.at[1:1 + 2 * couples:2].set(donor - passed).at[2:2 + 2 * couples:2].set(sink + passed)
    return lengths[jax.random.permutation(jax.random.fold_in(rng, 2), count)]


def bell_draw(key, extent, width, reach, cuts=(), kind=jnp.bfloat16):
    level = shard_levels(key, extent, cuts, -0.22, 0.18) if cuts else 1.0
    drawn = jax.random.normal(key, extent, jnp.float32) * width * level
    return jnp.minimum(jnp.maximum(drawn, -reach), reach).astype(kind)


def setup_inputs(seed: int = 0) -> dict:
    keys = jax.random.split(jax.random.key(seed), 16)
    return {
        "tokens": bell_draw(keys[0], (TOKENS, D), 1.0, 6.0, ((0, 32),)),
        "segments": jax.vmap(lambda own: jnp.searchsorted(jnp.cumsum(ragged(own, DOCS, LEN, DOC_MAX, 2)), jnp.arange(LEN), side="right"))(jax.random.split(keys[1], NSEQ)).reshape((NSEQ, LEN)).astype(jnp.int32),
        "gain_one": jnp.clip(1.0 + 0.15 * jax.random.normal(keys[2], (D,), jnp.float32), 0.25, 1.75).astype(jnp.bfloat16),
        "query_w": bell_draw(keys[3], (D, HEADS * HEAD_DIM), D ** -0.5, 0.15625, ((0, 8), (1, 4))),
        "query_b": bell_draw(keys[4], (HEADS * HEAD_DIM,), 0.5, 3.0, ((0, 4),)),
        "key_w": bell_draw(keys[5], (D, KV_HEADS * HEAD_DIM), D ** -0.5, 0.15625, ((0, 8),)),
        "key_b": bell_draw(keys[6], (KV_HEADS * HEAD_DIM,), 0.5, 3.0),
        "value_w": bell_draw(keys[7], (D, KV_HEADS * HEAD_DIM), D ** -0.5, 0.15625, ((0, 8),)),
        "value_b": bell_draw(keys[8], (KV_HEADS * HEAD_DIM,), 0.5, 3.0),
        "out_w": bell_draw(keys[9], (D, HEADS * HEAD_DIM), (HEADS * HEAD_DIM // 8) ** -0.5, 0.4375, ((0, 8), (1, 4))),
        "gain_two": jnp.clip(1.0 + 0.15 * jax.random.normal(keys[10], (D,), jnp.float32), 0.25, 1.75).astype(jnp.bfloat16),
        "gate_w": bell_draw(keys[11], (D, FF), D ** -0.5, 0.15625, ((0, 8), (1, 4))),
        "up_w": bell_draw(keys[12], (D, FF), D ** -0.5, 0.15625, ((0, 8), (1, 4))),
        "down_w": bell_draw(keys[13], (D, FF), FF ** -0.5, 0.0625, ((0, 8), (1, 4))),
        "cotangent": bell_draw(keys[14], (TOKENS, D), 1.0, 6.0, ((0, 32),)),
    }


@jax.custom_vjp
def low(v):
    return lax.optimization_barrier(v.astype(jnp.bfloat16)).astype(jnp.float32)

@jax.custom_vjp
def low_back(v):
    return v

def low_keep(v):
    return (low(v), None)

def low_pass(kept, grad):
    return (grad,)

def back_keep(v):
    return (v, None)

def back_low(kept, grad):
    return (low(grad),)
low.defvjp(low_keep, low_pass)
low_back.defvjp(back_keep, back_low)
EPSILON = 1e-06
ROPE_BASE = 1000000.0
NEGATIVE = -1e+30

def product(left, right):
    return jnp.dot(left, right, precision=lax.Precision.HIGHEST, preferred_element_type=jnp.float32)

def rms_scale(values, gain):
    inverse = lax.rsqrt(lax.optimization_barrier(jnp.mean(values * values, axis=-1, keepdims=True)) + EPSILON)
    return values * inverse * gain

def angle_tables(length, head_width):
    position = jnp.arange(length, dtype=jnp.float32)
    exponent = jnp.arange(head_width // 2, dtype=jnp.float32) * (2.0 / head_width)
    frequency = ROPE_BASE ** (-exponent)
    angle = position[:, None] * frequency[None, :]
    return (jnp.cos(angle), jnp.sin(angle))

def rotate(values, cosine, sine):
    half_width = values.shape[-1] // 2
    first_half = values[..., :half_width]
    second_half = values[..., half_width:]
    return jnp.concatenate([first_half * cosine - second_half * sine, second_half * cosine + first_half * sine], axis=-1)

def forward_sequence(params, inputs, segment):
    gain_one, query_w, query_b, key_w, key_b, value_w, value_b, out_w, gain_two, gate_w, up_w, down_w = params
    length = inputs.shape[0]
    group_size = HEADS // KV_HEADS
    normed = low(rms_scale(inputs, gain_one))
    query_lin = low_back(product(normed, query_w) + query_b)
    key_lin = low_back(product(normed, key_w) + key_b)
    value_all = low(low_back(product(normed, value_w) + value_b))
    cosine, sine = angle_tables(length, HEAD_DIM)
    query_rot = low(rotate(query_lin.reshape(length, HEADS, HEAD_DIM), cosine[:, None, :], sine[:, None, :]))
    key_rot = low(rotate(key_lin.reshape(length, KV_HEADS, HEAD_DIM), cosine[:, None, :], sine[:, None, :]))
    query_grp = query_rot.reshape(length, KV_HEADS, group_size, HEAD_DIM)
    value_grp = value_all.reshape(length, KV_HEADS, HEAD_DIM)
    scores = jnp.einsum('tagd,sad->agts', query_grp, key_rot, precision=lax.Precision.HIGHEST)
    scores = low_back(scores * HEAD_DIM ** (-0.5))
    positions = jnp.arange(length)
    allowed = (segment[:, None] == segment[None, :]) & (positions[None, :] <= positions[:, None])
    masked = jnp.where(allowed, scores, NEGATIVE)
    largest = lax.optimization_barrier(jnp.max(masked, axis=-1, keepdims=True))
    log_total = largest + jnp.log(lax.optimization_barrier(jnp.sum(jnp.exp(masked - largest), axis=-1, keepdims=True)))
    weights = low(jnp.exp(masked - log_total))
    context = jnp.einsum('agts,sad->tagd', weights, value_grp, precision=lax.Precision.HIGHEST)
    context = low(low_back(context.reshape(length, HEADS * HEAD_DIM)))
    attended = low_back(product(context, out_w.T))
    middle = inputs + attended
    second = low(rms_scale(middle, gain_two))
    gate = low_back(product(second, gate_w))
    upper = low_back(product(second, up_w))
    hidden = low(jax.nn.silu(gate) * upper)
    return middle + product(hidden, down_w.T)

def reference(tokens, segments, gain_one, query_w, query_b, key_w, key_b, value_w, value_b, out_w, gain_two, gate_w, up_w, down_w, cotangent):
    params = tuple((weight.astype(jnp.float32) for weight in (gain_one, query_w, query_b, key_w, key_b, value_w, value_b, out_w, gain_two, gate_w, up_w, down_w)))
    inputs = tokens.astype(jnp.float32).reshape(NSEQ, LEN, D)
    cotangents = cotangent.astype(jnp.float32).reshape(NSEQ, LEN, D)

    def one_sequence(running, batch):
        seq_inputs, seq_segment, seq_cot = batch

        def closed(weights_in, values_in):
            return forward_sequence(weights_in, values_in, seq_segment)
        output, pullback = jax.vjp(closed, params, seq_inputs)
        grad_params, grad_inputs = pullback(seq_cot)
        running = tuple((earlier + latest for earlier, latest in zip(running, grad_params)))
        return (running, (output.astype(jnp.bfloat16), grad_inputs.astype(jnp.bfloat16)))
    zeros = tuple((jnp.zeros(weight.shape, jnp.float32) for weight in params))
    sums, (outputs, grads) = lax.scan(one_sequence, zeros, (inputs, segments, cotangents))
    mixed = outputs.reshape(TOKENS, D)
    input_grad = grads.reshape(TOKENS, D)
    return (mixed, input_grad, sums[0], sums[1], sums[2], sums[3], sums[4], sums[5], sums[6], sums[7], sums[8], sums[9], sums[10], sums[11])
```

```python
import jax
import jax.numpy as jnp
from jax import lax
from jax.sharding import PartitionSpec as P

KV_HEADS = 2
HEAD_DIM = 128
DOC_MAX = 512
EPSILON = 1e-06
ROPE_BASE = 1000000.0
NEGATIVE = -1e30


def angle_tables(first, length, head_width):
    position = (first + jnp.arange(length)).astype(jnp.float32)
    exponent = jnp.arange(head_width // 2, dtype=jnp.float32) * (2.0 / head_width)
    frequency = ROPE_BASE ** (-exponent)
    angle = position[:, None] * frequency[None, :]
    return (jnp.cos(angle), jnp.sin(angle))


def rotate(values, cosine, sine):
    half_width = values.shape[-1] // 2
    first_half = values[..., :half_width]
    second_half = values[..., half_width:]
    return jnp.concatenate(
        [first_half * cosine - second_half * sine, second_half * cosine + first_half * sine],
        axis=-1,
    )


def rotate_back(grads, cosine, sine):
    return rotate(grads, cosine, -sine)


def dot_f32(left, right, dims):
    return lax.dot_general(left, right, (dims, ((), ())), preferred_element_type=jnp.float32)


def contract_rows(left, right):
    return dot_f32(left, right, ((0,), (0,)))


def contract_cols(left, right):
    return dot_f32(left, right, ((1,), (1,)))


def norm_back(upstream, unit, inverse, gain):
    scaled = upstream * gain
    gain_term = jnp.sum(upstream * unit, axis=0)
    input_term = inverse * (scaled - unit * jnp.mean(scaled * unit, axis=-1, keepdims=True))
    return (gain_term, input_term)


def local(
    tokens, segments, gain_one, query_w, query_b, key_w, key_b, value_w, value_b,
    out_w, gain_two, gate_w, up_w, down_w, cotangent,
):
    bf16, f32 = jnp.bfloat16, jnp.float32
    model_width = tokens.shape[1]
    rows = tokens.shape[0]
    tensor_size = lax.axis_size("tensor")
    rank = lax.axis_index("tensor")
    seq_length = rows * tensor_size
    kv_width = key_w.shape[1]
    query_width = query_w.shape[1] * tensor_size
    heads = query_width // HEAD_DIM
    group = heads // KV_HEADS
    scale = HEAD_DIM ** (-0.5)
    pair = lax.all_gather(jnp.stack([query_w, out_w]), "tensor", axis=2, tiled=True)
    joined = jnp.concatenate([pair[0], key_w, value_w, pair[1]], axis=1)
    joined = lax.all_gather(joined, "dp", axis=0, tiled=True)
    qkv_width = query_width + 2 * kv_width
    qkv_w = joined[:, :qkv_width]
    out_full = joined[:, qkv_width:]
    gains = lax.all_gather(jnp.stack([gain_one, gain_two]), "dp", axis=1, tiled=True).astype(f32)
    full_query_b = lax.all_gather(query_b, "tensor", axis=0, tiled=True)
    qkv_b = jnp.concatenate([full_query_b, key_b, value_b]).astype(f32)
    full_gate = lax.all_gather(gate_w, "dp", axis=0, tiled=True)
    full_up = lax.all_gather(up_w, "dp", axis=0, tiled=True)
    full_down = lax.all_gather(down_w, "dp", axis=0, tiled=True)
    cot_rows = lax.all_gather(cotangent, "tensor", axis=0, tiled=True)

    inputs = tokens.astype(f32)
    inverse_one = lax.rsqrt(jnp.mean(inputs * inputs, axis=-1, keepdims=True) + EPSILON)
    unit_one = inputs * inverse_one
    normed_one = (unit_one * gains[0]).astype(bf16)
    lin = jnp.dot(normed_one, qkv_w, preferred_element_type=f32) + qkv_b
    cosine, sine = angle_tables(rank * rows, rows, HEAD_DIM)
    cos_h, sin_h = cosine[:, None, :], sine[:, None, :]
    query_rot = rotate(lin[:, :query_width].reshape(rows, heads, HEAD_DIM), cos_h, sin_h).astype(bf16)
    key_rot = rotate(
        lin[:, query_width : query_width + kv_width].reshape(rows, KV_HEADS, HEAD_DIM), cos_h, sin_h
    ).astype(bf16)
    value_own = lin[:, query_width + kv_width :].astype(bf16)
    kv_own = jnp.concatenate([key_rot.reshape(rows, kv_width), value_own], axis=1)
    kv_all = lax.all_gather(kv_own, "tensor", axis=0, tiled=True)
    window = min(seq_length, rows + -(-DOC_MAX // rows) * rows)
    first = jnp.maximum((rank + 1) * rows - window, 0)
    kv_win = lax.dynamic_slice_in_dim(kv_all, first, window, 0)
    key_win = kv_win[:, :kv_width].reshape(window, KV_HEADS, HEAD_DIM)
    value_win = kv_win[:, kv_width:].reshape(window, KV_HEADS, HEAD_DIM)
    segment = segments[0]
    own_segment = lax.dynamic_slice_in_dim(segment, rank * rows, rows, 0)
    win_segment = lax.dynamic_slice_in_dim(segment, first, window, 0)
    own_pos = rank * rows + jnp.arange(rows)
    win_pos = first + jnp.arange(window)
    allowed = (own_segment[:, None] == win_segment[None, :]) & (win_pos[None, :] <= own_pos[:, None])
    grouped = query_rot.reshape(rows, KV_HEADS, group, HEAD_DIM)
    scores = jnp.einsum("tagd,sad->agts", grouped, key_win, preferred_element_type=f32) * scale
    masked = jnp.where(allowed, scores, NEGATIVE)
    largest = jnp.max(masked, axis=-1, keepdims=True)
    log_total = largest + jnp.log(jnp.sum(jnp.exp(masked - largest), axis=-1, keepdims=True))
    probs = jnp.exp(masked - log_total)
    probs_low = probs.astype(bf16)
    context = jnp.einsum("agts,sad->tagd", probs_low, value_win, preferred_element_type=f32)
    context = context.reshape(rows, query_width).astype(bf16)
    middle = inputs + contract_cols(context, out_full)
    inverse_two = lax.rsqrt(jnp.mean(middle * middle, axis=-1, keepdims=True) + EPSILON)
    unit_two = middle * inverse_two
    normed_two = (unit_two * gains[1]).astype(bf16)

    rows_two = lax.all_gather(normed_two, "tensor", axis=0, tiled=True)
    gate = jnp.dot(rows_two, full_gate, preferred_element_type=f32)
    upper = jnp.dot(rows_two, full_up, preferred_element_type=f32)
    sigmoid = jax.nn.sigmoid(gate)
    hidden_low = (gate * sigmoid * upper).astype(bf16)
    ffn_sum = lax.psum_scatter(
        contract_cols(hidden_low, full_down).astype(bf16), "tensor", scatter_dimension=0, tiled=True
    ).astype(f32)
    mixed = (middle + ffn_sum).astype(bf16)
    d_hidden = jnp.dot(cot_rows, full_down, preferred_element_type=f32)
    d_upper = (d_hidden * gate * sigmoid).astype(bf16)
    d_gate = (d_hidden * upper * sigmoid * (1.0 + gate * (1.0 - sigmoid))).astype(bf16)
    d_normed_two = lax.psum_scatter(
        (contract_cols(d_gate, full_gate) + contract_cols(d_upper, full_up)).astype(bf16),
        "tensor", scatter_dimension=0, tiled=True,
    ).astype(f32)
    grad_down = contract_rows(cot_rows, hidden_low).astype(bf16)
    grad_gate = contract_rows(rows_two, d_gate).astype(bf16)
    grad_up = contract_rows(rows_two, d_upper).astype(bf16)

    gain_two_term, d_from_two = norm_back(d_normed_two, unit_two, inverse_two, gains[1])
    d_middle = cotangent.astype(f32) + d_from_two
    d_attended = d_middle.astype(bf16)
    d_context = jnp.dot(d_attended, out_full, preferred_element_type=f32).astype(bf16)
    grad_out = contract_rows(d_attended, context).astype(bf16)
    d_context = d_context.reshape(rows, KV_HEADS, group, HEAD_DIM)
    d_probs = jnp.einsum("tagd,sad->agts", d_context, value_win, preferred_element_type=f32)
    row_delta = jnp.sum(probs * d_probs, axis=-1, keepdims=True)
    d_scores = (probs * (d_probs - row_delta)).astype(bf16)
    d_query_rot = jnp.einsum("agts,sad->tagd", d_scores, key_win, preferred_element_type=f32) * scale
    d_key_win = jnp.einsum("agts,tagd->sad", d_scores, grouped, preferred_element_type=f32) * scale
    d_value_win = jnp.einsum("agts,tagd->sad", probs_low, d_context, preferred_element_type=f32)
    d_query_lin = (
        rotate_back(d_query_rot.reshape(rows, heads, HEAD_DIM), cos_h, sin_h)
        .reshape(rows, query_width).astype(bf16)
    )
    d_kv_win = jnp.concatenate(
        [d_key_win.reshape(window, kv_width), d_value_win.reshape(window, kv_width)], axis=1
    ).astype(bf16)
    d_kv_all = lax.dynamic_update_slice(
        jnp.zeros((seq_length, 2 * kv_width), bf16), d_kv_win, (first, 0)
    )
    d_kv = lax.psum_scatter(d_kv_all, "tensor", scatter_dimension=0, tiled=True).astype(f32)
    d_key_lin = rotate_back(d_kv[:, :kv_width].reshape(rows, KV_HEADS, HEAD_DIM), cos_h, sin_h)
    d_lin = jnp.concatenate(
        [d_query_lin, d_key_lin.reshape(rows, kv_width).astype(bf16), d_kv[:, kv_width:].astype(bf16)],
        axis=1,
    )
    d_normed_one = contract_cols(d_lin, qkv_w)
    grad_qkv = contract_rows(normed_one, d_lin).astype(bf16)
    bias_term = jnp.sum(d_lin.astype(f32), axis=0)
    gain_one_term, d_from_one = norm_back(d_normed_one, unit_one, inverse_one, gains[0])
    input_grad = (d_middle + d_from_one).astype(bf16)

    def over_dp(grad):
        return lax.psum_scatter(grad, "dp", scatter_dimension=0, tiled=True)

    sum_gate, sum_up, sum_down = (over_dp(g).astype(f32) for g in (grad_gate, grad_up, grad_down))
    part = over_dp(jnp.concatenate([grad_qkv, grad_out], axis=1))
    pair = jnp.stack([part[:, :query_width], part[:, qkv_width:]])
    pair = lax.psum_scatter(pair, "tensor", scatter_dimension=2, tiled=True).astype(f32)
    kv_part = lax.psum_scatter(
        part[:, query_width:qkv_width], "tensor", scatter_dimension=0, tiled=True
    ).astype(f32)
    small = lax.psum(
        jnp.concatenate([bias_term, gain_one_term, gain_two_term]), ("dp", "tensor")
    )
    place = lax.axis_index("dp") * tensor_size + rank
    devices = lax.axis_size("dp") * tensor_size

    def own(start, size):
        share = size // devices
        return lax.dynamic_slice_in_dim(small, start + place * share, share, 0)

    return (
        mixed,
        input_grad,
        own(qkv_width, model_width),
        pair[0],
        own(0, query_width),
        kv_part[:, :kv_width],
        small[query_width : query_width + kv_width],
        kv_part[:, kv_width:],
        small[query_width + kv_width : qkv_width],
        pair[1],
        own(qkv_width + model_width, model_width),
        sum_gate,
        sum_up,
        sum_down,
    )


def solution(mesh):
    both = ("dp", "tensor")
    return jax.shard_map(
        local,
        mesh=mesh,
        in_specs=(
            P(both, None), P("dp", None), P("dp"), P("dp", "tensor"), P("tensor"), P("dp", None), P(),
            P("dp", None), P(), P("dp", "tensor"), P("dp"), P("dp", "tensor"), P("dp", "tensor"),
            P("dp", "tensor"), P(both, None),
        ),
        out_specs=(
            P(both, None), P(both, None), P(both), P("dp", "tensor"), P(both), P(both, None), P(),
            P(both, None), P(), P("dp", "tensor"), P(both), P("dp", "tensor"), P("dp", "tensor"),
            P("dp", "tensor"),
        ),
        check_vma=False,
    )
```

```python
import functools

import jax
import jax.numpy as jnp
from jax import lax
from jax.experimental import pallas as pl
from jax.experimental.pallas import tpu as pltpu
from jax.sharding import PartitionSpec as P

MESH = pl.DeviceIdType.MESH

KV_HEADS = 2
HEAD_DIM = 128
DOC_MAX = 512
EPSILON = 1e-06
ROPE_BASE = 1000000.0
NEGATIVE = -1e30


def angle_tables(first, length, head_width):
    position = (first + jnp.arange(length)).astype(jnp.float32)
    exponent = jnp.arange(head_width // 2, dtype=jnp.float32) * (2.0 / head_width)
    frequency = ROPE_BASE ** (-exponent)
    angle = position[:, None] * frequency[None, :]
    return (jnp.cos(angle), jnp.sin(angle))


def rotate(values, cosine, sine):
    half_width = values.shape[-1] // 2
    first_half = values[..., :half_width]
    second_half = values[..., half_width:]
    return jnp.concatenate(
        [first_half * cosine - second_half * sine, second_half * cosine + first_half * sine],
        axis=-1,
    )


def rotate_back(grads, cosine, sine):
    return rotate(grads, cosine, -sine)


def dot_f32(left, right, dims):
    return lax.dot_general(left, right, (dims, ((), ())), preferred_element_type=jnp.float32)


def contract_rows(left, right):
    return dot_f32(left, right, ((0,), (0,)))


def contract_cols(left, right):
    return dot_f32(left, right, ((1,), (1,)))


def norm_back(upstream, unit, inverse, gain):
    scaled = upstream * gain
    gain_term = jnp.sum(upstream * unit, axis=0)
    input_term = inverse * (scaled - unit * jnp.mean(scaled * unit, axis=-1, keepdims=True))
    return (gain_term, input_term)


def line_order(z, s):
    upper = z // 2
    near = z * (1 - upper) + (3 - z) * upper
    inner = (1 - s // 3) * ((s + 1) % 3) + (s // 3) * 3
    at = (1 - near) * s + near * inner
    return at * (1 - upper) + (3 - at) * upper


def ffn_body(
    two_ref, cot_ref, gate_ref, up_ref, down_ref,
    rows_out, hid_out, dg_out, du_out, sum_out, dn_out,
    rows_v, cot_v, gate_v, up_v, down_v, hid_v, dg_v, du_v, part, land, below, above, res_v,
    tile_sem, load_sem, ag_send, ag_recv, rs_send, rs_recv, own_recv, out_sem,
    *, axis, ft, nt,
):
    f32, bf16 = jnp.float32, jnp.bfloat16
    size = 4
    rows, width = two_ref.shape
    units = gate_ref.shape[1]
    n_f, n_n = units // ft, width // nt
    z = lax.axis_index(axis)
    has_low, has_high = z > 0, z < size - 1

    def to(dz):
        return {axis: z + dz}

    barrier = pltpu.get_barrier_semaphore()

    @pl.when(has_low)
    def _():
        pl.semaphore_signal(barrier, inc=1, device_id=to(-1), device_id_type=MESH)

    @pl.when(has_high)
    def _():
        pl.semaphore_signal(barrier, inc=1, device_id=to(1), device_id_type=MESH)

    own_load = pltpu.make_async_copy(two_ref, rows_v.at[z], load_sem.at[0])
    own_load.start()

    def tile_loads(f):
        cols = pl.ds(pl.multiple_of(f * ft, 128), ft)
        return [
            pltpu.make_async_copy(src.at[:, cols], dst.at[:, cols], tile_sem.at[k, f])
            for k, (src, dst) in enumerate(((gate_ref, gate_v), (up_ref, up_v), (down_ref, down_v)))
        ]

    cot_load = pltpu.make_async_copy(cot_ref, cot_v, load_sem.at[1])
    for f in range(n_f):
        for copy in tile_loads(f):
            copy.start()
        if f == 0:
            cot_load.start()

    pl.semaphore_wait(barrier, (z + size - 1) // size + (2 * size - 2 - z) // size)

    own_load.wait()

    def ag_copy(j, dz):
        way = (dz + 1) // 2
        return pltpu.make_async_remote_copy(
            src_ref=rows_v.at[j], dst_ref=rows_v.at[j], send_sem=ag_send.at[way, j],
            recv_sem=ag_recv.at[j], device_id=to(dz), device_id_type=MESH,
        )

    @pl.when(has_low)
    def _():
        ag_copy(z, -1).start()

    @pl.when(has_high)
    def _():
        ag_copy(z, 1).start()

    def rs_copy(j, n, dz, own):
        way = (dz + 1) // 2
        if own:
            dst = below.at[n] if dz == 1 else above.at[n]
            sem = own_recv.at[1 - way, n]
        else:
            dst, sem = land.at[j, n], rs_recv.at[j, n]
        return pltpu.make_async_remote_copy(
            src_ref=part.at[j, n], dst_ref=dst, send_sem=rs_send.at[j, n],
            recv_sem=sem, device_id=to(dz), device_id_type=MESH,
        )

    def pass_on(j, n, what):
        for dz in (1, -1):
            for own in (True, False):
                hop = j == z + dz
                going = (j > z) if dz == 1 else (j < z)
                near = hop if own else jnp.logical_not(hop)

                @pl.when(jnp.logical_and(going, near))
                def _(dz=dz, own=own):
                    copy = rs_copy(j, n, dz, own)
                    copy.start() if what == "start" else copy.wait_send()

    def out_copies(j):
        at = pl.ds(pl.multiple_of(j * rows, rows), rows)
        return [
            pltpu.make_async_copy(src.at[j], dst.at[at, :], out_sem.at[k, j])
            for k, (src, dst) in enumerate(
                ((rows_v, rows_out), (hid_v, hid_out), (dg_v, dg_out), (du_v, du_out))
            )
        ]

    def step(s, carry):
        for sign in (-1, 1):
            j = z + sign * s
            inside = jnp.logical_and(s > 0, (j >= 0) if sign == -1 else (j < size))

            @pl.when(inside)
            def _(j=j, sign=sign):
                ag_copy(j, -sign).wait_recv()

            onward = has_high if sign == -1 else has_low

            @pl.when(jnp.logical_and(inside, onward))
            def _(j=j, sign=sign):
                ag_copy(j, -sign).start()

        j = line_order(z, s)
        at = pl.ds(pl.multiple_of(j * rows, rows), rows)

        @pl.when(s == 0)
        def _():
            cot_load.wait()

        def units_tile(f, carry):
            @pl.when(s == 0)
            def _():
                for copy in tile_loads(f):
                    copy.wait()

            cols = pl.ds(pl.multiple_of(f * ft, 128), ft)
            mine = rows_v[j]
            gate = jnp.dot(mine, gate_v[:, cols], preferred_element_type=f32)
            upper = jnp.dot(mine, up_v[:, cols], preferred_element_type=f32)
            d_hidden = jnp.dot(cot_v[at, :], down_v[:, cols], preferred_element_type=f32)
            sig = 1.0 / (1.0 + jnp.exp(-gate))
            act = gate * sig
            hid_v[j, :, cols] = (act * upper).astype(bf16)
            du_v[j, :, cols] = (d_hidden * act).astype(bf16)
            dg_v[j, :, cols] = (d_hidden * upper * (sig + act * (1.0 - sig))).astype(bf16)
            return carry

        lax.fori_loop(0, n_f, units_tile, 0)
        for copy in out_copies(j):
            copy.start()
        ends = jnp.logical_and(s > 0, jnp.logical_not(jnp.logical_and(has_low, has_high)))

        def width_tile(n, carry):
            at_n = pl.ds(pl.multiple_of(n * nt, nt), nt)
            dims = (((1,), (1,)), ((), ()))
            total = lax.dot_general(dg_v[j], gate_v[at_n, :], dims, preferred_element_type=f32)
            total += lax.dot_general(du_v[j], up_v[at_n, :], dims, preferred_element_type=f32)
            part[j, n] = total.astype(bf16)

            @pl.when(ends)
            def _():
                pass_on(j, n, "start")

            return carry

        lax.fori_loop(0, n_n, width_tile, 0)
        return carry

    lax.fori_loop(0, size, step, 0)

    def down_tile(i, carry):
        j, n = i // n_n, i % n_n
        at_n = pl.ds(pl.multiple_of(n * nt, nt), nt)
        total = lax.dot_general(
            hid_v[j], down_v[at_n, :], (((1,), (1,)), ((), ())), preferred_element_type=f32
        )
        res_v[j, :, at_n] = total.astype(bf16)
        return carry

    def forward(j, n):
        pltpu.make_async_copy(land.at[j, n], land.at[j, n], rs_recv.at[j, n]).wait()
        part[j, n] = (part[j, n].astype(f32) + land[j, n].astype(f32)).astype(bf16)
        pass_on(j, n, "start")

    middle = jnp.logical_and(has_low, has_high)

    @pl.when(middle)
    def _():
        def first(n, carry):
            forward(3 - z, n)
            return carry

        lax.fori_loop(0, n_n, first, 0)

    lax.fori_loop(0, (size * n_n) // 2, down_tile, 0)

    @pl.when(middle)
    def _():
        def second(n, carry):
            forward(3 - 3 * (z // 2), n)
            forward(3 * (z // 2), n)
            return carry

        lax.fori_loop(0, n_n, second, 0)

    lax.fori_loop((size * n_n) // 2, size * n_n, down_tile, 0)
    sum_copies = [
        pltpu.make_async_copy(
            res_v.at[j], sum_out.at[pl.ds(j * rows, rows), :], load_sem.at[2 + j]
        )
        for j in range(size)
    ]
    for copy in sum_copies:
        copy.start()

    def last(n, carry):
        @pl.when(has_low)
        def _():
            pltpu.make_async_copy(below.at[n], below.at[n], own_recv.at[0, n]).wait()
            part[z, n] = (part[z, n].astype(f32) + below[n].astype(f32)).astype(bf16)

        @pl.when(has_high)
        def _():
            pltpu.make_async_copy(above.at[n], above.at[n], own_recv.at[1, n]).wait()
            part[z, n] = (part[z, n].astype(f32) + above[n].astype(f32)).astype(bf16)

        dn_out[:, pl.ds(pl.multiple_of(n * nt, nt), nt)] = part[z, n]
        return carry

    lax.fori_loop(0, n_n, last, 0)

    def drain(j, carry):
        for copy in out_copies(j):
            copy.wait()
        for dz in (-1, 1):
            came = jnp.logical_or(j == z, (j > z) if dz == -1 else (j < z))
            there = has_low if dz == -1 else has_high

            @pl.when(jnp.logical_and(came, there))
            def _(dz=dz):
                ag_copy(j, dz).wait_send()

        def sent(n, carry):
            @pl.when(j != z)
            def _():
                pltpu.make_async_copy(part.at[j, n], part.at[j, n], rs_send.at[j, n]).wait()

            return carry

        lax.fori_loop(0, n_n, sent, 0)
        return carry

    lax.fori_loop(0, size, drain, 0)
    for copy in sum_copies:
        copy.wait()


def ffn(two, cot_rows, gate, up, down, axis="tensor", ft=768, nt=512, collective_id=1, limit=66_000_000):
    rows, width = two.shape
    units = gate.shape[1]
    size = 4
    length = rows * size
    n_f, n_n = units // ft, width // nt
    bf16 = jnp.bfloat16
    hbm = pl.BlockSpec(memory_space=pl.ANY)
    vm = pltpu.VMEM
    dma = pltpu.SemaphoreType.DMA
    shape = lambda *s: jax.ShapeDtypeStruct(s, bf16)
    return pl.pallas_call(
        functools.partial(ffn_body, axis=axis, ft=ft, nt=nt),
        out_shape=(
            shape(length, width), shape(length, units), shape(length, units), shape(length, units),
            shape(length, width), shape(rows, width),
        ),
        in_specs=[hbm] * 5,
        out_specs=(hbm,) * 5 + (pl.BlockSpec(memory_space=pltpu.VMEM),),
        scratch_shapes=[
            vm((size, rows, width), bf16), vm((length, width), bf16),
            vm((width, units), bf16), vm((width, units), bf16), vm((width, units), bf16),
            vm((size, rows, units), bf16), vm((size, rows, units), bf16), vm((size, rows, units), bf16),
            vm((size, n_n, rows, nt), bf16), vm((size, n_n, rows, nt), bf16),
            vm((n_n, rows, nt), bf16), vm((n_n, rows, nt), bf16),
            vm((size, rows, width), bf16),
            dma((3, n_f)), dma((2 + size,)), dma((2, size)), dma((size,)), dma((size, n_n)), dma((size, n_n)),
            dma((2, n_n)), dma((4, size)),
        ],
        compiler_params=pltpu.CompilerParams(
            collective_id=collective_id, has_side_effects=True, vmem_limit_bytes=limit
        ),
        cost_estimate=pl.CostEstimate(
            flops=12 * length * width * units, bytes_accessed=8 * width * units + 8 * length * units,
            transcendentals=length * units,
        ),
        name="ffn",
    )(two, cot_rows, gate, up, down)


def local(
    tokens, segments, gain_one, query_w, query_b, key_w, key_b, value_w, value_b,
    out_w, gain_two, gate_w, up_w, down_w, cotangent,
):
    bf16, f32 = jnp.bfloat16, jnp.float32
    model_width = tokens.shape[1]
    rows = tokens.shape[0]
    tensor_size = lax.axis_size("tensor")
    rank = lax.axis_index("tensor")
    seq_length = rows * tensor_size
    kv_width = key_w.shape[1]
    query_width = query_w.shape[1] * tensor_size
    heads = query_width // HEAD_DIM
    group = heads // KV_HEADS
    scale = HEAD_DIM ** (-0.5)
    pair = lax.all_gather(jnp.stack([query_w, out_w]), "tensor", axis=2, tiled=True)
    joined = jnp.concatenate([pair[0], key_w, value_w, pair[1]], axis=1)
    joined = lax.all_gather(joined, "dp", axis=0, tiled=True)
    qkv_width = query_width + 2 * kv_width
    qkv_w = joined[:, :qkv_width]
    out_full = joined[:, qkv_width:]
    gains = lax.all_gather(jnp.stack([gain_one, gain_two]), "dp", axis=1, tiled=True).astype(f32)
    full_query_b = lax.all_gather(query_b, "tensor", axis=0, tiled=True)
    qkv_b = jnp.concatenate([full_query_b, key_b, value_b]).astype(f32)
    units = gate_w.shape[1]
    padded = -(-units // 768) * 768

    def whole(shard):
        shard = jnp.pad(shard, ((0, 0), (0, padded - units)))
        return lax.all_gather(shard, "dp", axis=0, tiled=True)

    full_gate, full_up, full_down = whole(gate_w), whole(up_w), whole(down_w)
    cot_rows = lax.all_gather(cotangent, "tensor", axis=0, tiled=True)

    inputs = tokens.astype(f32)
    inverse_one = lax.rsqrt(jnp.mean(inputs * inputs, axis=-1, keepdims=True) + EPSILON)
    unit_one = inputs * inverse_one
    normed_one = (unit_one * gains[0]).astype(bf16)
    lin = jnp.dot(normed_one, qkv_w, preferred_element_type=f32) + qkv_b
    cosine, sine = angle_tables(rank * rows, rows, HEAD_DIM)
    cos_h, sin_h = cosine[:, None, :], sine[:, None, :]
    query_rot = rotate(lin[:, :query_width].reshape(rows, heads, HEAD_DIM), cos_h, sin_h).astype(bf16)
    key_rot = rotate(
        lin[:, query_width : query_width + kv_width].reshape(rows, KV_HEADS, HEAD_DIM), cos_h, sin_h
    ).astype(bf16)
    value_own = lin[:, query_width + kv_width :].astype(bf16)
    kv_own = jnp.concatenate([key_rot.reshape(rows, kv_width), value_own], axis=1)
    kv_all = lax.all_gather(kv_own, "tensor", axis=0, tiled=True)
    window = min(seq_length, rows + -(-DOC_MAX // rows) * rows)
    first = jnp.maximum((rank + 1) * rows - window, 0)
    kv_win = lax.dynamic_slice_in_dim(kv_all, first, window, 0)
    key_win = kv_win[:, :kv_width].reshape(window, KV_HEADS, HEAD_DIM)
    value_win = kv_win[:, kv_width:].reshape(window, KV_HEADS, HEAD_DIM)
    segment = segments[0]
    own_segment = lax.dynamic_slice_in_dim(segment, rank * rows, rows, 0)
    win_segment = lax.dynamic_slice_in_dim(segment, first, window, 0)
    own_pos = rank * rows + jnp.arange(rows)
    win_pos = first + jnp.arange(window)
    allowed = (own_segment[:, None] == win_segment[None, :]) & (win_pos[None, :] <= own_pos[:, None])
    grouped = query_rot.reshape(rows, KV_HEADS, group, HEAD_DIM)
    scores = jnp.einsum("tagd,sad->agts", grouped, key_win, preferred_element_type=f32) * scale
    masked = jnp.where(allowed, scores, NEGATIVE)
    largest = jnp.max(masked, axis=-1, keepdims=True)
    log_total = largest + jnp.log(jnp.sum(jnp.exp(masked - largest), axis=-1, keepdims=True))
    probs = jnp.exp(masked - log_total)
    probs_low = probs.astype(bf16)
    context = jnp.einsum("agts,sad->tagd", probs_low, value_win, preferred_element_type=f32)
    context = context.reshape(rows, query_width).astype(bf16)
    middle = inputs + contract_cols(context, out_full)
    inverse_two = lax.rsqrt(jnp.mean(middle * middle, axis=-1, keepdims=True) + EPSILON)
    unit_two = middle * inverse_two
    normed_two = (unit_two * gains[1]).astype(bf16)

    rows_two, hidden_low, d_gate, d_upper, ffn_part, d_normed_two = ffn(
        normed_two, cot_rows, full_gate, full_up, full_down
    )
    ffn_sum = lax.psum_scatter(ffn_part, "tensor", scatter_dimension=0, tiled=True).astype(f32)
    mixed = (middle + ffn_sum).astype(bf16)
    d_normed_two = d_normed_two.astype(f32)
    grad_down = contract_rows(cot_rows, hidden_low).astype(bf16)
    grad_gate = contract_rows(rows_two, d_gate).astype(bf16)
    grad_up = contract_rows(rows_two, d_upper).astype(bf16)

    gain_two_term, d_from_two = norm_back(d_normed_two, unit_two, inverse_two, gains[1])
    d_middle = cotangent.astype(f32) + d_from_two
    d_attended = d_middle.astype(bf16)
    d_context = jnp.dot(d_attended, out_full, preferred_element_type=f32).astype(bf16)
    grad_out = contract_rows(d_attended, context).astype(bf16)
    d_context = d_context.reshape(rows, KV_HEADS, group, HEAD_DIM)
    d_probs = jnp.einsum("tagd,sad->agts", d_context, value_win, preferred_element_type=f32)
    row_delta = jnp.sum(probs * d_probs, axis=-1, keepdims=True)
    d_scores = (probs * (d_probs - row_delta)).astype(bf16)
    d_query_rot = jnp.einsum("agts,sad->tagd", d_scores, key_win, preferred_element_type=f32) * scale
    d_key_win = jnp.einsum("agts,tagd->sad", d_scores, grouped, preferred_element_type=f32) * scale
    d_value_win = jnp.einsum("agts,tagd->sad", probs_low, d_context, preferred_element_type=f32)
    d_query_lin = (
        rotate_back(d_query_rot.reshape(rows, heads, HEAD_DIM), cos_h, sin_h)
        .reshape(rows, query_width).astype(bf16)
    )
    d_kv_win = jnp.concatenate(
        [d_key_win.reshape(window, kv_width), d_value_win.reshape(window, kv_width)], axis=1
    ).astype(bf16)
    d_kv_all = lax.dynamic_update_slice(
        jnp.zeros((seq_length, 2 * kv_width), bf16), d_kv_win, (first, 0)
    )
    d_kv = lax.psum_scatter(d_kv_all, "tensor", scatter_dimension=0, tiled=True).astype(f32)
    d_key_lin = rotate_back(d_kv[:, :kv_width].reshape(rows, KV_HEADS, HEAD_DIM), cos_h, sin_h)
    d_lin = jnp.concatenate(
        [d_query_lin, d_key_lin.reshape(rows, kv_width).astype(bf16), d_kv[:, kv_width:].astype(bf16)],
        axis=1,
    )
    d_normed_one = contract_cols(d_lin, qkv_w)
    grad_qkv = contract_rows(normed_one, d_lin).astype(bf16)
    bias_term = jnp.sum(d_lin.astype(f32), axis=0)
    gain_one_term, d_from_one = norm_back(d_normed_one, unit_one, inverse_one, gains[0])
    input_grad = (d_middle + d_from_one).astype(bf16)

    def over_dp(grad):
        return lax.psum_scatter(grad, "dp", scatter_dimension=0, tiled=True)

    sum_gate, sum_up, sum_down = (over_dp(g)[:, :units].astype(f32) for g in (grad_gate, grad_up, grad_down))
    part = over_dp(jnp.concatenate([grad_qkv, grad_out], axis=1))
    pair = jnp.stack([part[:, :query_width], part[:, qkv_width:]])
    pair = lax.psum_scatter(pair, "tensor", scatter_dimension=2, tiled=True).astype(f32)
    kv_part = lax.psum_scatter(
        part[:, query_width:qkv_width], "tensor", scatter_dimension=0, tiled=True
    ).astype(f32)
    small = lax.psum(
        jnp.concatenate([bias_term, gain_one_term, gain_two_term]), ("dp", "tensor")
    )
    place = lax.axis_index("dp") * tensor_size + rank
    devices = lax.axis_size("dp") * tensor_size

    def own(start, size):
        share = size // devices
        return lax.dynamic_slice_in_dim(small, start + place * share, share, 0)

    return (
        mixed,
        input_grad,
        own(qkv_width, model_width),
        pair[0],
        own(0, query_width),
        kv_part[:, :kv_width],
        small[query_width : query_width + kv_width],
        kv_part[:, kv_width:],
        small[query_width + kv_width : qkv_width],
        pair[1],
        own(qkv_width + model_width, model_width),
        sum_gate,
        sum_up,
        sum_down,
    )


def solution(mesh):
    both = ("dp", "tensor")
    return jax.shard_map(
        local,
        mesh=mesh,
        in_specs=(
            P(both, None), P("dp", None), P("dp"), P("dp", "tensor"), P("tensor"), P("dp", None), P(),
            P("dp", None), P(), P("dp", "tensor"), P("dp"), P("dp", "tensor"), P("dp", "tensor"),
            P("dp", "tensor"), P(both, None),
        ),
        out_specs=(
            P(both, None), P(both, None), P(both), P("dp", "tensor"), P(both), P(both, None), P(),
            P(both, None), P(), P("dp", "tensor"), P(both), P("dp", "tensor"), P("dp", "tensor"),
            P("dp", "tensor"),
        ),
        check_vma=False,
    )
```

```python
import functools

import jax
import jax.numpy as jnp
from jax import lax
from jax.experimental import pallas as pl
from jax.experimental.pallas import tpu as pltpu
from jax.sharding import PartitionSpec as P

MESH = pl.DeviceIdType.MESH

KV_HEADS = 2
HEAD_DIM = 128
DOC_MAX = 512
EPSILON = 1e-06
ROPE_BASE = 1000000.0
NEGATIVE = -1e30


def angle_tables(first, length, head_width):
    position = (first + jnp.arange(length)).astype(jnp.float32)
    exponent = jnp.arange(head_width // 2, dtype=jnp.float32) * (2.0 / head_width)
    frequency = ROPE_BASE ** (-exponent)
    angle = position[:, None] * frequency[None, :]
    return (jnp.cos(angle), jnp.sin(angle))


def rotate(values, cosine, sine):
    half_width = values.shape[-1] // 2
    first_half = values[..., :half_width]
    second_half = values[..., half_width:]
    return jnp.concatenate(
        [first_half * cosine - second_half * sine, second_half * cosine + first_half * sine],
        axis=-1,
    )


def rotate_back(grads, cosine, sine):
    return rotate(grads, cosine, -sine)


def dot_f32(left, right, dims):
    return lax.dot_general(left, right, (dims, ((), ())), preferred_element_type=jnp.float32)


def contract_rows(left, right):
    return dot_f32(left, right, ((0,), (0,)))


def contract_cols(left, right):
    return dot_f32(left, right, ((1,), (1,)))


def norm_back(upstream, unit, inverse, gain):
    scaled = upstream * gain
    gain_term = jnp.sum(upstream * unit, axis=0)
    input_term = inverse * (scaled - unit * jnp.mean(scaled * unit, axis=-1, keepdims=True))
    return (gain_term, input_term)


def line_order(z, s):
    upper = z // 2
    near = z * (1 - upper) + (3 - z) * upper
    inner = (1 - s // 3) * ((s + 1) % 3) + (s // 3) * 3
    at = (1 - near) * s + near * inner
    return at * (1 - upper) + (3 - at) * upper


def ffn_body(
    two_ref, cot_ref, weights_ref,
    rows_out, hid_out, dg_out, du_out, sum_out, dn_out,
    rows_v, cot_v, gate_v, up_v, down_v, hid_v, dg_v, du_v, part, land, below, above, res_v,
    tile_sem, load_sem, ag_send, ag_recv, rs_send, rs_recv, own_recv, out_sem,
    *, axis, ft, nt,
):
    f32, bf16 = jnp.float32, jnp.bfloat16
    size = 4
    rows, width = two_ref.shape
    units = weights_ref.shape[1] // 3
    n_f, n_n = units // ft, width // nt
    z = lax.axis_index(axis)
    has_low, has_high = z > 0, z < size - 1

    def to(dz):
        return {axis: z + dz}

    barrier = pltpu.get_barrier_semaphore()

    @pl.when(has_low)
    def _():
        pl.semaphore_signal(barrier, inc=1, device_id=to(-1), device_id_type=MESH)

    @pl.when(has_high)
    def _():
        pl.semaphore_signal(barrier, inc=1, device_id=to(1), device_id_type=MESH)

    own_load = pltpu.make_async_copy(two_ref, rows_v.at[z], load_sem.at[0])
    own_load.start()

    def tile_loads(f):
        cols = pl.ds(pl.multiple_of(f * ft, 128), ft)
        return [
            pltpu.make_async_copy(
                weights_ref.at[:, pl.ds(pl.multiple_of(k * units + f * ft, 128), ft)],
                dst.at[:, cols], tile_sem.at[k, f],
            )
            for k, dst in enumerate((gate_v, up_v, down_v))
        ]

    cot_load = pltpu.make_async_copy(cot_ref, cot_v, load_sem.at[1])
    for f in range(n_f):
        for copy in tile_loads(f):
            copy.start()
        if f == 0:
            cot_load.start()

    pl.semaphore_wait(barrier, (z + size - 1) // size + (2 * size - 2 - z) // size)

    own_load.wait()

    def ag_copy(j, dz):
        way = (dz + 1) // 2
        return pltpu.make_async_remote_copy(
            src_ref=rows_v.at[j], dst_ref=rows_v.at[j], send_sem=ag_send.at[way, j],
            recv_sem=ag_recv.at[j], device_id=to(dz), device_id_type=MESH,
        )

    @pl.when(has_low)
    def _():
        ag_copy(z, -1).start()

    @pl.when(has_high)
    def _():
        ag_copy(z, 1).start()

    def rs_copy(j, n, dz, own):
        way = (dz + 1) // 2
        if own:
            dst = below.at[n] if dz == 1 else above.at[n]
            sem = own_recv.at[1 - way, n]
        else:
            dst, sem = land.at[j, n], rs_recv.at[j, n]
        return pltpu.make_async_remote_copy(
            src_ref=part.at[j, n], dst_ref=dst, send_sem=rs_send.at[j, n],
            recv_sem=sem, device_id=to(dz), device_id_type=MESH,
        )

    def pass_on(j, n, what):
        for dz in (1, -1):
            for own in (True, False):
                hop = j == z + dz
                going = (j > z) if dz == 1 else (j < z)
                near = hop if own else jnp.logical_not(hop)

                @pl.when(jnp.logical_and(going, near))
                def _(dz=dz, own=own):
                    copy = rs_copy(j, n, dz, own)
                    copy.start() if what == "start" else copy.wait_send()

    def out_copies(j):
        at = pl.ds(pl.multiple_of(j * rows, rows), rows)
        return [
            pltpu.make_async_copy(src.at[j], dst.at[at, :], out_sem.at[k, j])
            for k, (src, dst) in enumerate(
                ((rows_v, rows_out), (hid_v, hid_out), (dg_v, dg_out), (du_v, du_out))
            )
        ]

    def step(s, carry):
        for sign in (-1, 1):
            j = z + sign * s
            inside = jnp.logical_and(s > 0, (j >= 0) if sign == -1 else (j < size))

            @pl.when(inside)
            def _(j=j, sign=sign):
                ag_copy(j, -sign).wait_recv()

            onward = has_high if sign == -1 else has_low

            @pl.when(jnp.logical_and(inside, onward))
            def _(j=j, sign=sign):
                ag_copy(j, -sign).start()

        j = line_order(z, s)
        at = pl.ds(pl.multiple_of(j * rows, rows), rows)

        @pl.when(s == 0)
        def _():
            cot_load.wait()

        def units_tile(f, carry):
            @pl.when(s == 0)
            def _():
                for copy in tile_loads(f):
                    copy.wait()

            cols = pl.ds(pl.multiple_of(f * ft, 128), ft)
            mine = rows_v[j]
            gate = jnp.dot(mine, gate_v[:, cols], preferred_element_type=f32)
            upper = jnp.dot(mine, up_v[:, cols], preferred_element_type=f32)
            d_hidden = jnp.dot(cot_v[at, :], down_v[:, cols], preferred_element_type=f32)
            sig = 1.0 / (1.0 + jnp.exp(-gate))
            act = gate * sig
            hid_v[j, :, cols] = (act * upper).astype(bf16)
            du_v[j, :, cols] = (d_hidden * act).astype(bf16)
            dg_v[j, :, cols] = (d_hidden * upper * (sig + act * (1.0 - sig))).astype(bf16)
            return carry

        lax.fori_loop(0, n_f, units_tile, 0)
        for copy in out_copies(j):
            copy.start()
        ends = jnp.logical_and(s > 0, jnp.logical_not(jnp.logical_and(has_low, has_high)))

        def width_tile(n, carry):
            at_n = pl.ds(pl.multiple_of(n * nt, nt), nt)
            dims = (((1,), (1,)), ((), ()))
            total = lax.dot_general(dg_v[j], gate_v[at_n, :], dims, preferred_element_type=f32)
            total += lax.dot_general(du_v[j], up_v[at_n, :], dims, preferred_element_type=f32)
            part[j, n] = total.astype(bf16)

            @pl.when(ends)
            def _():
                pass_on(j, n, "start")

            return carry

        lax.fori_loop(0, n_n, width_tile, 0)
        return carry

    lax.fori_loop(0, size, step, 0)

    def down_tile(i, carry):
        j, n = i // n_n, i % n_n
        at_n = pl.ds(pl.multiple_of(n * nt, nt), nt)
        total = lax.dot_general(
            hid_v[j], down_v[at_n, :], (((1,), (1,)), ((), ())), preferred_element_type=f32
        )
        res_v[j, :, at_n] = total.astype(bf16)
        return carry

    def forward(j, n):
        pltpu.make_async_copy(land.at[j, n], land.at[j, n], rs_recv.at[j, n]).wait()
        part[j, n] = (part[j, n].astype(f32) + land[j, n].astype(f32)).astype(bf16)
        pass_on(j, n, "start")

    middle = jnp.logical_and(has_low, has_high)

    @pl.when(middle)
    def _():
        def first(n, carry):
            forward(3 - z, n)
            return carry

        lax.fori_loop(0, n_n, first, 0)

    lax.fori_loop(0, (size * n_n) // 2, down_tile, 0)

    @pl.when(middle)
    def _():
        def second(n, carry):
            forward(3 - 3 * (z // 2), n)
            forward(3 * (z // 2), n)
            return carry

        lax.fori_loop(0, n_n, second, 0)

    lax.fori_loop((size * n_n) // 2, size * n_n, down_tile, 0)
    sum_copies = [
        pltpu.make_async_copy(
            res_v.at[j], sum_out.at[pl.ds(j * rows, rows), :], load_sem.at[2 + j]
        )
        for j in range(size)
    ]
    for copy in sum_copies:
        copy.start()

    def last(n, carry):
        @pl.when(has_low)
        def _():
            pltpu.make_async_copy(below.at[n], below.at[n], own_recv.at[0, n]).wait()
            part[z, n] = (part[z, n].astype(f32) + below[n].astype(f32)).astype(bf16)

        @pl.when(has_high)
        def _():
            pltpu.make_async_copy(above.at[n], above.at[n], own_recv.at[1, n]).wait()
            part[z, n] = (part[z, n].astype(f32) + above[n].astype(f32)).astype(bf16)

        dn_out[:, pl.ds(pl.multiple_of(n * nt, nt), nt)] = part[z, n]
        return carry

    lax.fori_loop(0, n_n, last, 0)

    def drain(j, carry):
        for copy in out_copies(j):
            copy.wait()
        for dz in (-1, 1):
            came = jnp.logical_or(j == z, (j > z) if dz == -1 else (j < z))
            there = has_low if dz == -1 else has_high

            @pl.when(jnp.logical_and(came, there))
            def _(dz=dz):
                ag_copy(j, dz).wait_send()

        def sent(n, carry):
            @pl.when(j != z)
            def _():
                pltpu.make_async_copy(part.at[j, n], part.at[j, n], rs_send.at[j, n]).wait()

            return carry

        lax.fori_loop(0, n_n, sent, 0)
        return carry

    lax.fori_loop(0, size, drain, 0)
    for copy in sum_copies:
        copy.wait()


def ffn(two, cot_rows, weights, axis="tensor", ft=768, nt=512, collective_id=1, limit=66_000_000):
    rows, width = two.shape
    units = weights.shape[1] // 3
    size = 4
    length = rows * size
    n_f, n_n = units // ft, width // nt
    bf16 = jnp.bfloat16
    hbm = pl.BlockSpec(memory_space=pl.ANY)
    vm = pltpu.VMEM
    dma = pltpu.SemaphoreType.DMA
    shape = lambda *s: jax.ShapeDtypeStruct(s, bf16)
    return pl.pallas_call(
        functools.partial(ffn_body, axis=axis, ft=ft, nt=nt),
        out_shape=(
            shape(length, width), shape(length, units), shape(length, units), shape(length, units),
            shape(length, width), shape(rows, width),
        ),
        in_specs=[hbm] * 3,
        out_specs=(hbm,) * 5 + (pl.BlockSpec(memory_space=pltpu.VMEM),),
        scratch_shapes=[
            vm((size, rows, width), bf16), vm((length, width), bf16),
            vm((width, units), bf16), vm((width, units), bf16), vm((width, units), bf16),
            vm((size, rows, units), bf16), vm((size, rows, units), bf16), vm((size, rows, units), bf16),
            vm((size, n_n, rows, nt), bf16), vm((size, n_n, rows, nt), bf16),
            vm((n_n, rows, nt), bf16), vm((n_n, rows, nt), bf16),
            vm((size, rows, width), bf16),
            dma((3, n_f)), dma((2 + size,)), dma((2, size)), dma((size,)), dma((size, n_n)), dma((size, n_n)),
            dma((2, n_n)), dma((4, size)),
        ],
        compiler_params=pltpu.CompilerParams(
            collective_id=collective_id, has_side_effects=True, vmem_limit_bytes=limit
        ),
        cost_estimate=pl.CostEstimate(
            flops=12 * length * width * units, bytes_accessed=8 * width * units + 8 * length * units,
            transcendentals=length * units,
        ),
        name="ffn",
    )(two, cot_rows, weights)


def square(d):
    core, x, y = d % 2, (d // 2) % 2, d // 4
    by_x, by_y = d + 2 - 4 * x, d + 4 - 8 * y
    return by_x, by_y, d + 1 - 2 * core, by_x + 4 - 8 * y


def front_body(
    query_ref, out_ref, fixed_ref, ffn_ref, cot_ref,
    att_all, ffn_all, cot_all, extra_out,
    att_v, fill_sem, z_send, z_recv, cot_send, cot_recv, send, recv, keep_sem,
    *, att_w, ffn_w, order, lead,
):
    d, z = lax.axis_index("dp"), lax.axis_index("tensor")
    size = 4
    by_x, by_y, mate, across = square(d)
    rows = ffn_ref.shape[0]
    half = rows // 2
    part = query_ref.shape[1]
    fixed = fixed_ref.shape[1]
    chunk = cot_ref.shape[0]
    tall = query_ref.shape[0]

    barrier = pltpu.get_barrier_semaphore()
    for peer in (by_x, by_y, mate):
        pl.semaphore_signal(barrier, inc=1, device_id={"dp": peer}, device_id_type=MESH)
    for hop in range(1, size):
        pl.semaphore_signal(
            barrier, inc=1, device_id={"tensor": (z + hop) % size}, device_id_type=MESH
        )

    def place(of, owner):
        return pl.ds(pl.multiple_of(fixed + of * size * part + owner * part, 128), part)

    fills = [pltpu.make_async_copy(fixed_ref, att_v.at[pl.ds(0, rows), pl.ds(0, fixed)], fill_sem.at[0])]
    for of, ref in enumerate((query_ref, out_ref)):
        fills.append(pltpu.make_async_copy(ref, att_v.at[:, place(of, z)], fill_sem.at[1 + of]))
    at = pl.ds(pl.multiple_of(z * chunk, chunk), chunk)
    fills.append(pltpu.make_async_copy(cot_ref, cot_all.at[at, :], fill_sem.at[3]))
    for copy in fills:
        copy.start()

    pl.semaphore_wait(barrier, 3 + size - 1)

    def z_copy(of, hop):
        ref = (query_ref, out_ref)[of]
        return pltpu.make_async_remote_copy(
            src_ref=ref, dst_ref=att_v.at[:, place(of, z)], send_sem=z_send.at[of, hop - 1],
            recv_sem=z_recv.at[of, hop - 1], device_id={"tensor": (z + hop) % size},
            device_id_type=MESH,
        )

    def cot_copy(hop):
        return pltpu.make_async_remote_copy(
            src_ref=cot_ref, dst_ref=cot_all.at[at, :], send_sem=cot_send.at[hop - 1],
            recv_sem=cot_recv.at[hop - 1], device_id={"tensor": (z + hop) % size},
            device_id_type=MESH,
        )

    for of in range(2):
        for hop in range(1, size):
            z_copy(of, hop).start()
    fills[0].wait()

    def views(kind, p):
        src, dst, wide = ((att_v, att_all, att_w), (ffn_ref, ffn_all, ffn_w))[kind]
        return src, dst, pl.ds(pl.multiple_of(p * wide, 128), wide)

    def slot(kind, p):
        return p + kind * n_att

    n_att = att_all.shape[1] // att_w

    def block(dst, cols, owner, first=0, many=None):
        many = rows if many is None else many
        return dst.at[pl.ds(pl.multiple_of(owner * rows + first, 16), many), cols]

    def remote(src, dst, way, at_slot, peer):
        return pltpu.make_async_remote_copy(
            src_ref=src, dst_ref=dst, send_sem=send.at[way, at_slot], recv_sem=recv.at[way, at_slot],
            device_id={"dp": peer}, device_id_type=MESH,
        )

    def own(kind, p):
        src, dst, cols = views(kind, p)
        mine = src.at[pl.ds(0, rows), cols]
        there = block(dst, cols, d)
        s = slot(kind, p)
        return [
            remote(mine, there, 0, s, by_x), remote(mine, there, 1, s, by_y),
            remote(mine, there, 2, s, mate),
        ], pltpu.make_async_copy(mine, there, keep_sem.at[s])

    def relays(kind, p, group):
        _, dst, cols = views(kind, p)
        s = slot(kind, p)
        if group == 2:
            whole = block(dst, cols, across)
            return [remote(whole, whole, 7, s, mate)]
        owner, peer = ((by_x, by_y), (by_y, by_x))[group]
        piece, whole = block(dst, cols, owner, group * half, half), block(dst, cols, owner)
        way = 3 + 2 * group
        return [remote(piece, piece, way, s, peer), remote(whole, whole, way + 1, s, mate)]

    def arrived(kind, p, way):
        _, dst, cols = views(kind, p)
        many = half if way in (3, 5) else rows
        ref = block(dst, cols, d, 0, many)
        pltpu.make_async_copy(ref, ref, recv.at[way, slot(kind, p)]).wait()

    def begin(kind, p):
        copies, keep = own(kind, p)
        for copy in copies:
            copy.start()
        keep.start()

    def pass_on(kind, p):
        for group in range(2):
            arrived(kind, p, group)
            for copy in relays(kind, p, group):
                copy.start()

    def close(kind, p):
        arrived(kind, p, 3)
        arrived(kind, p, 5)
        relays(kind, p, 2)[0].start()

    def finish(kind, p):
        for way in (2, 4, 6, 7):
            arrived(kind, p, way)
        copies, keep = own(kind, p)
        for group in range(3):
            copies = copies + relays(kind, p, group)
        for copy in copies:
            copy.wait_send()
        keep.wait()

    state = {"begun": 0, "query": False, "out": False}

    def ready(kind, p):
        if kind == 1 or (p + 1) * att_w <= fixed:
            return
        need = 1 if (p + 1) * att_w <= fixed + size * part else 2
        for of in range(need):
            if not state[("query", "out")[of]]:
                state[("query", "out")[of]] = True
                fills[1 + of].wait()
                for hop in range(1, size):
                    ref = att_v.at[:, place(of, z)]
                    pltpu.make_async_copy(ref, ref, z_recv.at[of, hop - 1]).wait()
                if of == 1:
                    for hop in range(1, size):
                        cot_copy(hop).start()

    total = len(order)
    for i in range(total + 1):
        while state["begun"] < min(total, i + lead):
            ready(*order[state["begun"]])
            begin(*order[state["begun"]])
            state["begun"] += 1
        if i < total:
            pass_on(*order[i])
        if i > 0:
            close(*order[i - 1])
    for kind, p in order:
        finish(kind, p)
    keep = pltpu.make_async_copy(
        att_v.at[pl.ds(rows, tall - rows), pl.ds(fixed, size * part)], extra_out, fill_sem.at[0]
    )
    keep.start()
    for of in range(2):
        for hop in range(1, size):
            z_copy(of, hop).wait_send()
    for hop in range(1, size):
        pltpu.make_async_copy(cot_ref, cot_ref, cot_recv.at[hop - 1]).wait()
        cot_copy(hop).wait_send()
    fills[3].wait()
    keep.wait()


def front(query, out, fixed, ffn_w, cot, att_tile=512, ffn_tile=768, collective_id=2, limit=48_000_000):
    tall, part = query.shape
    rows, fixed_w = fixed.shape
    size, ways = 4, 8
    att_cols = fixed_w + 2 * size * part
    n_att, n_ffn = att_cols // att_tile, ffn_w.shape[1] // ffn_tile
    n_fixed = fixed_w // att_tile
    third = n_ffn // 3
    order = [(0, p) for p in range(n_fixed)] + [(1, p) for p in range(third)]
    order += [(0, p) for p in range(n_fixed, n_att)] + [(1, p) for p in range(third, n_ffn)]
    bf16 = jnp.bfloat16
    hbm = pl.BlockSpec(memory_space=pl.ANY)
    vmem = pl.BlockSpec(memory_space=pltpu.VMEM)
    dma = pltpu.SemaphoreType.DMA
    shape = lambda *s: jax.ShapeDtypeStruct(s, bf16)
    slots = n_att + n_ffn
    return pl.pallas_call(
        functools.partial(front_body, att_w=att_tile, ffn_w=ffn_tile, order=tuple(order), lead=3),
        out_shape=(
            shape(8 * rows, att_cols), shape(8 * rows, ffn_w.shape[1]),
            shape(size * cot.shape[0], cot.shape[1]), shape(tall - rows, size * part),
        ),
        in_specs=[vmem] * 5,
        out_specs=(hbm,) * 4,
        scratch_shapes=[
            pltpu.VMEM((tall, att_cols), bf16), dma((4,)), dma((2, size - 1)), dma((2, size - 1)),
            dma((size - 1,)), dma((size - 1,)), dma((ways, slots)), dma((ways, slots)), dma((slots,)),
        ],
        compiler_params=pltpu.CompilerParams(
            collective_id=collective_id, has_side_effects=True, vmem_limit_bytes=limit
        ),
        cost_estimate=pl.CostEstimate(
            flops=0, bytes_accessed=20 * rows * (att_cols + ffn_w.shape[1]), transcendentals=0
        ),
        name="front",
    )(query, out, fixed, ffn_w, cot)


def joined_units(gate_w, up_w, down_w, gain_one, gain_two, padded):
    gap = padded - gate_w.shape[1]
    wide = lambda w: jnp.pad(w, ((0, 0), (0, gap)))
    tail = jnp.pad(jnp.stack([gain_one, gain_two], axis=1), ((0, 0), (0, gap - 2)))
    return jnp.concatenate([wide(gate_w), wide(up_w), down_w, tail], axis=1)


def gather_weights(query_w, query_b, out_w, kv_w, ffn_w, cotangent):
    if lax.axis_size("dp") == 8 and lax.axis_size("tensor") == 4:
        tail = jnp.pad(query_b[None, :], ((0, 15), (0, 0)))
        tall_query = jnp.concatenate([query_w, tail], axis=0)
        tall_out = jnp.pad(out_w, ((0, 16), (0, 0)))
        att_all, ffn_all, cot_all, extra = front(tall_query, tall_out, kv_w, ffn_w, cotangent)
        return att_all, ffn_all, cot_all, extra[0]
    pair = lax.all_gather(jnp.stack([query_w, out_w]), "tensor", axis=2, tiled=True)
    att = jnp.concatenate([kv_w, pair[0], pair[1]], axis=1)
    return (
        lax.all_gather(att, "dp", axis=0, tiled=True),
        lax.all_gather(ffn_w, "dp", axis=0, tiled=True),
        lax.all_gather(cotangent, "tensor", axis=0, tiled=True),
        lax.all_gather(query_b, "tensor", axis=0, tiled=True),
    )


def local(
    tokens, segments, gain_one, query_w, query_b, key_w, key_b, value_w, value_b,
    out_w, gain_two, gate_w, up_w, down_w, cotangent,
):
    bf16, f32 = jnp.bfloat16, jnp.float32
    model_width = tokens.shape[1]
    rows = tokens.shape[0]
    tensor_size = lax.axis_size("tensor")
    rank = lax.axis_index("tensor")
    seq_length = rows * tensor_size
    kv_width = key_w.shape[1]
    query_width = query_w.shape[1] * tensor_size
    heads = query_width // HEAD_DIM
    group = heads // KV_HEADS
    scale = HEAD_DIM ** (-0.5)
    units = gate_w.shape[1]
    padded = -(-units // 768) * 768
    fixed_width = 2 * kv_width
    qkv_width = fixed_width + query_width
    att_w, ffn_w, cot_rows, full_query_b = gather_weights(
        query_w, query_b, out_w, jnp.concatenate([key_w, value_w], axis=1),
        joined_units(gate_w, up_w, down_w, gain_one, gain_two, padded), cotangent,
    )
    gains = ffn_w[:, 2 * padded + units : 2 * padded + units + 2].T.astype(f32)
    qkv_w = att_w[:, :qkv_width]
    out_full = att_w[:, qkv_width:]
    qkv_b = jnp.concatenate([key_b, value_b, full_query_b]).astype(f32)

    inputs = tokens.astype(f32)
    inverse_one = lax.rsqrt(jnp.mean(inputs * inputs, axis=-1, keepdims=True) + EPSILON)
    unit_one = inputs * inverse_one
    normed_one = (unit_one * gains[0]).astype(bf16)
    lin = jnp.dot(normed_one, qkv_w, preferred_element_type=f32) + qkv_b
    cosine, sine = angle_tables(rank * rows, rows, HEAD_DIM)
    cos_h, sin_h = cosine[:, None, :], sine[:, None, :]
    query_rot = rotate(lin[:, fixed_width:].reshape(rows, heads, HEAD_DIM), cos_h, sin_h).astype(bf16)
    key_rot = rotate(
        lin[:, :kv_width].reshape(rows, KV_HEADS, HEAD_DIM), cos_h, sin_h
    ).astype(bf16)
    value_own = lin[:, kv_width:fixed_width].astype(bf16)
    kv_own = jnp.concatenate([key_rot.reshape(rows, kv_width), value_own], axis=1)
    back = min(tensor_size - 1, -(-DOC_MAX // rows))
    window = (back + 1) * rows
    first = (rank - back) * rows

    def shift(value, hops):
        pairs = [(i, i + hops) for i in range(tensor_size) if 0 <= i + hops < tensor_size]
        return lax.ppermute(value, "tensor", pairs)

    kv_win = jnp.concatenate([shift(kv_own, hops) for hops in range(back, 0, -1)] + [kv_own], axis=0)
    key_win = kv_win[:, :kv_width].reshape(window, KV_HEADS, HEAD_DIM)
    value_win = kv_win[:, kv_width:].reshape(window, KV_HEADS, HEAD_DIM)
    segment = segments[0]
    own_segment = lax.dynamic_slice_in_dim(segment, rank * rows, rows, 0)
    win_segment = lax.dynamic_slice_in_dim(
        jnp.concatenate([jnp.full((back * rows,), -1, segment.dtype), segment]), rank * rows, window, 0
    )
    own_pos = rank * rows + jnp.arange(rows)
    win_pos = first + jnp.arange(window)
    allowed = (own_segment[:, None] == win_segment[None, :]) & (win_pos[None, :] <= own_pos[:, None])
    grouped = query_rot.reshape(rows, KV_HEADS, group, HEAD_DIM)
    scores = jnp.einsum("tagd,sad->agts", grouped, key_win, preferred_element_type=f32) * scale
    masked = jnp.where(allowed, scores, NEGATIVE)
    largest = jnp.max(masked, axis=-1, keepdims=True)
    log_total = largest + jnp.log(jnp.sum(jnp.exp(masked - largest), axis=-1, keepdims=True))
    probs = jnp.exp(masked - log_total)
    probs_low = probs.astype(bf16)
    context = jnp.einsum("agts,sad->tagd", probs_low, value_win, preferred_element_type=f32)
    context = context.reshape(rows, query_width).astype(bf16)
    middle = inputs + contract_cols(context, out_full)
    inverse_two = lax.rsqrt(jnp.mean(middle * middle, axis=-1, keepdims=True) + EPSILON)
    unit_two = middle * inverse_two
    normed_two = (unit_two * gains[1]).astype(bf16)

    rows_two, hidden_low, d_gate, d_upper, ffn_part, d_normed_two = ffn(
        normed_two, cot_rows, ffn_w
    )
    ffn_sum = lax.psum_scatter(ffn_part, "tensor", scatter_dimension=0, tiled=True).astype(f32)
    mixed = (middle + ffn_sum).astype(bf16)
    d_normed_two = d_normed_two.astype(f32)
    grad_down = contract_rows(cot_rows, hidden_low).astype(bf16)
    grad_gate = contract_rows(rows_two, d_gate).astype(bf16)
    grad_up = contract_rows(rows_two, d_upper).astype(bf16)

    gain_two_term, d_from_two = norm_back(d_normed_two, unit_two, inverse_two, gains[1])
    d_middle = cotangent.astype(f32) + d_from_two
    d_attended = d_middle.astype(bf16)
    d_context = jnp.dot(d_attended, out_full, preferred_element_type=f32).astype(bf16)
    grad_out = contract_rows(d_attended, context).astype(bf16)
    d_context = d_context.reshape(rows, KV_HEADS, group, HEAD_DIM)
    d_probs = jnp.einsum("tagd,sad->agts", d_context, value_win, preferred_element_type=f32)
    row_delta = jnp.sum(probs * d_probs, axis=-1, keepdims=True)
    d_scores = (probs * (d_probs - row_delta)).astype(bf16)
    d_query_rot = jnp.einsum("agts,sad->tagd", d_scores, key_win, preferred_element_type=f32) * scale
    d_key_win = jnp.einsum("agts,tagd->sad", d_scores, grouped, preferred_element_type=f32) * scale
    d_value_win = jnp.einsum("agts,tagd->sad", probs_low, d_context, preferred_element_type=f32)
    d_query_lin = (
        rotate_back(d_query_rot.reshape(rows, heads, HEAD_DIM), cos_h, sin_h)
        .reshape(rows, query_width).astype(bf16)
    )
    d_kv_win = jnp.concatenate(
        [d_key_win.reshape(window, kv_width), d_value_win.reshape(window, kv_width)], axis=1
    ).astype(bf16)
    d_kv = d_kv_win[back * rows :].astype(f32)
    for hops in range(1, back + 1):
        given = d_kv_win[(back - hops) * rows : (back - hops + 1) * rows]
        d_kv = d_kv + shift(given, -hops).astype(f32)
    d_key_lin = rotate_back(d_kv[:, :kv_width].reshape(rows, KV_HEADS, HEAD_DIM), cos_h, sin_h)
    d_lin = jnp.concatenate(
        [d_key_lin.reshape(rows, kv_width).astype(bf16), d_kv[:, kv_width:].astype(bf16), d_query_lin],
        axis=1,
    )
    d_normed_one = contract_cols(d_lin, qkv_w)
    grad_qkv = contract_rows(normed_one, d_lin).astype(bf16)
    bias_term = jnp.sum(d_lin.astype(f32), axis=0)
    gain_one_term, d_from_one = norm_back(d_normed_one, unit_one, inverse_one, gains[0])
    input_grad = (d_middle + d_from_one).astype(bf16)

    def over_dp(grad):
        return lax.psum_scatter(grad, "dp", scatter_dimension=0, tiled=True)

    sum_gate, sum_up, sum_down = (over_dp(g)[:, :units].astype(f32) for g in (grad_gate, grad_up, grad_down))
    part = over_dp(jnp.concatenate([grad_qkv, grad_out], axis=1))
    pair = jnp.stack([part[:, fixed_width:qkv_width], part[:, qkv_width:]])
    pair = lax.psum_scatter(pair, "tensor", scatter_dimension=2, tiled=True).astype(f32)
    kv_part = lax.psum_scatter(
        part[:, :fixed_width], "tensor", scatter_dimension=0, tiled=True
    ).astype(f32)
    small = lax.psum(
        jnp.concatenate([bias_term, gain_one_term, gain_two_term]), ("dp", "tensor")
    )
    place = lax.axis_index("dp") * tensor_size + rank
    devices = lax.axis_size("dp") * tensor_size

    def own(start, size):
        share = size // devices
        return lax.dynamic_slice_in_dim(small, start + place * share, share, 0)

    return (
        mixed,
        input_grad,
        own(qkv_width, model_width),
        pair[0],
        own(fixed_width, query_width),
        kv_part[:, :kv_width],
        small[:kv_width],
        kv_part[:, kv_width:],
        small[kv_width:fixed_width],
        pair[1],
        own(qkv_width + model_width, model_width),
        sum_gate,
        sum_up,
        sum_down,
    )


def solution(mesh):
    both = ("dp", "tensor")
    return jax.shard_map(
        local,
        mesh=mesh,
        in_specs=(
            P(both, None), P("dp", None), P("dp"), P("dp", "tensor"), P("tensor"), P("dp", None), P(),
            P("dp", None), P(), P("dp", "tensor"), P("dp"), P("dp", "tensor"), P("dp", "tensor"),
            P("dp", "tensor"), P(both, None),
        ),
        out_specs=(
            P(both, None), P(both, None), P(both), P("dp", "tensor"), P(both), P(both, None), P(),
            P(both, None), P(), P("dp", "tensor"), P(both), P("dp", "tensor"), P("dp", "tensor"),
            P("dp", "tensor"),
        ),
        check_vma=False,
    )
```

```python
import functools

import jax
import jax.numpy as jnp
from jax import lax
from jax.experimental import pallas as pl
from jax.experimental.pallas import tpu as pltpu
from jax.sharding import PartitionSpec as P

MESH = pl.DeviceIdType.MESH
KV_HEADS = 2
HEAD_DIM = 128
DOC_MAX = 512
EPSILON = 1e-06
ROPE_BASE = 1000000.0
NEGATIVE = -1e30


def square(d):
    core, x, y = d % 2, (d // 2) % 2, d // 4
    by_x, by_y = d + 2 - 4 * x, d + 4 - 8 * y
    return by_x, by_y, d + 1 - 2 * core, by_x + 4 - 8 * y


def front_body(
    query_ref, out_ref, fixed_ref, ffn_ref, cot_ref,
    att_all, ffn_all, cot_all, extra_out,
    att_v, fill_sem, z_send, z_recv, cot_send, cot_recv, send, recv, keep_sem,
    *, att_w, ffn_w, order, lead,
):
    d, z = lax.axis_index("dp"), lax.axis_index("tensor")
    size = 4
    by_x, by_y, mate, across = square(d)
    rows = ffn_ref.shape[0]
    half = rows // 2
    part = query_ref.shape[1]
    fixed = fixed_ref.shape[1]
    chunk = cot_ref.shape[0]
    tall = query_ref.shape[0]

    barrier = pltpu.get_barrier_semaphore()
    for peer in (by_x, by_y, mate):
        pl.semaphore_signal(barrier, inc=1, device_id={"dp": peer}, device_id_type=MESH)
    for hop in range(1, size):
        pl.semaphore_signal(
            barrier, inc=1, device_id={"tensor": (z + hop) % size}, device_id_type=MESH
        )

    def place(of, owner):
        return pl.ds(pl.multiple_of(fixed + of * size * part + owner * part, 128), part)

    fills = [pltpu.make_async_copy(fixed_ref, att_v.at[pl.ds(0, rows), pl.ds(0, fixed)], fill_sem.at[0])]
    for of, ref in enumerate((query_ref, out_ref)):
        fills.append(pltpu.make_async_copy(ref, att_v.at[:, place(of, z)], fill_sem.at[1 + of]))
    at = pl.ds(pl.multiple_of(z * chunk, chunk), chunk)
    fills.append(pltpu.make_async_copy(cot_ref, cot_all.at[at, :], fill_sem.at[3]))
    for copy in fills:
        copy.start()

    pl.semaphore_wait(barrier, 3 + size - 1)

    def z_copy(of, hop):
        ref = (query_ref, out_ref)[of]
        return pltpu.make_async_remote_copy(
            src_ref=ref, dst_ref=att_v.at[:, place(of, z)], send_sem=z_send.at[of, hop - 1],
            recv_sem=z_recv.at[of, hop - 1], device_id={"tensor": (z + hop) % size},
            device_id_type=MESH,
        )

    def cot_copy(hop):
        return pltpu.make_async_remote_copy(
            src_ref=cot_ref, dst_ref=cot_all.at[at, :], send_sem=cot_send.at[hop - 1],
            recv_sem=cot_recv.at[hop - 1], device_id={"tensor": (z + hop) % size},
            device_id_type=MESH,
        )

    for of in range(2):
        for hop in range(1, size):
            z_copy(of, hop).start()
    fills[0].wait()

    def views(kind, p):
        src, dst, wide = ((att_v, att_all, att_w), (ffn_ref, ffn_all, ffn_w))[kind]
        return src, dst, pl.ds(pl.multiple_of(p * wide, 128), wide)

    def slot(kind, p):
        return p + kind * n_att

    n_att = att_all.shape[1] // att_w

    def block(dst, cols, owner, first=0, many=None):
        many = rows if many is None else many
        return dst.at[pl.ds(pl.multiple_of(owner * rows + first, 16), many), cols]

    def remote(src, dst, way, at_slot, peer):
        return pltpu.make_async_remote_copy(
            src_ref=src, dst_ref=dst, send_sem=send.at[way, at_slot], recv_sem=recv.at[way, at_slot],
            device_id={"dp": peer}, device_id_type=MESH,
        )

    def own(kind, p):
        src, dst, cols = views(kind, p)
        mine = src.at[pl.ds(0, rows), cols]
        there = block(dst, cols, d)
        s = slot(kind, p)
        return [
            remote(mine, there, 0, s, by_x), remote(mine, there, 1, s, by_y),
            remote(mine, there, 2, s, mate),
        ], pltpu.make_async_copy(mine, there, keep_sem.at[s])

    def relays(kind, p, group):
        _, dst, cols = views(kind, p)
        s = slot(kind, p)
        if group == 2:
            whole = block(dst, cols, across)
            return [remote(whole, whole, 7, s, mate)]
        owner, peer = ((by_x, by_y), (by_y, by_x))[group]
        piece, whole = block(dst, cols, owner, group * half, half), block(dst, cols, owner)
        way = 3 + 2 * group
        return [remote(piece, piece, way, s, peer), remote(whole, whole, way + 1, s, mate)]

    def arrived(kind, p, way):
        _, dst, cols = views(kind, p)
        many = half if way in (3, 5) else rows
        ref = block(dst, cols, d, 0, many)
        pltpu.make_async_copy(ref, ref, recv.at[way, slot(kind, p)]).wait()

    def begin(kind, p):
        copies, keep = own(kind, p)
        for copy in copies:
            copy.start()
        keep.start()

    def pass_on(kind, p):
        for group in range(2):
            arrived(kind, p, group)
            for copy in relays(kind, p, group):
                copy.start()

    def close(kind, p):
        arrived(kind, p, 3)
        arrived(kind, p, 5)
        relays(kind, p, 2)[0].start()

    def finish(kind, p):
        for way in (2, 4, 6, 7):
            arrived(kind, p, way)
        copies, keep = own(kind, p)
        for group in range(3):
            copies = copies + relays(kind, p, group)
        for copy in copies:
            copy.wait_send()
        keep.wait()

    state = {"begun": 0, "query": False, "out": False}

    def ready(kind, p):
        if kind == 1 or (p + 1) * att_w <= fixed:
            return
        need = 1 if (p + 1) * att_w <= fixed + size * part else 2
        for of in range(need):
            if not state[("query", "out")[of]]:
                state[("query", "out")[of]] = True
                fills[1 + of].wait()
                for hop in range(1, size):
                    ref = att_v.at[:, place(of, z)]
                    pltpu.make_async_copy(ref, ref, z_recv.at[of, hop - 1]).wait()
                if of == 1:
                    for hop in range(1, size):
                        cot_copy(hop).start()

    total = len(order)
    for i in range(total + 1):
        while state["begun"] < min(total, i + lead):
            ready(*order[state["begun"]])
            begin(*order[state["begun"]])
            state["begun"] += 1
        if i < total:
            pass_on(*order[i])
        if i > 0:
            close(*order[i - 1])
    for kind, p in order:
        finish(kind, p)
    keep = pltpu.make_async_copy(
        att_v.at[pl.ds(rows, tall - rows), pl.ds(fixed, size * part)], extra_out, fill_sem.at[0]
    )
    keep.start()
    for of in range(2):
        for hop in range(1, size):
            z_copy(of, hop).wait_send()
    for hop in range(1, size):
        pltpu.make_async_copy(cot_ref, cot_ref, cot_recv.at[hop - 1]).wait()
        cot_copy(hop).wait_send()
    fills[3].wait()
    keep.wait()


def front(query, out, fixed, ffn_w, cot, att_tile=512, ffn_tile=768, collective_id=2, limit=48_000_000):
    tall, part = query.shape
    rows, fixed_w = fixed.shape
    size, ways = 4, 8
    att_cols = fixed_w + 2 * size * part
    n_att, n_ffn = att_cols // att_tile, ffn_w.shape[1] // ffn_tile
    n_fixed = fixed_w // att_tile
    third = n_ffn // 3
    order = [(0, p) for p in range(n_fixed)] + [(1, p) for p in range(third)]
    order += [(0, p) for p in range(n_fixed, n_att)] + [(1, p) for p in range(third, n_ffn)]
    bf16 = jnp.bfloat16
    hbm = pl.BlockSpec(memory_space=pl.ANY)
    vmem = pl.BlockSpec(memory_space=pltpu.VMEM)
    dma = pltpu.SemaphoreType.DMA
    shape = lambda *s: jax.ShapeDtypeStruct(s, bf16)
    slots = n_att + n_ffn
    return pl.pallas_call(
        functools.partial(front_body, att_w=att_tile, ffn_w=ffn_tile, order=tuple(order), lead=3),
        out_shape=(
            shape(8 * rows, att_cols), shape(8 * rows, ffn_w.shape[1]),
            shape(size * cot.shape[0], cot.shape[1]), shape(tall - rows, size * part),
        ),
        in_specs=[vmem] * 5,
        out_specs=(hbm,) * 4,
        scratch_shapes=[
            pltpu.VMEM((tall, att_cols), bf16), dma((4,)), dma((2, size - 1)), dma((2, size - 1)),
            dma((size - 1,)), dma((size - 1,)), dma((ways, slots)), dma((ways, slots)), dma((slots,)),
        ],
        compiler_params=pltpu.CompilerParams(
            collective_id=collective_id, has_side_effects=True, vmem_limit_bytes=limit
        ),
        cost_estimate=pl.CostEstimate(
            flops=0, bytes_accessed=20 * rows * (att_cols + ffn_w.shape[1]), transcendentals=0
        ),
        name="front",
    )(query, out, fixed, ffn_w, cot)


def line_order(z, s):
    upper = z // 2
    near = z * (1 - upper) + (3 - z) * upper
    inner = (1 - s // 3) * ((s + 1) % 3) + (s // 3) * 3
    at = (1 - near) * s + near * inner
    return at * (1 - upper) + (3 - at) * upper


def ffn_body(
    two_ref, cot_ref, weights_ref,
    rows_out, hid_out, dg_out, du_out, sum_out, dn_out,
    rows_v, cot_v, gate_v, up_v, down_v, hid_v, dg_v, du_v, part, land, below, above, res_v,
    tile_sem, load_sem, ag_send, ag_recv, rs_send, rs_recv, own_recv, out_sem,
    *, axis, ft, nt,
):
    f32, bf16 = jnp.float32, jnp.bfloat16
    size = 4
    rows, width = two_ref.shape
    units = weights_ref.shape[1] // 3
    n_f, n_n = units // ft, width // nt
    z = lax.axis_index(axis)
    has_low, has_high = z > 0, z < size - 1

    def to(dz):
        return {axis: z + dz}

    barrier = pltpu.get_barrier_semaphore()

    @pl.when(has_low)
    def _():
        pl.semaphore_signal(barrier, inc=1, device_id=to(-1), device_id_type=MESH)

    @pl.when(has_high)
    def _():
        pl.semaphore_signal(barrier, inc=1, device_id=to(1), device_id_type=MESH)

    own_load = pltpu.make_async_copy(two_ref, rows_v.at[z], load_sem.at[0])
    own_load.start()

    def tile_loads(f):
        cols = pl.ds(pl.multiple_of(f * ft, 128), ft)
        return [
            pltpu.make_async_copy(
                weights_ref.at[:, pl.ds(pl.multiple_of(k * units + f * ft, 128), ft)],
                dst.at[:, cols], tile_sem.at[k, f],
            )
            for k, dst in enumerate((gate_v, up_v, down_v))
        ]

    cot_load = pltpu.make_async_copy(cot_ref, cot_v, load_sem.at[1])
    for f in range(n_f):
        for copy in tile_loads(f):
            copy.start()
        if f == 0:
            cot_load.start()

    pl.semaphore_wait(barrier, (z + size - 1) // size + (2 * size - 2 - z) // size)

    own_load.wait()

    def ag_copy(j, dz):
        way = (dz + 1) // 2
        return pltpu.make_async_remote_copy(
            src_ref=rows_v.at[j], dst_ref=rows_v.at[j], send_sem=ag_send.at[way, j],
            recv_sem=ag_recv.at[j], device_id=to(dz), device_id_type=MESH,
        )

    @pl.when(has_low)
    def _():
        ag_copy(z, -1).start()

    @pl.when(has_high)
    def _():
        ag_copy(z, 1).start()

    def rs_copy(j, n, dz, own):
        way = (dz + 1) // 2
        if own:
            dst = below.at[n] if dz == 1 else above.at[n]
            sem = own_recv.at[1 - way, n]
        else:
            dst, sem = land.at[j, n], rs_recv.at[j, n]
        return pltpu.make_async_remote_copy(
            src_ref=part.at[j, n], dst_ref=dst, send_sem=rs_send.at[j, n],
            recv_sem=sem, device_id=to(dz), device_id_type=MESH,
        )

    def pass_on(j, n, what):
        for dz in (1, -1):
            for own in (True, False):
                hop = j == z + dz
                going = (j > z) if dz == 1 else (j < z)
                near = hop if own else jnp.logical_not(hop)

                @pl.when(jnp.logical_and(going, near))
                def _(dz=dz, own=own):
                    copy = rs_copy(j, n, dz, own)
                    copy.start() if what == "start" else copy.wait_send()

    def out_copies(j):
        at = pl.ds(pl.multiple_of(j * rows, rows), rows)
        return [
            pltpu.make_async_copy(src.at[j], dst.at[at, :], out_sem.at[k, j])
            for k, (src, dst) in enumerate(
                ((rows_v, rows_out), (hid_v, hid_out), (dg_v, dg_out), (du_v, du_out))
            )
        ]

    def step(s, carry):
        for sign in (-1, 1):
            j = z + sign * s
            inside = jnp.logical_and(s > 0, (j >= 0) if sign == -1 else (j < size))

            @pl.when(inside)
            def _(j=j, sign=sign):
                ag_copy(j, -sign).wait_recv()

            onward = has_high if sign == -1 else has_low

            @pl.when(jnp.logical_and(inside, onward))
            def _(j=j, sign=sign):
                ag_copy(j, -sign).start()

        j = line_order(z, s)
        at = pl.ds(pl.multiple_of(j * rows, rows), rows)

        @pl.when(s == 0)
        def _():
            cot_load.wait()

        def units_tile(f, carry):
            @pl.when(s == 0)
            def _():
                for copy in tile_loads(f):
                    copy.wait()

            cols = pl.ds(pl.multiple_of(f * ft, 128), ft)
            mine = rows_v[j]
            gate = jnp.dot(mine, gate_v[:, cols], preferred_element_type=f32)
            upper = jnp.dot(mine, up_v[:, cols], preferred_element_type=f32)
            d_hidden = jnp.dot(cot_v[at, :], down_v[:, cols], preferred_element_type=f32)
            sig = 1.0 / (1.0 + jnp.exp(-gate))
            act = gate * sig
            hid_v[j, :, cols] = (act * upper).astype(bf16)
            du_v[j, :, cols] = (d_hidden * act).astype(bf16)
            dg_v[j, :, cols] = (d_hidden * upper * (sig + act * (1.0 - sig))).astype(bf16)
            return carry

        lax.fori_loop(0, n_f, units_tile, 0)
        for copy in out_copies(j):
            copy.start()
        ends = jnp.logical_and(s > 0, jnp.logical_not(jnp.logical_and(has_low, has_high)))

        def width_tile(n, carry):
            at_n = pl.ds(pl.multiple_of(n * nt, nt), nt)
            dims = (((1,), (1,)), ((), ()))
            total = lax.dot_general(dg_v[j], gate_v[at_n, :], dims, preferred_element_type=f32)
            total += lax.dot_general(du_v[j], up_v[at_n, :], dims, preferred_element_type=f32)
            part[j, n] = total.astype(bf16)

            @pl.when(ends)
            def _():
                pass_on(j, n, "start")

            return carry

        lax.fori_loop(0, n_n, width_tile, 0)
        return carry

    lax.fori_loop(0, size, step, 0)

    def down_tile(i, carry):
        j, n = i // n_n, i % n_n
        at_n = pl.ds(pl.multiple_of(n * nt, nt), nt)
        total = lax.dot_general(
            hid_v[j], down_v[at_n, :], (((1,), (1,)), ((), ())), preferred_element_type=f32
        )
        res_v[j, :, at_n] = total.astype(bf16)
        return carry

    def forward(j, n):
        pltpu.make_async_copy(land.at[j, n], land.at[j, n], rs_recv.at[j, n]).wait()
        part[j, n] = (part[j, n].astype(f32) + land[j, n].astype(f32)).astype(bf16)
        pass_on(j, n, "start")

    middle = jnp.logical_and(has_low, has_high)

    @pl.when(middle)
    def _():
        def first(n, carry):
            forward(3 - z, n)
            return carry

        lax.fori_loop(0, n_n, first, 0)

    lax.fori_loop(0, (size * n_n) // 2, down_tile, 0)

    @pl.when(middle)
    def _():
        def second(n, carry):
            forward(3 - 3 * (z // 2), n)
            forward(3 * (z // 2), n)
            return carry

        lax.fori_loop(0, n_n, second, 0)

    lax.fori_loop((size * n_n) // 2, size * n_n, down_tile, 0)
    sum_copies = [
        pltpu.make_async_copy(
            res_v.at[j], sum_out.at[pl.ds(j * rows, rows), :], load_sem.at[2 + j]
        )
        for j in range(size)
    ]
    for copy in sum_copies:
        copy.start()

    def last(n, carry):
        @pl.when(has_low)
        def _():
            pltpu.make_async_copy(below.at[n], below.at[n], own_recv.at[0, n]).wait()
            part[z, n] = (part[z, n].astype(f32) + below[n].astype(f32)).astype(bf16)

        @pl.when(has_high)
        def _():
            pltpu.make_async_copy(above.at[n], above.at[n], own_recv.at[1, n]).wait()
            part[z, n] = (part[z, n].astype(f32) + above[n].astype(f32)).astype(bf16)

        dn_out[:, pl.ds(pl.multiple_of(n * nt, nt), nt)] = part[z, n]
        return carry

    lax.fori_loop(0, n_n, last, 0)

    def drain(j, carry):
        for copy in out_copies(j):
            copy.wait()
        for dz in (-1, 1):
            came = jnp.logical_or(j == z, (j > z) if dz == -1 else (j < z))
            there = has_low if dz == -1 else has_high

            @pl.when(jnp.logical_and(came, there))
            def _(dz=dz):
                ag_copy(j, dz).wait_send()

        def sent(n, carry):
            @pl.when(j != z)
            def _():
                pltpu.make_async_copy(part.at[j, n], part.at[j, n], rs_send.at[j, n]).wait()

            return carry

        lax.fori_loop(0, n_n, sent, 0)
        return carry

    lax.fori_loop(0, size, drain, 0)
    for copy in sum_copies:
        copy.wait()


def ffn(two, cot_rows, weights, axis="tensor", ft=768, nt=512, collective_id=1, limit=66_000_000):
    rows, width = two.shape
    units = weights.shape[1] // 3
    size = 4
    length = rows * size
    n_f, n_n = units // ft, width // nt
    bf16 = jnp.bfloat16
    hbm = pl.BlockSpec(memory_space=pl.ANY)
    vm = pltpu.VMEM
    dma = pltpu.SemaphoreType.DMA
    shape = lambda *s: jax.ShapeDtypeStruct(s, bf16)
    return pl.pallas_call(
        functools.partial(ffn_body, axis=axis, ft=ft, nt=nt),
        out_shape=(
            shape(length, width), shape(length, units), shape(length, units), shape(length, units),
            shape(length, width), shape(rows, width),
        ),
        in_specs=[hbm] * 3,
        out_specs=(hbm,) * 5 + (pl.BlockSpec(memory_space=pltpu.VMEM),),
        scratch_shapes=[
            vm((size, rows, width), bf16), vm((length, width), bf16),
            vm((width, units), bf16), vm((width, units), bf16), vm((width, units), bf16),
            vm((size, rows, units), bf16), vm((size, rows, units), bf16), vm((size, rows, units), bf16),
            vm((size, n_n, rows, nt), bf16), vm((size, n_n, rows, nt), bf16),
            vm((n_n, rows, nt), bf16), vm((n_n, rows, nt), bf16),
            vm((size, rows, width), bf16),
            dma((3, n_f)), dma((2 + size,)), dma((2, size)), dma((size,)), dma((size, n_n)), dma((size, n_n)),
            dma((2, n_n)), dma((4, size)),
        ],
        compiler_params=pltpu.CompilerParams(
            collective_id=collective_id, has_side_effects=True, vmem_limit_bytes=limit
        ),
        cost_estimate=pl.CostEstimate(
            flops=12 * length * width * units, bytes_accessed=8 * width * units + 8 * length * units,
            transcendentals=length * units,
        ),
        name="ffn",
    )(two, cot_rows, weights)


def back_body(
    two_ref, cot_ref, hid_ref, dg_ref, du_ref, lhs_ref, rhs_ref, part_ref, small_ref,
    ffn_out, query_out, out_out, kv_out, sum_out, small_out,
    left_v, right_v, grad, mate_land, core_sum, x_land, y_land, second, x_last, y_last, stage, fin,
    z_land, kv_land, sum_land, small_z, small_hop, small_next,
    left_sem, right_sem, mate_send, mate_recv, one_send, one_recv, two_send, two_recv, stage_sem,
    z_send, z_recv, kv_send, kv_recv, sum_send, sum_recv, own_sem, small_send, small_recv,
    hop_send, hop_recv, *, n_f, wide, cols_out,
):
    f32, bf16 = jnp.float32, jnp.bfloat16
    d, z = lax.axis_index("dp"), lax.axis_index("tensor")
    size = 4
    core, x, y = d % 2, (d // 2) % 2, d // 4
    by_x, by_y, mate, _ = square(d)
    here, at_x, at_y = 2 * y + x, 2 * y + 1 - x, 2 * (1 - y) + x
    cross = 3 - here
    block, half = core_sum.shape[2], core_sum.shape[2] // 2
    n_ffn, n_att = 3 * n_f, rhs_ref.shape[1] // wide
    total = n_ffn + n_att
    chunk = sum_out.shape[0]
    share = block // size
    part_w = wide // 2

    barrier = pltpu.get_barrier_semaphore()
    for peer in (by_x, by_y, mate):
        pl.semaphore_signal(barrier, inc=1, device_id={"dp": peer}, device_id_type=MESH)
    for hop in range(1, size):
        pl.semaphore_signal(
            barrier, inc=1, device_id={"tensor": (z + hop) % size}, device_id_type=MESH
        )

    lefts = [
        pltpu.make_async_copy(ref, left_v.at[k], left_sem.at[k])
        for k, ref in enumerate((cot_ref, two_ref))
    ]

    def right_load(i, what):
        cols = pl.ds(pl.multiple_of((i % n_f) * wide, 128), wide)
        for m, ref in enumerate((hid_ref, dg_ref, du_ref)):
            copy = pltpu.make_async_copy(ref.at[:, cols], right_v.at[i % 2], right_sem.at[i % 2])

            @pl.when(i // n_f == m)
            def _(copy=copy):
                copy.start() if what == "start" else copy.wait()

    lefts[0].start()
    right_load(jnp.int32(0), "start")
    lefts[1].start()

    def chunk_rows(j):
        return part_ref.at[pl.ds(pl.multiple_of(j * chunk, chunk), chunk), :]

    own_part = pltpu.make_async_copy(chunk_rows(z), sum_land.at[size - 1], own_sem.at[0])
    own_part.start()
    pl.semaphore_wait(barrier, 3 + size - 1)

    def dp_copy(src, dst, send_sem, recv_sem, peer):
        return pltpu.make_async_remote_copy(
            src_ref=src, dst_ref=dst, send_sem=send_sem, recv_sem=recv_sem,
            device_id={"dp": peer}, device_id_type=MESH,
        )

    def z_copy(src, dst, send_sem, recv_sem, peer):
        return pltpu.make_async_remote_copy(
            src_ref=src, dst_ref=dst, send_sem=send_sem, recv_sem=recv_sem,
            device_id={"tensor": peer}, device_id_type=MESH,
        )

    small_copies, sum_copies = [], []
    for hop in range(1, size):
        to, k = (z + hop) % size, hop - 1
        small_copies.append(
            z_copy(small_ref, small_z.at[k], small_send.at[k], small_recv.at[k], to)
        )
        sum_copies.append(
            z_copy(chunk_rows(to), sum_land.at[k], sum_send.at[k], sum_recv.at[k], to)
        )
    for copy in small_copies + sum_copies:
        copy.start()

    hops = (mate, by_x, by_y)

    def hop_copy(k):
        return dp_copy(small_next.at[k], small_hop.at[k], hop_send.at[k], hop_recv.at[k], hops[k])

    def mate_copy(i):
        return dp_copy(
            grad.at[i % 2, :, 1 - core], mate_land.at[i % 4], mate_send.at[i % 4],
            mate_recv.at[i % 4], mate,
        )

    def one_copies(i):
        s = core_sum.at[i % 4]
        first, last = pl.ds(0, half), pl.ds(half, half)
        plan = (
            (s.at[at_x, first, :], x_land.at[i, 0], by_x), (s.at[cross, first, :], x_land.at[i, 1], by_x),
            (s.at[at_y, last, :], y_land.at[i, 0], by_y), (s.at[cross, last, :], y_land.at[i, 1], by_y),
        )
        return [
            dp_copy(src, dst, one_send.at[k, i], one_recv.at[k, i], peer)
            for k, (src, dst, peer) in enumerate(plan)
        ]

    def two_copies(i):
        return [
            dp_copy(second.at[i % 4, 0], y_last.at[i], two_send.at[0, i], two_recv.at[0, i], by_y),
            dp_copy(second.at[i % 4, 1], x_last.at[i], two_send.at[1, i], two_recv.at[1, i], by_x),
        ]

    def stage_copy(i):
        cols = pl.ds(pl.multiple_of(i * wide, 128), wide)
        return pltpu.make_async_copy(stage.at[i % 2], ffn_out.at[:, cols], stage_sem.at[i % 2])

    def multiply(i):
        @pl.when(jnp.logical_and(i >= 2, i < total))
        def _():
            mate_copy(i - 2).wait_send()

        @pl.when(i + 1 < n_ffn)
        def _():
            right_load(i + 1, "start")

        dims = (((0,), (0,)), ((), ()))

        @pl.when(i < n_ffn)
        def _():
            @pl.when(i == 0)
            def _():
                lefts[0].wait()

            @pl.when(i == n_f)
            def _():
                lefts[1].wait()

            right_load(i, "wait")

            def rows(k, carry):
                at = pl.ds(pl.multiple_of(k * 2 * block, 128), 2 * block)
                value = lax.dot_general(
                    left_v[(i // n_f + 1) // 2, :, at], right_v[i % 2], dims, preferred_element_type=f32
                )
                grad[i % 2, k] = value.astype(bf16).reshape(2, block, wide)
                return carry

            lax.fori_loop(0, 4, rows, 0)

        @pl.when(jnp.logical_and(i >= n_ffn, i < total))
        def _():
            a = i - n_ffn
            cols = pl.ds(pl.multiple_of(a * wide, 128), wide)

            def rows(k, carry):
                at = pl.ds(pl.multiple_of(k * 2 * block, 128), 2 * block)
                value = lax.dot_general(
                    lhs_ref[(a // 2) % 2, :, at], rhs_ref[:, cols], dims, preferred_element_type=f32
                )
                grad[i % 2, k] = value.astype(bf16).reshape(2, block, wide)
                return carry

            lax.fori_loop(0, 4, rows, 0)

        @pl.when(i < total)
        def _():
            mate_copy(i).start()

    def sum_cores(i):
        mate_copy(i).wait_recv()
        for k in range(4):
            core_sum[i % 4, k] = (
                grad[i % 2, k, core].astype(f32) + mate_land[i % 4, k].astype(f32)
            ).astype(bf16)
        for copy in one_copies(i):
            copy.start()

    def sum_near(i):
        for copy in one_copies(i):
            copy.wait_recv()
        s = core_sum.at[i % 4]
        second[i % 4, 0] = (s[at_y, :half].astype(f32) + x_land[i, 1].astype(f32)).astype(bf16)
        second[i % 4, 1] = (s[at_x, half:].astype(f32) + y_land[i, 1].astype(f32)).astype(bf16)
        for copy in two_copies(i):
            copy.start()

    def z_sends(a, what):
        for h in range(2):
            owner = (a % 2) * 2 + h
            hop = (owner - z + size) % size
            src = fin.at[a, :, pl.ds(h * part_w, part_w)]

            @pl.when(jnp.logical_and(a < 4, hop > 0))
            def _(src=src, owner=owner, hop=hop, h=h):
                copy = z_copy(
                    src, z_land.at[a // 2, hop - 1], z_send.at[a, h], z_recv.at[a // 2, hop - 1], owner
                )
                copy.start() if what == "start" else copy.wait_send()

        @pl.when(a == 4)
        def _():
            for hop in range(1, size):
                to = (z + hop) % size
                rows = pl.ds(pl.multiple_of(to * share, 16), share)
                copy = z_copy(
                    fin.at[4, rows, :], kv_land.at[hop - 1], kv_send.at[hop - 1], kv_recv.at[hop - 1], to
                )
                copy.start() if what == "start" else copy.wait_send()

    def finish(i):
        for copy in two_copies(i):
            copy.wait_recv()
        own = core_sum.at[i % 4, here]
        top = own[:half].astype(f32) + x_land[i, 0].astype(f32) + y_last[i].astype(f32)
        low = own[half:].astype(f32) + y_land[i, 0].astype(f32) + x_last[i].astype(f32)

        @pl.when(i < n_ffn)
        def _():
            @pl.when(i >= 2)
            def _():
                stage_copy(i - 2).wait()

            stage[i % 2, :half] = top
            stage[i % 2, half:] = low
            stage_copy(i).start()

        @pl.when(i >= n_ffn)
        def _():
            a = i - n_ffn
            fin[a, :half] = top.astype(bf16)
            fin[a, half:] = low.astype(bf16)
            z_sends(a, "start")

        for copy in one_copies(i) + two_copies(i):
            copy.wait_send()

    def small_step(i):
        @pl.when(i == 2)
        def _():
            for copy in small_copies:
                copy.wait_recv()
            small_next[0] = small_ref[...] + small_z[0] + small_z[1] + small_z[2]
            hop_copy(0).start()

        for k in range(2):

            @pl.when(i == 3 + k)
            def _(k=k):
                hop_copy(k).wait_recv()
                small_next[k + 1] = small_next[k] + small_hop[k]
                hop_copy(k + 1).start()

        @pl.when(i == 5)
        def _():
            hop_copy(2).wait_recv()
            small_out[...] = small_next[2] + small_hop[2]

    def turn(i, carry):
        multiply(i)
        for lag, work in ((1, sum_cores), (2, sum_near), (3, finish)):

            @pl.when(jnp.logical_and(i >= lag, i - lag < total))
            def _(lag=lag, work=work):
                work(i - lag)

        small_step(i)
        return carry

    lax.fori_loop(0, total + 3, turn, 0)
    for i in (total - 2, total - 1):
        mate_copy(i).wait_send()
    for i in (n_ffn - 2, n_ffn - 1):
        stage_copy(i).wait()
    own_part.wait()
    for copy in sum_copies:
        copy.wait_recv()
    acc = sum_land[size - 1].astype(f32)
    for k in range(size - 1):
        acc += sum_land[k].astype(f32)
    sum_out[...] = acc.astype(bf16)
    for of, dst in ((0, query_out), (1, out_out)):
        for k in range(size - 1):
            ref = z_land.at[of, k]
            pltpu.make_async_copy(ref, ref, z_recv.at[of, k]).wait()
        for h in range(4):

            @pl.when(z == h)
            def _(of=of, dst=dst, h=h):
                acc = fin[2 * of + h // 2, :, (h % 2) * part_w : (h % 2 + 1) * part_w].astype(f32)
                for k in range(size - 1):
                    acc += z_land[of, k].astype(f32)
                dst[...] = acc

    for k in range(size - 1):
        pltpu.make_async_copy(kv_land.at[k], kv_land.at[k], kv_recv.at[k]).wait()
    rows = pl.ds(pl.multiple_of(z * share, 16), share)
    acc = fin[4, rows, :].astype(f32)
    for k in range(size - 1):
        acc += kv_land[k].astype(f32)
    kv_out[...] = acc
    for a in range(n_att):
        z_sends(a, "wait")
    for copy in sum_copies + small_copies:
        copy.wait_send()
    for k in range(3):
        hop_copy(k).wait_send()


def back(two, cot_rows, hid, dg, du, lhs, rhs, ffn_part, small, wide=768, collective_id=3, limit=67_000_000):
    length, width = two.shape
    size, chunk, block = 4, lhs.shape[1], width // 8
    units = hid.shape[1]
    n_f, n_att = units // wide, rhs.shape[1] // wide
    n_ffn = 3 * n_f
    total = n_ffn + n_att
    half, part_w, share = block // 2, wide // 2, block // size
    bf16, f32 = jnp.bfloat16, jnp.float32
    hbm = pl.BlockSpec(memory_space=pl.ANY)
    vmem = pl.BlockSpec(memory_space=pltpu.VMEM)
    vm = pltpu.VMEM
    dma = pltpu.SemaphoreType.DMA
    shape = jax.ShapeDtypeStruct
    return pl.pallas_call(
        functools.partial(back_body, n_f=n_f, wide=wide, cols_out=3 * units),
        out_shape=(
            shape((block, 3 * units), f32), shape((block, part_w), f32), shape((block, part_w), f32),
            shape((share, wide), f32), shape((chunk, width), bf16), shape(small.shape, f32),
        ),
        in_specs=[hbm] * 5 + [vmem, vmem, hbm, vmem],
        out_specs=(hbm,) + (vmem,) * 5,
        scratch_shapes=[
            vm((2, length, width), bf16), vm((2, length, wide), bf16), vm((2, 4, 2, block, wide), bf16),
            vm((4, 4, block, wide), bf16), vm((4, 4, block, wide), bf16),
            vm((total, 2, half, wide), bf16), vm((total, 2, half, wide), bf16),
            vm((4, 2, half, wide), bf16), vm((total, half, wide), bf16), vm((total, half, wide), bf16),
            vm((2, block, wide), f32), vm((n_att, block, wide), bf16),
            vm((2, size - 1, block, part_w), bf16), vm((size - 1, share, wide), bf16),
            vm((size, chunk, width), bf16), vm((3,) + small.shape, f32), vm((3,) + small.shape, f32),
            vm((3,) + small.shape, f32),
            dma((2,)), dma((2,)), dma((4,)), dma((4,)), dma((4, total)), dma((4, total)),
            dma((2, total)), dma((2, total)), dma((2,)),
            dma((4, 2)), dma((2, size - 1)), dma((size - 1,)), dma((size - 1,)), dma((size - 1,)),
            dma((size - 1,)), dma((1,)), dma((size - 1,)), dma((size - 1,)), dma((3,)), dma((3,)),
        ],
        compiler_params=pltpu.CompilerParams(
            collective_id=collective_id, has_side_effects=True, vmem_limit_bytes=limit
        ),
        cost_estimate=pl.CostEstimate(
            flops=6 * length * width * units, bytes_accessed=8 * length * units, transcendentals=0
        ),
        name="back",
    )(two, cot_rows, hid, dg, du, lhs, rhs, ffn_part, small)


def angle_tables(first, length, head_width):
    position = (first + jnp.arange(length)).astype(jnp.float32)
    exponent = jnp.arange(head_width // 2, dtype=jnp.float32) * (2.0 / head_width)
    frequency = ROPE_BASE ** (-exponent)
    angle = position[:, None] * frequency[None, :]
    return (jnp.cos(angle), jnp.sin(angle))


def rotate(values, cosine, sine):
    half_width = values.shape[-1] // 2
    first_half = values[..., :half_width]
    second_half = values[..., half_width:]
    return jnp.concatenate(
        [first_half * cosine - second_half * sine, second_half * cosine + first_half * sine],
        axis=-1,
    )


def rotate_back(grads, cosine, sine):
    return rotate(grads, cosine, -sine)


def dot_f32(left, right, dims):
    return lax.dot_general(left, right, (dims, ((), ())), preferred_element_type=jnp.float32)


def contract_rows(left, right):
    return dot_f32(left, right, ((0,), (0,)))


def contract_cols(left, right):
    return dot_f32(left, right, ((1,), (1,)))


def norm_back(upstream, unit, inverse, gain):
    scaled = upstream * gain
    gain_term = jnp.sum(upstream * unit, axis=0)
    input_term = inverse * (scaled - unit * jnp.mean(scaled * unit, axis=-1, keepdims=True))
    return (gain_term, input_term)


def joined_units(gate_w, up_w, down_w, gain_one, gain_two, padded):
    gap = padded - gate_w.shape[1]
    wide = lambda w: jnp.pad(w, ((0, 0), (0, gap)))
    tail = jnp.pad(jnp.stack([gain_one, gain_two], axis=1), ((0, 0), (0, gap - 2)))
    return jnp.concatenate([wide(gate_w), wide(up_w), down_w, tail], axis=1)


def gather_weights(query_w, query_b, out_w, kv_w, ffn_w, cotangent):
    if lax.axis_size("dp") == 8 and lax.axis_size("tensor") == 4:
        tail = jnp.pad(query_b[None, :], ((0, 15), (0, 0)))
        tall_query = jnp.concatenate([query_w, tail], axis=0)
        tall_out = jnp.pad(out_w, ((0, 16), (0, 0)))
        att_all, ffn_all, cot_all, extra = front(tall_query, tall_out, kv_w, ffn_w, cotangent)
        return att_all, ffn_all, cot_all, extra[0]
    pair = lax.all_gather(jnp.stack([query_w, out_w]), "tensor", axis=2, tiled=True)
    att = jnp.concatenate([kv_w, pair[0], pair[1]], axis=1)
    return (
        lax.all_gather(att, "dp", axis=0, tiled=True),
        lax.all_gather(ffn_w, "dp", axis=0, tiled=True),
        lax.all_gather(cotangent, "tensor", axis=0, tiled=True),
        lax.all_gather(query_b, "tensor", axis=0, tiled=True),
    )


def sum_grads(two, cot_rows, hid, dg, du, normed_one, d_attended, d_lin, context, ffn_part, small):
    f32, bf16 = jnp.float32, jnp.bfloat16
    padded = hid.shape[1]
    fixed = d_lin.shape[1] - context.shape[1]
    d_query = d_lin[:, fixed:]
    if lax.axis_size("dp") == 8 and lax.axis_size("tensor") == 4:
        gap = context.shape[1] // 2 - fixed
        rhs = jnp.concatenate([d_query, context, jnp.pad(d_lin[:, :fixed], ((0, 0), (0, gap)))], axis=1)
        lhs = jnp.stack([normed_one, d_attended])
        flat, query, out, kv, ffn_sum, total = back(
            two, cot_rows, hid, dg, du, lhs, rhs, ffn_part, small.reshape(-1, 128)
        )
        flat = [flat[:, k * padded : (k + 1) * padded] for k in range(3)]
        return (*flat, query, out, kv, ffn_sum, total.reshape(-1))

    def over_dp(left, right):
        return lax.psum_scatter(
            contract_rows(left, right).astype(bf16), "dp", scatter_dimension=0, tiled=True
        )

    def over_tensor(value, axis):
        return lax.psum_scatter(value, "tensor", scatter_dimension=axis, tiled=True).astype(f32)

    return (
        over_dp(cot_rows, hid).astype(f32),
        over_dp(two, dg).astype(f32),
        over_dp(two, du).astype(f32),
        over_tensor(over_dp(normed_one, d_query), 1),
        over_tensor(over_dp(d_attended, context), 1),
        over_tensor(over_dp(normed_one, d_lin[:, :fixed]), 0),
        over_tensor(ffn_part, 0),
        lax.psum(small, ("dp", "tensor")),
    )


def local(
    tokens, segments, gain_one, query_w, query_b, key_w, key_b, value_w, value_b,
    out_w, gain_two, gate_w, up_w, down_w, cotangent,
):
    bf16, f32 = jnp.bfloat16, jnp.float32
    model_width = tokens.shape[1]
    rows = tokens.shape[0]
    tensor_size = lax.axis_size("tensor")
    rank = lax.axis_index("tensor")
    seq_length = rows * tensor_size
    kv_width = key_w.shape[1]
    query_width = query_w.shape[1] * tensor_size
    heads = query_width // HEAD_DIM
    group = heads // KV_HEADS
    scale = HEAD_DIM ** (-0.5)
    units = gate_w.shape[1]
    padded = -(-units // 768) * 768
    fixed_width = 2 * kv_width
    qkv_width = fixed_width + query_width
    att_w, ffn_w, cot_rows, full_query_b = gather_weights(
        query_w, query_b, out_w, jnp.concatenate([key_w, value_w], axis=1),
        joined_units(gate_w, up_w, down_w, gain_one, gain_two, padded), cotangent,
    )
    gains = ffn_w[:, 2 * padded + units : 2 * padded + units + 2].T.astype(f32)
    qkv_w = att_w[:, :qkv_width]
    out_full = att_w[:, qkv_width:]
    qkv_b = jnp.concatenate([key_b, value_b, full_query_b]).astype(f32)

    inputs = tokens.astype(f32)
    inverse_one = lax.rsqrt(jnp.mean(inputs * inputs, axis=-1, keepdims=True) + EPSILON)
    unit_one = inputs * inverse_one
    normed_one = (unit_one * gains[0]).astype(bf16)
    lin = jnp.dot(normed_one, qkv_w, preferred_element_type=f32) + qkv_b
    cosine, sine = angle_tables(rank * rows, rows, HEAD_DIM)
    cos_h, sin_h = cosine[:, None, :], sine[:, None, :]
    query_rot = rotate(lin[:, fixed_width:].reshape(rows, heads, HEAD_DIM), cos_h, sin_h).astype(bf16)
    key_rot = rotate(
        lin[:, :kv_width].reshape(rows, KV_HEADS, HEAD_DIM), cos_h, sin_h
    ).astype(bf16)
    value_own = lin[:, kv_width:fixed_width].astype(bf16)
    kv_own = jnp.concatenate([key_rot.reshape(rows, kv_width), value_own], axis=1)
    back = min(tensor_size - 1, -(-DOC_MAX // rows))
    window = (back + 1) * rows
    first = (rank - back) * rows

    def shift(value, hops):
        pairs = [(i, i + hops) for i in range(tensor_size) if 0 <= i + hops < tensor_size]
        return lax.ppermute(value, "tensor", pairs)

    kv_win = jnp.concatenate([shift(kv_own, hops) for hops in range(back, 0, -1)] + [kv_own], axis=0)
    key_win = kv_win[:, :kv_width].reshape(window, KV_HEADS, HEAD_DIM)
    value_win = kv_win[:, kv_width:].reshape(window, KV_HEADS, HEAD_DIM)
    segment = segments[0]
    own_segment = lax.dynamic_slice_in_dim(segment, rank * rows, rows, 0)
    win_segment = lax.dynamic_slice_in_dim(
        jnp.concatenate([jnp.full((back * rows,), -1, segment.dtype), segment]), rank * rows, window, 0
    )
    own_pos = rank * rows + jnp.arange(rows)
    win_pos = first + jnp.arange(window)
    allowed = (own_segment[:, None] == win_segment[None, :]) & (win_pos[None, :] <= own_pos[:, None])
    grouped = query_rot.reshape(rows, KV_HEADS, group, HEAD_DIM)
    scores = jnp.einsum("tagd,sad->agts", grouped, key_win, preferred_element_type=f32) * scale
    masked = jnp.where(allowed, scores, NEGATIVE)
    largest = jnp.max(masked, axis=-1, keepdims=True)
    log_total = largest + jnp.log(jnp.sum(jnp.exp(masked - largest), axis=-1, keepdims=True))
    probs = jnp.exp(masked - log_total)
    probs_low = probs.astype(bf16)
    context = jnp.einsum("agts,sad->tagd", probs_low, value_win, preferred_element_type=f32)
    context = context.reshape(rows, query_width).astype(bf16)
    middle = inputs + contract_cols(context, out_full)
    inverse_two = lax.rsqrt(jnp.mean(middle * middle, axis=-1, keepdims=True) + EPSILON)
    unit_two = middle * inverse_two
    normed_two = (unit_two * gains[1]).astype(bf16)

    rows_two, hidden_low, d_gate, d_upper, ffn_part, d_normed_two = ffn(
        normed_two, cot_rows, ffn_w
    )
    d_normed_two = d_normed_two.astype(f32)
    gain_two_term, d_from_two = norm_back(d_normed_two, unit_two, inverse_two, gains[1])
    d_middle = cotangent.astype(f32) + d_from_two
    d_attended = d_middle.astype(bf16)
    d_context = jnp.dot(d_attended, out_full, preferred_element_type=f32).astype(bf16)
    d_context = d_context.reshape(rows, KV_HEADS, group, HEAD_DIM)
    d_probs = jnp.einsum("tagd,sad->agts", d_context, value_win, preferred_element_type=f32)
    row_delta = jnp.sum(probs * d_probs, axis=-1, keepdims=True)
    d_scores = (probs * (d_probs - row_delta)).astype(bf16)
    d_query_rot = jnp.einsum("agts,sad->tagd", d_scores, key_win, preferred_element_type=f32) * scale
    d_key_win = jnp.einsum("agts,tagd->sad", d_scores, grouped, preferred_element_type=f32) * scale
    d_value_win = jnp.einsum("agts,tagd->sad", probs_low, d_context, preferred_element_type=f32)
    d_query_lin = (
        rotate_back(d_query_rot.reshape(rows, heads, HEAD_DIM), cos_h, sin_h)
        .reshape(rows, query_width).astype(bf16)
    )
    d_kv_win = jnp.concatenate(
        [d_key_win.reshape(window, kv_width), d_value_win.reshape(window, kv_width)], axis=1
    ).astype(bf16)
    d_kv = d_kv_win[back * rows :].astype(f32)
    for hops in range(1, back + 1):
        given = d_kv_win[(back - hops) * rows : (back - hops + 1) * rows]
        d_kv = d_kv + shift(given, -hops).astype(f32)
    d_key_lin = rotate_back(d_kv[:, :kv_width].reshape(rows, KV_HEADS, HEAD_DIM), cos_h, sin_h)
    d_lin = jnp.concatenate(
        [d_key_lin.reshape(rows, kv_width).astype(bf16), d_kv[:, kv_width:].astype(bf16), d_query_lin],
        axis=1,
    )
    d_normed_one = contract_cols(d_lin, qkv_w)
    bias_term = jnp.sum(d_lin.astype(f32), axis=0)
    gain_one_term, d_from_one = norm_back(d_normed_one, unit_one, inverse_one, gains[0])
    input_grad = (d_middle + d_from_one).astype(bf16)

    sums = sum_grads(
        rows_two, cot_rows, hidden_low, d_gate, d_upper, normed_one, d_attended, d_lin, context,
        ffn_part, jnp.concatenate([bias_term, gain_one_term, gain_two_term]),
    )
    sum_down, sum_gate, sum_up, sum_query, sum_out, sum_kv, ffn_sum, small = sums
    mixed = (middle + ffn_sum.astype(f32)).astype(bf16)
    place = lax.axis_index("dp") * tensor_size + rank
    devices = lax.axis_size("dp") * tensor_size

    def own(start, size):
        share = size // devices
        return lax.dynamic_slice_in_dim(small, start + place * share, share, 0)

    return (
        mixed,
        input_grad,
        own(qkv_width, model_width),
        sum_query,
        own(fixed_width, query_width),
        sum_kv[:, :kv_width],
        small[:kv_width],
        sum_kv[:, kv_width : 2 * kv_width],
        small[kv_width:fixed_width],
        sum_out,
        own(qkv_width + model_width, model_width),
        sum_gate[:, :units],
        sum_up[:, :units],
        sum_down[:, :units],
    )


def solution(mesh):
    both = ("dp", "tensor")
    return jax.shard_map(
        local,
        mesh=mesh,
        in_specs=(
            P(both, None), P("dp", None), P("dp"), P("dp", "tensor"), P("tensor"), P("dp", None), P(),
            P("dp", None), P(), P("dp", "tensor"), P("dp"), P("dp", "tensor"), P("dp", "tensor"),
            P("dp", "tensor"), P(both, None),
        ),
        out_specs=(
            P(both, None), P(both, None), P(both), P("dp", "tensor"), P(both), P(both, None), P(),
            P(both, None), P(), P("dp", "tensor"), P(both), P("dp", "tensor"), P("dp", "tensor"),
            P("dp", "tensor"),
        ),
        check_vma=False,
    )
```

```python
import functools

import jax
import jax.numpy as jnp
from jax import lax
from jax.experimental import pallas as pl
from jax.experimental.pallas import tpu as pltpu
from jax.sharding import PartitionSpec as P

MESH = pl.DeviceIdType.MESH
KV_HEADS = 2
HEAD_DIM = 128
DOC_MAX = 512
EPSILON = 1e-06
ROPE_BASE = 1000000.0
NEGATIVE = -1e30


def square(d):
    core, x, y = d % 2, (d // 2) % 2, d // 4
    by_x, by_y = d + 2 - 4 * x, d + 4 - 8 * y
    return by_x, by_y, d + 1 - 2 * core, by_x + 4 - 8 * y


def front_body(
    x_ref, turn_ref, mask_ref, bias_ref, query_ref, out_ref, fixed_ref, ffn_ref, cot_ref,
    att_all, ffn_all, cot_all, two_out, mid_out, one_out, query_rot, kv_win, lse_out, ctx_out, gain_out,
    att_v, w_v, one_v, q_v, kv_v, ctx_v, mid_v, two_v,
    fill_sem, z_send, z_recv, cot_send, cot_recv, send, recv, keep_sem, w_sem, kv_send, kv_recv, save_sem,
    *, pieces, order, lead,
):
    f32, bf16 = jnp.float32, jnp.bfloat16
    d, z = lax.axis_index("dp"), lax.axis_index("tensor")
    size = 4
    by_x, by_y, mate, across = square(d)
    rows = ffn_ref.shape[0]
    half = rows // 2
    part = query_ref.shape[1]
    fixed = fixed_ref.shape[1]
    chunk = cot_ref.shape[0]
    tall = query_ref.shape[0]

    barrier = pltpu.get_barrier_semaphore()
    for peer in (by_x, by_y, mate):
        pl.semaphore_signal(barrier, inc=1, device_id={"dp": peer}, device_id_type=MESH)
    for hop in range(1, size):
        pl.semaphore_signal(
            barrier, inc=1, device_id={"tensor": (z + hop) % size}, device_id_type=MESH
        )

    def place(of, owner):
        return pl.ds(pl.multiple_of(fixed + of * size * part + owner * part, 128), part)

    fills = [pltpu.make_async_copy(fixed_ref, att_v.at[pl.ds(0, rows), pl.ds(0, fixed)], fill_sem.at[0])]
    for of, ref in enumerate((query_ref, out_ref)):
        fills.append(pltpu.make_async_copy(ref, att_v.at[:, place(of, z)], fill_sem.at[1 + of]))
    at = pl.ds(pl.multiple_of(z * chunk, chunk), chunk)
    fills.append(pltpu.make_async_copy(cot_ref, cot_all.at[at, :], fill_sem.at[3]))
    for copy in fills:
        copy.start()

    pl.semaphore_wait(barrier, 3 + size - 1)

    def z_copy(of, hop):
        ref = (query_ref, out_ref)[of]
        return pltpu.make_async_remote_copy(
            src_ref=ref, dst_ref=att_v.at[:, place(of, z)], send_sem=z_send.at[of, hop - 1],
            recv_sem=z_recv.at[of, hop - 1], device_id={"tensor": (z + hop) % size},
            device_id_type=MESH,
        )

    def cot_copy(hop):
        return pltpu.make_async_remote_copy(
            src_ref=cot_ref, dst_ref=cot_all.at[at, :], send_sem=cot_send.at[hop - 1],
            recv_sem=cot_recv.at[hop - 1], device_id={"tensor": (z + hop) % size},
            device_id_type=MESH,
        )

    for of in range(2):
        for hop in range(1, size):
            z_copy(of, hop).start()
    fills[0].wait()

    def views(kind, p):
        src, dst = ((att_v, att_all), (ffn_ref, ffn_all))[kind]
        return src, dst, pl.ds(*pieces[kind][p])

    def slot(kind, p):
        return p + kind * len(pieces[0])

    def block(dst, cols, owner, first=0, many=None):
        many = rows if many is None else many
        return dst.at[pl.ds(pl.multiple_of(owner * rows + first, 16), many), cols]

    def remote(src, dst, way, at_slot, peer):
        return pltpu.make_async_remote_copy(
            src_ref=src, dst_ref=dst, send_sem=send.at[way, at_slot], recv_sem=recv.at[way, at_slot],
            device_id={"dp": peer}, device_id_type=MESH,
        )

    def own(kind, p):
        src, dst, cols = views(kind, p)
        mine = src.at[pl.ds(0, rows), cols]
        there = block(dst, cols, d)
        s = slot(kind, p)
        return [
            remote(mine, there, 0, s, by_x), remote(mine, there, 1, s, by_y),
            remote(mine, there, 2, s, mate),
        ], pltpu.make_async_copy(mine, there, keep_sem.at[s])

    def relays(kind, p, group):
        _, dst, cols = views(kind, p)
        s = slot(kind, p)
        if group == 2:
            whole = block(dst, cols, across)
            return [remote(whole, whole, 7, s, mate)]
        owner, peer = ((by_x, by_y), (by_y, by_x))[group]
        piece, whole = block(dst, cols, owner, group * half, half), block(dst, cols, owner)
        way = 3 + 2 * group
        return [remote(piece, piece, way, s, peer), remote(whole, whole, way + 1, s, mate)]

    def arrived(kind, p, way):
        _, dst, cols = views(kind, p)
        many = half if way in (3, 5) else rows
        ref = block(dst, cols, d, 0, many)
        pltpu.make_async_copy(ref, ref, recv.at[way, slot(kind, p)]).wait()

    def begin(kind, p):
        copies, keep = own(kind, p)
        for copy in copies:
            copy.start()
        keep.start()

    def pass_on(kind, p):
        for group in range(2):
            arrived(kind, p, group)
            for copy in relays(kind, p, group):
                copy.start()

    def close(kind, p):
        arrived(kind, p, 3)
        arrived(kind, p, 5)
        relays(kind, p, 2)[0].start()

    def settle(kind, p):
        for way in (2, 4, 6, 7):
            arrived(kind, p, way)
        own(kind, p)[1].wait()

    def finish(kind, p):
        copies = own(kind, p)[0]
        for group in range(3):
            copies = copies + relays(kind, p, group)
        for copy in copies:
            copy.wait_send()

    state = {"begun": 0, "query": False, "out": False}

    def ready(kind, p):
        end = sum(pieces[kind][p])
        if kind == 1 or end <= fixed:
            return
        need = 1 if end <= fixed + size * part else 2
        for of in range(need):
            if not state[("query", "out")[of]]:
                state[("query", "out")[of]] = True
                fills[1 + of].wait()
                for hop in range(1, size):
                    ref = att_v.at[:, place(of, z)]
                    pltpu.make_async_copy(ref, ref, z_recv.at[of, hop - 1]).wait()
                if of == 1:
                    for hop in range(1, size):
                        cot_copy(hop).start()

    def weight_load(p):
        cols = pl.ds(*pieces[0][p])
        return pltpu.make_async_copy(att_all.at[:, cols], w_v.at[:, cols], w_sem.at[p])

    def take(first, last):
        for p in range(first, last):
            settle(0, p)
            weight_load(p).start()

    def held(first, last):
        for p in range(first, last):
            weight_load(p).wait()

    saves = []

    def save(src, dst):
        copy = pltpu.make_async_copy(src, dst, save_sem.at[len(saves)])
        copy.start()
        saves.append(copy)

    part_rows = max(16, chunk // 4)

    def norm(value_of, row, dst):
        gain = gain_out[row : row + 1, :]

        def some(r, carry):
            at_r = pl.ds(pl.multiple_of(r * part_rows, part_rows), part_rows)
            value = value_of(at_r)
            inverse = lax.rsqrt(jnp.mean(value * value, axis=-1, keepdims=True) + EPSILON)
            dst[at_r, :] = (value * inverse * gain).astype(bf16)
            return carry

        lax.fori_loop(0, chunk // part_rows, some, 0)

    def turned(value):
        return value * turn_ref[0] + pltpu.roll(value, HEAD_DIM // 2, 1) * turn_ref[1]

    lead_w = fixed - 2 * KV_HEADS * HEAD_DIM
    kv_w = KV_HEADS * HEAD_DIM
    heads = size * part // HEAD_DIM
    scale = HEAD_DIM ** (-0.5)

    def kv_copy(hop):
        return pltpu.make_async_remote_copy(
            src_ref=kv_v.at[2], dst_ref=kv_v.at[2 - hop], send_sem=kv_send.at[hop - 1],
            recv_sem=kv_recv.at[hop - 1], device_id={"tensor": z + hop}, device_id_type=MESH,
        )

    def keys():
        pick = (
            lax.broadcasted_iota(jnp.int32, (8, lead_w), 0)
            == lax.broadcasted_iota(jnp.int32, (8, lead_w), 1)
        ).astype(bf16)
        gain_out[...] = lax.dot_general(
            pick, w_v[:, :lead_w], (((1,), (1,)), ((), ())), preferred_element_type=f32
        )
        norm(lambda at_r: x_ref[at_r, :].astype(f32), 0, one_v)
        save(one_v, one_out)
        lin = jnp.dot(one_v[...], w_v[:, lead_w:fixed], preferred_element_type=f32) + bias_ref[0:1, :]
        for g in range(KV_HEADS):
            cols = slice(g * HEAD_DIM, (g + 1) * HEAD_DIM)
            kv_v[2, :, cols] = turned(lin[:, cols]).astype(bf16)
        kv_v[2, :, kv_w:] = lin[:, kv_w:].astype(bf16)
        for hop in (1, 2):

            @pl.when(z + hop < size)
            def _(hop=hop):
                kv_copy(hop).start()

            @pl.when(z < hop)
            def _(hop=hop):
                kv_v[2 - hop] = jnp.zeros(kv_v.shape[1:], bf16)

    def queries():
        def pair(h, carry):
            cols = pl.ds(pl.multiple_of(h * 2 * HEAD_DIM, 128), 2 * HEAD_DIM)
            from_w = pl.ds(pl.multiple_of(fixed + h * 2 * HEAD_DIM, 128), 2 * HEAD_DIM)
            lin = jnp.dot(one_v[...], w_v[:, from_w], preferred_element_type=f32)
            lin += att_v[pl.ds(rows, 16), from_w][0:1, :].astype(f32)
            for k in range(2):
                out_cols = pl.ds(pl.multiple_of(h * 2 * HEAD_DIM + k * HEAD_DIM, 128), HEAD_DIM)
                q_v[:, out_cols] = turned(lin[:, k * HEAD_DIM : (k + 1) * HEAD_DIM]).astype(bf16)
            return carry

        lax.fori_loop(0, heads // 2, pair, 0)
        save(q_v, query_rot)

    def kv_wait():
        for hop in (1, 2):

            @pl.when(z >= hop)
            def _(hop=hop):
                pltpu.make_async_copy(kv_v.at[2 - hop], kv_v.at[2 - hop], kv_recv.at[hop - 1]).wait()

        save(kv_v, kv_win)

    def attend(first, last):
        def head(h, carry):
            cols = pl.ds(pl.multiple_of(h * HEAD_DIM, 128), HEAD_DIM)
            group = h // (heads // KV_HEADS)
            key_cols = pl.ds(pl.multiple_of(group * HEAD_DIM, 128), HEAD_DIM)
            value_cols = pl.ds(pl.multiple_of(kv_w + group * HEAD_DIM, 128), HEAD_DIM)
            key = kv_v[:, :, key_cols].reshape(3 * chunk, HEAD_DIM)
            value = kv_v[:, :, value_cols].reshape(3 * chunk, HEAD_DIM)
            scores = lax.dot_general(
                q_v[:, cols], key, (((1,), (1,)), ((), ())), preferred_element_type=f32
            )
            scores = scores * scale + mask_ref[...]
            largest = jnp.max(scores, axis=-1, keepdims=True)
            powers = jnp.exp(scores - largest)
            mass = jnp.sum(powers, axis=-1, keepdims=True)
            lse_out[h] = largest + jnp.log(mass)
            probs = (powers * (1.0 / mass)).astype(bf16)
            ctx_v[:, cols] = jnp.dot(probs, value, preferred_element_type=f32).astype(bf16)
            return carry

        lax.fori_loop(first, last, head, 0)

    def project():
        save(ctx_v, ctx_out)
        tile = min(512, w_v.shape[0])

        def some(n, carry):
            at_n = pl.ds(pl.multiple_of(n * tile, tile), tile)
            added = lax.dot_general(
                ctx_v[...], w_v[at_n, fixed + size * part :], (((1,), (1,)), ((), ())),
                preferred_element_type=f32,
            )
            mid_v[:, at_n] = x_ref[:, at_n].astype(f32) + added
            return carry

        lax.fori_loop(0, w_v.shape[0] // tile, some, 0)
        save(mid_v, mid_out)
        norm(lambda at_r: mid_v[at_r, :], 1, two_v)
        save(two_v, two_out)

    n_att = len(pieces[0])
    n_qkv = 1 + (n_att - 1) // 2
    third = heads // 3 + (heads % 3 > 0)
    last_q = order.index((0, n_qkv - 1))
    last_out = order.index((0, n_att - 1))
    work = [
        (last_q + 1, lambda: take(0, n_qkv)),
        (last_q + 2, lambda: held(0, n_qkv)),
        (last_q + 2, keys),
        (last_q + 3, queries),
        (last_out + 1, lambda: take(n_qkv, n_att)),
        (last_out + 1, kv_wait),
        (last_out + 1, lambda: attend(0, third)),
        (last_out + 2, lambda: attend(third, 2 * third)),
        (last_out + 3, lambda: attend(2 * third, heads)),
        (last_out + 4, lambda: held(n_qkv, n_att)),
        (last_out + 4, project),
    ]
    total = len(order)
    for i in range(total + 1):
        while state["begun"] < min(total, i + lead):
            ready(*order[state["begun"]])
            begin(*order[state["begun"]])
            state["begun"] += 1
        if i < total:
            pass_on(*order[i])
        if i > 0:
            close(*order[i - 1])
        while work and (work[0][0] <= i or i == total):
            work.pop(0)[1]()
    for kind, p in order:
        if kind == 1:
            settle(kind, p)
    for kind, p in order:
        finish(kind, p)
    for copy in saves:
        copy.wait()
    for hop in (1, 2):

        @pl.when(z + hop < size)
        def _(hop=hop):
            kv_copy(hop).wait_send()

    for of in range(2):
        for hop in range(1, size):
            z_copy(of, hop).wait_send()
    for hop in range(1, size):
        pltpu.make_async_copy(cot_ref, cot_ref, cot_recv.at[hop - 1]).wait()
        cot_copy(hop).wait_send()
    fills[3].wait()


def front(
    tokens, turn, mask, kv_bias, query, out, fixed, ffn_w, cot, att_tile=512, ffn_tile=768,
    collective_id=2, limit=60_000_000,
):
    tall, part = query.shape
    rows, fixed_w = fixed.shape
    chunk, width = tokens.shape
    size, ways = 4, 8
    query_w = size * part
    att_cols = fixed_w + 2 * query_w
    pieces = (
        [(0, fixed_w)] + [(fixed_w + p * att_tile, att_tile) for p in range(2 * query_w // att_tile)],
        [(p * ffn_tile, ffn_tile) for p in range(ffn_w.shape[1] // ffn_tile)],
    )
    n_att, n_ffn = len(pieces[0]), len(pieces[1])
    early = min(2, n_ffn)
    order = [(0, 0)] + [(1, p) for p in range(early)] + [(0, p) for p in range(1, n_att)]
    order += [(1, p) for p in range(early, n_ffn)]
    bf16, f32 = jnp.bfloat16, jnp.float32
    hbm = pl.BlockSpec(memory_space=pl.ANY)
    vmem = pl.BlockSpec(memory_space=pltpu.VMEM)
    vm = pltpu.VMEM
    dma = pltpu.SemaphoreType.DMA
    shape = lambda *s: jax.ShapeDtypeStruct(s, bf16)
    wide = lambda *s: jax.ShapeDtypeStruct(s, f32)
    slots = n_att + n_ffn
    kv_w = 2 * KV_HEADS * HEAD_DIM
    heads = query_w // HEAD_DIM
    return pl.pallas_call(
        functools.partial(front_body, pieces=pieces, order=order, lead=3),
        out_shape=(
            shape(8 * rows, att_cols), shape(8 * rows, ffn_w.shape[1]),
            shape(size * cot.shape[0], cot.shape[1]),
            shape(chunk, width), wide(chunk, width), shape(chunk, width), shape(chunk, query_w),
            shape(3, chunk, kv_w), wide(heads, chunk, 1), shape(chunk, query_w), wide(8, width),
        ),
        in_specs=[vmem] * 9,
        out_specs=(hbm,) * 8 + (vmem, hbm, vmem),
        scratch_shapes=[
            vm((tall, att_cols), bf16), vm((8 * rows, att_cols), bf16), vm((chunk, width), bf16),
            vm((chunk, query_w), bf16), vm((3, chunk, kv_w), bf16), vm((chunk, query_w), bf16),
            vm((chunk, width), f32), vm((chunk, width), bf16),
            dma((4,)), dma((2, size - 1)), dma((2, size - 1)),
            dma((size - 1,)), dma((size - 1,)), dma((ways, slots)), dma((ways, slots)), dma((slots,)),
            dma((n_att,)), dma((2,)), dma((2,)), dma((6,)),
        ],
        compiler_params=pltpu.CompilerParams(
            collective_id=collective_id, has_side_effects=True, vmem_limit_bytes=limit
        ),
        cost_estimate=pl.CostEstimate(
            flops=2 * chunk * width * att_cols, bytes_accessed=20 * rows * (att_cols + ffn_w.shape[1]),
            transcendentals=0,
        ),
        name="front",
    )(tokens, turn, mask, kv_bias, query, out, fixed, ffn_w, cot)


def line_order(z, s):
    upper = z // 2
    near = z * (1 - upper) + (3 - z) * upper
    inner = (1 - s // 3) * ((s + 1) % 3) + (s // 3) * 3
    at = (1 - near) * s + near * inner
    return at * (1 - upper) + (3 - at) * upper


def ffn_body(
    two_ref, cot_ref, weights_ref,
    rows_out, hid_out, dg_out, du_out, sum_out, dn_out,
    rows_v, cot_v, gate_v, up_v, down_v, hid_v, dg_v, du_v, part, land, below, above, res_v,
    tile_sem, load_sem, ag_send, ag_recv, rs_send, rs_recv, own_recv, out_sem,
    *, axis, ft, nt,
):
    f32, bf16 = jnp.float32, jnp.bfloat16
    size = 4
    rows, width = two_ref.shape
    units = weights_ref.shape[1] // 3
    n_f, n_n = units // ft, width // nt
    z = lax.axis_index(axis)
    has_low, has_high = z > 0, z < size - 1

    def to(dz):
        return {axis: z + dz}

    barrier = pltpu.get_barrier_semaphore()

    @pl.when(has_low)
    def _():
        pl.semaphore_signal(barrier, inc=1, device_id=to(-1), device_id_type=MESH)

    @pl.when(has_high)
    def _():
        pl.semaphore_signal(barrier, inc=1, device_id=to(1), device_id_type=MESH)

    own_load = pltpu.make_async_copy(two_ref, rows_v.at[z], load_sem.at[0])
    own_load.start()

    def tile_loads(f):
        cols = pl.ds(pl.multiple_of(f * ft, 128), ft)
        return [
            pltpu.make_async_copy(
                weights_ref.at[:, pl.ds(pl.multiple_of(k * units + f * ft, 128), ft)],
                dst.at[:, cols], tile_sem.at[k, f],
            )
            for k, dst in enumerate((gate_v, up_v, down_v))
        ]

    cot_load = pltpu.make_async_copy(cot_ref, cot_v, load_sem.at[1])
    for f in range(n_f):
        for copy in tile_loads(f):
            copy.start()
        if f == 0:
            cot_load.start()

    pl.semaphore_wait(barrier, (z + size - 1) // size + (2 * size - 2 - z) // size)

    own_load.wait()

    def ag_copy(j, dz):
        way = (dz + 1) // 2
        return pltpu.make_async_remote_copy(
            src_ref=rows_v.at[j], dst_ref=rows_v.at[j], send_sem=ag_send.at[way, j],
            recv_sem=ag_recv.at[j], device_id=to(dz), device_id_type=MESH,
        )

    @pl.when(has_low)
    def _():
        ag_copy(z, -1).start()

    @pl.when(has_high)
    def _():
        ag_copy(z, 1).start()

    def rs_copy(j, n, dz, own):
        way = (dz + 1) // 2
        if own:
            dst = below.at[n] if dz == 1 else above.at[n]
            sem = own_recv.at[1 - way, n]
        else:
            dst, sem = land.at[j, n], rs_recv.at[j, n]
        return pltpu.make_async_remote_copy(
            src_ref=part.at[j, n], dst_ref=dst, send_sem=rs_send.at[j, n],
            recv_sem=sem, device_id=to(dz), device_id_type=MESH,
        )

    def pass_on(j, n, what):
        for dz in (1, -1):
            for own in (True, False):
                hop = j == z + dz
                going = (j > z) if dz == 1 else (j < z)
                near = hop if own else jnp.logical_not(hop)

                @pl.when(jnp.logical_and(going, near))
                def _(dz=dz, own=own):
                    copy = rs_copy(j, n, dz, own)
                    copy.start() if what == "start" else copy.wait_send()

    def out_copies(j):
        at = pl.ds(pl.multiple_of(j * rows, rows), rows)
        return [
            pltpu.make_async_copy(src.at[j], dst.at[at, :], out_sem.at[k, j])
            for k, (src, dst) in enumerate(
                ((rows_v, rows_out), (hid_v, hid_out), (dg_v, dg_out), (du_v, du_out))
            )
        ]

    def step(s, carry):
        for sign in (-1, 1):
            j = z + sign * s
            inside = jnp.logical_and(s > 0, (j >= 0) if sign == -1 else (j < size))

            @pl.when(inside)
            def _(j=j, sign=sign):
                ag_copy(j, -sign).wait_recv()

            onward = has_high if sign == -1 else has_low

            @pl.when(jnp.logical_and(inside, onward))
            def _(j=j, sign=sign):
                ag_copy(j, -sign).start()

        j = line_order(z, s)
        at = pl.ds(pl.multiple_of(j * rows, rows), rows)

        @pl.when(s == 0)
        def _():
            cot_load.wait()

        def units_tile(f, carry):
            @pl.when(s == 0)
            def _():
                for copy in tile_loads(f):
                    copy.wait()

            cols = pl.ds(pl.multiple_of(f * ft, 128), ft)
            mine = rows_v[j]
            gate = jnp.dot(mine, gate_v[:, cols], preferred_element_type=f32)
            upper = jnp.dot(mine, up_v[:, cols], preferred_element_type=f32)
            d_hidden = jnp.dot(cot_v[at, :], down_v[:, cols], preferred_element_type=f32)
            sig = 1.0 / (1.0 + jnp.exp(-gate))
            act = gate * sig
            hid_v[j, :, cols] = (act * upper).astype(bf16)
            du_v[j, :, cols] = (d_hidden * act).astype(bf16)
            dg_v[j, :, cols] = (d_hidden * upper * (sig + act * (1.0 - sig))).astype(bf16)
            return carry

        lax.fori_loop(0, n_f, units_tile, 0)
        for copy in out_copies(j):
            copy.start()
        ends = jnp.logical_and(s > 0, jnp.logical_not(jnp.logical_and(has_low, has_high)))

        def width_tile(n, carry):
            at_n = pl.ds(pl.multiple_of(n * nt, nt), nt)
            dims = (((1,), (1,)), ((), ()))
            total = lax.dot_general(dg_v[j], gate_v[at_n, :], dims, preferred_element_type=f32)
            total += lax.dot_general(du_v[j], up_v[at_n, :], dims, preferred_element_type=f32)
            part[j, n] = total.astype(bf16)

            @pl.when(ends)
            def _():
                pass_on(j, n, "start")

            return carry

        lax.fori_loop(0, n_n, width_tile, 0)
        return carry

    lax.fori_loop(0, size, step, 0)

    def down_tile(i, carry):
        j, n = i // n_n, i % n_n
        at_n = pl.ds(pl.multiple_of(n * nt, nt), nt)
        total = lax.dot_general(
            hid_v[j], down_v[at_n, :], (((1,), (1,)), ((), ())), preferred_element_type=f32
        )
        res_v[j, :, at_n] = total.astype(bf16)
        return carry

    def forward(j, n):
        pltpu.make_async_copy(land.at[j, n], land.at[j, n], rs_recv.at[j, n]).wait()
        part[j, n] = (part[j, n].astype(f32) + land[j, n].astype(f32)).astype(bf16)
        pass_on(j, n, "start")

    middle = jnp.logical_and(has_low, has_high)

    @pl.when(middle)
    def _():
        def first(n, carry):
            forward(3 - z, n)
            return carry

        lax.fori_loop(0, n_n, first, 0)

    lax.fori_loop(0, (size * n_n) // 2, down_tile, 0)

    @pl.when(middle)
    def _():
        def second(n, carry):
            forward(3 - 3 * (z // 2), n)
            forward(3 * (z // 2), n)
            return carry

        lax.fori_loop(0, n_n, second, 0)

    lax.fori_loop((size * n_n) // 2, size * n_n, down_tile, 0)
    sum_copies = [
        pltpu.make_async_copy(
            res_v.at[j], sum_out.at[pl.ds(j * rows, rows), :], load_sem.at[2 + j]
        )
        for j in range(size)
    ]
    for copy in sum_copies:
        copy.start()

    def last(n, carry):
        @pl.when(has_low)
        def _():
            pltpu.make_async_copy(below.at[n], below.at[n], own_recv.at[0, n]).wait()
            part[z, n] = (part[z, n].astype(f32) + below[n].astype(f32)).astype(bf16)

        @pl.when(has_high)
        def _():
            pltpu.make_async_copy(above.at[n], above.at[n], own_recv.at[1, n]).wait()
            part[z, n] = (part[z, n].astype(f32) + above[n].astype(f32)).astype(bf16)

        dn_out[:, pl.ds(pl.multiple_of(n * nt, nt), nt)] = part[z, n]
        return carry

    lax.fori_loop(0, n_n, last, 0)

    def drain(j, carry):
        for copy in out_copies(j):
            copy.wait()
        for dz in (-1, 1):
            came = jnp.logical_or(j == z, (j > z) if dz == -1 else (j < z))
            there = has_low if dz == -1 else has_high

            @pl.when(jnp.logical_and(came, there))
            def _(dz=dz):
                ag_copy(j, dz).wait_send()

        def sent(n, carry):
            @pl.when(j != z)
            def _():
                pltpu.make_async_copy(part.at[j, n], part.at[j, n], rs_send.at[j, n]).wait()

            return carry

        lax.fori_loop(0, n_n, sent, 0)
        return carry

    lax.fori_loop(0, size, drain, 0)
    for copy in sum_copies:
        copy.wait()


def ffn(two, cot_rows, weights, axis="tensor", ft=768, nt=512, collective_id=1, limit=66_000_000):
    rows, width = two.shape
    units = weights.shape[1] // 3
    size = 4
    length = rows * size
    n_f, n_n = units // ft, width // nt
    bf16 = jnp.bfloat16
    hbm = pl.BlockSpec(memory_space=pl.ANY)
    vm = pltpu.VMEM
    dma = pltpu.SemaphoreType.DMA
    shape = lambda *s: jax.ShapeDtypeStruct(s, bf16)
    return pl.pallas_call(
        functools.partial(ffn_body, axis=axis, ft=ft, nt=nt),
        out_shape=(
            shape(length, width), shape(length, units), shape(length, units), shape(length, units),
            shape(length, width), shape(rows, width),
        ),
        in_specs=[hbm] * 3,
        out_specs=(hbm,) * 5 + (pl.BlockSpec(memory_space=pltpu.VMEM),),
        scratch_shapes=[
            vm((size, rows, width), bf16), vm((length, width), bf16),
            vm((width, units), bf16), vm((width, units), bf16), vm((width, units), bf16),
            vm((size, rows, units), bf16), vm((size, rows, units), bf16), vm((size, rows, units), bf16),
            vm((size, n_n, rows, nt), bf16), vm((size, n_n, rows, nt), bf16),
            vm((n_n, rows, nt), bf16), vm((n_n, rows, nt), bf16),
            vm((size, rows, width), bf16),
            dma((3, n_f)), dma((2 + size,)), dma((2, size)), dma((size,)), dma((size, n_n)), dma((size, n_n)),
            dma((2, n_n)), dma((4, size)),
        ],
        compiler_params=pltpu.CompilerParams(
            collective_id=collective_id, has_side_effects=True, vmem_limit_bytes=limit
        ),
        cost_estimate=pl.CostEstimate(
            flops=12 * length * width * units, bytes_accessed=8 * width * units + 8 * length * units,
            transcendentals=length * units,
        ),
        name="ffn",
    )(two, cot_rows, weights)


def back_body(
    two_ref, cot_ref, hid_ref, dg_ref, du_ref, lhs_ref, rhs_ref, part_ref, small_ref,
    ffn_out, query_out, out_out, kv_out, sum_out, small_out,
    left_v, right_v, grad, mate_land, core_sum, x_land, y_land, second, x_last, y_last, stage, fin,
    z_land, kv_land, sum_land, small_z, small_hop, small_next,
    left_sem, right_sem, mate_send, mate_recv, one_send, one_recv, two_send, two_recv, stage_sem,
    z_send, z_recv, kv_send, kv_recv, sum_send, sum_recv, own_sem, small_send, small_recv,
    hop_send, hop_recv, *, n_f, wide, cols_out,
):
    f32, bf16 = jnp.float32, jnp.bfloat16
    d, z = lax.axis_index("dp"), lax.axis_index("tensor")
    size = 4
    core, x, y = d % 2, (d // 2) % 2, d // 4
    by_x, by_y, mate, _ = square(d)
    here, at_x, at_y = 2 * y + x, 2 * y + 1 - x, 2 * (1 - y) + x
    cross = 3 - here
    block, half = core_sum.shape[2], core_sum.shape[2] // 2
    n_ffn, n_att = 3 * n_f, rhs_ref.shape[1] // wide
    total = n_ffn + n_att
    chunk = sum_out.shape[0]
    share = block // size
    part_w = wide // 2

    barrier = pltpu.get_barrier_semaphore()
    for peer in (by_x, by_y, mate):
        pl.semaphore_signal(barrier, inc=1, device_id={"dp": peer}, device_id_type=MESH)
    for hop in range(1, size):
        pl.semaphore_signal(
            barrier, inc=1, device_id={"tensor": (z + hop) % size}, device_id_type=MESH
        )

    lefts = [
        pltpu.make_async_copy(ref, left_v.at[k], left_sem.at[k])
        for k, ref in enumerate((cot_ref, two_ref))
    ]

    def right_load(i, what):
        cols = pl.ds(pl.multiple_of((i % n_f) * wide, 128), wide)
        for m, ref in enumerate((hid_ref, dg_ref, du_ref)):
            copy = pltpu.make_async_copy(ref.at[:, cols], right_v.at[i % 2], right_sem.at[i % 2])

            @pl.when(i // n_f == m)
            def _(copy=copy):
                copy.start() if what == "start" else copy.wait()

    lefts[0].start()
    right_load(jnp.int32(0), "start")
    lefts[1].start()

    def chunk_rows(j):
        return part_ref.at[pl.ds(pl.multiple_of(j * chunk, chunk), chunk), :]

    own_part = pltpu.make_async_copy(chunk_rows(z), sum_land.at[size - 1], own_sem.at[0])
    own_part.start()
    pl.semaphore_wait(barrier, 3 + size - 1)

    def dp_copy(src, dst, send_sem, recv_sem, peer):
        return pltpu.make_async_remote_copy(
            src_ref=src, dst_ref=dst, send_sem=send_sem, recv_sem=recv_sem,
            device_id={"dp": peer}, device_id_type=MESH,
        )

    def z_copy(src, dst, send_sem, recv_sem, peer):
        return pltpu.make_async_remote_copy(
            src_ref=src, dst_ref=dst, send_sem=send_sem, recv_sem=recv_sem,
            device_id={"tensor": peer}, device_id_type=MESH,
        )

    small_copies, sum_copies = [], []
    for hop in range(1, size):
        to, k = (z + hop) % size, hop - 1
        small_copies.append(
            z_copy(small_ref, small_z.at[k], small_send.at[k], small_recv.at[k], to)
        )
        sum_copies.append(
            z_copy(chunk_rows(to), sum_land.at[k], sum_send.at[k], sum_recv.at[k], to)
        )
    for copy in small_copies + sum_copies:
        copy.start()

    hops = (mate, by_x, by_y)

    def hop_copy(k):
        return dp_copy(small_next.at[k], small_hop.at[k], hop_send.at[k], hop_recv.at[k], hops[k])

    def mate_copy(i):
        return dp_copy(
            grad.at[i % 2, :, 1 - core], mate_land.at[i % 4], mate_send.at[i % 4],
            mate_recv.at[i % 4], mate,
        )

    def one_copies(i):
        s = core_sum.at[i % 4]
        first, last = pl.ds(0, half), pl.ds(half, half)
        plan = (
            (s.at[at_x, first, :], x_land.at[i, 0], by_x), (s.at[cross, first, :], x_land.at[i, 1], by_x),
            (s.at[at_y, last, :], y_land.at[i, 0], by_y), (s.at[cross, last, :], y_land.at[i, 1], by_y),
        )
        return [
            dp_copy(src, dst, one_send.at[k, i], one_recv.at[k, i], peer)
            for k, (src, dst, peer) in enumerate(plan)
        ]

    def two_copies(i):
        return [
            dp_copy(second.at[i % 4, 0], y_last.at[i], two_send.at[0, i], two_recv.at[0, i], by_y),
            dp_copy(second.at[i % 4, 1], x_last.at[i], two_send.at[1, i], two_recv.at[1, i], by_x),
        ]

    def stage_copy(i):
        cols = pl.ds(pl.multiple_of(i * wide, 128), wide)
        return pltpu.make_async_copy(stage.at[i % 2], ffn_out.at[:, cols], stage_sem.at[i % 2])

    def multiply(i):
        @pl.when(jnp.logical_and(i >= 2, i < total))
        def _():
            mate_copy(i - 2).wait_send()

        @pl.when(i + 1 < n_ffn)
        def _():
            right_load(i + 1, "start")

        dims = (((0,), (0,)), ((), ()))

        @pl.when(i < n_ffn)
        def _():
            @pl.when(i == 0)
            def _():
                lefts[0].wait()

            @pl.when(i == n_f)
            def _():
                lefts[1].wait()

            right_load(i, "wait")

            def rows(k, carry):
                at = pl.ds(pl.multiple_of(k * 2 * block, 128), 2 * block)
                value = lax.dot_general(
                    left_v[(i // n_f + 1) // 2, :, at], right_v[i % 2], dims, preferred_element_type=f32
                )
                grad[i % 2, k] = value.astype(bf16).reshape(2, block, wide)
                return carry

            lax.fori_loop(0, 4, rows, 0)

        @pl.when(jnp.logical_and(i >= n_ffn, i < total))
        def _():
            a = i - n_ffn
            cols = pl.ds(pl.multiple_of(a * wide, 128), wide)

            def rows(k, carry):
                at = pl.ds(pl.multiple_of(k * 2 * block, 128), 2 * block)
                value = lax.dot_general(
                    lhs_ref[(a // 2) % 2, :, at], rhs_ref[:, cols], dims, preferred_element_type=f32
                )
                grad[i % 2, k] = value.astype(bf16).reshape(2, block, wide)
                return carry

            lax.fori_loop(0, 4, rows, 0)

        @pl.when(i < total)
        def _():
            mate_copy(i).start()

    def sum_cores(i):
        mate_copy(i).wait_recv()
        for k in range(4):
            core_sum[i % 4, k] = (
                grad[i % 2, k, core].astype(f32) + mate_land[i % 4, k].astype(f32)
            ).astype(bf16)
        for copy in one_copies(i):
            copy.start()

    def sum_near(i):
        for copy in one_copies(i):
            copy.wait_recv()
        s = core_sum.at[i % 4]
        second[i % 4, 0] = (s[at_y, :half].astype(f32) + x_land[i, 1].astype(f32)).astype(bf16)
        second[i % 4, 1] = (s[at_x, half:].astype(f32) + y_land[i, 1].astype(f32)).astype(bf16)
        for copy in two_copies(i):
            copy.start()

    def z_sends(a, what):
        for h in range(2):
            owner = (a % 2) * 2 + h
            hop = (owner - z + size) % size
            src = fin.at[a, :, pl.ds(h * part_w, part_w)]

            @pl.when(jnp.logical_and(a < 4, hop > 0))
            def _(src=src, owner=owner, hop=hop, h=h):
                copy = z_copy(
                    src, z_land.at[a // 2, hop - 1], z_send.at[a, h], z_recv.at[a // 2, hop - 1], owner
                )
                copy.start() if what == "start" else copy.wait_send()

        @pl.when(a == 4)
        def _():
            for hop in range(1, size):
                to = (z + hop) % size
                rows = pl.ds(pl.multiple_of(to * share, 16), share)
                copy = z_copy(
                    fin.at[4, rows, :], kv_land.at[hop - 1], kv_send.at[hop - 1], kv_recv.at[hop - 1], to
                )
                copy.start() if what == "start" else copy.wait_send()

    def finish(i):
        for copy in two_copies(i):
            copy.wait_recv()
        own = core_sum.at[i % 4, here]
        top = own[:half].astype(f32) + x_land[i, 0].astype(f32) + y_last[i].astype(f32)
        low = own[half:].astype(f32) + y_land[i, 0].astype(f32) + x_last[i].astype(f32)

        @pl.when(i < n_ffn)
        def _():
            @pl.when(i >= 2)
            def _():
                stage_copy(i - 2).wait()

            stage[i % 2, :half] = top
            stage[i % 2, half:] = low
            stage_copy(i).start()

        @pl.when(i >= n_ffn)
        def _():
            a = i - n_ffn
            fin[a, :half] = top.astype(bf16)
            fin[a, half:] = low.astype(bf16)
            z_sends(a, "start")

        for copy in one_copies(i) + two_copies(i):
            copy.wait_send()

    def small_step(i):
        @pl.when(i == 2)
        def _():
            for copy in small_copies:
                copy.wait_recv()
            small_next[0] = small_ref[...] + small_z[0] + small_z[1] + small_z[2]
            hop_copy(0).start()

        for k in range(2):

            @pl.when(i == 3 + k)
            def _(k=k):
                hop_copy(k).wait_recv()
                small_next[k + 1] = small_next[k] + small_hop[k]
                hop_copy(k + 1).start()

        @pl.when(i == 5)
        def _():
            hop_copy(2).wait_recv()
            small_out[...] = small_next[2] + small_hop[2]

    def turn(i, carry):
        multiply(i)
        for lag, work in ((1, sum_cores), (2, sum_near), (3, finish)):

            @pl.when(jnp.logical_and(i >= lag, i - lag < total))
            def _(lag=lag, work=work):
                work(i - lag)

        small_step(i)
        return carry

    lax.fori_loop(0, total + 3, turn, 0)
    for i in (total - 2, total - 1):
        mate_copy(i).wait_send()
    for i in (n_ffn - 2, n_ffn - 1):
        stage_copy(i).wait()
    own_part.wait()
    for copy in sum_copies:
        copy.wait_recv()
    acc = sum_land[size - 1].astype(f32)
    for k in range(size - 1):
        acc += sum_land[k].astype(f32)
    sum_out[...] = acc.astype(bf16)
    for of, dst in ((0, query_out), (1, out_out)):
        for k in range(size - 1):
            ref = z_land.at[of, k]
            pltpu.make_async_copy(ref, ref, z_recv.at[of, k]).wait()
        for h in range(4):

            @pl.when(z == h)
            def _(of=of, dst=dst, h=h):
                acc = fin[2 * of + h // 2, :, (h % 2) * part_w : (h % 2 + 1) * part_w].astype(f32)
                for k in range(size - 1):
                    acc += z_land[of, k].astype(f32)
                dst[...] = acc

    for k in range(size - 1):
        pltpu.make_async_copy(kv_land.at[k], kv_land.at[k], kv_recv.at[k]).wait()
    rows = pl.ds(pl.multiple_of(z * share, 16), share)
    acc = fin[4, rows, :].astype(f32)
    for k in range(size - 1):
        acc += kv_land[k].astype(f32)
    kv_out[...] = acc
    for a in range(n_att):
        z_sends(a, "wait")
    for copy in sum_copies + small_copies:
        copy.wait_send()
    for k in range(3):
        hop_copy(k).wait_send()


def back(two, cot_rows, hid, dg, du, lhs, rhs, ffn_part, small, wide=768, collective_id=3, limit=67_000_000):
    length, width = two.shape
    size, chunk, block = 4, lhs.shape[1], width // 8
    units = hid.shape[1]
    n_f, n_att = units // wide, rhs.shape[1] // wide
    n_ffn = 3 * n_f
    total = n_ffn + n_att
    half, part_w, share = block // 2, wide // 2, block // size
    bf16, f32 = jnp.bfloat16, jnp.float32
    hbm = pl.BlockSpec(memory_space=pl.ANY)
    vmem = pl.BlockSpec(memory_space=pltpu.VMEM)
    vm = pltpu.VMEM
    dma = pltpu.SemaphoreType.DMA
    shape = jax.ShapeDtypeStruct
    return pl.pallas_call(
        functools.partial(back_body, n_f=n_f, wide=wide, cols_out=3 * units),
        out_shape=(
            shape((block, 3 * units), f32), shape((block, part_w), f32), shape((block, part_w), f32),
            shape((share, wide), f32), shape((chunk, width), bf16), shape(small.shape, f32),
        ),
        in_specs=[hbm] * 5 + [vmem, vmem, hbm, vmem],
        out_specs=(hbm,) + (vmem,) * 5,
        scratch_shapes=[
            vm((2, length, width), bf16), vm((2, length, wide), bf16), vm((2, 4, 2, block, wide), bf16),
            vm((4, 4, block, wide), bf16), vm((4, 4, block, wide), bf16),
            vm((total, 2, half, wide), bf16), vm((total, 2, half, wide), bf16),
            vm((4, 2, half, wide), bf16), vm((total, half, wide), bf16), vm((total, half, wide), bf16),
            vm((2, block, wide), f32), vm((n_att, block, wide), bf16),
            vm((2, size - 1, block, part_w), bf16), vm((size - 1, share, wide), bf16),
            vm((size, chunk, width), bf16), vm((3,) + small.shape, f32), vm((3,) + small.shape, f32),
            vm((3,) + small.shape, f32),
            dma((2,)), dma((2,)), dma((4,)), dma((4,)), dma((4, total)), dma((4, total)),
            dma((2, total)), dma((2, total)), dma((2,)),
            dma((4, 2)), dma((2, size - 1)), dma((size - 1,)), dma((size - 1,)), dma((size - 1,)),
            dma((size - 1,)), dma((1,)), dma((size - 1,)), dma((size - 1,)), dma((3,)), dma((3,)),
        ],
        compiler_params=pltpu.CompilerParams(
            collective_id=collective_id, has_side_effects=True, vmem_limit_bytes=limit
        ),
        cost_estimate=pl.CostEstimate(
            flops=6 * length * width * units, bytes_accessed=8 * length * units, transcendentals=0
        ),
        name="back",
    )(two, cot_rows, hid, dg, du, lhs, rhs, ffn_part, small)


def angle_tables(first, length, head_width):
    position = (first + jnp.arange(length)).astype(jnp.float32)
    exponent = jnp.arange(head_width // 2, dtype=jnp.float32) * (2.0 / head_width)
    frequency = ROPE_BASE ** (-exponent)
    angle = position[:, None] * frequency[None, :]
    return (jnp.cos(angle), jnp.sin(angle))


def rotate(values, cosine, sine):
    half_width = values.shape[-1] // 2
    first_half = values[..., :half_width]
    second_half = values[..., half_width:]
    return jnp.concatenate(
        [first_half * cosine - second_half * sine, second_half * cosine + first_half * sine],
        axis=-1,
    )


def rotate_back(grads, cosine, sine):
    return rotate(grads, cosine, -sine)


def dot_f32(left, right, dims):
    return lax.dot_general(left, right, (dims, ((), ())), preferred_element_type=jnp.float32)


def contract_rows(left, right):
    return dot_f32(left, right, ((0,), (0,)))


def contract_cols(left, right):
    return dot_f32(left, right, ((1,), (1,)))


def norm_back(upstream, unit, inverse, gain):
    scaled = upstream * gain
    gain_term = jnp.sum(upstream * unit, axis=0)
    input_term = inverse * (scaled - unit * jnp.mean(scaled * unit, axis=-1, keepdims=True))
    return (gain_term, input_term)


def joined_units(gate_w, up_w, down_w):
    units = gate_w.shape[1]
    gap = -(-units // 768) * 768 - units
    wide = lambda w: jnp.pad(w, ((0, 0), (0, gap)))
    return jnp.concatenate([wide(gate_w), wide(up_w), wide(down_w)], axis=1)


def attention_branch(tokens, cosine, sine, mask, gains_w, query_w, query_b, kv_w, kv_b, out_w, ffn_w, cotangent):
    f32, bf16 = jnp.float32, jnp.bfloat16
    rows = tokens.shape[0]
    size = lax.axis_size("tensor")
    fixed_w = jnp.concatenate([gains_w, kv_w], axis=1)
    if lax.axis_size("dp") == 8 and size == 4:
        tall_query = jnp.concatenate([query_w, jnp.pad(query_b[None, :], ((0, 15), (0, 0)))], axis=0)
        tall_out = jnp.pad(out_w, ((0, 16), (0, 0)))
        turn = jnp.stack(
            [jnp.concatenate([cosine, cosine], axis=1), jnp.concatenate([-sine, sine], axis=1)]
        )
        att_w, ffn_all, cot_rows, two, middle, one, query_rot, kv_win, lse, context, gains = front(
            tokens, turn, mask, kv_b[None, :], tall_query, tall_out, fixed_w, ffn_w, cotangent
        )
        kv_win = kv_win.reshape(3 * rows, kv_w.shape[1])
        return att_w, ffn_all, cot_rows, two, middle, one, query_rot, kv_win, lse, context, gains[:2]
    pair = lax.all_gather(jnp.stack([query_w, out_w]), "tensor", axis=2, tiled=True)
    att_w = jnp.concatenate([fixed_w, pair[0], pair[1]], axis=1)
    att_w = lax.all_gather(att_w, "dp", axis=0, tiled=True)
    ffn_all = lax.all_gather(ffn_w, "dp", axis=0, tiled=True)
    cot_rows = lax.all_gather(cotangent, "tensor", axis=0, tiled=True)
    full_query_b = lax.all_gather(query_b, "tensor", axis=0, tiled=True).astype(f32)
    ahead = gains_w.shape[1]
    kv_width = kv_w.shape[1] // 2
    qkv_width = 2 * kv_width + full_query_b.shape[0]
    heads = full_query_b.shape[0] // HEAD_DIM
    gains = att_w[:, :2].T.astype(f32)
    inputs = tokens.astype(f32)
    inverse = lax.rsqrt(jnp.mean(inputs * inputs, axis=-1, keepdims=True) + EPSILON)
    one = (inputs * inverse * gains[0]).astype(bf16)
    lin = jnp.dot(one, att_w[:, ahead : ahead + qkv_width], preferred_element_type=f32)
    lin = lin + jnp.concatenate([kv_b, full_query_b])
    cos_h, sin_h = cosine[:, None, :], sine[:, None, :]
    query_rot = rotate(lin[:, 2 * kv_width :].reshape(rows, heads, HEAD_DIM), cos_h, sin_h).astype(bf16)
    key_rot = rotate(lin[:, :kv_width].reshape(rows, KV_HEADS, HEAD_DIM), cos_h, sin_h).astype(bf16)
    kv_own = jnp.concatenate(
        [key_rot.reshape(rows, kv_width), lin[:, kv_width : 2 * kv_width].astype(bf16)], axis=1
    )
    back_chunks = mask.shape[1] // rows - 1
    kv_win = jnp.concatenate(
        [shift(kv_own, hops) for hops in range(back_chunks, 0, -1)] + [kv_own], axis=0
    )
    window = kv_win.shape[0]
    key_win = kv_win[:, :kv_width].reshape(window, KV_HEADS, HEAD_DIM)
    value_win = kv_win[:, kv_width:].reshape(window, KV_HEADS, HEAD_DIM)
    grouped = query_rot.reshape(rows, KV_HEADS, heads // KV_HEADS, HEAD_DIM)
    scores = jnp.einsum("tagd,sad->agts", grouped, key_win, preferred_element_type=f32)
    scores = scores * HEAD_DIM ** (-0.5) + mask
    largest = jnp.max(scores, axis=-1, keepdims=True)
    lse = largest + jnp.log(jnp.sum(jnp.exp(scores - largest), axis=-1, keepdims=True))
    probs = jnp.exp(scores - lse).astype(bf16)
    context = jnp.einsum("agts,sad->tagd", probs, value_win, preferred_element_type=f32)
    context = context.reshape(rows, heads * HEAD_DIM).astype(bf16)
    middle = inputs + contract_cols(context, att_w[:, ahead + qkv_width :])
    inverse = lax.rsqrt(jnp.mean(middle * middle, axis=-1, keepdims=True) + EPSILON)
    two = (middle * inverse * gains[1]).astype(bf16)
    query_rot = query_rot.reshape(rows, heads * HEAD_DIM)
    return att_w, ffn_all, cot_rows, two, middle, one, query_rot, kv_win, lse, context, gains


def shift(value, hops):
    size = lax.axis_size("tensor")
    pairs = [(i, i + hops) for i in range(size) if 0 <= i + hops < size]
    return lax.ppermute(value, "tensor", pairs)


def sum_grads(two, cot_rows, hid, dg, du, normed_one, d_attended, d_lin, context, ffn_part, small):
    f32, bf16 = jnp.float32, jnp.bfloat16
    padded = hid.shape[1]
    fixed = d_lin.shape[1] - context.shape[1]
    d_query = d_lin[:, fixed:]
    if lax.axis_size("dp") == 8 and lax.axis_size("tensor") == 4:
        gap = context.shape[1] // 2 - fixed
        rhs = jnp.concatenate([d_query, context, jnp.pad(d_lin[:, :fixed], ((0, 0), (0, gap)))], axis=1)
        lhs = jnp.stack([normed_one, d_attended])
        flat, query, out, kv, ffn_sum, total = back(
            two, cot_rows, hid, dg, du, lhs, rhs, ffn_part, small.reshape(-1, 128)
        )
        flat = [flat[:, k * padded : (k + 1) * padded] for k in range(3)]
        return (*flat, query, out, kv, ffn_sum, total.reshape(-1))

    def over_dp(left, right):
        return lax.psum_scatter(
            contract_rows(left, right).astype(bf16), "dp", scatter_dimension=0, tiled=True
        )

    def over_tensor(value, axis):
        return lax.psum_scatter(value, "tensor", scatter_dimension=axis, tiled=True).astype(f32)

    return (
        over_dp(cot_rows, hid).astype(f32),
        over_dp(two, dg).astype(f32),
        over_dp(two, du).astype(f32),
        over_tensor(over_dp(normed_one, d_query), 1),
        over_tensor(over_dp(d_attended, context), 1),
        over_tensor(over_dp(normed_one, d_lin[:, :fixed]), 0),
        over_tensor(ffn_part, 0),
        lax.psum(small, ("dp", "tensor")),
    )


def local(
    tokens, segments, gain_one, query_w, query_b, key_w, key_b, value_w, value_b,
    out_w, gain_two, gate_w, up_w, down_w, cotangent,
):
    bf16, f32 = jnp.bfloat16, jnp.float32
    rows, model_width = tokens.shape
    tensor_size = lax.axis_size("tensor")
    rank = lax.axis_index("tensor")
    kv_width = key_w.shape[1]
    fixed_width = 2 * kv_width
    query_width = query_w.shape[1] * tensor_size
    qkv_width = fixed_width + query_width
    heads = query_width // HEAD_DIM
    group = heads // KV_HEADS
    scale = HEAD_DIM ** (-0.5)
    units = gate_w.shape[1]
    back_chunks = min(tensor_size - 1, -(-DOC_MAX // rows))
    window = (back_chunks + 1) * rows
    cosine, sine = angle_tables(rank * rows, rows, HEAD_DIM)
    cos_h, sin_h = cosine[:, None, :], sine[:, None, :]
    segment = segments[0]
    own_segment = lax.dynamic_slice_in_dim(segment, rank * rows, rows, 0)
    before = jnp.full((back_chunks * rows,), -1, segment.dtype)
    win_segment = lax.dynamic_slice_in_dim(jnp.concatenate([before, segment]), rank * rows, window, 0)
    own_pos = back_chunks * rows + jnp.arange(rows)
    win_pos = jnp.arange(window)
    allowed = (own_segment[:, None] == win_segment[None, :]) & (win_pos[None, :] <= own_pos[:, None])
    mask = jnp.where(allowed, 0.0, NEGATIVE).astype(f32)
    ahead = 128
    gains_w = jnp.pad(jnp.stack([gain_one, gain_two], axis=1), ((0, 0), (0, ahead - 2)))
    (
        att_w, ffn_w, cot_rows, normed_two, middle, normed_one, query_rot, kv_win, lse, context, gains,
    ) = attention_branch(
        tokens, cosine, sine, mask, gains_w, query_w, query_b, jnp.concatenate([key_w, value_w], axis=1),
        jnp.concatenate([key_b, value_b]).astype(f32), out_w, joined_units(gate_w, up_w, down_w), cotangent,
    )
    qkv_w = att_w[:, ahead : ahead + qkv_width]
    out_full = att_w[:, ahead + qkv_width :]
    rows_two, hidden_low, d_gate, d_upper, ffn_part, d_normed_two = ffn(
        normed_two, cot_rows, ffn_w
    )
    d_normed_two = d_normed_two.astype(f32)
    inputs = tokens.astype(f32)
    inverse_one = lax.rsqrt(jnp.mean(inputs * inputs, axis=-1, keepdims=True) + EPSILON)
    unit_one = inputs * inverse_one
    inverse_two = lax.rsqrt(jnp.mean(middle * middle, axis=-1, keepdims=True) + EPSILON)
    unit_two = middle * inverse_two
    gain_two_term, d_from_two = norm_back(d_normed_two, unit_two, inverse_two, gains[1])
    d_middle = cotangent.astype(f32) + d_from_two
    d_attended = d_middle.astype(bf16)
    d_context = jnp.dot(d_attended, out_full, preferred_element_type=f32).astype(bf16)
    d_context = d_context.reshape(rows, KV_HEADS, group, HEAD_DIM)
    key_win = kv_win[:, :kv_width].reshape(window, KV_HEADS, HEAD_DIM)
    value_win = kv_win[:, kv_width:].reshape(window, KV_HEADS, HEAD_DIM)
    grouped = query_rot.reshape(rows, KV_HEADS, group, HEAD_DIM)
    scores = jnp.einsum("tagd,sad->agts", grouped, key_win, preferred_element_type=f32) * scale + mask
    probs = jnp.exp(scores - lse.reshape(KV_HEADS, group, rows, 1))
    probs_low = probs.astype(bf16)
    d_probs = jnp.einsum("tagd,sad->agts", d_context, value_win, preferred_element_type=f32)
    row_delta = jnp.sum(probs * d_probs, axis=-1, keepdims=True)
    d_scores = (probs * (d_probs - row_delta)).astype(bf16)
    d_query_rot = jnp.einsum("agts,sad->tagd", d_scores, key_win, preferred_element_type=f32) * scale
    d_key_win = jnp.einsum("agts,tagd->sad", d_scores, grouped, preferred_element_type=f32) * scale
    d_value_win = jnp.einsum("agts,tagd->sad", probs_low, d_context, preferred_element_type=f32)
    d_query_lin = (
        rotate_back(d_query_rot.reshape(rows, heads, HEAD_DIM), cos_h, sin_h)
        .reshape(rows, query_width).astype(bf16)
    )
    d_kv_win = jnp.concatenate(
        [d_key_win.reshape(window, kv_width), d_value_win.reshape(window, kv_width)], axis=1
    ).astype(bf16)
    d_kv = d_kv_win[back_chunks * rows :].astype(f32)
    for hops in range(1, back_chunks + 1):
        given = d_kv_win[(back_chunks - hops) * rows : (back_chunks - hops + 1) * rows]
        d_kv = d_kv + shift(given, -hops).astype(f32)
    d_key_lin = rotate_back(d_kv[:, :kv_width].reshape(rows, KV_HEADS, HEAD_DIM), cos_h, sin_h)
    d_lin = jnp.concatenate(
        [d_key_lin.reshape(rows, kv_width).astype(bf16), d_kv[:, kv_width:].astype(bf16), d_query_lin],
        axis=1,
    )
    d_normed_one = contract_cols(d_lin, qkv_w)
    bias_term = jnp.sum(d_lin.astype(f32), axis=0)
    gain_one_term, d_from_one = norm_back(d_normed_one, unit_one, inverse_one, gains[0])
    input_grad = (d_middle + d_from_one).astype(bf16)

    sums = sum_grads(
        rows_two, cot_rows, hidden_low, d_gate, d_upper, normed_one, d_attended, d_lin, context,
        ffn_part, jnp.concatenate([bias_term, gain_one_term, gain_two_term]),
    )
    sum_down, sum_gate, sum_up, sum_query, sum_out, sum_kv, ffn_sum, small = sums
    mixed = (middle + ffn_sum.astype(f32)).astype(bf16)
    place = lax.axis_index("dp") * tensor_size + rank
    devices = lax.axis_size("dp") * tensor_size

    def own(start, size):
        share = size // devices
        return lax.dynamic_slice_in_dim(small, start + place * share, share, 0)

    return (
        mixed,
        input_grad,
        own(qkv_width, model_width),
        sum_query,
        own(fixed_width, query_width),
        sum_kv[:, :kv_width],
        small[:kv_width],
        sum_kv[:, kv_width : 2 * kv_width],
        small[kv_width:fixed_width],
        sum_out,
        own(qkv_width + model_width, model_width),
        sum_gate[:, :units],
        sum_up[:, :units],
        sum_down[:, :units],
    )


def solution(mesh):
    both = ("dp", "tensor")
    return jax.shard_map(
        local,
        mesh=mesh,
        in_specs=(
            P(both, None), P("dp", None), P("dp"), P("dp", "tensor"), P("tensor"), P("dp", None), P(),
            P("dp", None), P(), P("dp", "tensor"), P("dp"), P("dp", "tensor"), P("dp", "tensor"),
            P("dp", "tensor"), P(both, None),
        ),
        out_specs=(
            P(both, None), P(both, None), P(both), P("dp", "tensor"), P(both), P(both, None), P(),
            P(both, None), P(), P("dp", "tensor"), P(both), P("dp", "tensor"), P("dp", "tensor"),
            P("dp", "tensor"),
        ),
        check_vma=False,
    )
```

```python
import functools

import jax
import jax.numpy as jnp
from jax import lax
from jax.experimental import pallas as pl
from jax.experimental.pallas import tpu as pltpu
from jax.sharding import PartitionSpec as P

MESH = pl.DeviceIdType.MESH
KV_HEADS = 2
HEAD_DIM = 128
DOC_MAX = 512
EPSILON = 1e-06
ROPE_BASE = 1000000.0
NEGATIVE = -1e30


def square(d):
    core, x, y = d % 2, (d // 2) % 2, d // 4
    by_x, by_y = d + 2 - 4 * x, d + 4 - 8 * y
    return by_x, by_y, d + 1 - 2 * core, by_x + 4 - 8 * y


def front_body(
    x_ref, turn_ref, mask_ref, bias_ref, query_ref, out_ref, fixed_ref, ffn_ref, cot_ref,
    att_all, ffn_all, cot_all, two_out, mid_out, one_out, query_rot, kv_win, lse_out, ctx_out, gain_out,
    att_v, w_v, one_v, q_v, kv_v, ctx_v, mid_v, two_v,
    fill_sem, z_send, z_recv, cot_send, cot_recv, send, recv, keep_sem, w_sem, kv_send, kv_recv, save_sem,
    *, pieces, order, lead,
):
    f32, bf16 = jnp.float32, jnp.bfloat16
    d, z = lax.axis_index("dp"), lax.axis_index("tensor")
    size = 4
    by_x, by_y, mate, across = square(d)
    rows = ffn_ref.shape[0]
    half = rows // 2
    part = query_ref.shape[1]
    fixed = fixed_ref.shape[1]
    chunk = cot_ref.shape[0]
    tall = query_ref.shape[0]

    barrier = pltpu.get_barrier_semaphore()
    for peer in (by_x, by_y, mate):
        pl.semaphore_signal(barrier, inc=1, device_id={"dp": peer}, device_id_type=MESH)
    for hop in range(1, size):
        pl.semaphore_signal(
            barrier, inc=1, device_id={"tensor": (z + hop) % size}, device_id_type=MESH
        )

    def place(of, owner):
        return pl.ds(pl.multiple_of(fixed + of * size * part + owner * part, 128), part)

    fills = [pltpu.make_async_copy(fixed_ref, att_v.at[pl.ds(0, rows), pl.ds(0, fixed)], fill_sem.at[0])]
    for of, ref in enumerate((query_ref, out_ref)):
        fills.append(pltpu.make_async_copy(ref, att_v.at[:, place(of, z)], fill_sem.at[1 + of]))
    at = pl.ds(pl.multiple_of(z * chunk, chunk), chunk)
    fills.append(pltpu.make_async_copy(cot_ref, cot_all.at[at, :], fill_sem.at[3]))
    for copy in fills:
        copy.start()

    pl.semaphore_wait(barrier, 3 + size - 1)

    def z_copy(of, hop):
        ref = (query_ref, out_ref)[of]
        return pltpu.make_async_remote_copy(
            src_ref=ref, dst_ref=att_v.at[:, place(of, z)], send_sem=z_send.at[of, hop - 1],
            recv_sem=z_recv.at[of, hop - 1], device_id={"tensor": (z + hop) % size},
            device_id_type=MESH,
        )

    has_low, has_high = z > 0, z < size - 1

    def cot_copy(j, dz):
        ref = cot_all.at[pl.ds(pl.multiple_of(j * chunk, chunk), chunk), :]
        return pltpu.make_async_remote_copy(
            src_ref=ref, dst_ref=ref, send_sem=cot_send.at[(dz + 1) // 2, j], recv_sem=cot_recv.at[j],
            device_id={"tensor": z + dz}, device_id_type=MESH,
        )

    def cot_start():
        fills[3].wait()
        for dz, there in ((-1, has_low), (1, has_high)):

            @pl.when(there)
            def _(dz=dz):
                cot_copy(z, dz).start()

    def cot_step(hop):
        for sign, onward in ((-1, has_high), (1, has_low)):
            j = z + sign * hop
            inside = (j >= 0) if sign == -1 else (j < size)

            @pl.when(inside)
            def _(j=j, sign=sign):
                cot_copy(j, -sign).wait_recv()

            @pl.when(jnp.logical_and(inside, onward))
            def _(j=j, sign=sign):
                cot_copy(j, -sign).start()

    for of in range(2):
        for hop in range(1, size):
            z_copy(of, hop).start()
    fills[0].wait()

    def views(kind, p):
        src, dst = ((att_v, att_all), (ffn_ref, ffn_all))[kind]
        return src, dst, pl.ds(*pieces[kind][p])

    def slot(kind, p):
        return p + kind * len(pieces[0])

    def block(dst, cols, owner, first=0, many=None):
        many = rows if many is None else many
        return dst.at[pl.ds(pl.multiple_of(owner * rows + first, 16), many), cols]

    def remote(src, dst, way, at_slot, peer):
        return pltpu.make_async_remote_copy(
            src_ref=src, dst_ref=dst, send_sem=send.at[way, at_slot], recv_sem=recv.at[way, at_slot],
            device_id={"dp": peer}, device_id_type=MESH,
        )

    def own(kind, p):
        src, dst, cols = views(kind, p)
        mine = src.at[pl.ds(0, rows), cols]
        there = block(dst, cols, d)
        s = slot(kind, p)
        return [
            remote(mine, there, 0, s, by_x), remote(mine, there, 1, s, by_y),
            remote(mine, there, 2, s, mate),
        ], pltpu.make_async_copy(mine, there, keep_sem.at[s])

    def relays(kind, p, group):
        _, dst, cols = views(kind, p)
        s = slot(kind, p)
        if group == 2:
            whole = block(dst, cols, across)
            return [remote(whole, whole, 7, s, mate)]
        owner, peer = ((by_x, by_y), (by_y, by_x))[group]
        piece, whole = block(dst, cols, owner, group * half, half), block(dst, cols, owner)
        way = 3 + 2 * group
        return [remote(piece, piece, way, s, peer), remote(whole, whole, way + 1, s, mate)]

    def arrived(kind, p, way):
        _, dst, cols = views(kind, p)
        many = half if way in (3, 5) else rows
        ref = block(dst, cols, d, 0, many)
        pltpu.make_async_copy(ref, ref, recv.at[way, slot(kind, p)]).wait()

    def begin(kind, p):
        copies, keep = own(kind, p)
        for copy in copies:
            copy.start()
        keep.start()

    def pass_on(kind, p):
        for group in range(2):
            arrived(kind, p, group)
            for copy in relays(kind, p, group):
                copy.start()

    def close(kind, p):
        arrived(kind, p, 3)
        arrived(kind, p, 5)
        relays(kind, p, 2)[0].start()

    def settle(kind, p):
        for way in (2, 4, 6, 7):
            arrived(kind, p, way)
        own(kind, p)[1].wait()

    def finish(kind, p):
        copies = own(kind, p)[0]
        for group in range(3):
            copies = copies + relays(kind, p, group)
        for copy in copies:
            copy.wait_send()

    state = {"begun": 0, "query": False, "out": False}

    def ready(kind, p):
        end = sum(pieces[kind][p])
        if kind == 1 or end <= fixed:
            return
        need = 1 if end <= fixed + size * part else 2
        for of in range(need):
            if not state[("query", "out")[of]]:
                state[("query", "out")[of]] = True
                fills[1 + of].wait()
                for hop in range(1, size):
                    ref = att_v.at[:, place(of, z)]
                    pltpu.make_async_copy(ref, ref, z_recv.at[of, hop - 1]).wait()
                if of == 1:
                    cot_start()

    def weight_load(p):
        cols = pl.ds(*pieces[0][p])
        return pltpu.make_async_copy(att_all.at[:, cols], w_v.at[:, cols], w_sem.at[p])

    def take(first, last):
        for p in range(first, last):
            settle(0, p)
            weight_load(p).start()

    def held(first, last):
        for p in range(first, last):
            weight_load(p).wait()

    saves = []

    def save(src, dst):
        copy = pltpu.make_async_copy(src, dst, save_sem.at[len(saves)])
        copy.start()
        saves.append(copy)

    part_rows = max(16, chunk // 4)

    def norm(value_of, row, dst):
        gain = gain_out[row : row + 1, :]

        def some(r, carry):
            at_r = pl.ds(pl.multiple_of(r * part_rows, part_rows), part_rows)
            value = value_of(at_r)
            inverse = lax.rsqrt(jnp.mean(value * value, axis=-1, keepdims=True) + EPSILON)
            dst[at_r, :] = (value * inverse * gain).astype(bf16)
            return carry

        lax.fori_loop(0, chunk // part_rows, some, 0)

    def turned(value):
        return value * turn_ref[0] + pltpu.roll(value, HEAD_DIM // 2, 1) * turn_ref[1]

    lead_w = fixed - 2 * KV_HEADS * HEAD_DIM
    kv_w = KV_HEADS * HEAD_DIM
    heads = size * part // HEAD_DIM
    scale = HEAD_DIM ** (-0.5)

    def kv_copy(hop):
        return pltpu.make_async_remote_copy(
            src_ref=kv_v.at[2], dst_ref=kv_v.at[2 - hop], send_sem=kv_send.at[hop - 1],
            recv_sem=kv_recv.at[hop - 1], device_id={"tensor": z + hop}, device_id_type=MESH,
        )

    def keys():
        pick = (
            lax.broadcasted_iota(jnp.int32, (8, lead_w), 0)
            == lax.broadcasted_iota(jnp.int32, (8, lead_w), 1)
        ).astype(bf16)
        gain_out[...] = lax.dot_general(
            pick, w_v[:, :lead_w], (((1,), (1,)), ((), ())), preferred_element_type=f32
        )
        norm(lambda at_r: x_ref[at_r, :].astype(f32), 0, one_v)
        save(one_v, one_out)
        lin = jnp.dot(one_v[...], w_v[:, lead_w:fixed], preferred_element_type=f32) + bias_ref[0:1, :]
        for g in range(KV_HEADS):
            cols = slice(g * HEAD_DIM, (g + 1) * HEAD_DIM)
            kv_v[2, :, cols] = turned(lin[:, cols]).astype(bf16)
        kv_v[2, :, kv_w:] = lin[:, kv_w:].astype(bf16)
        for hop in (1, 2):

            @pl.when(z + hop < size)
            def _(hop=hop):
                kv_copy(hop).start()

            @pl.when(z < hop)
            def _(hop=hop):
                kv_v[2 - hop] = jnp.zeros(kv_v.shape[1:], bf16)

    def queries():
        def pair(h, carry):
            cols = pl.ds(pl.multiple_of(h * 2 * HEAD_DIM, 128), 2 * HEAD_DIM)
            from_w = pl.ds(pl.multiple_of(fixed + h * 2 * HEAD_DIM, 128), 2 * HEAD_DIM)
            lin = jnp.dot(one_v[...], w_v[:, from_w], preferred_element_type=f32)
            lin += att_v[pl.ds(rows, 16), from_w][0:1, :].astype(f32)
            for k in range(2):
                out_cols = pl.ds(pl.multiple_of(h * 2 * HEAD_DIM + k * HEAD_DIM, 128), HEAD_DIM)
                q_v[:, out_cols] = turned(lin[:, k * HEAD_DIM : (k + 1) * HEAD_DIM]).astype(bf16)
            return carry

        lax.fori_loop(0, heads // 2, pair, 0)
        save(q_v, query_rot)

    def kv_wait():
        for hop in (1, 2):

            @pl.when(z >= hop)
            def _(hop=hop):
                pltpu.make_async_copy(kv_v.at[2 - hop], kv_v.at[2 - hop], kv_recv.at[hop - 1]).wait()

        save(kv_v, kv_win)

    def attend(first, last):
        def head(h, carry):
            cols = pl.ds(pl.multiple_of(h * HEAD_DIM, 128), HEAD_DIM)
            group = h // (heads // KV_HEADS)
            key_cols = pl.ds(pl.multiple_of(group * HEAD_DIM, 128), HEAD_DIM)
            value_cols = pl.ds(pl.multiple_of(kv_w + group * HEAD_DIM, 128), HEAD_DIM)
            key = kv_v[:, :, key_cols].reshape(3 * chunk, HEAD_DIM)
            value = kv_v[:, :, value_cols].reshape(3 * chunk, HEAD_DIM)
            scores = lax.dot_general(
                q_v[:, cols], key, (((1,), (1,)), ((), ())), preferred_element_type=f32
            )
            scores = scores * scale + mask_ref[...]
            largest = jnp.max(scores, axis=-1, keepdims=True)
            powers = jnp.exp(scores - largest)
            mass = jnp.sum(powers, axis=-1, keepdims=True)
            lse_out[h] = largest + jnp.log(mass)
            probs = (powers * (1.0 / mass)).astype(bf16)
            ctx_v[:, cols] = jnp.dot(probs, value, preferred_element_type=f32).astype(bf16)
            return carry

        lax.fori_loop(first, last, head, 0)

    def project():
        save(ctx_v, ctx_out)
        tile = min(512, w_v.shape[0])

        def some(n, carry):
            at_n = pl.ds(pl.multiple_of(n * tile, tile), tile)
            added = lax.dot_general(
                ctx_v[...], w_v[at_n, fixed + size * part :], (((1,), (1,)), ((), ())),
                preferred_element_type=f32,
            )
            mid_v[:, at_n] = x_ref[:, at_n].astype(f32) + added
            return carry

        lax.fori_loop(0, w_v.shape[0] // tile, some, 0)
        save(mid_v, mid_out)
        norm(lambda at_r: mid_v[at_r, :], 1, two_v)
        save(two_v, two_out)

    n_att = len(pieces[0])
    n_qkv = 1 + (n_att - 1) // 2
    third = heads // 3 + (heads % 3 > 0)
    last_q = order.index((0, n_qkv - 1))
    last_out = order.index((0, n_att - 1))
    work = [
        (last_q - 1, lambda: cot_step(1)),
        (last_q + 1, lambda: cot_step(2)),
        (last_q + 1, lambda: take(0, n_qkv)),
        (last_q + 2, lambda: held(0, n_qkv)),
        (last_q + 2, keys),
        (last_q + 3, queries),
        (last_out + 1, lambda: take(n_qkv, n_att)),
        (last_out + 1, kv_wait),
        (last_out + 1, lambda: attend(0, third)),
        (last_out + 2, lambda: attend(third, 2 * third)),
        (last_out + 3, lambda: attend(2 * third, heads)),
        (last_out + 4, lambda: held(n_qkv, n_att)),
        (last_out + 4, project),
        (last_out + 5, lambda: cot_step(3)),
    ]
    total = len(order)
    for i in range(total + 1):
        while state["begun"] < min(total, i + lead):
            ready(*order[state["begun"]])
            begin(*order[state["begun"]])
            state["begun"] += 1
        if i < total:
            pass_on(*order[i])
        if i > 0:
            close(*order[i - 1])
        while work and (work[0][0] <= i or i == total):
            work.pop(0)[1]()
    for kind, p in order:
        if kind == 1:
            settle(kind, p)
    for kind, p in order:
        finish(kind, p)
    for copy in saves:
        copy.wait()
    for hop in (1, 2):

        @pl.when(z + hop < size)
        def _(hop=hop):
            kv_copy(hop).wait_send()

    for of in range(2):
        for hop in range(1, size):
            z_copy(of, hop).wait_send()
    for j in range(size):
        for dz, there in ((-1, has_low), (1, has_high)):
            came = jnp.logical_and((z <= j) if dz == -1 else (z >= j), there)

            @pl.when(came)
            def _(j=j, dz=dz):
                cot_copy(j, dz).wait_send()


def front(
    tokens, turn, mask, kv_bias, query, out, fixed, ffn_w, cot, att_tile=512, ffn_tile=768,
    collective_id=2, limit=60_000_000,
):
    tall, part = query.shape
    rows, fixed_w = fixed.shape
    chunk, width = tokens.shape
    size, ways = 4, 8
    query_w = size * part
    att_cols = fixed_w + 2 * query_w
    pieces = (
        [(0, fixed_w)] + [(fixed_w + p * att_tile, att_tile) for p in range(2 * query_w // att_tile)],
        [(p * ffn_tile, ffn_tile) for p in range(ffn_w.shape[1] // ffn_tile)],
    )
    n_att, n_ffn = len(pieces[0]), len(pieces[1])
    early = min(2, n_ffn)
    order = [(0, 0)] + [(1, p) for p in range(early)] + [(0, p) for p in range(1, n_att)]
    order += [(1, p) for p in range(early, n_ffn)]
    bf16, f32 = jnp.bfloat16, jnp.float32
    hbm = pl.BlockSpec(memory_space=pl.ANY)
    vmem = pl.BlockSpec(memory_space=pltpu.VMEM)
    vm = pltpu.VMEM
    dma = pltpu.SemaphoreType.DMA
    shape = lambda *s: jax.ShapeDtypeStruct(s, bf16)
    wide = lambda *s: jax.ShapeDtypeStruct(s, f32)
    slots = n_att + n_ffn
    kv_w = 2 * KV_HEADS * HEAD_DIM
    heads = query_w // HEAD_DIM
    return pl.pallas_call(
        functools.partial(front_body, pieces=pieces, order=order, lead=3),
        out_shape=(
            shape(8 * rows, att_cols), shape(8 * rows, ffn_w.shape[1]),
            shape(size * cot.shape[0], cot.shape[1]),
            shape(chunk, width), wide(chunk, width), shape(chunk, width), shape(chunk, query_w),
            shape(3, chunk, kv_w), wide(heads, chunk, 1), shape(chunk, query_w), wide(8, width),
        ),
        in_specs=[vmem] * 9,
        out_specs=(hbm,) * 8 + (vmem, hbm, vmem),
        scratch_shapes=[
            vm((tall, att_cols), bf16), vm((8 * rows, att_cols), bf16), vm((chunk, width), bf16),
            vm((chunk, query_w), bf16), vm((3, chunk, kv_w), bf16), vm((chunk, query_w), bf16),
            vm((chunk, width), f32), vm((chunk, width), bf16),
            dma((4,)), dma((2, size - 1)), dma((2, size - 1)),
            dma((2, size)), dma((size,)), dma((ways, slots)), dma((ways, slots)), dma((slots,)),
            dma((n_att,)), dma((2,)), dma((2,)), dma((6,)),
        ],
        compiler_params=pltpu.CompilerParams(
            collective_id=collective_id, has_side_effects=True, vmem_limit_bytes=limit
        ),
        cost_estimate=pl.CostEstimate(
            flops=2 * chunk * width * att_cols, bytes_accessed=20 * rows * (att_cols + ffn_w.shape[1]),
            transcendentals=0,
        ),
        name="front",
    )(tokens, turn, mask, kv_bias, query, out, fixed, ffn_w, cot)


def line_order(z, s):
    upper = z // 2
    near = z * (1 - upper) + (3 - z) * upper
    inner = (1 - s // 3) * ((s + 1) % 3) + (s // 3) * 3
    at = (1 - near) * s + near * inner
    return at * (1 - upper) + (3 - at) * upper


def ffn_body(
    two_ref, cot_ref, weights_ref,
    rows_out, hid_out, dg_out, du_out, sum_out, dn_out,
    rows_v, cot_v, gate_v, up_v, down_v, hid_v, dg_v, du_v, part, land, below, above, res_v,
    tile_sem, load_sem, ag_send, ag_recv, rs_send, rs_recv, own_recv, out_sem,
    *, axis, ft, nt,
):
    f32, bf16 = jnp.float32, jnp.bfloat16
    size = 4
    rows, width = two_ref.shape
    units = weights_ref.shape[1] // 3
    n_f, n_n = units // ft, width // nt
    z = lax.axis_index(axis)
    has_low, has_high = z > 0, z < size - 1

    def to(dz):
        return {axis: z + dz}

    barrier = pltpu.get_barrier_semaphore()

    @pl.when(has_low)
    def _():
        pl.semaphore_signal(barrier, inc=1, device_id=to(-1), device_id_type=MESH)

    @pl.when(has_high)
    def _():
        pl.semaphore_signal(barrier, inc=1, device_id=to(1), device_id_type=MESH)

    own_load = pltpu.make_async_copy(two_ref, rows_v.at[z], load_sem.at[0])
    own_load.start()

    def tile_loads(f):
        cols = pl.ds(pl.multiple_of(f * ft, 128), ft)
        return [
            pltpu.make_async_copy(
                weights_ref.at[:, pl.ds(pl.multiple_of(k * units + f * ft, 128), ft)],
                dst.at[:, cols], tile_sem.at[k, f],
            )
            for k, dst in enumerate((gate_v, up_v, down_v))
        ]

    cot_load = pltpu.make_async_copy(cot_ref, cot_v, load_sem.at[1])
    for f in range(n_f):
        for copy in tile_loads(f):
            copy.start()
        if f == 0:
            cot_load.start()

    pl.semaphore_wait(barrier, (z + size - 1) // size + (2 * size - 2 - z) // size)

    own_load.wait()

    def ag_copy(j, dz):
        way = (dz + 1) // 2
        return pltpu.make_async_remote_copy(
            src_ref=rows_v.at[j], dst_ref=rows_v.at[j], send_sem=ag_send.at[way, j],
            recv_sem=ag_recv.at[j], device_id=to(dz), device_id_type=MESH,
        )

    @pl.when(has_low)
    def _():
        ag_copy(z, -1).start()

    @pl.when(has_high)
    def _():
        ag_copy(z, 1).start()

    def rs_copy(j, n, dz, own):
        way = (dz + 1) // 2
        if own:
            dst = below.at[n] if dz == 1 else above.at[n]
            sem = own_recv.at[1 - way, n]
        else:
            dst, sem = land.at[j, n], rs_recv.at[j, n]
        return pltpu.make_async_remote_copy(
            src_ref=part.at[j, n], dst_ref=dst, send_sem=rs_send.at[j, n],
            recv_sem=sem, device_id=to(dz), device_id_type=MESH,
        )

    def pass_on(j, n, what):
        for dz in (1, -1):
            for own in (True, False):
                hop = j == z + dz
                going = (j > z) if dz == 1 else (j < z)
                near = hop if own else jnp.logical_not(hop)

                @pl.when(jnp.logical_and(going, near))
                def _(dz=dz, own=own):
                    copy = rs_copy(j, n, dz, own)
                    copy.start() if what == "start" else copy.wait_send()

    def out_copies(j):
        at = pl.ds(pl.multiple_of(j * rows, rows), rows)
        return [
            pltpu.make_async_copy(src.at[j], dst.at[at, :], out_sem.at[k, j])
            for k, (src, dst) in enumerate(
                ((rows_v, rows_out), (hid_v, hid_out), (dg_v, dg_out), (du_v, du_out))
            )
        ]

    def step(s, carry):
        for sign in (-1, 1):
            j = z + sign * s
            inside = jnp.logical_and(s > 0, (j >= 0) if sign == -1 else (j < size))

            @pl.when(inside)
            def _(j=j, sign=sign):
                ag_copy(j, -sign).wait_recv()

            onward = has_high if sign == -1 else has_low

            @pl.when(jnp.logical_and(inside, onward))
            def _(j=j, sign=sign):
                ag_copy(j, -sign).start()

        j = line_order(z, s)
        at = pl.ds(pl.multiple_of(j * rows, rows), rows)

        @pl.when(s == 0)
        def _():
            cot_load.wait()

        def units_tile(f, carry):
            @pl.when(s == 0)
            def _():
                for copy in tile_loads(f):
                    copy.wait()

            cols = pl.ds(pl.multiple_of(f * ft, 128), ft)
            mine = rows_v[j]
            gate = jnp.dot(mine, gate_v[:, cols], preferred_element_type=f32)
            upper = jnp.dot(mine, up_v[:, cols], preferred_element_type=f32)
            d_hidden = jnp.dot(cot_v[at, :], down_v[:, cols], preferred_element_type=f32)
            sig = 1.0 / (1.0 + jnp.exp(-gate))
            act = gate * sig
            hid_v[j, :, cols] = (act * upper).astype(bf16)
            du_v[j, :, cols] = (d_hidden * act).astype(bf16)
            dg_v[j, :, cols] = (d_hidden * upper * (sig + act * (1.0 - sig))).astype(bf16)
            return carry

        lax.fori_loop(0, n_f, units_tile, 0)
        for copy in out_copies(j):
            copy.start()
        ends = jnp.logical_and(s > 0, jnp.logical_not(jnp.logical_and(has_low, has_high)))

        def width_tile(n, carry):
            at_n = pl.ds(pl.multiple_of(n * nt, nt), nt)
            dims = (((1,), (1,)), ((), ()))
            total = lax.dot_general(dg_v[j], gate_v[at_n, :], dims, preferred_element_type=f32)
            total += lax.dot_general(du_v[j], up_v[at_n, :], dims, preferred_element_type=f32)
            part[j, n] = total.astype(bf16)

            @pl.when(ends)
            def _():
                pass_on(j, n, "start")

            return carry

        lax.fori_loop(0, n_n, width_tile, 0)
        return carry

    lax.fori_loop(0, size, step, 0)

    def down_tile(i, carry):
        j, n = i // n_n, i % n_n
        at_n = pl.ds(pl.multiple_of(n * nt, nt), nt)
        total = lax.dot_general(
            hid_v[j], down_v[at_n, :], (((1,), (1,)), ((), ())), preferred_element_type=f32
        )
        res_v[j, :, at_n] = total.astype(bf16)
        return carry

    def forward(j, n):
        pltpu.make_async_copy(land.at[j, n], land.at[j, n], rs_recv.at[j, n]).wait()
        part[j, n] = (part[j, n].astype(f32) + land[j, n].astype(f32)).astype(bf16)
        pass_on(j, n, "start")

    middle = jnp.logical_and(has_low, has_high)

    @pl.when(middle)
    def _():
        def first(n, carry):
            forward(3 - z, n)
            return carry

        lax.fori_loop(0, n_n, first, 0)

    lax.fori_loop(0, (size * n_n) // 2, down_tile, 0)

    @pl.when(middle)
    def _():
        def second(n, carry):
            forward(3 - 3 * (z // 2), n)
            forward(3 * (z // 2), n)
            return carry

        lax.fori_loop(0, n_n, second, 0)

    lax.fori_loop((size * n_n) // 2, size * n_n, down_tile, 0)
    sum_copies = [
        pltpu.make_async_copy(
            res_v.at[j], sum_out.at[pl.ds(j * rows, rows), :], load_sem.at[2 + j]
        )
        for j in range(size)
    ]
    for copy in sum_copies:
        copy.start()

    def last(n, carry):
        @pl.when(has_low)
        def _():
            pltpu.make_async_copy(below.at[n], below.at[n], own_recv.at[0, n]).wait()
            part[z, n] = (part[z, n].astype(f32) + below[n].astype(f32)).astype(bf16)

        @pl.when(has_high)
        def _():
            pltpu.make_async_copy(above.at[n], above.at[n], own_recv.at[1, n]).wait()
            part[z, n] = (part[z, n].astype(f32) + above[n].astype(f32)).astype(bf16)

        dn_out[:, pl.ds(pl.multiple_of(n * nt, nt), nt)] = part[z, n]
        return carry

    lax.fori_loop(0, n_n, last, 0)

    def drain(j, carry):
        for copy in out_copies(j):
            copy.wait()
        for dz in (-1, 1):
            came = jnp.logical_or(j == z, (j > z) if dz == -1 else (j < z))
            there = has_low if dz == -1 else has_high

            @pl.when(jnp.logical_and(came, there))
            def _(dz=dz):
                ag_copy(j, dz).wait_send()

        def sent(n, carry):
            @pl.when(j != z)
            def _():
                pltpu.make_async_copy(part.at[j, n], part.at[j, n], rs_send.at[j, n]).wait()

            return carry

        lax.fori_loop(0, n_n, sent, 0)
        return carry

    lax.fori_loop(0, size, drain, 0)
    for copy in sum_copies:
        copy.wait()


def ffn(two, cot_rows, weights, axis="tensor", ft=768, nt=512, collective_id=1, limit=66_000_000):
    rows, width = two.shape
    units = weights.shape[1] // 3
    size = 4
    length = rows * size
    n_f, n_n = units // ft, width // nt
    bf16 = jnp.bfloat16
    hbm = pl.BlockSpec(memory_space=pl.ANY)
    vm = pltpu.VMEM
    dma = pltpu.SemaphoreType.DMA
    shape = lambda *s: jax.ShapeDtypeStruct(s, bf16)
    return pl.pallas_call(
        functools.partial(ffn_body, axis=axis, ft=ft, nt=nt),
        out_shape=(
            shape(length, width), shape(length, units), shape(length, units), shape(length, units),
            shape(length, width), shape(rows, width),
        ),
        in_specs=[hbm] * 3,
        out_specs=(hbm,) * 5 + (pl.BlockSpec(memory_space=pltpu.VMEM),),
        scratch_shapes=[
            vm((size, rows, width), bf16), vm((length, width), bf16),
            vm((width, units), bf16), vm((width, units), bf16), vm((width, units), bf16),
            vm((size, rows, units), bf16), vm((size, rows, units), bf16), vm((size, rows, units), bf16),
            vm((size, n_n, rows, nt), bf16), vm((size, n_n, rows, nt), bf16),
            vm((n_n, rows, nt), bf16), vm((n_n, rows, nt), bf16),
            vm((size, rows, width), bf16),
            dma((3, n_f)), dma((2 + size,)), dma((2, size)), dma((size,)), dma((size, n_n)), dma((size, n_n)),
            dma((2, n_n)), dma((4, size)),
        ],
        compiler_params=pltpu.CompilerParams(
            collective_id=collective_id, has_side_effects=True, vmem_limit_bytes=limit
        ),
        cost_estimate=pl.CostEstimate(
            flops=12 * length * width * units, bytes_accessed=8 * width * units + 8 * length * units,
            transcendentals=length * units,
        ),
        name="ffn",
    )(two, cot_rows, weights)


def back_body(
    two_ref, cot_ref, hid_ref, dg_ref, du_ref, part_ref, up_ref, x_ref, mid_ref, gain_ref, att_ref,
    query_ref, win_ref, lse_ref, ctx_ref, one_ref, mask_ref, turn_ref,
    ffn_out, query_out, out_out, kv_out, mixed_out, input_out, small_out,
    up_v, own_v, x_v, mid_v, gain_v, w_v, query_v, win_v, lse_v, mask_v, turn_v, lhs_ref, rhs_ref,
    d_mid, d_ctx, d_win, kv_give, kv_take, d_one, small_ref,
    left_v, right_v, grad, mate_land, core_sum, x_land, y_land, second, x_last, y_last, stage, fin,
    z_land, kv_land, sum_land, small_z, small_hop, small_next, in_sem, give_send, give_recv,
    left_sem, right_sem, mate_send, mate_recv, one_send, one_recv, two_send, two_recv, stage_sem,
    z_send, z_recv, kv_send, kv_recv, sum_send, sum_recv, own_sem, small_send, small_recv,
    hop_send, hop_recv, *, n_f, wide,
):
    f32, bf16 = jnp.float32, jnp.bfloat16
    d, z = lax.axis_index("dp"), lax.axis_index("tensor")
    size = 4
    core, x, y = d % 2, (d // 2) % 2, d // 4
    by_x, by_y, mate, _ = square(d)
    here, at_x, at_y = 2 * y + x, 2 * y + 1 - x, 2 * (1 - y) + x
    cross = 3 - here
    block, half = core_sum.shape[2], core_sum.shape[2] // 2
    n_ffn, n_att = 3 * n_f, rhs_ref.shape[1] // wide
    ring = x_land.shape[0]
    total = n_ffn + n_att
    chunk, width = mixed_out.shape
    share = block // size
    part_w = wide // 2

    barrier = pltpu.get_barrier_semaphore()
    for peer in (by_x, by_y, mate):
        pl.semaphore_signal(barrier, inc=1, device_id={"dp": peer}, device_id_type=MESH)
    for hop in range(1, size):
        pl.semaphore_signal(
            barrier, inc=1, device_id={"tensor": (z + hop) % size}, device_id_type=MESH
        )

    lefts = [
        pltpu.make_async_copy(ref, left_v, left_sem.at[k]) for k, ref in enumerate((cot_ref, two_ref))
    ]
    query_w = query_ref.shape[1]
    kv_w = KV_HEADS * HEAD_DIM
    heads = query_w // HEAD_DIM
    scale = HEAD_DIM ** (-0.5)
    ahead = att_ref.shape[1] - 2 * query_w - 2 * kv_w
    own_rows = pl.ds(pl.multiple_of(z * chunk, chunk), chunk)
    ctx_cols = pl.ds(query_w, query_w)
    plan = (
        (up_ref, up_v), (cot_ref.at[own_rows, :], own_v), (mid_ref, mid_v), (gain_ref, gain_v),
        (att_ref.at[:, pl.ds(ahead + 2 * kv_w + query_w, query_w)], w_v.at[:, pl.ds(0, query_w)]),
        (query_ref, query_v), (win_ref, win_v), (lse_ref, lse_v), (mask_ref, mask_v), (turn_ref, turn_v),
        (ctx_ref, rhs_ref.at[:, ctx_cols]), (x_ref, x_v), (one_ref, lhs_ref.at[0]),
        (att_ref.at[:, pl.ds(ahead, 2 * kv_w + query_w)], w_v),
    )
    loads = [pltpu.make_async_copy(src, dst, in_sem.at[k]) for k, (src, dst) in enumerate(plan)]

    def right_load(i, what):
        cols = pl.ds(pl.multiple_of((i % n_f) * wide, 128), wide)
        for m, ref in enumerate((hid_ref, dg_ref, du_ref)):
            copy = pltpu.make_async_copy(ref.at[:, cols], right_v.at[i % 2], right_sem.at[i % 2])

            @pl.when(i // n_f == m)
            def _(copy=copy):
                copy.start() if what == "start" else copy.wait()

    lefts[0].start()
    right_load(jnp.int32(0), "start")
    for copy in loads[:-1]:
        copy.start()

    def chunk_rows(j):
        return part_ref.at[pl.ds(pl.multiple_of(j * chunk, chunk), chunk), :]

    own_part = pltpu.make_async_copy(chunk_rows(z), sum_land.at[size - 1], own_sem.at[0])
    own_part.start()
    pl.semaphore_wait(barrier, 3 + size - 1)

    def dp_copy(src, dst, send_sem, recv_sem, peer):
        return pltpu.make_async_remote_copy(
            src_ref=src, dst_ref=dst, send_sem=send_sem, recv_sem=recv_sem,
            device_id={"dp": peer}, device_id_type=MESH,
        )

    def z_copy(src, dst, send_sem, recv_sem, peer):
        return pltpu.make_async_remote_copy(
            src_ref=src, dst_ref=dst, send_sem=send_sem, recv_sem=recv_sem,
            device_id={"tensor": peer}, device_id_type=MESH,
        )

    small_copies, sum_copies = [], []
    for hop in range(1, size):
        to, k = (z + hop) % size, hop - 1
        small_copies.append(
            z_copy(small_ref, small_z.at[k], small_send.at[k], small_recv.at[k], to)
        )
        sum_copies.append(
            z_copy(chunk_rows(to), sum_land.at[k], sum_send.at[k], sum_recv.at[k], to)
        )
    for copy in sum_copies:
        copy.start()
    rhs_ref[:, 2 * query_w + 2 * kv_w :] = jnp.zeros((chunk, rhs_ref.shape[1] - 2 * query_w - 2 * kv_w), bf16)

    hops = (mate, by_x, by_y)

    def hop_copy(k):
        return dp_copy(small_next.at[k], small_hop.at[k], hop_send.at[k], hop_recv.at[k], hops[k])

    def mate_copy(i):
        return dp_copy(
            grad.at[i % 2, :, 1 - core], mate_land.at[i % 4], mate_send.at[i % 4],
            mate_recv.at[i % 4], mate,
        )

    def one_copies(i):
        s = core_sum.at[i % 4]
        first, last = pl.ds(0, half), pl.ds(half, half)
        plan = (
            (s.at[at_x, first, :], x_land.at[i % ring, 0], by_x), (s.at[cross, first, :], x_land.at[i % ring, 1], by_x),
            (s.at[at_y, last, :], y_land.at[i % ring, 0], by_y), (s.at[cross, last, :], y_land.at[i % ring, 1], by_y),
        )
        return [
            dp_copy(src, dst, one_send.at[k, i % ring], one_recv.at[k, i % ring], peer)
            for k, (src, dst, peer) in enumerate(plan)
        ]

    def two_copies(i):
        return [
            dp_copy(second.at[i % 4, 0], y_last.at[i % ring], two_send.at[0, i % ring], two_recv.at[0, i % ring], by_y),
            dp_copy(second.at[i % 4, 1], x_last.at[i % ring], two_send.at[1, i % ring], two_recv.at[1, i % ring], by_x),
        ]

    def stage_copy(i):
        cols = pl.ds(pl.multiple_of(i * wide, 128), wide)
        return pltpu.make_async_copy(stage.at[i % 2], ffn_out.at[:, cols], stage_sem.at[i % 2])

    def multiply(i):
        @pl.when(jnp.logical_and(i >= 2, i < total))
        def _():
            mate_copy(i - 2).wait_send()

        @pl.when(i + 1 < n_ffn)
        def _():
            right_load(i + 1, "start")

        dims = (((0,), (0,)), ((), ()))

        @pl.when(i < n_ffn)
        def _():
            @pl.when(i == 0)
            def _():
                lefts[0].wait()

            @pl.when(i == n_f)
            def _():
                lefts[1].start()
                lefts[1].wait()

            right_load(i, "wait")

            def rows(k, carry):
                at = pl.ds(pl.multiple_of(k * 2 * block, 128), 2 * block)
                value = lax.dot_general(
                    left_v[:, at], right_v[i % 2], dims, preferred_element_type=f32
                )
                grad[i % 2, k] = value.astype(bf16).reshape(2, block, wide)
                return carry

            lax.fori_loop(0, 4, rows, 0)

        @pl.when(jnp.logical_and(i >= n_ffn, i < total))
        def _():
            a = i - n_ffn
            cols = pl.ds(pl.multiple_of(a * wide, 128), wide)

            def rows(k, carry):
                at = pl.ds(pl.multiple_of(k * 2 * block, 128), 2 * block)
                value = lax.dot_general(
                    lhs_ref[(a // 2) % 2, :, at], rhs_ref[:, cols], dims, preferred_element_type=f32
                )
                grad[i % 2, k] = value.astype(bf16).reshape(2, block, wide)
                return carry

            lax.fori_loop(0, 4, rows, 0)

        @pl.when(i < total)
        def _():
            mate_copy(i).start()

    def sum_cores(i):
        mate_copy(i).wait_recv()
        for k in range(4):
            core_sum[i % 4, k] = (
                grad[i % 2, k, core].astype(f32) + mate_land[i % 4, k].astype(f32)
            ).astype(bf16)
        for copy in one_copies(i):
            copy.start()

    def sum_near(i):
        for copy in one_copies(i):
            copy.wait_recv()
        s = core_sum.at[i % 4]
        second[i % 4, 0] = (s[at_y, :half].astype(f32) + x_land[i % ring, 1].astype(f32)).astype(bf16)
        second[i % 4, 1] = (s[at_x, half:].astype(f32) + y_land[i % ring, 1].astype(f32)).astype(bf16)
        for copy in two_copies(i):
            copy.start()

    def z_sends(a, what):
        for h in range(2):
            owner = (a % 2) * 2 + h
            hop = (owner - z + size) % size
            src = fin.at[a, :, pl.ds(h * part_w, part_w)]

            @pl.when(jnp.logical_and(a < 4, hop > 0))
            def _(src=src, owner=owner, hop=hop, h=h):
                copy = z_copy(
                    src, z_land.at[a // 2, hop - 1], z_send.at[a, h], z_recv.at[a // 2, hop - 1], owner
                )
                copy.start() if what == "start" else copy.wait_send()

        @pl.when(a == 4)
        def _():
            for hop in range(1, size):
                to = (z + hop) % size
                rows = pl.ds(pl.multiple_of(to * share, 16), share)
                copy = z_copy(
                    fin.at[4, rows, :], kv_land.at[hop - 1], kv_send.at[hop - 1], kv_recv.at[hop - 1], to
                )
                copy.start() if what == "start" else copy.wait_send()

    def finish(i):
        for copy in two_copies(i):
            copy.wait_recv()
        own = core_sum.at[i % 4, here]
        top = own[:half].astype(f32) + x_land[i % ring, 0].astype(f32) + y_last[i % ring].astype(f32)
        low = own[half:].astype(f32) + y_land[i % ring, 0].astype(f32) + x_last[i % ring].astype(f32)

        @pl.when(i < n_ffn)
        def _():
            @pl.when(i >= 2)
            def _():
                stage_copy(i - 2).wait()

            stage[i % 2, :half] = top
            stage[i % 2, half:] = low
            stage_copy(i).start()

        @pl.when(i >= n_ffn)
        def _():
            a = i - n_ffn
            fin[a, :half] = top.astype(bf16)
            fin[a, half:] = low.astype(bf16)
            z_sends(a, "start")

        for copy in one_copies(i) + two_copies(i):
            copy.wait_send()

    def back_norm(upstream, value, gain, base, col):
        inverse = lax.rsqrt(jnp.mean(value * value, axis=-1, keepdims=True) + EPSILON)
        unit = value * inverse
        scaled = upstream * gain
        term = jnp.sum(upstream * unit, axis=0, keepdims=True)
        small_ref[:, pl.ds(col, width)] += jnp.broadcast_to(term, (8, width))
        return base + inverse * (scaled - unit * jnp.mean(scaled * unit, axis=-1, keepdims=True))

    some_rows = max(16, chunk // 4)

    def by_rows(work):
        def some(r, carry):
            work(pl.ds(pl.multiple_of(r * some_rows, some_rows), some_rows))
            return carry

        lax.fori_loop(0, chunk // some_rows, some, 0)

    gain_one_at, gain_two_at = query_w + 2 * kv_w, query_w + 2 * kv_w + width

    def open_branch():
        for k in (0, 1, 2, 3):
            loads[k].wait()
        small_ref[...] = jnp.zeros_like(small_ref)

        def work(at):
            value = back_norm(
                up_v[at, :].astype(f32), mid_v[at, :], gain_v[1:2, :], own_v[at, :].astype(f32), gain_two_at
            )
            d_mid[at, :] = value
            lhs_ref[1, at, :] = value.astype(bf16)

        by_rows(work)

    def context_grads():
        loads[4].wait()
        tile = min(512, query_w)

        def some(n, carry):
            cols = pl.ds(pl.multiple_of(n * tile, tile), tile)
            d_ctx[:, cols] = jnp.dot(lhs_ref[1], w_v[:, cols], preferred_element_type=f32).astype(bf16)
            return carry

        lax.fori_loop(0, query_w // tile, some, 0)
        loads[-1].start()
        for k in (5, 6, 7, 8, 9):
            loads[k].wait()
        d_win[...] = jnp.zeros_like(d_win)

    def turned_back(value):
        return value * turn_v[0] - pltpu.roll(value, HEAD_DIM // 2, 1) * turn_v[1]

    def attend_back(first, last):
        def head(h, carry):
            cols = pl.ds(pl.multiple_of(h * HEAD_DIM, 128), HEAD_DIM)
            group = h // (heads // KV_HEADS)
            key_cols = pl.ds(pl.multiple_of(group * HEAD_DIM, 128), HEAD_DIM)
            value_cols = pl.ds(pl.multiple_of(kv_w + group * HEAD_DIM, 128), HEAD_DIM)
            key = win_v[:, :, key_cols].reshape(3 * chunk, HEAD_DIM)
            value = win_v[:, :, value_cols].reshape(3 * chunk, HEAD_DIM)
            query, given = query_v[:, cols], d_ctx[:, cols]
            across, down = (((1,), (1,)), ((), ())), (((0,), (0,)), ((), ()))
            scores = lax.dot_general(query, key, across, preferred_element_type=f32)
            probs = jnp.exp(scores * scale + mask_v[...] - lse_v[h])
            d_probs = lax.dot_general(given, value, across, preferred_element_type=f32)
            delta = jnp.sum(probs * d_probs, axis=-1, keepdims=True)
            d_scores = (probs * (d_probs - delta)).astype(bf16)
            d_query = jnp.dot(d_scores, key, preferred_element_type=f32) * scale
            rhs_ref[:, cols] = turned_back(d_query).astype(bf16)
            d_key = lax.dot_general(d_scores, query, down, preferred_element_type=f32) * scale
            d_value = lax.dot_general(probs.astype(bf16), given, down, preferred_element_type=f32)
            d_win[:, :, key_cols] += d_key.reshape(3, chunk, HEAD_DIM)
            d_win[:, :, value_cols] += d_value.reshape(3, chunk, HEAD_DIM)
            return carry

        lax.fori_loop(first, last, head, 0)

    def give_copy(hop):
        return z_copy(
            kv_give.at[hop - 1], kv_take.at[hop - 1], give_send.at[hop - 1], give_recv.at[hop - 1], z - hop
        )

    def give():
        for hop in (1, 2):

            @pl.when(z >= hop)
            def _(hop=hop):
                kv_give[hop - 1] = d_win[2 - hop].astype(bf16)
                give_copy(hop).start()

    def take():
        for hop in (1, 2):

            @pl.when(z + hop < size)
            def _(hop=hop):
                pltpu.make_async_copy(kv_take.at[hop - 1], kv_take.at[hop - 1], give_recv.at[hop - 1]).wait()
                d_win[2] += kv_take[hop - 1].astype(f32)

        for g in range(KV_HEADS):
            cols = slice(g * HEAD_DIM, (g + 1) * HEAD_DIM)
            out_cols = slice(2 * query_w + g * HEAD_DIM, 2 * query_w + (g + 1) * HEAD_DIM)
            rhs_ref[:, out_cols] = turned_back(d_win[2, :, cols]).astype(bf16)
        rhs_ref[:, 2 * query_w + kv_w : 2 * query_w + 2 * kv_w] = d_win[2, :, kv_w:].astype(bf16)
        ones = jnp.ones((8, chunk), bf16)
        small_ref[:, :query_w] = jnp.dot(ones, rhs_ref[:, :query_w], preferred_element_type=f32)
        small_ref[:, query_w : query_w + 2 * kv_w] = jnp.dot(
            ones, rhs_ref[:, 2 * query_w : 2 * query_w + 2 * kv_w], preferred_element_type=f32
        )

    def one_grads():
        loads[-1].wait()
        tile = min(512, width)
        across = (((1,), (1,)), ((), ()))

        def some(n, carry):
            at_n = pl.ds(pl.multiple_of(n * tile, tile), tile)
            d_one[:, at_n] = lax.dot_general(
                rhs_ref[:, :query_w], w_v[at_n, 2 * kv_w :], across, preferred_element_type=f32
            ) + lax.dot_general(
                rhs_ref[:, 2 * query_w : 2 * query_w + 2 * kv_w], w_v[at_n, : 2 * kv_w], across,
                preferred_element_type=f32,
            )
            return carry

        lax.fori_loop(0, width // tile, some, 0)

    def close_branch():
        loads[11].wait()

        def work(at):
            input_out[at, :] = back_norm(
                d_one[at, :], x_v[at, :].astype(f32), gain_v[0:1, :], d_mid[at, :], gain_one_at
            ).astype(bf16)

        by_rows(work)
        for copy in small_copies:
            copy.start()

    def small_first():
        for copy in small_copies:
            copy.wait_recv()
        small_next[0] = small_ref[...] + small_z[0] + small_z[1] + small_z[2]
        hop_copy(0).start()

    def small_then(k):
        hop_copy(k).wait_recv()
        small_next[k + 1] = small_next[k] + small_hop[k]
        hop_copy(k + 1).start()

    def small_last():
        hop_copy(2).wait_recv()
        small_out[...] = small_next[2] + small_hop[2]

    span = n_ffn - 1
    quarter = heads // 4

    def at_turn(k):
        return min(k, span)

    steps = [
        (0, open_branch), (at_turn(1), context_grads),
        (at_turn(2), lambda: attend_back(0, quarter)),
        (at_turn(3), lambda: attend_back(quarter, 2 * quarter)),
        (at_turn(4), lambda: attend_back(2 * quarter, 3 * quarter)),
        (at_turn(5), lambda: attend_back(3 * quarter, heads)),
        (at_turn(5), give),
        (at_turn(7), take), (at_turn(7), lambda: [loads[k].wait() for k in (10, 12)]),
        (n_ffn + 1, one_grads), (n_ffn + 2, close_branch),
        (n_ffn + 4, small_first), (n_ffn + 5, lambda: small_then(0)), (n_ffn + 6, lambda: small_then(1)),
        (n_ffn + 7, small_last),
    ]

    def small_step(i):
        for when, step in steps:

            @pl.when(i == when)
            def _(step=step):
                step()

    def turn(i, carry):
        multiply(i)
        for lag, work in ((1, sum_cores), (2, sum_near), (3, finish)):

            @pl.when(jnp.logical_and(i >= lag, i - lag < total))
            def _(lag=lag, work=work):
                work(i - lag)

        small_step(i)
        return carry

    lax.fori_loop(0, total + 3, turn, 0)
    for i in (total - 2, total - 1):
        mate_copy(i).wait_send()
    for i in (n_ffn - 2, n_ffn - 1):
        stage_copy(i).wait()
    own_part.wait()
    for copy in sum_copies:
        copy.wait_recv()
    acc = sum_land[size - 1].astype(f32)
    for k in range(size - 1):
        acc += sum_land[k].astype(f32)
    mixed_out[...] = (mid_v[...] + acc).astype(bf16)
    for of, dst in ((0, query_out), (1, out_out)):
        for k in range(size - 1):
            ref = z_land.at[of, k]
            pltpu.make_async_copy(ref, ref, z_recv.at[of, k]).wait()
        for h in range(4):

            @pl.when(z == h)
            def _(of=of, dst=dst, h=h):
                acc = fin[2 * of + h // 2, :, (h % 2) * part_w : (h % 2 + 1) * part_w].astype(f32)
                for k in range(size - 1):
                    acc += z_land[of, k].astype(f32)
                dst[...] = acc

    for k in range(size - 1):
        pltpu.make_async_copy(kv_land.at[k], kv_land.at[k], kv_recv.at[k]).wait()
    rows = pl.ds(pl.multiple_of(z * share, 16), share)
    acc = fin[4, rows, :].astype(f32)
    for k in range(size - 1):
        acc += kv_land[k].astype(f32)
    kv_out[...] = acc
    for a in range(n_att):
        z_sends(a, "wait")
    for copy in sum_copies + small_copies:
        copy.wait_send()
    for k in range(3):
        hop_copy(k).wait_send()
    for hop in (1, 2):

        @pl.when(z >= hop)
        def _(hop=hop):
            give_copy(hop).wait_send()


def back(
    two, cot_rows, hid, dg, du, ffn_part, up, tokens, middle, gains, att_w, query_rot, kv_win, lse, context,
    normed_one, mask, turn, wide=768, collective_id=3, limit=67_000_000,
):
    length, width = two.shape
    size, chunk, block = 4, tokens.shape[0], width // 8
    units, query_w, kv_w = hid.shape[1], context.shape[1], kv_win.shape[2]
    n_f, n_att = units // wide, (2 * query_w + wide) // wide
    total = 3 * n_f + n_att
    half, part_w, share = block // 2, wide // 2, block // size
    heads = lse.shape[0]
    bf16, f32 = jnp.bfloat16, jnp.float32
    small = (8, query_w + kv_w + 2 * width)
    ring = 5
    hbm = pl.BlockSpec(memory_space=pl.ANY)
    vmem = pl.BlockSpec(memory_space=pltpu.VMEM)
    vm = pltpu.VMEM
    dma = pltpu.SemaphoreType.DMA
    shape = jax.ShapeDtypeStruct
    return pl.pallas_call(
        functools.partial(back_body, n_f=n_f, wide=wide),
        out_shape=(
            shape((block, 3 * units), f32), shape((block, part_w), f32), shape((block, part_w), f32),
            shape((share, wide), f32), shape((chunk, width), bf16), shape((chunk, width), bf16),
            shape(small, f32),
        ),
        in_specs=[hbm] * 18,
        out_specs=(hbm,) + (vmem,) * 6,
        scratch_shapes=[
            vm((chunk, width), bf16), vm((chunk, width), bf16), vm((chunk, width), bf16),
            vm((chunk, width), f32), vm(gains.shape, f32), vm((width, kv_w + query_w), bf16),
            vm((chunk, query_w), bf16), vm(kv_win.shape, bf16), vm((heads, chunk, 1), f32),
            vm(mask.shape, f32), vm(turn.shape, f32), vm((2, chunk, width), bf16),
            vm((chunk, 2 * query_w + wide), bf16), vm((chunk, width), f32), vm((chunk, query_w), bf16),
            vm(kv_win.shape, f32), vm((2, chunk, kv_w), bf16), vm((2, chunk, kv_w), bf16),
            vm((chunk, width), f32), vm(small, f32),
            vm((length, width), bf16), vm((2, length, wide), bf16), vm((2, 4, 2, block, wide), bf16),
            vm((4, 4, block, wide), bf16), vm((4, 4, block, wide), bf16),
            vm((ring, 2, half, wide), bf16), vm((ring, 2, half, wide), bf16),
            vm((4, 2, half, wide), bf16), vm((ring, half, wide), bf16), vm((ring, half, wide), bf16),
            vm((2, block, wide), f32), vm((n_att, block, wide), bf16),
            vm((2, size - 1, block, part_w), bf16), vm((size - 1, share, wide), bf16),
            vm((size, chunk, width), bf16), vm((3,) + small, f32), vm((3,) + small, f32),
            vm((3,) + small, f32), dma((14,)), dma((2,)), dma((2,)),
            dma((2,)), dma((2,)), dma((4,)), dma((4,)), dma((4, ring)), dma((4, ring)),
            dma((2, ring)), dma((2, ring)), dma((2,)),
            dma((4, 2)), dma((2, size - 1)), dma((size - 1,)), dma((size - 1,)), dma((size - 1,)),
            dma((size - 1,)), dma((1,)), dma((size - 1,)), dma((size - 1,)), dma((3,)), dma((3,)),
        ],
        compiler_params=pltpu.CompilerParams(
            collective_id=collective_id, has_side_effects=True, vmem_limit_bytes=limit
        ),
        cost_estimate=pl.CostEstimate(
            flops=6 * length * width * units, bytes_accessed=8 * length * units, transcendentals=0
        ),
        name="back",
    )(
        two, cot_rows, hid, dg, du, ffn_part, up, tokens, middle, gains, att_w, query_rot, kv_win, lse, context,
        normed_one, mask, turn,
    )


def angle_tables(first, length, head_width):
    position = (first + jnp.arange(length)).astype(jnp.float32)
    exponent = jnp.arange(head_width // 2, dtype=jnp.float32) * (2.0 / head_width)
    frequency = ROPE_BASE ** (-exponent)
    angle = position[:, None] * frequency[None, :]
    return (jnp.cos(angle), jnp.sin(angle))


def rotate(values, cosine, sine):
    half_width = values.shape[-1] // 2
    first_half = values[..., :half_width]
    second_half = values[..., half_width:]
    return jnp.concatenate(
        [first_half * cosine - second_half * sine, second_half * cosine + first_half * sine],
        axis=-1,
    )


def rotate_back(grads, cosine, sine):
    return rotate(grads, cosine, -sine)


def dot_f32(left, right, dims):
    return lax.dot_general(left, right, (dims, ((), ())), preferred_element_type=jnp.float32)


def contract_rows(left, right):
    return dot_f32(left, right, ((0,), (0,)))


def contract_cols(left, right):
    return dot_f32(left, right, ((1,), (1,)))


def norm_back(upstream, unit, inverse, gain):
    scaled = upstream * gain
    gain_term = jnp.sum(upstream * unit, axis=0)
    input_term = inverse * (scaled - unit * jnp.mean(scaled * unit, axis=-1, keepdims=True))
    return (gain_term, input_term)


def joined_units(gate_w, up_w, down_w):
    units = gate_w.shape[1]
    gap = -(-units // 768) * 768 - units
    wide = lambda w: jnp.pad(w, ((0, 0), (0, gap)))
    return jnp.concatenate([wide(gate_w), wide(up_w), wide(down_w)], axis=1)


def attention_branch(tokens, cosine, sine, mask, gains_w, query_w, query_b, kv_w, kv_b, out_w, ffn_w, cotangent):
    f32, bf16 = jnp.float32, jnp.bfloat16
    rows = tokens.shape[0]
    size = lax.axis_size("tensor")
    fixed_w = jnp.concatenate([gains_w, kv_w], axis=1)
    if lax.axis_size("dp") == 8 and size == 4:
        tall_query = jnp.concatenate([query_w, jnp.pad(query_b[None, :], ((0, 15), (0, 0)))], axis=0)
        tall_out = jnp.pad(out_w, ((0, 16), (0, 0)))
        turn = jnp.stack(
            [jnp.concatenate([cosine, cosine], axis=1), jnp.concatenate([-sine, sine], axis=1)]
        )
        att_w, ffn_all, cot_rows, two, middle, one, query_rot, kv_win, lse, context, gains = front(
            tokens, turn, mask, kv_b[None, :], tall_query, tall_out, fixed_w, ffn_w, cotangent
        )
        kv_win = kv_win.reshape(3 * rows, kv_w.shape[1])
        return att_w, ffn_all, cot_rows, two, middle, one, query_rot, kv_win, lse, context, gains
    pair = lax.all_gather(jnp.stack([query_w, out_w]), "tensor", axis=2, tiled=True)
    att_w = jnp.concatenate([fixed_w, pair[0], pair[1]], axis=1)
    att_w = lax.all_gather(att_w, "dp", axis=0, tiled=True)
    ffn_all = lax.all_gather(ffn_w, "dp", axis=0, tiled=True)
    cot_rows = lax.all_gather(cotangent, "tensor", axis=0, tiled=True)
    full_query_b = lax.all_gather(query_b, "tensor", axis=0, tiled=True).astype(f32)
    ahead = gains_w.shape[1]
    kv_width = kv_w.shape[1] // 2
    qkv_width = 2 * kv_width + full_query_b.shape[0]
    heads = full_query_b.shape[0] // HEAD_DIM
    gains = att_w[:, :2].T.astype(f32)
    inputs = tokens.astype(f32)
    inverse = lax.rsqrt(jnp.mean(inputs * inputs, axis=-1, keepdims=True) + EPSILON)
    one = (inputs * inverse * gains[0]).astype(bf16)
    lin = jnp.dot(one, att_w[:, ahead : ahead + qkv_width], preferred_element_type=f32)
    lin = lin + jnp.concatenate([kv_b, full_query_b])
    cos_h, sin_h = cosine[:, None, :], sine[:, None, :]
    query_rot = rotate(lin[:, 2 * kv_width :].reshape(rows, heads, HEAD_DIM), cos_h, sin_h).astype(bf16)
    key_rot = rotate(lin[:, :kv_width].reshape(rows, KV_HEADS, HEAD_DIM), cos_h, sin_h).astype(bf16)
    kv_own = jnp.concatenate(
        [key_rot.reshape(rows, kv_width), lin[:, kv_width : 2 * kv_width].astype(bf16)], axis=1
    )
    back_chunks = mask.shape[1] // rows - 1
    kv_win = jnp.concatenate(
        [shift(kv_own, hops) for hops in range(back_chunks, 0, -1)] + [kv_own], axis=0
    )
    window = kv_win.shape[0]
    key_win = kv_win[:, :kv_width].reshape(window, KV_HEADS, HEAD_DIM)
    value_win = kv_win[:, kv_width:].reshape(window, KV_HEADS, HEAD_DIM)
    grouped = query_rot.reshape(rows, KV_HEADS, heads // KV_HEADS, HEAD_DIM)
    scores = jnp.einsum("tagd,sad->agts", grouped, key_win, preferred_element_type=f32)
    scores = scores * HEAD_DIM ** (-0.5) + mask
    largest = jnp.max(scores, axis=-1, keepdims=True)
    lse = largest + jnp.log(jnp.sum(jnp.exp(scores - largest), axis=-1, keepdims=True))
    probs = jnp.exp(scores - lse).astype(bf16)
    context = jnp.einsum("agts,sad->tagd", probs, value_win, preferred_element_type=f32)
    context = context.reshape(rows, heads * HEAD_DIM).astype(bf16)
    middle = inputs + contract_cols(context, att_w[:, ahead + qkv_width :])
    inverse = lax.rsqrt(jnp.mean(middle * middle, axis=-1, keepdims=True) + EPSILON)
    two = (middle * inverse * gains[1]).astype(bf16)
    query_rot = query_rot.reshape(rows, heads * HEAD_DIM)
    return att_w, ffn_all, cot_rows, two, middle, one, query_rot, kv_win, lse, context, gains


def shift(value, hops):
    size = lax.axis_size("tensor")
    pairs = [(i, i + hops) for i in range(size) if 0 <= i + hops < size]
    return lax.ppermute(value, "tensor", pairs)


def sum_grads(two, cot_rows, hid, dg, du, normed_one, d_attended, d_lin, context, ffn_part, small):
    f32, bf16 = jnp.float32, jnp.bfloat16
    fixed = d_lin.shape[1] - context.shape[1]
    d_query = d_lin[:, fixed:]
    def over_dp(left, right):
        return lax.psum_scatter(
            contract_rows(left, right).astype(bf16), "dp", scatter_dimension=0, tiled=True
        )

    def over_tensor(value, axis):
        return lax.psum_scatter(value, "tensor", scatter_dimension=axis, tiled=True).astype(f32)

    return (
        over_dp(cot_rows, hid).astype(f32),
        over_dp(two, dg).astype(f32),
        over_dp(two, du).astype(f32),
        over_tensor(over_dp(normed_one, d_query), 1),
        over_tensor(over_dp(d_attended, context), 1),
        over_tensor(over_dp(normed_one, d_lin[:, :fixed]), 0),
        over_tensor(ffn_part, 0),
        lax.psum(small, ("dp", "tensor")),
    )


def branch_back(
    tokens, cosine, sine, mask, att_w, cot_rows, rows_two, hidden_low, d_gate, d_upper, ffn_part,
    d_normed_two, cotangent, middle, normed_one, query_rot, kv_win, lse, context, gains,
):
    f32, bf16 = jnp.float32, jnp.bfloat16
    rows = tokens.shape[0]
    kv_width, query_width = kv_win.shape[1] // 2, query_rot.shape[1]
    qkv_width = 2 * kv_width + query_width
    ahead = att_w.shape[1] - qkv_width - query_width
    heads, padded = query_width // HEAD_DIM, hidden_low.shape[1]
    if lax.axis_size("dp") == 8 and lax.axis_size("tensor") == 4:
        turn = jnp.stack(
            [jnp.concatenate([cosine, cosine], axis=1), jnp.concatenate([-sine, sine], axis=1)]
        )
        flat, sum_query, sum_out, sum_kv, mixed, input_grad, small = back(
            rows_two, cot_rows, hidden_low, d_gate, d_upper, ffn_part, d_normed_two, tokens, middle, gains,
            att_w, query_rot, kv_win.reshape(-1, rows, 2 * kv_width), lse, context, normed_one, mask, turn,
        )
        flat = [flat[:, k * padded : (k + 1) * padded] for k in range(3)]
        return mixed, input_grad, *flat, sum_query, sum_out, sum_kv, small[0]
    group = heads // KV_HEADS
    window = kv_win.shape[0]
    back_chunks = window // rows - 1
    scale = HEAD_DIM ** (-0.5)
    cos_h, sin_h = cosine[:, None, :], sine[:, None, :]
    d_normed_two = d_normed_two.astype(f32)
    qkv_w = att_w[:, ahead : ahead + qkv_width]
    out_full = att_w[:, ahead + qkv_width :]
    inputs = tokens.astype(f32)
    inverse_one = lax.rsqrt(jnp.mean(inputs * inputs, axis=-1, keepdims=True) + EPSILON)
    unit_one = inputs * inverse_one
    inverse_two = lax.rsqrt(jnp.mean(middle * middle, axis=-1, keepdims=True) + EPSILON)
    unit_two = middle * inverse_two
    gain_two_term, d_from_two = norm_back(d_normed_two, unit_two, inverse_two, gains[1])
    d_middle = cotangent.astype(f32) + d_from_two
    d_attended = d_middle.astype(bf16)
    d_context = jnp.dot(d_attended, out_full, preferred_element_type=f32).astype(bf16)
    d_context = d_context.reshape(rows, KV_HEADS, group, HEAD_DIM)
    key_win = kv_win[:, :kv_width].reshape(window, KV_HEADS, HEAD_DIM)
    value_win = kv_win[:, kv_width:].reshape(window, KV_HEADS, HEAD_DIM)
    grouped = query_rot.reshape(rows, KV_HEADS, group, HEAD_DIM)
    scores = jnp.einsum("tagd,sad->agts", grouped, key_win, preferred_element_type=f32) * scale + mask
    probs = jnp.exp(scores - lse.reshape(KV_HEADS, group, rows, 1))
    probs_low = probs.astype(bf16)
    d_probs = jnp.einsum("tagd,sad->agts", d_context, value_win, preferred_element_type=f32)
    row_delta = jnp.sum(probs * d_probs, axis=-1, keepdims=True)
    d_scores = (probs * (d_probs - row_delta)).astype(bf16)
    d_query_rot = jnp.einsum("agts,sad->tagd", d_scores, key_win, preferred_element_type=f32) * scale
    d_key_win = jnp.einsum("agts,tagd->sad", d_scores, grouped, preferred_element_type=f32) * scale
    d_value_win = jnp.einsum("agts,tagd->sad", probs_low, d_context, preferred_element_type=f32)
    d_query_lin = (
        rotate_back(d_query_rot.reshape(rows, heads, HEAD_DIM), cos_h, sin_h)
        .reshape(rows, query_width).astype(bf16)
    )
    d_kv_win = jnp.concatenate(
        [d_key_win.reshape(window, kv_width), d_value_win.reshape(window, kv_width)], axis=1
    ).astype(bf16)
    d_kv = d_kv_win[back_chunks * rows :].astype(f32)
    for hops in range(1, back_chunks + 1):
        given = d_kv_win[(back_chunks - hops) * rows : (back_chunks - hops + 1) * rows]
        d_kv = d_kv + shift(given, -hops).astype(f32)
    d_key_lin = rotate_back(d_kv[:, :kv_width].reshape(rows, KV_HEADS, HEAD_DIM), cos_h, sin_h)
    d_lin = jnp.concatenate(
        [d_key_lin.reshape(rows, kv_width).astype(bf16), d_kv[:, kv_width:].astype(bf16), d_query_lin],
        axis=1,
    )
    d_normed_one = contract_cols(d_lin, qkv_w)
    bias_term = jnp.sum(d_lin.astype(f32), axis=0)
    gain_one_term, d_from_one = norm_back(d_normed_one, unit_one, inverse_one, gains[0])
    input_grad = (d_middle + d_from_one).astype(bf16)

    sums = sum_grads(
        rows_two, cot_rows, hidden_low, d_gate, d_upper, normed_one, d_attended, d_lin, context,
        ffn_part, jnp.concatenate([bias_term[2 * kv_width :], bias_term[: 2 * kv_width], gain_one_term, gain_two_term]),
    )
    sum_down, sum_gate, sum_up, sum_query, sum_out, sum_kv, ffn_sum, small = sums
    mixed = (middle + ffn_sum.astype(f32)).astype(bf16)
    return mixed, input_grad, sum_down, sum_gate, sum_up, sum_query, sum_out, sum_kv, small


def local(
    tokens, segments, gain_one, query_w, query_b, key_w, key_b, value_w, value_b,
    out_w, gain_two, gate_w, up_w, down_w, cotangent,
):
    bf16, f32 = jnp.bfloat16, jnp.float32
    rows, model_width = tokens.shape
    tensor_size = lax.axis_size("tensor")
    rank = lax.axis_index("tensor")
    kv_width = key_w.shape[1]
    fixed_width = 2 * kv_width
    query_width = query_w.shape[1] * tensor_size
    qkv_width = fixed_width + query_width
    units = gate_w.shape[1]
    back_chunks = min(tensor_size - 1, -(-DOC_MAX // rows))
    window = (back_chunks + 1) * rows
    cosine, sine = angle_tables(rank * rows, rows, HEAD_DIM)
    segment = segments[0]
    own_segment = lax.dynamic_slice_in_dim(segment, rank * rows, rows, 0)
    before = jnp.full((back_chunks * rows,), -1, segment.dtype)
    win_segment = lax.dynamic_slice_in_dim(jnp.concatenate([before, segment]), rank * rows, window, 0)
    own_pos = back_chunks * rows + jnp.arange(rows)
    win_pos = jnp.arange(window)
    allowed = (own_segment[:, None] == win_segment[None, :]) & (win_pos[None, :] <= own_pos[:, None])
    mask = jnp.where(allowed, 0.0, NEGATIVE).astype(f32)
    ahead = 128
    gains_w = jnp.pad(jnp.stack([gain_one, gain_two], axis=1), ((0, 0), (0, ahead - 2)))
    (
        att_w, ffn_w, cot_rows, normed_two, middle, normed_one, query_rot, kv_win, lse, context, gains,
    ) = attention_branch(
        tokens, cosine, sine, mask, gains_w, query_w, query_b, jnp.concatenate([key_w, value_w], axis=1),
        jnp.concatenate([key_b, value_b]).astype(f32), out_w, joined_units(gate_w, up_w, down_w), cotangent,
    )
    rows_two, hidden_low, d_gate, d_upper, ffn_part, d_normed_two = ffn(
        normed_two, cot_rows, ffn_w
    )
    mixed, input_grad, sum_down, sum_gate, sum_up, sum_query, sum_out, sum_kv, small = branch_back(
        tokens, cosine, sine, mask, att_w, cot_rows, rows_two, hidden_low, d_gate, d_upper, ffn_part,
        d_normed_two, cotangent, middle, normed_one, query_rot, kv_win, lse, context, gains,
    )
    place = lax.axis_index("dp") * tensor_size + rank
    devices = lax.axis_size("dp") * tensor_size

    def own(start, size):
        share = size // devices
        return lax.dynamic_slice_in_dim(small, start + place * share, share, 0)

    return (
        mixed,
        input_grad,
        own(qkv_width, model_width),
        sum_query,
        own(0, query_width),
        sum_kv[:, :kv_width],
        small[query_width : query_width + kv_width],
        sum_kv[:, kv_width : 2 * kv_width],
        small[query_width + kv_width : qkv_width],
        sum_out,
        own(qkv_width + model_width, model_width),
        sum_gate[:, :units],
        sum_up[:, :units],
        sum_down[:, :units],
    )


def solution(mesh):
    both = ("dp", "tensor")
    return jax.shard_map(
        local,
        mesh=mesh,
        in_specs=(
            P(both, None), P("dp", None), P("dp"), P("dp", "tensor"), P("tensor"), P("dp", None), P(),
            P("dp", None), P(), P("dp", "tensor"), P("dp"), P("dp", "tensor"), P("dp", "tensor"),
            P("dp", "tensor"), P(both, None),
        ),
        out_specs=(
            P(both, None), P(both, None), P(both), P("dp", "tensor"), P(both), P(both, None), P(),
            P(both, None), P(), P("dp", "tensor"), P(both), P("dp", "tensor"), P("dp", "tensor"),
            P("dp", "tensor"),
        ),
        check_vma=False,
    )
```

```python
import functools

import jax
import jax.numpy as jnp
from jax import lax
from jax.experimental import pallas as pl
from jax.experimental.pallas import tpu as pltpu
from jax.sharding import PartitionSpec as P

MESH = pl.DeviceIdType.MESH
KV_HEADS = 2
HEAD_DIM = 128
DOC_MAX = 512
EPSILON = 1e-06
ROPE_BASE = 1000000.0
NEGATIVE = -1e30


def square(d):
    core, x, y = d % 2, (d // 2) % 2, d // 4
    by_x, by_y = d + 2 - 4 * x, d + 4 - 8 * y
    return by_x, by_y, d + 1 - 2 * core, by_x + 4 - 8 * y


def front_body(
    x_ref, turn_ref, mask_ref, bias_ref, query_ref, out_ref, fixed_ref, ffn_ref, cot_ref,
    att_all, ffn_all, cot_all, two_all, mid_out, one_out, query_rot, kv_win, lse_out, ctx_out, gain_out,
    att_v, w_v, one_v, q_v, kv_v, ctx_v, mid_v, two_v,
    fill_sem, z_send, z_recv, cot_send, cot_recv, send, recv, keep_sem, w_sem, kv_send, kv_recv, save_sem,
    two_send, two_recv,
    *, pieces, order, lead,
):
    f32, bf16 = jnp.float32, jnp.bfloat16
    d, z = lax.axis_index("dp"), lax.axis_index("tensor")
    size = 4
    by_x, by_y, mate, across = square(d)
    rows = ffn_ref.shape[0]
    half = rows // 2
    part = query_ref.shape[1]
    fixed = fixed_ref.shape[1]
    chunk = cot_ref.shape[0]
    tall = query_ref.shape[0]

    barrier = pltpu.get_barrier_semaphore()
    for peer in (by_x, by_y, mate):
        pl.semaphore_signal(barrier, inc=1, device_id={"dp": peer}, device_id_type=MESH)
    for hop in range(1, size):
        pl.semaphore_signal(
            barrier, inc=1, device_id={"tensor": (z + hop) % size}, device_id_type=MESH
        )

    def place(of, owner):
        return pl.ds(pl.multiple_of(fixed + of * size * part + owner * part, 128), part)

    fills = [pltpu.make_async_copy(fixed_ref, att_v.at[pl.ds(0, rows), pl.ds(0, fixed)], fill_sem.at[0])]
    for of, ref in enumerate((query_ref, out_ref)):
        fills.append(pltpu.make_async_copy(ref, att_v.at[:, place(of, z)], fill_sem.at[1 + of]))
    at = pl.ds(pl.multiple_of(z * chunk, chunk), chunk)
    fills.append(pltpu.make_async_copy(cot_ref, cot_all.at[at, :], fill_sem.at[3]))
    for copy in fills:
        copy.start()

    pl.semaphore_wait(barrier, 3 + size - 1)

    def z_copy(of, hop):
        ref = (query_ref, out_ref)[of]
        return pltpu.make_async_remote_copy(
            src_ref=ref, dst_ref=att_v.at[:, place(of, z)], send_sem=z_send.at[of, hop - 1],
            recv_sem=z_recv.at[of, hop - 1], device_id={"tensor": (z + hop) % size},
            device_id_type=MESH,
        )

    has_low, has_high = z > 0, z < size - 1

    def cot_copy(j, dz):
        ref = cot_all.at[pl.ds(pl.multiple_of(j * chunk, chunk), chunk), :]
        return pltpu.make_async_remote_copy(
            src_ref=ref, dst_ref=ref, send_sem=cot_send.at[(dz + 1) // 2, j], recv_sem=cot_recv.at[j],
            device_id={"tensor": z + dz}, device_id_type=MESH,
        )

    def cot_start():
        fills[3].wait()
        for dz, there in ((-1, has_low), (1, has_high)):

            @pl.when(there)
            def _(dz=dz):
                cot_copy(z, dz).start()

    def cot_step(hop):
        for sign, onward in ((-1, has_high), (1, has_low)):
            j = z + sign * hop
            inside = (j >= 0) if sign == -1 else (j < size)

            @pl.when(inside)
            def _(j=j, sign=sign):
                cot_copy(j, -sign).wait_recv()

            @pl.when(jnp.logical_and(inside, onward))
            def _(j=j, sign=sign):
                cot_copy(j, -sign).start()

    def two_copy(j, dz, own):
        ref = two_all.at[pl.ds(pl.multiple_of(j * chunk, chunk), chunk), :]
        return pltpu.make_async_remote_copy(
            src_ref=two_v if own else ref, dst_ref=ref, send_sem=two_send.at[(dz + 1) // 2, j],
            recv_sem=two_recv.at[j], device_id={"tensor": z + dz}, device_id_type=MESH,
        )

    def two_start():
        for dz, there in ((-1, has_low), (1, has_high)):

            @pl.when(there)
            def _(dz=dz):
                two_copy(z, dz, True).start()

    def two_step(hop):
        for sign, onward in ((-1, has_high), (1, has_low)):
            j = z + sign * hop
            inside = (j >= 0) if sign == -1 else (j < size)

            @pl.when(inside)
            def _(j=j, sign=sign):
                two_copy(j, -sign, False).wait_recv()

            if hop == 1:

                @pl.when(jnp.logical_and(inside, onward))
                def _(j=j, sign=sign):
                    two_copy(j, -sign, False).start()

    for of in range(2):
        for hop in range(1, size):
            z_copy(of, hop).start()
    fills[0].wait()

    def views(kind, p):
        src, dst = ((att_v, att_all), (ffn_ref, ffn_all))[kind]
        return src, dst, pl.ds(*pieces[kind][p])

    def slot(kind, p):
        return p + kind * len(pieces[0])

    def block(dst, cols, owner, first=0, many=None):
        many = rows if many is None else many
        return dst.at[pl.ds(pl.multiple_of(owner * rows + first, 16), many), cols]

    def remote(src, dst, way, at_slot, peer):
        return pltpu.make_async_remote_copy(
            src_ref=src, dst_ref=dst, send_sem=send.at[way, at_slot], recv_sem=recv.at[way, at_slot],
            device_id={"dp": peer}, device_id_type=MESH,
        )

    def own(kind, p):
        src, dst, cols = views(kind, p)
        mine = src.at[pl.ds(0, rows), cols]
        there = block(dst, cols, d)
        s = slot(kind, p)
        return [
            remote(mine, there, 0, s, by_x), remote(mine, there, 1, s, by_y),
            remote(mine, there, 2, s, mate),
        ], pltpu.make_async_copy(mine, there, keep_sem.at[s])

    def relays(kind, p, group):
        _, dst, cols = views(kind, p)
        s = slot(kind, p)
        if group == 2:
            whole = block(dst, cols, across)
            return [remote(whole, whole, 7, s, mate)]
        owner, peer = ((by_x, by_y), (by_y, by_x))[group]
        piece, whole = block(dst, cols, owner, group * half, half), block(dst, cols, owner)
        way = 3 + 2 * group
        return [remote(piece, piece, way, s, peer), remote(whole, whole, way + 1, s, mate)]

    def arrived(kind, p, way):
        _, dst, cols = views(kind, p)
        many = half if way in (3, 5) else rows
        ref = block(dst, cols, d, 0, many)
        pltpu.make_async_copy(ref, ref, recv.at[way, slot(kind, p)]).wait()

    def begin(kind, p):
        copies, keep = own(kind, p)
        for copy in copies:
            copy.start()
        keep.start()

    def pass_on(kind, p):
        for group in range(2):
            arrived(kind, p, group)
            for copy in relays(kind, p, group):
                copy.start()

    def close(kind, p):
        arrived(kind, p, 3)
        arrived(kind, p, 5)
        relays(kind, p, 2)[0].start()

    def settle(kind, p):
        for way in (2, 4, 6, 7):
            arrived(kind, p, way)
        own(kind, p)[1].wait()

    def finish(kind, p):
        copies = own(kind, p)[0]
        for group in range(3):
            copies = copies + relays(kind, p, group)
        for copy in copies:
            copy.wait_send()

    state = {"begun": 0, "query": False, "out": False}

    def ready(kind, p):
        end = sum(pieces[kind][p])
        if kind == 1 or end <= fixed:
            return
        need = 1 if end <= fixed + size * part else 2
        for of in range(need):
            if not state[("query", "out")[of]]:
                state[("query", "out")[of]] = True
                fills[1 + of].wait()
                for hop in range(1, size):
                    ref = att_v.at[:, place(of, z)]
                    pltpu.make_async_copy(ref, ref, z_recv.at[of, hop - 1]).wait()
                if of == 1:
                    cot_start()

    def weight_load(p):
        cols = pl.ds(*pieces[0][p])
        return pltpu.make_async_copy(att_all.at[:, cols], w_v.at[:, cols], w_sem.at[p])

    def take(first, last):
        for p in range(first, last):
            settle(0, p)
            weight_load(p).start()

    def held(first, last):
        for p in range(first, last):
            weight_load(p).wait()

    saves = []

    def save(src, dst):
        copy = pltpu.make_async_copy(src, dst, save_sem.at[len(saves)])
        copy.start()
        saves.append(copy)

    part_rows = max(16, chunk // 4)

    def norm(value_of, row, dst):
        gain = gain_out[row : row + 1, :]

        def some(r, carry):
            at_r = pl.ds(pl.multiple_of(r * part_rows, part_rows), part_rows)
            value = value_of(at_r)
            inverse = lax.rsqrt(jnp.mean(value * value, axis=-1, keepdims=True) + EPSILON)
            dst[at_r, :] = (value * inverse * gain).astype(bf16)
            return carry

        lax.fori_loop(0, chunk // part_rows, some, 0)

    def turned(value):
        return value * turn_ref[0] + pltpu.roll(value, HEAD_DIM // 2, 1) * turn_ref[1]

    lead_w = fixed - 2 * KV_HEADS * HEAD_DIM
    kv_w = KV_HEADS * HEAD_DIM
    heads = size * part // HEAD_DIM
    scale = HEAD_DIM ** (-0.5)

    def kv_copy(hop):
        return pltpu.make_async_remote_copy(
            src_ref=kv_v.at[2], dst_ref=kv_v.at[2 - hop], send_sem=kv_send.at[hop - 1],
            recv_sem=kv_recv.at[hop - 1], device_id={"tensor": z + hop}, device_id_type=MESH,
        )

    def keys():
        pick = (
            lax.broadcasted_iota(jnp.int32, (8, lead_w), 0)
            == lax.broadcasted_iota(jnp.int32, (8, lead_w), 1)
        ).astype(bf16)
        gain_out[...] = lax.dot_general(
            pick, w_v[:, :lead_w], (((1,), (1,)), ((), ())), preferred_element_type=f32
        )
        norm(lambda at_r: x_ref[at_r, :].astype(f32), 0, one_v)
        save(one_v, one_out)
        lin = jnp.dot(one_v[...], w_v[:, lead_w:fixed], preferred_element_type=f32) + bias_ref[0:1, :]
        for g in range(KV_HEADS):
            cols = slice(g * HEAD_DIM, (g + 1) * HEAD_DIM)
            kv_v[2, :, cols] = turned(lin[:, cols]).astype(bf16)
        kv_v[2, :, kv_w:] = lin[:, kv_w:].astype(bf16)
        for hop in (1, 2):

            @pl.when(z + hop < size)
            def _(hop=hop):
                kv_copy(hop).start()

            @pl.when(z < hop)
            def _(hop=hop):
                kv_v[2 - hop] = jnp.zeros(kv_v.shape[1:], bf16)

    def queries():
        def pair(h, carry):
            cols = pl.ds(pl.multiple_of(h * 2 * HEAD_DIM, 128), 2 * HEAD_DIM)
            from_w = pl.ds(pl.multiple_of(fixed + h * 2 * HEAD_DIM, 128), 2 * HEAD_DIM)
            lin = jnp.dot(one_v[...], w_v[:, from_w], preferred_element_type=f32)
            lin += att_v[pl.ds(rows, 16), from_w][0:1, :].astype(f32)
            for k in range(2):
                out_cols = pl.ds(pl.multiple_of(h * 2 * HEAD_DIM + k * HEAD_DIM, 128), HEAD_DIM)
                q_v[:, out_cols] = turned(lin[:, k * HEAD_DIM : (k + 1) * HEAD_DIM]).astype(bf16)
            return carry

        lax.fori_loop(0, heads // 2, pair, 0)
        save(q_v, query_rot)

    def kv_wait():
        for hop in (1, 2):

            @pl.when(z >= hop)
            def _(hop=hop):
                pltpu.make_async_copy(kv_v.at[2 - hop], kv_v.at[2 - hop], kv_recv.at[hop - 1]).wait()

        save(kv_v, kv_win)

    def attend(first, last):
        def head(h, carry):
            cols = pl.ds(pl.multiple_of(h * HEAD_DIM, 128), HEAD_DIM)
            group = h // (heads // KV_HEADS)
            key_cols = pl.ds(pl.multiple_of(group * HEAD_DIM, 128), HEAD_DIM)
            value_cols = pl.ds(pl.multiple_of(kv_w + group * HEAD_DIM, 128), HEAD_DIM)
            key = kv_v[:, :, key_cols].reshape(3 * chunk, HEAD_DIM)
            value = kv_v[:, :, value_cols].reshape(3 * chunk, HEAD_DIM)
            scores = lax.dot_general(
                q_v[:, cols], key, (((1,), (1,)), ((), ())), preferred_element_type=f32
            )
            scores = scores * scale + mask_ref[...]
            largest = jnp.max(scores, axis=-1, keepdims=True)
            powers = jnp.exp(scores - largest)
            mass = jnp.sum(powers, axis=-1, keepdims=True)
            lse_out[h] = largest + jnp.log(mass)
            probs = (powers * (1.0 / mass)).astype(bf16)
            ctx_v[:, cols] = jnp.dot(probs, value, preferred_element_type=f32).astype(bf16)
            return carry

        lax.fori_loop(first, last, head, 0)

    def project():
        save(ctx_v, ctx_out)
        tile = min(512, w_v.shape[0])

        def some(n, carry):
            at_n = pl.ds(pl.multiple_of(n * tile, tile), tile)
            added = lax.dot_general(
                ctx_v[...], w_v[at_n, fixed + size * part :], (((1,), (1,)), ((), ())),
                preferred_element_type=f32,
            )
            mid_v[:, at_n] = x_ref[:, at_n].astype(f32) + added
            return carry

        lax.fori_loop(0, w_v.shape[0] // tile, some, 0)
        save(mid_v, mid_out)
        norm(lambda at_r: mid_v[at_r, :], 1, two_v)
        save(two_v, two_all.at[at, :])
        two_start()

    n_att = len(pieces[0])
    n_qkv = 1 + (n_att - 1) // 2
    third = heads // 3 + (heads % 3 > 0)
    last_q = order.index((0, n_qkv - 1))
    last_out = order.index((0, n_att - 1))
    work = [
        (last_q - 1, lambda: cot_step(1)),
        (last_q + 1, lambda: cot_step(2)),
        (last_q + 1, lambda: take(0, n_qkv)),
        (last_q + 2, lambda: held(0, n_qkv)),
        (last_q + 2, keys),
        (last_q + 2, queries),
        (last_q + 3, kv_wait),
        (last_q + 3, lambda: attend(0, third)),
        (last_out + 1, lambda: take(n_qkv, n_att)),
        (last_out + 1, lambda: attend(third, 2 * third)),
        (last_out + 2, lambda: cot_step(3)),
        (last_out + 2, lambda: attend(2 * third, heads)),
        (last_out + 3, lambda: held(n_qkv, n_att)),
        (last_out + 3, project),
        (last_out + 5, lambda: two_step(1)),
        (last_out + 20, lambda: two_step(2)),
    ]
    total = len(order)
    for i in range(total + 1):
        while state["begun"] < min(total, i + (lead if i <= last_q else 2 * lead)):
            ready(*order[state["begun"]])
            begin(*order[state["begun"]])
            state["begun"] += 1
        if i < total:
            pass_on(*order[i])
        if i > 0:
            close(*order[i - 1])
        while work and (work[0][0] <= i or i == total):
            work.pop(0)[1]()
    for kind, p in order:
        if kind == 1:
            settle(kind, p)
    for kind, p in order:
        finish(kind, p)
    for copy in saves:
        copy.wait()
    for hop in (1, 2):

        @pl.when(z + hop < size)
        def _(hop=hop):
            kv_copy(hop).wait_send()

    for of in range(2):
        for hop in range(1, size):
            z_copy(of, hop).wait_send()
    for j in range(size):
        for dz, there in ((-1, has_low), (1, has_high)):
            came = jnp.logical_and((z <= j) if dz == -1 else (z >= j), there)

            @pl.when(came)
            def _(j=j, dz=dz):
                cot_copy(j, dz).wait_send()

            near = jnp.logical_and(came, (j - z <= 1) if dz == -1 else (z - j <= 1))

            @pl.when(near)
            def _(j=j, dz=dz):
                two_copy(j, dz, False).wait_send()


def front(
    tokens, turn, mask, kv_bias, query, out, fixed, ffn_w, cot, att_tile=512, ffn_tile=768,
    collective_id=2, limit=60_000_000,
):
    tall, part = query.shape
    rows, fixed_w = fixed.shape
    chunk, width = tokens.shape
    size, ways = 4, 8
    query_w = size * part
    att_cols = fixed_w + 2 * query_w
    pieces = (
        [(0, fixed_w)] + [(fixed_w + p * att_tile, att_tile) for p in range(2 * query_w // att_tile)],
        [(p * ffn_tile, ffn_tile) for p in range(ffn_w.shape[1] // ffn_tile)],
    )
    n_att, n_ffn = len(pieces[0]), len(pieces[1])
    early = min(2, n_ffn)
    order = [(0, 0)] + [(1, p) for p in range(early)] + [(0, p) for p in range(1, n_att)]
    order += [(1, p) for p in range(early, n_ffn)]
    bf16, f32 = jnp.bfloat16, jnp.float32
    hbm = pl.BlockSpec(memory_space=pl.ANY)
    vmem = pl.BlockSpec(memory_space=pltpu.VMEM)
    vm = pltpu.VMEM
    dma = pltpu.SemaphoreType.DMA
    shape = lambda *s: jax.ShapeDtypeStruct(s, bf16)
    wide = lambda *s: jax.ShapeDtypeStruct(s, f32)
    slots = n_att + n_ffn
    kv_w = 2 * KV_HEADS * HEAD_DIM
    heads = query_w // HEAD_DIM
    return pl.pallas_call(
        functools.partial(front_body, pieces=pieces, order=order, lead=3),
        out_shape=(
            shape(8 * rows, att_cols), shape(8 * rows, ffn_w.shape[1]),
            shape(size * cot.shape[0], cot.shape[1]),
            shape(size * chunk, width), wide(chunk, width), shape(chunk, width), shape(chunk, query_w),
            shape(3, chunk, kv_w), wide(heads, chunk, 1), shape(chunk, query_w), wide(8, width),
        ),
        in_specs=[vmem] * 9,
        out_specs=(hbm,) * 8 + (vmem, hbm, vmem),
        scratch_shapes=[
            vm((tall, att_cols), bf16), vm((8 * rows, att_cols), bf16), vm((chunk, width), bf16),
            vm((chunk, query_w), bf16), vm((3, chunk, kv_w), bf16), vm((chunk, query_w), bf16),
            vm((chunk, width), f32), vm((chunk, width), bf16),
            dma((4,)), dma((2, size - 1)), dma((2, size - 1)),
            dma((2, size)), dma((size,)), dma((ways, slots)), dma((ways, slots)), dma((slots,)),
            dma((n_att,)), dma((2,)), dma((2,)), dma((6,)), dma((2, size)), dma((size,)),
        ],
        compiler_params=pltpu.CompilerParams(
            collective_id=collective_id, has_side_effects=True, vmem_limit_bytes=limit
        ),
        cost_estimate=pl.CostEstimate(
            flops=2 * chunk * width * att_cols, bytes_accessed=20 * rows * (att_cols + ffn_w.shape[1]),
            transcendentals=0,
        ),
        name="front",
    )(tokens, turn, mask, kv_bias, query, out, fixed, ffn_w, cot)


def line_order(z, s):
    upper = z // 2
    near = z * (1 - upper) + (3 - z) * upper
    late = s // 2
    at = (1 - late) * (2 + s) + late * ((3 - s) * (1 - near) + (s - 2) * near)
    return at * (1 - upper) + (3 - at) * upper


def ffn_body(
    two_ref, cot_ref, weights_ref,
    rows_out, hid_out, dg_out, du_out, sum_out, dn_out,
    rows_v, cot_v, gate_v, up_v, down_v, hid_v, dg_v, du_v, part, land, below, above, res_v,
    tile_sem, load_sem, row_sem, ag_send, ag_recv, rs_send, rs_recv, own_recv, out_sem,
    *, axis, ft, nt,
):
    f32, bf16 = jnp.float32, jnp.bfloat16
    size = 4
    rows, width = two_ref.shape[0] // size, two_ref.shape[1]
    units = weights_ref.shape[1] // 3
    n_f, n_n = units // ft, width // nt
    z = lax.axis_index(axis)
    has_low, has_high = z > 0, z < size - 1

    def to(dz):
        return {axis: z + dz}

    barrier = pltpu.get_barrier_semaphore()

    @pl.when(has_low)
    def _():
        pl.semaphore_signal(barrier, inc=1, device_id=to(-1), device_id_type=MESH)

    @pl.when(has_high)
    def _():
        pl.semaphore_signal(barrier, inc=1, device_id=to(1), device_id_type=MESH)

    def chunk_rows(j):
        return two_ref.at[pl.ds(pl.multiple_of(j * rows, rows), rows), :]

    def far(j):
        return jnp.logical_or(j - z == 3, z - j == 3)

    def row_load(j):
        return pltpu.make_async_copy(chunk_rows(j), rows_v.at[j], row_sem.at[j])

    def load_rows(s):
        j = line_order(z, s)

        @pl.when(jnp.logical_not(far(j)))
        def _():
            row_load(j).start()

    load_rows(0)

    def tile_loads(f):
        cols = pl.ds(pl.multiple_of(f * ft, 128), ft)
        return [
            pltpu.make_async_copy(
                weights_ref.at[:, pl.ds(pl.multiple_of(k * units + f * ft, 128), ft)],
                dst.at[:, cols], tile_sem.at[k, f],
            )
            for k, dst in enumerate((gate_v, up_v, down_v))
        ]

    cot_load = pltpu.make_async_copy(cot_ref, cot_v, load_sem.at[1])
    for f in range(n_f):
        for copy in tile_loads(f):
            copy.start()
        if f == 0:
            cot_load.start()
            for s in range(1, size):
                load_rows(s)

    pl.semaphore_wait(barrier, (z + size - 1) // size + (2 * size - 2 - z) // size)

    def far_copy():
        j = 3 - 3 * (z // 2)
        return pltpu.make_async_remote_copy(
            src_ref=chunk_rows(j), dst_ref=rows_v.at[j], send_sem=ag_send.at[0], recv_sem=ag_recv.at[0],
            device_id=to(2 * (z // 2) - 1), device_id_type=MESH,
        )

    middle = jnp.logical_and(has_low, has_high)

    @pl.when(middle)
    def _():
        far_copy().start()

    def rs_copy(j, n, dz, own):
        way = (dz + 1) // 2
        if own:
            dst = below.at[n] if dz == 1 else above.at[n]
            sem = own_recv.at[1 - way, n]
        else:
            dst, sem = land.at[j, n], rs_recv.at[j, n]
        return pltpu.make_async_remote_copy(
            src_ref=part.at[j, n], dst_ref=dst, send_sem=rs_send.at[j, n],
            recv_sem=sem, device_id=to(dz), device_id_type=MESH,
        )

    def pass_on(j, n, what):
        for dz in (1, -1):
            for own in (True, False):
                hop = j == z + dz
                going = (j > z) if dz == 1 else (j < z)
                near = hop if own else jnp.logical_not(hop)

                @pl.when(jnp.logical_and(going, near))
                def _(dz=dz, own=own):
                    copy = rs_copy(j, n, dz, own)
                    copy.start() if what == "start" else copy.wait_send()

    def out_copies(j):
        at = pl.ds(pl.multiple_of(j * rows, rows), rows)
        return [
            pltpu.make_async_copy(src.at[j], dst.at[at, :], out_sem.at[k, j])
            for k, (src, dst) in enumerate(
                ((rows_v, rows_out), (hid_v, hid_out), (dg_v, dg_out), (du_v, du_out))
            )
        ]

    def forward(j, n):
        pltpu.make_async_copy(land.at[j, n], land.at[j, n], rs_recv.at[j, n]).wait()
        part[j, n] = (part[j, n].astype(f32) + land[j, n].astype(f32)).astype(bf16)
        pass_on(j, n, "start")

    def forward_all(j):
        def some(n, carry):
            forward(j, n)
            return carry

        lax.fori_loop(0, n_n, some, 0)

    def step(s, carry):
        j = line_order(z, s)

        @pl.when(far(j))
        def _():
            pltpu.make_async_copy(rows_v.at[j], rows_v.at[j], ag_recv.at[0]).wait()

        @pl.when(jnp.logical_not(far(j)))
        def _():
            row_load(j).wait()

        at = pl.ds(pl.multiple_of(j * rows, rows), rows)

        @pl.when(s == 0)
        def _():
            cot_load.wait()

        def units_tile(f, carry):
            @pl.when(s == 0)
            def _():
                for copy in tile_loads(f):
                    copy.wait()

            cols = pl.ds(pl.multiple_of(f * ft, 128), ft)
            mine = rows_v[j]
            gate = jnp.dot(mine, gate_v[:, cols], preferred_element_type=f32)
            upper = jnp.dot(mine, up_v[:, cols], preferred_element_type=f32)
            d_hidden = jnp.dot(cot_v[at, :], down_v[:, cols], preferred_element_type=f32)
            sig = 1.0 / (1.0 + jnp.exp(-gate))
            act = gate * sig
            hid_v[j, :, cols] = (act * upper).astype(bf16)
            du_v[j, :, cols] = (d_hidden * act).astype(bf16)
            dg_v[j, :, cols] = (d_hidden * upper * (sig + act * (1.0 - sig))).astype(bf16)
            return carry

        lax.fori_loop(0, n_f, units_tile, 0)
        for copy in out_copies(j):
            copy.start()
        ends = jnp.logical_and(s < 3, jnp.logical_not(middle))

        @pl.when(jnp.logical_and(middle, s == 3))
        def _():
            forward_all(3 - z)
            forward_all(3 - 3 * (z // 2))


        def width_tile(n, carry):
            at_n = pl.ds(pl.multiple_of(n * nt, nt), nt)
            dims = (((1,), (1,)), ((), ()))
            total = lax.dot_general(dg_v[j], gate_v[at_n, :], dims, preferred_element_type=f32)
            total += lax.dot_general(du_v[j], up_v[at_n, :], dims, preferred_element_type=f32)
            part[j, n] = total.astype(bf16)

            @pl.when(ends)
            def _():
                pass_on(j, n, "start")

            return carry

        lax.fori_loop(0, n_n, width_tile, 0)
        return carry

    lax.fori_loop(0, size, step, 0)

    def down_tile(i, carry):
        j, n = i // n_n, i % n_n
        at_n = pl.ds(pl.multiple_of(n * nt, nt), nt)
        total = lax.dot_general(
            hid_v[j], down_v[at_n, :], (((1,), (1,)), ((), ())), preferred_element_type=f32
        )
        res_v[j, :, at_n] = total.astype(bf16)
        return carry

    tiles = size * n_n
    done = tiles // 3
    lax.fori_loop(0, done, down_tile, 0)
    for n in range(n_n):
        until = tiles if n == n_n - 1 else done + (n + 1) * (tiles - done) // n_n

        @pl.when(middle)
        def _(n=n):
            forward(3 * (z // 2), n)

        lax.fori_loop(done + n * (tiles - done) // n_n, until, down_tile, 0)
    sum_copies = [
        pltpu.make_async_copy(
            res_v.at[j], sum_out.at[pl.ds(j * rows, rows), :], load_sem.at[2 + j]
        )
        for j in range(size)
    ]
    for copy in sum_copies:
        copy.start()

    def last(n, carry):
        @pl.when(has_low)
        def _():
            pltpu.make_async_copy(below.at[n], below.at[n], own_recv.at[0, n]).wait()
            part[z, n] = (part[z, n].astype(f32) + below[n].astype(f32)).astype(bf16)

        @pl.when(has_high)
        def _():
            pltpu.make_async_copy(above.at[n], above.at[n], own_recv.at[1, n]).wait()
            part[z, n] = (part[z, n].astype(f32) + above[n].astype(f32)).astype(bf16)

        dn_out[:, pl.ds(pl.multiple_of(n * nt, nt), nt)] = part[z, n]
        return carry

    lax.fori_loop(0, n_n, last, 0)

    def drain(j, carry):
        for copy in out_copies(j):
            copy.wait()
        def sent(n, carry):
            @pl.when(j != z)
            def _():
                pltpu.make_async_copy(part.at[j, n], part.at[j, n], rs_send.at[j, n]).wait()

            return carry

        lax.fori_loop(0, n_n, sent, 0)
        return carry

    lax.fori_loop(0, size, drain, 0)

    @pl.when(middle)
    def _():
        far_copy().wait_send()

    for copy in sum_copies:
        copy.wait()


def ffn(two, cot_rows, weights, axis="tensor", ft=768, nt=512, collective_id=1, limit=66_000_000):
    size = 4
    length, width = two.shape
    rows = length // size
    units = weights.shape[1] // 3
    n_f, n_n = units // ft, width // nt
    bf16 = jnp.bfloat16
    hbm = pl.BlockSpec(memory_space=pl.ANY)
    vm = pltpu.VMEM
    dma = pltpu.SemaphoreType.DMA
    shape = lambda *s: jax.ShapeDtypeStruct(s, bf16)
    return pl.pallas_call(
        functools.partial(ffn_body, axis=axis, ft=ft, nt=nt),
        out_shape=(
            shape(length, width), shape(length, units), shape(length, units), shape(length, units),
            shape(length, width), shape(rows, width),
        ),
        in_specs=[hbm] * 3,
        out_specs=(hbm,) * 5 + (pl.BlockSpec(memory_space=pltpu.VMEM),),
        scratch_shapes=[
            vm((size, rows, width), bf16), vm((length, width), bf16),
            vm((width, units), bf16), vm((width, units), bf16), vm((width, units), bf16),
            vm((size, rows, units), bf16), vm((size, rows, units), bf16), vm((size, rows, units), bf16),
            vm((size, n_n, rows, nt), bf16), vm((size, n_n, rows, nt), bf16),
            vm((n_n, rows, nt), bf16), vm((n_n, rows, nt), bf16),
            vm((size, rows, width), bf16),
            dma((3, n_f)), dma((2 + size,)), dma((size,)), dma((1,)), dma((1,)), dma((size, n_n)), dma((size, n_n)),
            dma((2, n_n)), dma((4, size)),
        ],
        compiler_params=pltpu.CompilerParams(
            collective_id=collective_id, has_side_effects=True, vmem_limit_bytes=limit
        ),
        cost_estimate=pl.CostEstimate(
            flops=12 * length * width * units, bytes_accessed=8 * width * units + 8 * length * units,
            transcendentals=length * units,
        ),
        name="ffn",
    )(two, cot_rows, weights)


def back_body(
    two_ref, cot_ref, hid_ref, dg_ref, du_ref, part_ref, up_ref, x_ref, mid_ref, gain_ref, att_ref,
    query_ref, win_ref, lse_ref, ctx_ref, one_ref, mask_ref, turn_ref,
    ffn_out, query_out, out_out, kv_out, mixed_out, input_out, small_out,
    up_v, own_v, x_v, mid_v, gain_v, w_v, query_v, win_v, lse_v, mask_v, turn_v, lhs_ref, rhs_ref,
    d_mid, d_ctx, d_win, kv_give, kv_take, d_one, small_ref,
    left_v, right_v, grad, mate_land, core_sum, x_land, y_land, second, x_last, y_last, stage, fin,
    z_land, kv_land, sum_land, small_z, small_hop, small_next, in_sem, give_send, give_recv,
    left_sem, right_sem, mate_send, mate_recv, one_send, one_recv, two_send, two_recv, stage_sem,
    z_send, z_recv, kv_send, kv_recv, sum_send, sum_recv, own_sem, small_send, small_recv,
    hop_send, hop_recv, *, n_f, wide,
):
    f32, bf16 = jnp.float32, jnp.bfloat16
    d, z = lax.axis_index("dp"), lax.axis_index("tensor")
    size = 4
    core, x, y = d % 2, (d // 2) % 2, d // 4
    by_x, by_y, mate, _ = square(d)
    here, at_x, at_y = 2 * y + x, 2 * y + 1 - x, 2 * (1 - y) + x
    cross = 3 - here
    block, half = core_sum.shape[2], core_sum.shape[2] // 2
    n_ffn, n_att = 3 * n_f, rhs_ref.shape[1] // wide
    ring, n_sum, n_last = x_land.shape[0], core_sum.shape[0], x_last.shape[0]
    total = n_ffn + n_att
    chunk, width = mixed_out.shape
    share = block // size
    part_w = wide // 2

    barrier = pltpu.get_barrier_semaphore()
    for peer in (by_x, by_y, mate):
        pl.semaphore_signal(barrier, inc=1, device_id={"dp": peer}, device_id_type=MESH)
    for hop in range(1, size):
        pl.semaphore_signal(
            barrier, inc=1, device_id={"tensor": (z + hop) % size}, device_id_type=MESH
        )

    lefts = [
        pltpu.make_async_copy(ref, left_v, left_sem.at[k]) for k, ref in enumerate((cot_ref, two_ref))
    ]
    query_w = query_ref.shape[1]
    kv_w = KV_HEADS * HEAD_DIM
    heads = query_w // HEAD_DIM
    scale = HEAD_DIM ** (-0.5)
    ahead = att_ref.shape[1] - 2 * query_w - 2 * kv_w
    own_rows = pl.ds(pl.multiple_of(z * chunk, chunk), chunk)
    ctx_cols = pl.ds(query_w, query_w)
    plan = (
        (up_ref, up_v), (cot_ref.at[own_rows, :], own_v), (mid_ref, mid_v), (gain_ref, gain_v),
        (att_ref.at[:, pl.ds(ahead + 2 * kv_w + query_w, query_w)], w_v.at[:, pl.ds(0, query_w)]),
        (query_ref, query_v), (win_ref, win_v), (lse_ref, lse_v), (mask_ref, mask_v), (turn_ref, turn_v),
        (ctx_ref, rhs_ref.at[:, ctx_cols]), (x_ref, x_v), (one_ref, lhs_ref.at[0]),
        (att_ref.at[:, pl.ds(ahead, 2 * kv_w + query_w)], w_v),
    )
    loads = [pltpu.make_async_copy(src, dst, in_sem.at[k]) for k, (src, dst) in enumerate(plan)]

    def right_load(i, what):
        cols = pl.ds(pl.multiple_of((i % n_f) * wide, 128), wide)
        for m, ref in enumerate((hid_ref, dg_ref, du_ref)):
            copy = pltpu.make_async_copy(ref.at[:, cols], right_v.at[i % 2], right_sem.at[i % 2])

            @pl.when(i // n_f == m)
            def _(copy=copy):
                copy.start() if what == "start" else copy.wait()

    lefts[0].start()
    right_load(jnp.int32(0), "start")
    for copy in loads[:-1]:
        copy.start()

    def chunk_rows(j):
        return part_ref.at[pl.ds(pl.multiple_of(j * chunk, chunk), chunk), :]

    own_part = pltpu.make_async_copy(chunk_rows(z), sum_land.at[size - 1], own_sem.at[0])
    own_part.start()
    pl.semaphore_wait(barrier, 3 + size - 1)

    def dp_copy(src, dst, send_sem, recv_sem, peer):
        return pltpu.make_async_remote_copy(
            src_ref=src, dst_ref=dst, send_sem=send_sem, recv_sem=recv_sem,
            device_id={"dp": peer}, device_id_type=MESH,
        )

    def z_copy(src, dst, send_sem, recv_sem, peer):
        return pltpu.make_async_remote_copy(
            src_ref=src, dst_ref=dst, send_sem=send_sem, recv_sem=recv_sem,
            device_id={"tensor": peer}, device_id_type=MESH,
        )

    small_copies, sum_copies = [], []
    for hop in range(1, size):
        to, k = (z + hop) % size, hop - 1
        small_copies.append(
            z_copy(small_ref, small_z.at[k], small_send.at[k], small_recv.at[k], to)
        )
        sum_copies.append(
            z_copy(chunk_rows(to), sum_land.at[k], sum_send.at[k], sum_recv.at[k], to)
        )
    for copy in sum_copies:
        copy.start()
    rhs_ref[:, 2 * query_w + 2 * kv_w :] = jnp.zeros((chunk, rhs_ref.shape[1] - 2 * query_w - 2 * kv_w), bf16)

    hops = (mate, by_x, by_y)

    def hop_copy(k):
        return dp_copy(small_next.at[k], small_hop.at[k], hop_send.at[k], hop_recv.at[k], hops[k])

    def mate_copy(i):
        return dp_copy(
            grad.at[i % 2, :, 1 - core], mate_land.at[i % 4], mate_send.at[i % 4],
            mate_recv.at[i % 4], mate,
        )

    def one_copies(i):
        s = core_sum.at[i % n_sum]
        first, last = pl.ds(0, half), pl.ds(half, half)
        plan = (
            (s.at[at_x, first, :], x_land.at[i % ring, 0], by_x), (s.at[cross, first, :], x_land.at[i % ring, 1], by_x),
            (s.at[at_y, last, :], y_land.at[i % ring, 0], by_y), (s.at[cross, last, :], y_land.at[i % ring, 1], by_y),
        )
        return [
            dp_copy(src, dst, one_send.at[k, i % ring], one_recv.at[k, i % ring], peer)
            for k, (src, dst, peer) in enumerate(plan)
        ]

    def two_copies(i):
        return [
            dp_copy(second.at[i % 4, 0], y_last.at[i % n_last], two_send.at[0, i % ring], two_recv.at[0, i % ring], by_y),
            dp_copy(second.at[i % 4, 1], x_last.at[i % n_last], two_send.at[1, i % ring], two_recv.at[1, i % ring], by_x),
        ]

    def stage_copy(i):
        cols = pl.ds(pl.multiple_of(i * wide, 128), wide)
        return pltpu.make_async_copy(stage.at[i % 2], ffn_out.at[:, cols], stage_sem.at[i % 2])

    def multiply(i):
        @pl.when(jnp.logical_and(i >= 2, i < total))
        def _():
            mate_copy(i - 2).wait_send()

        @pl.when(i + 1 < n_ffn)
        def _():
            right_load(i + 1, "start")

        dims = (((0,), (0,)), ((), ()))

        @pl.when(i < n_ffn)
        def _():
            @pl.when(i == 0)
            def _():
                lefts[0].wait()

            @pl.when(i == n_f)
            def _():
                lefts[1].start()
                lefts[1].wait()

            right_load(i, "wait")

            def rows(k, carry):
                at = pl.ds(pl.multiple_of(k * 2 * block, 128), 2 * block)
                value = lax.dot_general(
                    left_v[:, at], right_v[i % 2], dims, preferred_element_type=f32
                )
                grad[i % 2, k] = value.astype(bf16).reshape(2, block, wide)
                return carry

            lax.fori_loop(0, 4, rows, 0)

        @pl.when(jnp.logical_and(i >= n_ffn, i < total))
        def _():
            a = i - n_ffn
            cols = pl.ds(pl.multiple_of(a * wide, 128), wide)

            def rows(k, carry):
                at = pl.ds(pl.multiple_of(k * 2 * block, 128), 2 * block)
                value = lax.dot_general(
                    lhs_ref[(a // 2) % 2, :, at], rhs_ref[:, cols], dims, preferred_element_type=f32
                )
                grad[i % 2, k] = value.astype(bf16).reshape(2, block, wide)
                return carry

            lax.fori_loop(0, 4, rows, 0)

        @pl.when(i < total)
        def _():
            mate_copy(i).start()

    def sum_cores(i):
        mate_copy(i).wait_recv()
        for k in range(4):
            core_sum[i % n_sum, k] = (
                grad[i % 2, k, core].astype(f32) + mate_land[i % 4, k].astype(f32)
            ).astype(bf16)
        for copy in one_copies(i):
            copy.start()

    def sum_near(i):
        for copy in one_copies(i):
            copy.wait_recv()
        s = core_sum.at[i % n_sum]
        second[i % 4, 0] = (s[at_y, :half].astype(f32) + x_land[i % ring, 1].astype(f32)).astype(bf16)
        second[i % 4, 1] = (s[at_x, half:].astype(f32) + y_land[i % ring, 1].astype(f32)).astype(bf16)
        for copy in two_copies(i):
            copy.start()

    def z_sends(a, what):
        for h in range(2):
            owner = (a % 2) * 2 + h
            hop = (owner - z + size) % size
            src = fin.at[a, :, pl.ds(h * part_w, part_w)]

            @pl.when(jnp.logical_and(a < 4, hop > 0))
            def _(src=src, owner=owner, hop=hop, h=h):
                copy = z_copy(
                    src, z_land.at[a // 2, hop - 1], z_send.at[a, h], z_recv.at[a // 2, hop - 1], owner
                )
                copy.start() if what == "start" else copy.wait_send()

        @pl.when(a == 4)
        def _():
            for hop in range(1, size):
                to = (z + hop) % size
                rows = pl.ds(pl.multiple_of(to * share, 16), share)
                copy = z_copy(
                    fin.at[4, rows, :], kv_land.at[hop - 1], kv_send.at[hop - 1], kv_recv.at[hop - 1], to
                )
                copy.start() if what == "start" else copy.wait_send()

    def finish(i):
        for copy in two_copies(i):
            copy.wait_recv()
        own = core_sum.at[i % n_sum, here]
        top = own[:half].astype(f32) + x_land[i % ring, 0].astype(f32) + y_last[i % n_last].astype(f32)
        low = own[half:].astype(f32) + y_land[i % ring, 0].astype(f32) + x_last[i % n_last].astype(f32)

        @pl.when(i < n_ffn)
        def _():
            @pl.when(i >= 2)
            def _():
                stage_copy(i - 2).wait()

            stage[i % 2, :half] = top
            stage[i % 2, half:] = low
            stage_copy(i).start()

        @pl.when(i >= n_ffn)
        def _():
            a = i - n_ffn
            fin[a, :half] = top.astype(bf16)
            fin[a, half:] = low.astype(bf16)
            z_sends(a, "start")

        for copy in one_copies(i) + two_copies(i):
            copy.wait_send()

    def back_norm(upstream, value, gain, base, col):
        inverse = lax.rsqrt(jnp.mean(value * value, axis=-1, keepdims=True) + EPSILON)
        unit = value * inverse
        scaled = upstream * gain
        term = jnp.sum(upstream * unit, axis=0, keepdims=True)
        small_ref[:, pl.ds(col, width)] += jnp.broadcast_to(term, (8, width))
        return base + inverse * (scaled - unit * jnp.mean(scaled * unit, axis=-1, keepdims=True))

    some_rows = max(16, chunk // 4)

    def by_rows(work):
        def some(r, carry):
            work(pl.ds(pl.multiple_of(r * some_rows, some_rows), some_rows))
            return carry

        lax.fori_loop(0, chunk // some_rows, some, 0)

    gain_one_at, gain_two_at = query_w + 2 * kv_w, query_w + 2 * kv_w + width

    def open_branch():
        for k in (0, 1, 2, 3):
            loads[k].wait()
        small_ref[...] = jnp.zeros_like(small_ref)

        def work(at):
            value = back_norm(
                up_v[at, :].astype(f32), mid_v[at, :], gain_v[1:2, :], own_v[at, :].astype(f32), gain_two_at
            )
            d_mid[at, :] = value
            lhs_ref[1, at, :] = value.astype(bf16)

        by_rows(work)

    def context_grads():
        loads[4].wait()
        tile = min(512, query_w)

        def some(n, carry):
            cols = pl.ds(pl.multiple_of(n * tile, tile), tile)
            d_ctx[:, cols] = jnp.dot(lhs_ref[1], w_v[:, cols], preferred_element_type=f32).astype(bf16)
            return carry

        lax.fori_loop(0, query_w // tile, some, 0)
        loads[-1].start()
        for k in (5, 6, 7, 8, 9):
            loads[k].wait()
        d_win[...] = jnp.zeros_like(d_win)

    def turned_back(value):
        return value * turn_v[0] - pltpu.roll(value, HEAD_DIM // 2, 1) * turn_v[1]

    def attend_back(first, last):
        def head(h, carry):
            cols = pl.ds(pl.multiple_of(h * HEAD_DIM, 128), HEAD_DIM)
            group = h // (heads // KV_HEADS)
            key_cols = pl.ds(pl.multiple_of(group * HEAD_DIM, 128), HEAD_DIM)
            value_cols = pl.ds(pl.multiple_of(kv_w + group * HEAD_DIM, 128), HEAD_DIM)
            key = win_v[:, :, key_cols].reshape(3 * chunk, HEAD_DIM)
            value = win_v[:, :, value_cols].reshape(3 * chunk, HEAD_DIM)
            query, given = query_v[:, cols], d_ctx[:, cols]
            across, down = (((1,), (1,)), ((), ())), (((0,), (0,)), ((), ()))
            scores = lax.dot_general(query, key, across, preferred_element_type=f32)
            probs = jnp.exp(scores * scale + mask_v[...] - lse_v[h])
            d_probs = lax.dot_general(given, value, across, preferred_element_type=f32)
            delta = jnp.sum(probs * d_probs, axis=-1, keepdims=True)
            d_scores = (probs * (d_probs - delta)).astype(bf16)
            d_query = jnp.dot(d_scores, key, preferred_element_type=f32) * scale
            rhs_ref[:, cols] = turned_back(d_query).astype(bf16)
            d_key = lax.dot_general(d_scores, query, down, preferred_element_type=f32) * scale
            d_value = lax.dot_general(probs.astype(bf16), given, down, preferred_element_type=f32)
            d_win[:, :, key_cols] += d_key.reshape(3, chunk, HEAD_DIM)
            d_win[:, :, value_cols] += d_value.reshape(3, chunk, HEAD_DIM)
            return carry

        lax.fori_loop(first, last, head, 0)

    def give_copy(hop):
        return z_copy(
            kv_give.at[hop - 1], kv_take.at[hop - 1], give_send.at[hop - 1], give_recv.at[hop - 1], z - hop
        )

    def give():
        for hop in (1, 2):

            @pl.when(z >= hop)
            def _(hop=hop):
                kv_give[hop - 1] = d_win[2 - hop].astype(bf16)
                give_copy(hop).start()

    def take():
        for hop in (1, 2):

            @pl.when(z + hop < size)
            def _(hop=hop):
                pltpu.make_async_copy(kv_take.at[hop - 1], kv_take.at[hop - 1], give_recv.at[hop - 1]).wait()
                d_win[2] += kv_take[hop - 1].astype(f32)

        for g in range(KV_HEADS):
            cols = slice(g * HEAD_DIM, (g + 1) * HEAD_DIM)
            out_cols = slice(2 * query_w + g * HEAD_DIM, 2 * query_w + (g + 1) * HEAD_DIM)
            rhs_ref[:, out_cols] = turned_back(d_win[2, :, cols]).astype(bf16)
        rhs_ref[:, 2 * query_w + kv_w : 2 * query_w + 2 * kv_w] = d_win[2, :, kv_w:].astype(bf16)
        ones = jnp.ones((8, chunk), bf16)
        small_ref[:, :query_w] = jnp.dot(ones, rhs_ref[:, :query_w], preferred_element_type=f32)
        small_ref[:, query_w : query_w + 2 * kv_w] = jnp.dot(
            ones, rhs_ref[:, 2 * query_w : 2 * query_w + 2 * kv_w], preferred_element_type=f32
        )

    def one_grads():
        loads[-1].wait()
        tile = min(512, width)
        across = (((1,), (1,)), ((), ()))

        def some(n, carry):
            at_n = pl.ds(pl.multiple_of(n * tile, tile), tile)
            d_one[:, at_n] = lax.dot_general(
                rhs_ref[:, :query_w], w_v[at_n, 2 * kv_w :], across, preferred_element_type=f32
            ) + lax.dot_general(
                rhs_ref[:, 2 * query_w : 2 * query_w + 2 * kv_w], w_v[at_n, : 2 * kv_w], across,
                preferred_element_type=f32,
            )
            return carry

        lax.fori_loop(0, width // tile, some, 0)

    def close_branch():
        loads[11].wait()

        def work(at):
            input_out[at, :] = back_norm(
                d_one[at, :], x_v[at, :].astype(f32), gain_v[0:1, :], d_mid[at, :], gain_one_at
            ).astype(bf16)

        by_rows(work)
        for copy in small_copies:
            copy.start()

    def small_first():
        for copy in small_copies:
            copy.wait_recv()
        small_next[0] = small_ref[...] + small_z[0] + small_z[1] + small_z[2]
        hop_copy(0).start()

    def small_then(k):
        hop_copy(k).wait_recv()
        small_next[k + 1] = small_next[k] + small_hop[k]
        hop_copy(k + 1).start()

    def small_last():
        hop_copy(2).wait_recv()
        small_out[...] = small_next[2] + small_hop[2]

    span = n_ffn - 1
    quarter = heads // 4

    def at_turn(k):
        return min(k, span)

    steps = [
        (0, open_branch), (at_turn(1), context_grads),
        (at_turn(2), lambda: attend_back(0, quarter)),
        (at_turn(3), lambda: attend_back(quarter, 2 * quarter)),
        (at_turn(4), lambda: attend_back(2 * quarter, 3 * quarter)),
        (at_turn(5), lambda: attend_back(3 * quarter, heads)),
        (at_turn(5), give),
        (at_turn(7), take), (at_turn(7), lambda: [loads[k].wait() for k in (10, 12)]),
        (n_ffn + 1, one_grads), (n_ffn + 2, close_branch),
        (n_ffn + 4, small_first), (n_ffn + 5, lambda: small_then(0)), (n_ffn + 6, lambda: small_then(1)),
        (n_ffn + 7, small_last),
    ]

    def small_step(i):
        for when, step in steps:

            @pl.when(i == when)
            def _(step=step):
                step()

    def turn(i, carry):
        multiply(i)
        for lag, work in ((1, sum_cores), (3, sum_near), (5, finish)):

            @pl.when(jnp.logical_and(i >= lag, i - lag < total))
            def _(lag=lag, work=work):
                work(i - lag)

        small_step(i)
        return carry

    lax.fori_loop(0, total + 5, turn, 0)
    for i in (total - 2, total - 1):
        mate_copy(i).wait_send()
    for i in (n_ffn - 2, n_ffn - 1):
        stage_copy(i).wait()
    own_part.wait()
    for copy in sum_copies:
        copy.wait_recv()
    acc = sum_land[size - 1].astype(f32)
    for k in range(size - 1):
        acc += sum_land[k].astype(f32)
    mixed_out[...] = (mid_v[...] + acc).astype(bf16)
    for of, dst in ((0, query_out), (1, out_out)):
        for k in range(size - 1):
            ref = z_land.at[of, k]
            pltpu.make_async_copy(ref, ref, z_recv.at[of, k]).wait()
        for h in range(4):

            @pl.when(z == h)
            def _(of=of, dst=dst, h=h):
                acc = fin[2 * of + h // 2, :, (h % 2) * part_w : (h % 2 + 1) * part_w].astype(f32)
                for k in range(size - 1):
                    acc += z_land[of, k].astype(f32)
                dst[...] = acc

    for k in range(size - 1):
        pltpu.make_async_copy(kv_land.at[k], kv_land.at[k], kv_recv.at[k]).wait()
    rows = pl.ds(pl.multiple_of(z * share, 16), share)
    acc = fin[4, rows, :].astype(f32)
    for k in range(size - 1):
        acc += kv_land[k].astype(f32)
    kv_out[...] = acc
    for a in range(n_att):
        z_sends(a, "wait")
    for copy in sum_copies + small_copies:
        copy.wait_send()
    for k in range(3):
        hop_copy(k).wait_send()
    for hop in (1, 2):

        @pl.when(z >= hop)
        def _(hop=hop):
            give_copy(hop).wait_send()


def back(
    two, cot_rows, hid, dg, du, ffn_part, up, tokens, middle, gains, att_w, query_rot, kv_win, lse, context,
    normed_one, mask, turn, wide=768, collective_id=3, limit=67_000_000,
):
    length, width = two.shape
    size, chunk, block = 4, tokens.shape[0], width // 8
    units, query_w, kv_w = hid.shape[1], context.shape[1], kv_win.shape[2]
    n_f, n_att = units // wide, (2 * query_w + wide) // wide
    total = 3 * n_f + n_att
    half, part_w, share = block // 2, wide // 2, block // size
    heads = lse.shape[0]
    bf16, f32 = jnp.bfloat16, jnp.float32
    small = (8, query_w + kv_w + 2 * width)
    ring = 8
    hbm = pl.BlockSpec(memory_space=pl.ANY)
    vmem = pl.BlockSpec(memory_space=pltpu.VMEM)
    vm = pltpu.VMEM
    dma = pltpu.SemaphoreType.DMA
    shape = jax.ShapeDtypeStruct
    return pl.pallas_call(
        functools.partial(back_body, n_f=n_f, wide=wide),
        out_shape=(
            shape((block, 3 * units), f32), shape((block, part_w), f32), shape((block, part_w), f32),
            shape((share, wide), f32), shape((chunk, width), bf16), shape((chunk, width), bf16),
            shape(small, f32),
        ),
        in_specs=[hbm] * 18,
        out_specs=(hbm,) + (vmem,) * 6,
        scratch_shapes=[
            vm((chunk, width), bf16), vm((chunk, width), bf16), vm((chunk, width), bf16),
            vm((chunk, width), f32), vm(gains.shape, f32), vm((width, kv_w + query_w), bf16),
            vm((chunk, query_w), bf16), vm(kv_win.shape, bf16), vm((heads, chunk, 1), f32),
            vm(mask.shape, f32), vm(turn.shape, f32), vm((2, chunk, width), bf16),
            vm((chunk, 2 * query_w + wide), bf16), vm((chunk, width), f32), vm((chunk, query_w), bf16),
            vm(kv_win.shape, f32), vm((2, chunk, kv_w), bf16), vm((2, chunk, kv_w), bf16),
            vm((chunk, width), f32), vm(small, f32),
            vm((length, width), bf16), vm((2, length, wide), bf16), vm((2, 4, 2, block, wide), bf16),
            vm((4, 4, block, wide), bf16), vm((5, 4, block, wide), bf16),
            vm((ring, 2, half, wide), bf16), vm((ring, 2, half, wide), bf16),
            vm((4, 2, half, wide), bf16), vm((6, half, wide), bf16), vm((6, half, wide), bf16),
            vm((2, block, wide), f32), vm((n_att, block, wide), bf16),
            vm((2, size - 1, block, part_w), bf16), vm((size - 1, share, wide), bf16),
            vm((size, chunk, width), bf16), vm((3,) + small, f32), vm((3,) + small, f32),
            vm((3,) + small, f32), dma((14,)), dma((2,)), dma((2,)),
            dma((2,)), dma((2,)), dma((4,)), dma((4,)), dma((4, ring)), dma((4, ring)),
            dma((2, ring)), dma((2, ring)), dma((2,)),
            dma((4, 2)), dma((2, size - 1)), dma((size - 1,)), dma((size - 1,)), dma((size - 1,)),
            dma((size - 1,)), dma((1,)), dma((size - 1,)), dma((size - 1,)), dma((3,)), dma((3,)),
        ],
        compiler_params=pltpu.CompilerParams(
            collective_id=collective_id, has_side_effects=True, vmem_limit_bytes=limit
        ),
        cost_estimate=pl.CostEstimate(
            flops=6 * length * width * units, bytes_accessed=8 * length * units, transcendentals=0
        ),
        name="back",
    )(
        two, cot_rows, hid, dg, du, ffn_part, up, tokens, middle, gains, att_w, query_rot, kv_win, lse, context,
        normed_one, mask, turn,
    )


def angle_tables(first, length, head_width):
    position = (first + jnp.arange(length)).astype(jnp.float32)
    exponent = jnp.arange(head_width // 2, dtype=jnp.float32) * (2.0 / head_width)
    frequency = ROPE_BASE ** (-exponent)
    angle = position[:, None] * frequency[None, :]
    return (jnp.cos(angle), jnp.sin(angle))


def rotate(values, cosine, sine):
    half_width = values.shape[-1] // 2
    first_half = values[..., :half_width]
    second_half = values[..., half_width:]
    return jnp.concatenate(
        [first_half * cosine - second_half * sine, second_half * cosine + first_half * sine],
        axis=-1,
    )


def rotate_back(grads, cosine, sine):
    return rotate(grads, cosine, -sine)


def dot_f32(left, right, dims):
    return lax.dot_general(left, right, (dims, ((), ())), preferred_element_type=jnp.float32)


def contract_rows(left, right):
    return dot_f32(left, right, ((0,), (0,)))


def contract_cols(left, right):
    return dot_f32(left, right, ((1,), (1,)))


def norm_back(upstream, unit, inverse, gain):
    scaled = upstream * gain
    gain_term = jnp.sum(upstream * unit, axis=0)
    input_term = inverse * (scaled - unit * jnp.mean(scaled * unit, axis=-1, keepdims=True))
    return (gain_term, input_term)


def joined_units(gate_w, up_w, down_w):
    units = gate_w.shape[1]
    gap = -(-units // 768) * 768 - units
    wide = lambda w: jnp.pad(w, ((0, 0), (0, gap)))
    return jnp.concatenate([wide(gate_w), wide(up_w), wide(down_w)], axis=1)


def attention_branch(tokens, cosine, sine, mask, gains_w, query_w, query_b, kv_w, kv_b, out_w, ffn_w, cotangent):
    f32, bf16 = jnp.float32, jnp.bfloat16
    rows = tokens.shape[0]
    size = lax.axis_size("tensor")
    fixed_w = jnp.concatenate([gains_w, kv_w], axis=1)
    if lax.axis_size("dp") == 8 and size == 4:
        tall_query = jnp.concatenate([query_w, jnp.pad(query_b[None, :], ((0, 15), (0, 0)))], axis=0)
        tall_out = jnp.pad(out_w, ((0, 16), (0, 0)))
        turn = jnp.stack(
            [jnp.concatenate([cosine, cosine], axis=1), jnp.concatenate([-sine, sine], axis=1)]
        )
        att_w, ffn_all, cot_rows, two, middle, one, query_rot, kv_win, lse, context, gains = front(
            tokens, turn, mask, kv_b[None, :], tall_query, tall_out, fixed_w, ffn_w, cotangent
        )
        kv_win = kv_win.reshape(3 * rows, kv_w.shape[1])
        return att_w, ffn_all, cot_rows, two, middle, one, query_rot, kv_win, lse, context, gains
    pair = lax.all_gather(jnp.stack([query_w, out_w]), "tensor", axis=2, tiled=True)
    att_w = jnp.concatenate([fixed_w, pair[0], pair[1]], axis=1)
    att_w = lax.all_gather(att_w, "dp", axis=0, tiled=True)
    ffn_all = lax.all_gather(ffn_w, "dp", axis=0, tiled=True)
    cot_rows = lax.all_gather(cotangent, "tensor", axis=0, tiled=True)
    full_query_b = lax.all_gather(query_b, "tensor", axis=0, tiled=True).astype(f32)
    ahead = gains_w.shape[1]
    kv_width = kv_w.shape[1] // 2
    qkv_width = 2 * kv_width + full_query_b.shape[0]
    heads = full_query_b.shape[0] // HEAD_DIM
    gains = att_w[:, :2].T.astype(f32)
    inputs = tokens.astype(f32)
    inverse = lax.rsqrt(jnp.mean(inputs * inputs, axis=-1, keepdims=True) + EPSILON)
    one = (inputs * inverse * gains[0]).astype(bf16)
    lin = jnp.dot(one, att_w[:, ahead : ahead + qkv_width], preferred_element_type=f32)
    lin = lin + jnp.concatenate([kv_b, full_query_b])
    cos_h, sin_h = cosine[:, None, :], sine[:, None, :]
    query_rot = rotate(lin[:, 2 * kv_width :].reshape(rows, heads, HEAD_DIM), cos_h, sin_h).astype(bf16)
    key_rot = rotate(lin[:, :kv_width].reshape(rows, KV_HEADS, HEAD_DIM), cos_h, sin_h).astype(bf16)
    kv_own = jnp.concatenate(
        [key_rot.reshape(rows, kv_width), lin[:, kv_width : 2 * kv_width].astype(bf16)], axis=1
    )
    back_chunks = mask.shape[1] // rows - 1
    kv_win = jnp.concatenate(
        [shift(kv_own, hops) for hops in range(back_chunks, 0, -1)] + [kv_own], axis=0
    )
    window = kv_win.shape[0]
    key_win = kv_win[:, :kv_width].reshape(window, KV_HEADS, HEAD_DIM)
    value_win = kv_win[:, kv_width:].reshape(window, KV_HEADS, HEAD_DIM)
    grouped = query_rot.reshape(rows, KV_HEADS, heads // KV_HEADS, HEAD_DIM)
    scores = jnp.einsum("tagd,sad->agts", grouped, key_win, preferred_element_type=f32)
    scores = scores * HEAD_DIM ** (-0.5) + mask
    largest = jnp.max(scores, axis=-1, keepdims=True)
    lse = largest + jnp.log(jnp.sum(jnp.exp(scores - largest), axis=-1, keepdims=True))
    probs = jnp.exp(scores - lse).astype(bf16)
    context = jnp.einsum("agts,sad->tagd", probs, value_win, preferred_element_type=f32)
    context = context.reshape(rows, heads * HEAD_DIM).astype(bf16)
    middle = inputs + contract_cols(context, att_w[:, ahead + qkv_width :])
    inverse = lax.rsqrt(jnp.mean(middle * middle, axis=-1, keepdims=True) + EPSILON)
    two = (middle * inverse * gains[1]).astype(bf16)
    two = lax.all_gather(two, "tensor", axis=0, tiled=True)
    query_rot = query_rot.reshape(rows, heads * HEAD_DIM)
    return att_w, ffn_all, cot_rows, two, middle, one, query_rot, kv_win, lse, context, gains


def shift(value, hops):
    size = lax.axis_size("tensor")
    pairs = [(i, i + hops) for i in range(size) if 0 <= i + hops < size]
    return lax.ppermute(value, "tensor", pairs)


def sum_grads(two, cot_rows, hid, dg, du, normed_one, d_attended, d_lin, context, ffn_part, small):
    f32, bf16 = jnp.float32, jnp.bfloat16
    fixed = d_lin.shape[1] - context.shape[1]
    d_query = d_lin[:, fixed:]
    def over_dp(left, right):
        return lax.psum_scatter(
            contract_rows(left, right).astype(bf16), "dp", scatter_dimension=0, tiled=True
        )

    def over_tensor(value, axis):
        return lax.psum_scatter(value, "tensor", scatter_dimension=axis, tiled=True).astype(f32)

    return (
        over_dp(cot_rows, hid).astype(f32),
        over_dp(two, dg).astype(f32),
        over_dp(two, du).astype(f32),
        over_tensor(over_dp(normed_one, d_query), 1),
        over_tensor(over_dp(d_attended, context), 1),
        over_tensor(over_dp(normed_one, d_lin[:, :fixed]), 0),
        over_tensor(ffn_part, 0),
        lax.psum(small, ("dp", "tensor")),
    )


def branch_back(
    tokens, cosine, sine, mask, att_w, cot_rows, rows_two, hidden_low, d_gate, d_upper, ffn_part,
    d_normed_two, cotangent, middle, normed_one, query_rot, kv_win, lse, context, gains,
):
    f32, bf16 = jnp.float32, jnp.bfloat16
    rows = tokens.shape[0]
    kv_width, query_width = kv_win.shape[1] // 2, query_rot.shape[1]
    qkv_width = 2 * kv_width + query_width
    ahead = att_w.shape[1] - qkv_width - query_width
    heads, padded = query_width // HEAD_DIM, hidden_low.shape[1]
    if lax.axis_size("dp") == 8 and lax.axis_size("tensor") == 4:
        turn = jnp.stack(
            [jnp.concatenate([cosine, cosine], axis=1), jnp.concatenate([-sine, sine], axis=1)]
        )
        flat, sum_query, sum_out, sum_kv, mixed, input_grad, small = back(
            rows_two, cot_rows, hidden_low, d_gate, d_upper, ffn_part, d_normed_two, tokens, middle, gains,
            att_w, query_rot, kv_win.reshape(-1, rows, 2 * kv_width), lse, context, normed_one, mask, turn,
        )
        flat = [flat[:, k * padded : (k + 1) * padded] for k in range(3)]
        return mixed, input_grad, *flat, sum_query, sum_out, sum_kv, small[0]
    group = heads // KV_HEADS
    window = kv_win.shape[0]
    back_chunks = window // rows - 1
    scale = HEAD_DIM ** (-0.5)
    cos_h, sin_h = cosine[:, None, :], sine[:, None, :]
    d_normed_two = d_normed_two.astype(f32)
    qkv_w = att_w[:, ahead : ahead + qkv_width]
    out_full = att_w[:, ahead + qkv_width :]
    inputs = tokens.astype(f32)
    inverse_one = lax.rsqrt(jnp.mean(inputs * inputs, axis=-1, keepdims=True) + EPSILON)
    unit_one = inputs * inverse_one
    inverse_two = lax.rsqrt(jnp.mean(middle * middle, axis=-1, keepdims=True) + EPSILON)
    unit_two = middle * inverse_two
    gain_two_term, d_from_two = norm_back(d_normed_two, unit_two, inverse_two, gains[1])
    d_middle = cotangent.astype(f32) + d_from_two
    d_attended = d_middle.astype(bf16)
    d_context = jnp.dot(d_attended, out_full, preferred_element_type=f32).astype(bf16)
    d_context = d_context.reshape(rows, KV_HEADS, group, HEAD_DIM)
    key_win = kv_win[:, :kv_width].reshape(window, KV_HEADS, HEAD_DIM)
    value_win = kv_win[:, kv_width:].reshape(window, KV_HEADS, HEAD_DIM)
    grouped = query_rot.reshape(rows, KV_HEADS, group, HEAD_DIM)
    scores = jnp.einsum("tagd,sad->agts", grouped, key_win, preferred_element_type=f32) * scale + mask
    probs = jnp.exp(scores - lse.reshape(KV_HEADS, group, rows, 1))
    probs_low = probs.astype(bf16)
    d_probs = jnp.einsum("tagd,sad->agts", d_context, value_win, preferred_element_type=f32)
    row_delta = jnp.sum(probs * d_probs, axis=-1, keepdims=True)
    d_scores = (probs * (d_probs - row_delta)).astype(bf16)
    d_query_rot = jnp.einsum("agts,sad->tagd", d_scores, key_win, preferred_element_type=f32) * scale
    d_key_win = jnp.einsum("agts,tagd->sad", d_scores, grouped, preferred_element_type=f32) * scale
    d_value_win = jnp.einsum("agts,tagd->sad", probs_low, d_context, preferred_element_type=f32)
    d_query_lin = (
        rotate_back(d_query_rot.reshape(rows, heads, HEAD_DIM), cos_h, sin_h)
        .reshape(rows, query_width).astype(bf16)
    )
    d_kv_win = jnp.concatenate(
        [d_key_win.reshape(window, kv_width), d_value_win.reshape(window, kv_width)], axis=1
    ).astype(bf16)
    d_kv = d_kv_win[back_chunks * rows :].astype(f32)
    for hops in range(1, back_chunks + 1):
        given = d_kv_win[(back_chunks - hops) * rows : (back_chunks - hops + 1) * rows]
        d_kv = d_kv + shift(given, -hops).astype(f32)
    d_key_lin = rotate_back(d_kv[:, :kv_width].reshape(rows, KV_HEADS, HEAD_DIM), cos_h, sin_h)
    d_lin = jnp.concatenate(
        [d_key_lin.reshape(rows, kv_width).astype(bf16), d_kv[:, kv_width:].astype(bf16), d_query_lin],
        axis=1,
    )
    d_normed_one = contract_cols(d_lin, qkv_w)
    bias_term = jnp.sum(d_lin.astype(f32), axis=0)
    gain_one_term, d_from_one = norm_back(d_normed_one, unit_one, inverse_one, gains[0])
    input_grad = (d_middle + d_from_one).astype(bf16)

    sums = sum_grads(
        rows_two, cot_rows, hidden_low, d_gate, d_upper, normed_one, d_attended, d_lin, context,
        ffn_part, jnp.concatenate([bias_term[2 * kv_width :], bias_term[: 2 * kv_width], gain_one_term, gain_two_term]),
    )
    sum_down, sum_gate, sum_up, sum_query, sum_out, sum_kv, ffn_sum, small = sums
    mixed = (middle + ffn_sum.astype(f32)).astype(bf16)
    return mixed, input_grad, sum_down, sum_gate, sum_up, sum_query, sum_out, sum_kv, small


def local(
    tokens, segments, gain_one, query_w, query_b, key_w, key_b, value_w, value_b,
    out_w, gain_two, gate_w, up_w, down_w, cotangent,
):
    bf16, f32 = jnp.bfloat16, jnp.float32
    rows, model_width = tokens.shape
    tensor_size = lax.axis_size("tensor")
    rank = lax.axis_index("tensor")
    kv_width = key_w.shape[1]
    fixed_width = 2 * kv_width
    query_width = query_w.shape[1] * tensor_size
    qkv_width = fixed_width + query_width
    units = gate_w.shape[1]
    back_chunks = min(tensor_size - 1, -(-DOC_MAX // rows))
    window = (back_chunks + 1) * rows
    cosine, sine = angle_tables(rank * rows, rows, HEAD_DIM)
    segment = segments[0]
    own_segment = lax.dynamic_slice_in_dim(segment, rank * rows, rows, 0)
    before = jnp.full((back_chunks * rows,), -1, segment.dtype)
    win_segment = lax.dynamic_slice_in_dim(jnp.concatenate([before, segment]), rank * rows, window, 0)
    own_pos = back_chunks * rows + jnp.arange(rows)
    win_pos = jnp.arange(window)
    allowed = (own_segment[:, None] == win_segment[None, :]) & (win_pos[None, :] <= own_pos[:, None])
    mask = jnp.where(allowed, 0.0, NEGATIVE).astype(f32)
    ahead = 128
    gains_w = jnp.pad(jnp.stack([gain_one, gain_two], axis=1), ((0, 0), (0, ahead - 2)))
    (
        att_w, ffn_w, cot_rows, normed_two, middle, normed_one, query_rot, kv_win, lse, context, gains,
    ) = attention_branch(
        tokens, cosine, sine, mask, gains_w, query_w, query_b, jnp.concatenate([key_w, value_w], axis=1),
        jnp.concatenate([key_b, value_b]).astype(f32), out_w, joined_units(gate_w, up_w, down_w), cotangent,
    )
    rows_two, hidden_low, d_gate, d_upper, ffn_part, d_normed_two = ffn(
        normed_two, cot_rows, ffn_w
    )
    mixed, input_grad, sum_down, sum_gate, sum_up, sum_query, sum_out, sum_kv, small = branch_back(
        tokens, cosine, sine, mask, att_w, cot_rows, rows_two, hidden_low, d_gate, d_upper, ffn_part,
        d_normed_two, cotangent, middle, normed_one, query_rot, kv_win, lse, context, gains,
    )
    place = lax.axis_index("dp") * tensor_size + rank
    devices = lax.axis_size("dp") * tensor_size

    def own(start, size):
        share = size // devices
        return lax.dynamic_slice_in_dim(small, start + place * share, share, 0)

    return (
        mixed,
        input_grad,
        own(qkv_width, model_width),
        sum_query,
        own(0, query_width),
        sum_kv[:, :kv_width],
        small[query_width : query_width + kv_width],
        sum_kv[:, kv_width : 2 * kv_width],
        small[query_width + kv_width : qkv_width],
        sum_out,
        own(qkv_width + model_width, model_width),
        sum_gate[:, :units],
        sum_up[:, :units],
        sum_down[:, :units],
    )


def solution(mesh):
    both = ("dp", "tensor")
    return jax.shard_map(
        local,
        mesh=mesh,
        in_specs=(
            P(both, None), P("dp", None), P("dp"), P("dp", "tensor"), P("tensor"), P("dp", None), P(),
            P("dp", None), P(), P("dp", "tensor"), P("dp"), P("dp", "tensor"), P("dp", "tensor"),
            P("dp", "tensor"), P(both, None),
        ),
        out_specs=(
            P(both, None), P(both, None), P(both), P("dp", "tensor"), P(both), P(both, None), P(),
            P(both, None), P(), P("dp", "tensor"), P(both), P("dp", "tensor"), P("dp", "tensor"),
            P("dp", "tensor"),
        ),
        check_vma=False,
    )
```

```python
import functools

import jax
import jax.numpy as jnp
from jax import lax
from jax.experimental import pallas as pl
from jax.experimental.pallas import tpu as pltpu
from jax.sharding import PartitionSpec as P

MESH = pl.DeviceIdType.MESH
KV_HEADS = 2
HEAD_DIM = 128
DOC_MAX = 512
EPSILON = 1e-06
ROPE_BASE = 1000000.0
NEGATIVE = -1e30


def square(d):
    core, x, y = d % 2, (d // 2) % 2, d // 4
    by_x, by_y = d + 2 - 4 * x, d + 4 - 8 * y
    return by_x, by_y, d + 1 - 2 * core, by_x + 4 - 8 * y


def front_body(
    x_ref, turn_ref, mask_ref, bias_ref, query_ref, out_ref, fixed_ref, ffn_ref, cot_ref,
    att_all, ffn_all, cot_all, two_all, mid_out, one_out, query_rot, kv_win, lse_out, ctx_out, gain_out,
    att_v, w_v, one_v, q_v, kv_v, ctx_v, mid_v, two_v,
    fill_sem, z_send, z_recv, cot_send, cot_recv, send, recv, keep_sem, w_sem, kv_send, kv_recv, save_sem,
    two_send, two_recv,
    *, pieces, order, lead,
):
    f32, bf16 = jnp.float32, jnp.bfloat16
    d, z = lax.axis_index("dp"), lax.axis_index("tensor")
    size = 4
    by_x, by_y, mate, across = square(d)
    rows = ffn_ref.shape[0]
    half = rows // 2
    part = query_ref.shape[1]
    fixed = fixed_ref.shape[1]
    chunk = cot_ref.shape[0]
    tall = query_ref.shape[0]

    barrier = pltpu.get_barrier_semaphore()
    for peer in (by_x, by_y, mate):
        pl.semaphore_signal(barrier, inc=1, device_id={"dp": peer}, device_id_type=MESH)
    for hop in range(1, size):
        pl.semaphore_signal(
            barrier, inc=1, device_id={"tensor": (z + hop) % size}, device_id_type=MESH
        )

    def place(of, owner):
        return pl.ds(pl.multiple_of(fixed + of * size * part + owner * part, 128), part)

    fills = [pltpu.make_async_copy(fixed_ref, att_v.at[pl.ds(0, rows), pl.ds(0, fixed)], fill_sem.at[0])]
    for of, ref in enumerate((query_ref, out_ref)):
        fills.append(pltpu.make_async_copy(ref, att_v.at[:, place(of, z)], fill_sem.at[1 + of]))
    at = pl.ds(pl.multiple_of(z * chunk, chunk), chunk)
    fills.append(pltpu.make_async_copy(cot_ref, cot_all.at[at, :], fill_sem.at[3]))
    for copy in fills:
        copy.start()

    pl.semaphore_wait(barrier, 3 + size - 1)

    def z_copy(of, j, dz, own):
        ref = att_v.at[:, place(of, j)]
        return pltpu.make_async_remote_copy(
            src_ref=(query_ref, out_ref)[of] if own else ref, dst_ref=ref,
            send_sem=z_send.at[of, (dz + 1) // 2, j], recv_sem=z_recv.at[of, j],
            device_id={"tensor": z + dz}, device_id_type=MESH,
        )

    def z_start(of):
        for dz, there in ((-1, has_low), (1, has_high)):

            @pl.when(there)
            def _(dz=dz):
                z_copy(of, z, dz, True).start()

    def z_step(of, hop):
        for sign, onward in ((-1, has_high), (1, has_low)):
            j = z + sign * hop
            inside = (j >= 0) if sign == -1 else (j < size)

            @pl.when(inside)
            def _(j=j, sign=sign):
                z_copy(of, j, -sign, False).wait_recv()

            @pl.when(jnp.logical_and(inside, onward))
            def _(j=j, sign=sign):
                z_copy(of, j, -sign, False).start()

    has_low, has_high = z > 0, z < size - 1

    def cot_copy(j, dz):
        ref = cot_all.at[pl.ds(pl.multiple_of(j * chunk, chunk), chunk), :]
        return pltpu.make_async_remote_copy(
            src_ref=ref, dst_ref=ref, send_sem=cot_send.at[(dz + 1) // 2, j], recv_sem=cot_recv.at[j],
            device_id={"tensor": z + dz}, device_id_type=MESH,
        )

    def cot_start():
        fills[3].wait()
        for dz, there in ((-1, has_low), (1, has_high)):

            @pl.when(there)
            def _(dz=dz):
                cot_copy(z, dz).start()

    def cot_step(hop):
        for sign, onward in ((-1, has_high), (1, has_low)):
            j = z + sign * hop
            inside = (j >= 0) if sign == -1 else (j < size)

            @pl.when(inside)
            def _(j=j, sign=sign):
                cot_copy(j, -sign).wait_recv()

            @pl.when(jnp.logical_and(inside, onward))
            def _(j=j, sign=sign):
                cot_copy(j, -sign).start()

    def two_copy(j, dz, own):
        ref = two_all.at[pl.ds(pl.multiple_of(j * chunk, chunk), chunk), :]
        return pltpu.make_async_remote_copy(
            src_ref=two_v if own else ref, dst_ref=ref, send_sem=two_send.at[(dz + 1) // 2, j],
            recv_sem=two_recv.at[j], device_id={"tensor": z + dz}, device_id_type=MESH,
        )

    def two_start():
        for dz, there in ((-1, has_low), (1, has_high)):

            @pl.when(there)
            def _(dz=dz):
                two_copy(z, dz, True).start()

    def two_step(hop):
        for sign, onward in ((-1, has_high), (1, has_low)):
            j = z + sign * hop
            inside = (j >= 0) if sign == -1 else (j < size)

            @pl.when(inside)
            def _(j=j, sign=sign):
                two_copy(j, -sign, False).wait_recv()

            if hop == 1:

                @pl.when(jnp.logical_and(inside, onward))
                def _(j=j, sign=sign):
                    two_copy(j, -sign, False).start()

    for of in range(2):
        z_start(of)
    fills[0].wait()

    def views(kind, p):
        src, dst = ((att_v, att_all), (ffn_ref, ffn_all))[kind]
        return src, dst, pl.ds(*pieces[kind][p])

    def slot(kind, p):
        return p + kind * len(pieces[0])

    def block(dst, cols, owner, first=0, many=None):
        many = rows if many is None else many
        return dst.at[pl.ds(pl.multiple_of(owner * rows + first, 16), many), cols]

    def remote(src, dst, way, at_slot, peer):
        return pltpu.make_async_remote_copy(
            src_ref=src, dst_ref=dst, send_sem=send.at[way, at_slot], recv_sem=recv.at[way, at_slot],
            device_id={"dp": peer}, device_id_type=MESH,
        )

    def own(kind, p):
        src, dst, cols = views(kind, p)
        mine = src.at[pl.ds(0, rows), cols]
        there = block(dst, cols, d)
        s = slot(kind, p)
        return [
            remote(mine, there, 0, s, by_x), remote(mine, there, 1, s, by_y),
            remote(mine, there, 2, s, mate),
        ], pltpu.make_async_copy(mine, there, keep_sem.at[s])

    def relays(kind, p, group):
        _, dst, cols = views(kind, p)
        s = slot(kind, p)
        if group == 2:
            whole = block(dst, cols, across)
            return [remote(whole, whole, 7, s, mate)]
        owner, peer = ((by_x, by_y), (by_y, by_x))[group]
        piece, whole = block(dst, cols, owner, group * half, half), block(dst, cols, owner)
        way = 3 + 2 * group
        return [remote(piece, piece, way, s, peer), remote(whole, whole, way + 1, s, mate)]

    def arrived(kind, p, way):
        _, dst, cols = views(kind, p)
        many = half if way in (3, 5) else rows
        ref = block(dst, cols, d, 0, many)
        pltpu.make_async_copy(ref, ref, recv.at[way, slot(kind, p)]).wait()

    def begin(kind, p):
        copies, keep = own(kind, p)
        for copy in copies:
            copy.start()
        keep.start()

    def pass_on(kind, p):
        for group in range(2):
            arrived(kind, p, group)
            for copy in relays(kind, p, group):
                copy.start()

    def close(kind, p):
        arrived(kind, p, 3)
        arrived(kind, p, 5)
        relays(kind, p, 2)[0].start()

    def settle(kind, p):
        for way in (2, 4, 6, 7):
            arrived(kind, p, way)
        own(kind, p)[1].wait()

    def finish(kind, p):
        copies = own(kind, p)[0]
        for group in range(3):
            copies = copies + relays(kind, p, group)
        for copy in copies:
            copy.wait_send()

    state = {"begun": 0, "query": False, "out": False}

    def ready(kind, p):
        end = sum(pieces[kind][p])
        if kind == 1 or end <= fixed:
            return
        need = 1 if end <= fixed + size * part else 2
        for of in range(need):
            if not state[("query", "out")[of]]:
                state[("query", "out")[of]] = True
                fills[1 + of].wait()
                if of == 1:
                    cot_start()

    def weight_load(p):
        cols = pl.ds(*pieces[0][p])
        return pltpu.make_async_copy(att_all.at[:, cols], w_v.at[:, cols], w_sem.at[p])

    def take(first, last):
        for p in range(first, last):
            settle(0, p)
            weight_load(p).start()

    def held(first, last):
        for p in range(first, last):
            weight_load(p).wait()

    saves = []

    def save(src, dst):
        copy = pltpu.make_async_copy(src, dst, save_sem.at[len(saves)])
        copy.start()
        saves.append(copy)

    part_rows = max(16, chunk // 4)

    def norm(value_of, row, dst):
        gain = gain_out[row : row + 1, :]

        def some(r, carry):
            at_r = pl.ds(pl.multiple_of(r * part_rows, part_rows), part_rows)
            value = value_of(at_r)
            inverse = lax.rsqrt(jnp.mean(value * value, axis=-1, keepdims=True) + EPSILON)
            dst[at_r, :] = (value * inverse * gain).astype(bf16)
            return carry

        lax.fori_loop(0, chunk // part_rows, some, 0)

    def turned(value):
        return value * turn_ref[0] + pltpu.roll(value, HEAD_DIM // 2, 1) * turn_ref[1]

    lead_w = fixed - 2 * KV_HEADS * HEAD_DIM
    kv_w = KV_HEADS * HEAD_DIM
    heads = size * part // HEAD_DIM
    scale = HEAD_DIM ** (-0.5)

    def kv_copy(hop):
        return pltpu.make_async_remote_copy(
            src_ref=kv_v.at[2], dst_ref=kv_v.at[2 - hop], send_sem=kv_send.at[hop - 1],
            recv_sem=kv_recv.at[hop - 1], device_id={"tensor": z + hop}, device_id_type=MESH,
        )

    def keys():
        pick = (
            lax.broadcasted_iota(jnp.int32, (8, lead_w), 0)
            == lax.broadcasted_iota(jnp.int32, (8, lead_w), 1)
        ).astype(bf16)
        gain_out[...] = lax.dot_general(
            pick, w_v[:, :lead_w], (((1,), (1,)), ((), ())), preferred_element_type=f32
        )
        norm(lambda at_r: x_ref[at_r, :].astype(f32), 0, one_v)
        save(one_v, one_out)
        lin = jnp.dot(one_v[...], w_v[:, lead_w:fixed], preferred_element_type=f32) + bias_ref[0:1, :]
        for g in range(KV_HEADS):
            cols = slice(g * HEAD_DIM, (g + 1) * HEAD_DIM)
            kv_v[2, :, cols] = turned(lin[:, cols]).astype(bf16)
        kv_v[2, :, kv_w:] = lin[:, kv_w:].astype(bf16)
        for hop in (1, 2):

            @pl.when(z + hop < size)
            def _(hop=hop):
                kv_copy(hop).start()

            @pl.when(z < hop)
            def _(hop=hop):
                kv_v[2 - hop] = jnp.zeros(kv_v.shape[1:], bf16)

    per = pieces[0][1][1] // HEAD_DIM

    def queries(first):
        def pair(k, carry):
            h = first + 2 * k
            cols = pl.ds(pl.multiple_of(h * HEAD_DIM, 128), 2 * HEAD_DIM)
            from_w = pl.ds(pl.multiple_of(fixed + h * HEAD_DIM, 128), 2 * HEAD_DIM)
            lin = jnp.dot(one_v[...], w_v[:, from_w], preferred_element_type=f32)
            lin += att_v[pl.ds(rows, 16), from_w][0:1, :].astype(f32)
            q_v[:, cols] = jnp.concatenate(
                [turned(lin[:, :HEAD_DIM]), turned(lin[:, HEAD_DIM:])], axis=1
            ).astype(bf16)
            return carry

        lax.fori_loop(0, per // 2, pair, 0)

    def kv_wait():
        for hop in (1, 2):

            @pl.when(z >= hop)
            def _(hop=hop):
                pltpu.make_async_copy(kv_v.at[2 - hop], kv_v.at[2 - hop], kv_recv.at[hop - 1]).wait()

        save(kv_v, kv_win)

    def attend(first, last):
        def head(h, carry):
            cols = pl.ds(pl.multiple_of(h * HEAD_DIM, 128), HEAD_DIM)
            group = h // (heads // KV_HEADS)
            key_cols = pl.ds(pl.multiple_of(group * HEAD_DIM, 128), HEAD_DIM)
            value_cols = pl.ds(pl.multiple_of(kv_w + group * HEAD_DIM, 128), HEAD_DIM)
            key = kv_v[:, :, key_cols].reshape(3 * chunk, HEAD_DIM)
            value = kv_v[:, :, value_cols].reshape(3 * chunk, HEAD_DIM)
            scores = lax.dot_general(
                q_v[:, cols], key, (((1,), (1,)), ((), ())), preferred_element_type=f32
            )
            scores = scores * scale + mask_ref[...]
            largest = jnp.max(scores, axis=-1, keepdims=True)
            powers = jnp.exp(scores - largest)
            mass = jnp.sum(powers, axis=-1, keepdims=True)
            lse_out[h] = largest + jnp.log(mass)
            probs = (powers * (1.0 / mass)).astype(bf16)
            ctx_v[:, cols] = jnp.dot(probs, value, preferred_element_type=f32).astype(bf16)
            return carry

        lax.fori_loop(first, last, head, 0)

    def project(k):
        tile = min(512, w_v.shape[0])
        wide = per * HEAD_DIM

        def some(n, carry):
            at_n = pl.ds(pl.multiple_of(n * tile, tile), tile)
            added = lax.dot_general(
                ctx_v[:, k * wide : (k + 1) * wide],
                w_v[at_n, fixed + size * part + k * wide : fixed + size * part + (k + 1) * wide],
                (((1,), (1,)), ((), ())), preferred_element_type=f32,
            )
            so_far = mid_v[:, at_n] if k else x_ref[:, at_n].astype(f32)
            mid_v[:, at_n] = so_far + added
            return carry

        lax.fori_loop(0, w_v.shape[0] // tile, some, 0)

    def second_norm():
        norm(lambda at_r: mid_v[at_r, :], 1, two_v)
        save(two_v, two_all.at[at, :])
        two_start()
        save(mid_v, mid_out)
        save(q_v, query_rot)
        save(ctx_v, ctx_out)

    n_att = len(pieces[0])
    n_q = (n_att - 1) // 2
    when_q, when_out = [[order.index((0, 1 + of * n_q + k)) for k in range(n_q)] for of in range(2)]
    last_q, last_out = when_q[-1], when_out[-1]
    work = [(2, lambda: take(0, 1)), (2, lambda: held(0, 1)), (2, keys)]
    work += [(last_q + 1, lambda: cot_step(1)), (last_q + 4, lambda: cot_step(2)), (last_q + 6, lambda: cot_step(3))]
    work += [(when_q[0] + 2, kv_wait)]
    for k in range(n_q):
        work += [
            (when_q[k] + 2, lambda k=k: take(1 + k, 2 + k)), (when_q[k] + 3, lambda k=k: held(1 + k, 2 + k)),
            (when_q[k] + 3, lambda k=k: queries(k * per)),
            (when_q[k] + 3, lambda k=k: attend(k * per, (k + 1) * per)),
        ]
        late = 3 if k < n_q - 1 else 2
        work += [
            (when_out[k] + 2, lambda k=k: take(1 + n_q + k, 2 + n_q + k)),
            (when_out[k] + late, lambda k=k: held(1 + n_q + k, 2 + n_q + k)),
            (when_out[k] + late, lambda k=k: project(k)),
        ]
    work += [
        (last_out + 2, second_norm), (last_out + 5, lambda: two_step(1)), (last_out + 20, lambda: two_step(2)),
    ]
    work.sort(key=lambda step: step[0])
    total = len(order)
    for i in range(total + 1):
        while state["begun"] < min(total, i + (lead if i <= last_out else 2 * lead)):
            ready(*order[state["begun"]])
            begin(*order[state["begun"]])
            state["begun"] += 1
        if i == 0:
            for hop in range(1, size):
                for of in range(2):
                    z_step(of, hop)
                if hop < size - 1:
                    pass_on(*order[hop - 1])
        if size - 2 <= i < total:
            pass_on(*order[i])
        if i > 0:
            close(*order[i - 1])
        while work and (work[0][0] <= i or i == total):
            work.pop(0)[1]()
    for kind, p in order:
        if kind == 1:
            settle(kind, p)
    for kind, p in order:
        finish(kind, p)
    for copy in saves:
        copy.wait()
    for hop in (1, 2):

        @pl.when(z + hop < size)
        def _(hop=hop):
            kv_copy(hop).wait_send()

    for j in range(size):
        for dz, there in ((-1, has_low), (1, has_high)):
            came = jnp.logical_and((z <= j) if dz == -1 else (z >= j), there)

            @pl.when(came)
            def _(j=j, dz=dz):
                cot_copy(j, dz).wait_send()
                for of in range(2):
                    z_copy(of, j, dz, False).wait_send()

            near = jnp.logical_and(came, (j - z <= 1) if dz == -1 else (z - j <= 1))

            @pl.when(near)
            def _(j=j, dz=dz):
                two_copy(j, dz, False).wait_send()


def front(
    tokens, turn, mask, kv_bias, query, out, fixed, ffn_w, cot, att_tile=512, ffn_tile=768,
    collective_id=2, limit=60_000_000,
):
    tall, part = query.shape
    rows, fixed_w = fixed.shape
    chunk, width = tokens.shape
    size, ways = 4, 8
    query_w = size * part
    att_cols = fixed_w + 2 * query_w
    pieces = (
        [(0, fixed_w)] + [(fixed_w + p * att_tile, att_tile) for p in range(2 * query_w // att_tile)],
        [(p * ffn_tile, ffn_tile) for p in range(ffn_w.shape[1] // ffn_tile)],
    )
    n_att, n_ffn = len(pieces[0]), len(pieces[1])
    early = min(2, n_ffn)
    order = [(0, 0)] + [(1, p) for p in range(early)] + [(0, p) for p in range(1, n_att)]
    order += [(1, p) for p in range(early, n_ffn)]
    bf16, f32 = jnp.bfloat16, jnp.float32
    hbm = pl.BlockSpec(memory_space=pl.ANY)
    vmem = pl.BlockSpec(memory_space=pltpu.VMEM)
    vm = pltpu.VMEM
    dma = pltpu.SemaphoreType.DMA
    shape = lambda *s: jax.ShapeDtypeStruct(s, bf16)
    wide = lambda *s: jax.ShapeDtypeStruct(s, f32)
    slots = n_att + n_ffn
    kv_w = 2 * KV_HEADS * HEAD_DIM
    heads = query_w // HEAD_DIM
    return pl.pallas_call(
        functools.partial(front_body, pieces=pieces, order=order, lead=3),
        out_shape=(
            shape(8 * rows, att_cols), shape(8 * rows, ffn_w.shape[1]),
            shape(size * cot.shape[0], cot.shape[1]),
            shape(size * chunk, width), wide(chunk, width), shape(chunk, width), shape(chunk, query_w),
            shape(3, chunk, kv_w), wide(heads, chunk, 1), shape(chunk, query_w), wide(8, width),
        ),
        in_specs=[vmem] * 9,
        out_specs=(hbm,) * 8 + (vmem, hbm, vmem),
        scratch_shapes=[
            vm((tall, att_cols), bf16), vm((8 * rows, att_cols), bf16), vm((chunk, width), bf16),
            vm((chunk, query_w), bf16), vm((3, chunk, kv_w), bf16), vm((chunk, query_w), bf16),
            vm((chunk, width), f32), vm((chunk, width), bf16),
            dma((4,)), dma((2, 2, size)), dma((2, size)),
            dma((2, size)), dma((size,)), dma((ways, slots)), dma((ways, slots)), dma((slots,)),
            dma((n_att,)), dma((2,)), dma((2,)), dma((6,)), dma((2, size)), dma((size,)),
        ],
        compiler_params=pltpu.CompilerParams(
            collective_id=collective_id, has_side_effects=True, vmem_limit_bytes=limit
        ),
        cost_estimate=pl.CostEstimate(
            flops=2 * chunk * width * att_cols, bytes_accessed=20 * rows * (att_cols + ffn_w.shape[1]),
            transcendentals=0,
        ),
        name="front",
    )(tokens, turn, mask, kv_bias, query, out, fixed, ffn_w, cot)


def line_order(z, s):
    upper = z // 2
    near = z * (1 - upper) + (3 - z) * upper
    late = s // 2
    at = (1 - late) * (2 + s) + late * ((3 - s) * (1 - near) + (s - 2) * near)
    return at * (1 - upper) + (3 - at) * upper


def ffn_body(
    two_ref, cot_ref, weights_ref,
    rows_out, hid_out, dg_out, du_out, sum_out, dn_out,
    rows_v, cot_v, gate_v, up_v, down_v, hid_v, dg_v, du_v, part, land, below, above, res_v,
    tile_sem, load_sem, row_sem, ag_send, ag_recv, rs_send, rs_recv, own_recv, out_sem,
    *, axis, ft, nt,
):
    f32, bf16 = jnp.float32, jnp.bfloat16
    size = 4
    rows, width = two_ref.shape[0] // size, two_ref.shape[1]
    units = weights_ref.shape[1] // 3
    n_f, n_n = units // ft, width // nt
    z = lax.axis_index(axis)
    has_low, has_high = z > 0, z < size - 1

    def to(dz):
        return {axis: z + dz}

    barrier = pltpu.get_barrier_semaphore()

    @pl.when(has_low)
    def _():
        pl.semaphore_signal(barrier, inc=1, device_id=to(-1), device_id_type=MESH)

    @pl.when(has_high)
    def _():
        pl.semaphore_signal(barrier, inc=1, device_id=to(1), device_id_type=MESH)

    def chunk_rows(j):
        return two_ref.at[pl.ds(pl.multiple_of(j * rows, rows), rows), :]

    def far(j):
        return jnp.logical_or(j - z == 3, z - j == 3)

    def row_load(j):
        return pltpu.make_async_copy(chunk_rows(j), rows_v.at[j], row_sem.at[j])

    def load_rows(s):
        j = line_order(z, s)

        @pl.when(jnp.logical_not(far(j)))
        def _():
            row_load(j).start()

    load_rows(0)

    def tile_loads(f):
        cols = pl.ds(pl.multiple_of(f * ft, 128), ft)
        return [
            pltpu.make_async_copy(
                weights_ref.at[:, pl.ds(pl.multiple_of(k * units + f * ft, 128), ft)],
                dst.at[:, cols], tile_sem.at[k, f],
            )
            for k, dst in enumerate((gate_v, up_v, down_v))
        ]

    cot_load = pltpu.make_async_copy(cot_ref, cot_v, load_sem.at[1])
    for f in range(n_f):
        for copy in tile_loads(f):
            copy.start()
        if f == 0:
            cot_load.start()
            for s in range(1, size):
                load_rows(s)

    pl.semaphore_wait(barrier, (z + size - 1) // size + (2 * size - 2 - z) // size)

    def far_copy():
        j = 3 - 3 * (z // 2)
        return pltpu.make_async_remote_copy(
            src_ref=chunk_rows(j), dst_ref=rows_v.at[j], send_sem=ag_send.at[0], recv_sem=ag_recv.at[0],
            device_id=to(2 * (z // 2) - 1), device_id_type=MESH,
        )

    middle = jnp.logical_and(has_low, has_high)

    @pl.when(middle)
    def _():
        far_copy().start()

    def rs_copy(j, n, dz, own):
        way = (dz + 1) // 2
        if own:
            dst = below.at[n] if dz == 1 else above.at[n]
            sem = own_recv.at[1 - way, n]
        else:
            dst, sem = land.at[j, n], rs_recv.at[j, n]
        return pltpu.make_async_remote_copy(
            src_ref=part.at[j, n], dst_ref=dst, send_sem=rs_send.at[j, n],
            recv_sem=sem, device_id=to(dz), device_id_type=MESH,
        )

    def pass_on(j, n, what):
        for dz in (1, -1):
            for own in (True, False):
                hop = j == z + dz
                going = (j > z) if dz == 1 else (j < z)
                near = hop if own else jnp.logical_not(hop)

                @pl.when(jnp.logical_and(going, near))
                def _(dz=dz, own=own):
                    copy = rs_copy(j, n, dz, own)
                    copy.start() if what == "start" else copy.wait_send()

    def out_copies(j):
        at = pl.ds(pl.multiple_of(j * rows, rows), rows)
        return [
            pltpu.make_async_copy(src.at[j], dst.at[at, :], out_sem.at[k, j])
            for k, (src, dst) in enumerate(
                ((rows_v, rows_out), (hid_v, hid_out), (dg_v, dg_out), (du_v, du_out))
            )
        ]

    def forward(j, n):
        pltpu.make_async_copy(land.at[j, n], land.at[j, n], rs_recv.at[j, n]).wait()
        part[j, n] = (part[j, n].astype(f32) + land[j, n].astype(f32)).astype(bf16)
        pass_on(j, n, "start")

    def forward_all(j):
        def some(n, carry):
            forward(j, n)
            return carry

        lax.fori_loop(0, n_n, some, 0)

    def step(s, carry):
        j = line_order(z, s)

        @pl.when(far(j))
        def _():
            pltpu.make_async_copy(rows_v.at[j], rows_v.at[j], ag_recv.at[0]).wait()

        @pl.when(jnp.logical_not(far(j)))
        def _():
            row_load(j).wait()

        at = pl.ds(pl.multiple_of(j * rows, rows), rows)

        @pl.when(s == 0)
        def _():
            cot_load.wait()

        def units_tile(f, carry):
            @pl.when(s == 0)
            def _():
                for copy in tile_loads(f):
                    copy.wait()

            cols = pl.ds(pl.multiple_of(f * ft, 128), ft)
            mine = rows_v[j]
            gate = jnp.dot(mine, gate_v[:, cols], preferred_element_type=f32)
            upper = jnp.dot(mine, up_v[:, cols], preferred_element_type=f32)
            d_hidden = jnp.dot(cot_v[at, :], down_v[:, cols], preferred_element_type=f32)
            sig = 1.0 / (1.0 + jnp.exp(-gate))
            act = gate * sig
            hid_v[j, :, cols] = (act * upper).astype(bf16)
            du_v[j, :, cols] = (d_hidden * act).astype(bf16)
            dg_v[j, :, cols] = (d_hidden * upper * (sig + act * (1.0 - sig))).astype(bf16)
            return carry

        lax.fori_loop(0, n_f, units_tile, 0)
        for copy in out_copies(j):
            copy.start()
        ends = jnp.logical_and(s < 3, jnp.logical_not(middle))

        @pl.when(jnp.logical_and(middle, s == 3))
        def _():
            forward_all(3 - z)
            forward_all(3 - 3 * (z // 2))


        def width_tile(n, carry):
            at_n = pl.ds(pl.multiple_of(n * nt, nt), nt)
            dims = (((1,), (1,)), ((), ()))
            total = lax.dot_general(dg_v[j], gate_v[at_n, :], dims, preferred_element_type=f32)
            total += lax.dot_general(du_v[j], up_v[at_n, :], dims, preferred_element_type=f32)
            part[j, n] = total.astype(bf16)

            @pl.when(ends)
            def _():
                pass_on(j, n, "start")

            return carry

        lax.fori_loop(0, n_n, width_tile, 0)
        return carry

    lax.fori_loop(0, size, step, 0)

    def down_tile(i, carry):
        j, n = i // n_n, i % n_n
        at_n = pl.ds(pl.multiple_of(n * nt, nt), nt)
        total = lax.dot_general(
            hid_v[j], down_v[at_n, :], (((1,), (1,)), ((), ())), preferred_element_type=f32
        )
        res_v[j, :, at_n] = total.astype(bf16)
        return carry

    tiles = size * n_n
    done = tiles // 3
    lax.fori_loop(0, done, down_tile, 0)
    for n in range(n_n):
        until = tiles if n == n_n - 1 else done + (n + 1) * (tiles - done) // n_n

        @pl.when(middle)
        def _(n=n):
            forward(3 * (z // 2), n)

        lax.fori_loop(done + n * (tiles - done) // n_n, until, down_tile, 0)
    sum_copies = [
        pltpu.make_async_copy(
            res_v.at[j], sum_out.at[pl.ds(j * rows, rows), :], load_sem.at[2 + j]
        )
        for j in range(size)
    ]
    for copy in sum_copies:
        copy.start()

    def last(n, carry):
        @pl.when(has_low)
        def _():
            pltpu.make_async_copy(below.at[n], below.at[n], own_recv.at[0, n]).wait()
            part[z, n] = (part[z, n].astype(f32) + below[n].astype(f32)).astype(bf16)

        @pl.when(has_high)
        def _():
            pltpu.make_async_copy(above.at[n], above.at[n], own_recv.at[1, n]).wait()
            part[z, n] = (part[z, n].astype(f32) + above[n].astype(f32)).astype(bf16)

        dn_out[:, pl.ds(pl.multiple_of(n * nt, nt), nt)] = part[z, n]
        return carry

    lax.fori_loop(0, n_n, last, 0)

    def drain(j, carry):
        for copy in out_copies(j):
            copy.wait()
        def sent(n, carry):
            @pl.when(j != z)
            def _():
                pltpu.make_async_copy(part.at[j, n], part.at[j, n], rs_send.at[j, n]).wait()

            return carry

        lax.fori_loop(0, n_n, sent, 0)
        return carry

    lax.fori_loop(0, size, drain, 0)

    @pl.when(middle)
    def _():
        far_copy().wait_send()

    for copy in sum_copies:
        copy.wait()


def ffn(two, cot_rows, weights, axis="tensor", ft=768, nt=512, collective_id=1, limit=66_000_000):
    size = 4
    length, width = two.shape
    rows = length // size
    units = weights.shape[1] // 3
    n_f, n_n = units // ft, width // nt
    bf16 = jnp.bfloat16
    hbm = pl.BlockSpec(memory_space=pl.ANY)
    vm = pltpu.VMEM
    dma = pltpu.SemaphoreType.DMA
    shape = lambda *s: jax.ShapeDtypeStruct(s, bf16)
    return pl.pallas_call(
        functools.partial(ffn_body, axis=axis, ft=ft, nt=nt),
        out_shape=(
            shape(length, width), shape(length, units), shape(length, units), shape(length, units),
            shape(length, width), shape(rows, width),
        ),
        in_specs=[hbm] * 3,
        out_specs=(hbm,) * 5 + (pl.BlockSpec(memory_space=pltpu.VMEM),),
        scratch_shapes=[
            vm((size, rows, width), bf16), vm((length, width), bf16),
            vm((width, units), bf16), vm((width, units), bf16), vm((width, units), bf16),
            vm((size, rows, units), bf16), vm((size, rows, units), bf16), vm((size, rows, units), bf16),
            vm((size, n_n, rows, nt), bf16), vm((size, n_n, rows, nt), bf16),
            vm((n_n, rows, nt), bf16), vm((n_n, rows, nt), bf16),
            vm((size, rows, width), bf16),
            dma((3, n_f)), dma((2 + size,)), dma((size,)), dma((1,)), dma((1,)), dma((size, n_n)), dma((size, n_n)),
            dma((2, n_n)), dma((4, size)),
        ],
        compiler_params=pltpu.CompilerParams(
            collective_id=collective_id, has_side_effects=True, vmem_limit_bytes=limit
        ),
        cost_estimate=pl.CostEstimate(
            flops=12 * length * width * units, bytes_accessed=8 * width * units + 8 * length * units,
            transcendentals=length * units,
        ),
        name="ffn",
    )(two, cot_rows, weights)


def back_body(
    two_ref, cot_ref, hid_ref, dg_ref, du_ref, part_ref, up_ref, x_ref, mid_ref, gain_ref, att_ref,
    query_ref, win_ref, lse_ref, ctx_ref, one_ref, mask_ref, turn_ref,
    ffn_out, query_out, out_out, kv_out, mixed_out, input_out, small_out,
    up_v, own_v, mid_v, gain_v, w_v, query_v, win_v, lse_v, mask_v, turn_v, lhs_ref, rhs_ref,
    d_mid, d_ctx, d_win, kv_give, kv_take, small_ref,
    left_v, right_v, grad, mate_land, core_sum, x_land, y_land, second, x_last, y_last, stage, fin,
    z_land, kv_land, fold_land, fold_last, fold_own, small_z, small_hop, small_next, in_sem, give_send, give_recv,
    left_sem, right_sem, mate_send, mate_recv, one_send, one_recv, two_send, two_recv, stage_sem,
    z_send, z_recv, kv_send, kv_recv, fold_send, fold_recv, last_recv, own_sem, small_send, small_recv,
    hop_send, hop_recv, *, n_f, wide,
):
    f32, bf16 = jnp.float32, jnp.bfloat16
    d, z = lax.axis_index("dp"), lax.axis_index("tensor")
    size = 4
    core, x, y = d % 2, (d // 2) % 2, d // 4
    by_x, by_y, mate, _ = square(d)
    here, at_x, at_y = 2 * y + x, 2 * y + 1 - x, 2 * (1 - y) + x
    cross = 3 - here
    block, half = core_sum.shape[2], core_sum.shape[2] // 2
    n_ffn, n_att = 3 * n_f, rhs_ref.shape[1] // wide
    ring, n_sum, n_last = x_land.shape[0], core_sum.shape[0], x_last.shape[0]
    n_grad, n_mate = grad.shape[0], mate_land.shape[0]
    total = n_ffn + n_att
    chunk, width = mixed_out.shape
    share = block // size
    part_w = wide // 2

    barrier = pltpu.get_barrier_semaphore()
    for peer in (by_x, by_y, mate):
        pl.semaphore_signal(barrier, inc=1, device_id={"dp": peer}, device_id_type=MESH)
    for hop in range(1, size):
        pl.semaphore_signal(
            barrier, inc=1, device_id={"tensor": (z + hop) % size}, device_id_type=MESH
        )

    lefts = [
        pltpu.make_async_copy(ref, left_v, left_sem.at[k]) for k, ref in enumerate((cot_ref, two_ref))
    ]
    query_w = query_ref.shape[1]
    kv_w = KV_HEADS * HEAD_DIM
    heads = query_w // HEAD_DIM
    scale = HEAD_DIM ** (-0.5)
    ahead = att_ref.shape[1] - 2 * query_w - 2 * kv_w
    own_rows = pl.ds(pl.multiple_of(z * chunk, chunk), chunk)
    ctx_cols = pl.ds(query_w, query_w)
    plan = (
        (up_ref, up_v), (cot_ref.at[own_rows, :], own_v), (mid_ref, mid_v), (gain_ref, gain_v),
        (att_ref.at[:, pl.ds(ahead + 2 * kv_w + query_w, query_w)], w_v.at[:, pl.ds(0, query_w)]),
        (query_ref, query_v), (win_ref, win_v), (lse_ref, lse_v), (mask_ref, mask_v), (turn_ref, turn_v),
        (ctx_ref, rhs_ref.at[:, ctx_cols]), (one_ref, lhs_ref.at[0]), (x_ref, up_v),
        (att_ref.at[:, pl.ds(ahead, 2 * kv_w + query_w)], w_v),
    )
    loads = [pltpu.make_async_copy(src, dst, in_sem.at[k]) for k, (src, dst) in enumerate(plan)]

    def right_load(i, what):
        cols = pl.ds(pl.multiple_of((i % n_f) * wide, 128), wide)
        for m, ref in enumerate((hid_ref, dg_ref, du_ref)):
            copy = pltpu.make_async_copy(ref.at[:, cols], right_v.at[i % 2], right_sem.at[i % 2])

            @pl.when(i // n_f == m)
            def _(copy=copy):
                copy.start() if what == "start" else copy.wait()

    lefts[0].start()
    right_load(jnp.int32(0), "start")
    for copy in loads[:-2]:
        copy.start()

    def chunk_rows(j):
        return part_ref.at[pl.ds(pl.multiple_of(j * chunk, chunk), chunk), :]

    upper = z // 2
    inward = 1 - 2 * upper
    middle = jnp.logical_and(z > 0, z < size - 1)

    def fold_load(j):
        return pltpu.make_async_copy(chunk_rows(j), fold_own, own_sem.at[0])

    def fold_copy(k, first):
        if first:
            j = (3 - 3 * upper, 2 - upper, z + inward)[k]
            src, to = chunk_rows(j), z + inward
            dst = (fold_land.at[0], fold_land.at[1], fold_last.at[0])[k]
            sem = (fold_recv.at[0], fold_recv.at[1], last_recv.at[0])[k]
        else:
            src, to = fold_land.at[k], z + (inward, inward, -inward)[k]
            dst = (fold_land.at[2], fold_last.at[1], fold_last.at[1])[k]
            sem = (fold_recv.at[2], last_recv.at[1], last_recv.at[1])[k]
        return pltpu.make_async_remote_copy(
            src_ref=src, dst_ref=dst, send_sem=fold_send.at[k], recv_sem=sem,
            device_id={"tensor": to}, device_id_type=MESH,
        )

    def fold(k):
        @pl.when(middle)
        def _():
            pltpu.make_async_copy(fold_land.at[k], fold_land.at[k], fold_recv.at[k]).wait()
            fold_load(z).wait()
            fold_land[k] = (fold_land[k].astype(f32) + fold_own[...].astype(f32)).astype(bf16)
            fold_copy(k, False).start()
            fold_load((2 - upper, 3 * upper, z)[k]).start()
    pl.semaphore_wait(barrier, 3 + size - 1)

    def dp_copy(src, dst, send_sem, recv_sem, peer):
        return pltpu.make_async_remote_copy(
            src_ref=src, dst_ref=dst, send_sem=send_sem, recv_sem=recv_sem,
            device_id={"dp": peer}, device_id_type=MESH,
        )

    def z_copy(src, dst, send_sem, recv_sem, peer):
        return pltpu.make_async_remote_copy(
            src_ref=src, dst_ref=dst, send_sem=send_sem, recv_sem=recv_sem,
            device_id={"tensor": peer}, device_id_type=MESH,
        )

    small_copies = []
    for hop in range(1, size):
        to, k = (z + hop) % size, hop - 1
        small_copies.append(
            z_copy(small_ref, small_z.at[k], small_send.at[k], small_recv.at[k], to)
        )

    @pl.when(jnp.logical_not(middle))
    def _():
        for k in range(3):
            fold_copy(k, True).start()
        fold_load(z).start()

    @pl.when(middle)
    def _():
        fold_load(3 - 3 * upper).start()

    rhs_ref[:, 2 * query_w + 2 * kv_w :] = jnp.zeros((chunk, rhs_ref.shape[1] - 2 * query_w - 2 * kv_w), bf16)

    hops = (mate, by_x, by_y)

    def hop_copy(k):
        return dp_copy(small_next.at[k], small_hop.at[k], hop_send.at[k], hop_recv.at[k], hops[k])

    def mate_copy(i):
        return dp_copy(
            grad.at[i % n_grad, :, 1 - core], mate_land.at[i % n_mate], mate_send.at[i % n_mate],
            mate_recv.at[i % n_mate], mate,
        )

    def one_copies(i):
        s = core_sum.at[i % n_sum]
        first, last = pl.ds(0, half), pl.ds(half, half)
        plan = (
            (s.at[at_x, first, :], x_land.at[i % ring, 0], by_x), (s.at[cross, first, :], x_land.at[i % ring, 1], by_x),
            (s.at[at_y, last, :], y_land.at[i % ring, 0], by_y), (s.at[cross, last, :], y_land.at[i % ring, 1], by_y),
        )
        return [
            dp_copy(src, dst, one_send.at[k, i % ring], one_recv.at[k, i % ring], peer)
            for k, (src, dst, peer) in enumerate(plan)
        ]

    def two_copies(i):
        return [
            dp_copy(second.at[i % 2, 0], y_last.at[i % n_last], two_send.at[0, i % ring], two_recv.at[0, i % ring], by_y),
            dp_copy(second.at[i % 2, 1], x_last.at[i % n_last], two_send.at[1, i % ring], two_recv.at[1, i % ring], by_x),
        ]

    def stage_copy(i):
        cols = pl.ds(pl.multiple_of(i * wide, 128), wide)
        return pltpu.make_async_copy(stage.at[i % 2], ffn_out.at[:, cols], stage_sem.at[i % 2])

    def multiply(i):
        @pl.when(jnp.logical_and(i >= n_grad, i < total))
        def _():
            mate_copy(i - n_grad).wait_send()

        @pl.when(i + 1 < n_ffn)
        def _():
            right_load(i + 1, "start")

        dims = (((0,), (0,)), ((), ()))

        @pl.when(i < n_ffn)
        def _():
            @pl.when(i == 0)
            def _():
                lefts[0].wait()

            @pl.when(i == n_f)
            def _():
                lefts[1].start()
                lefts[1].wait()

            right_load(i, "wait")

            def rows(k, carry):
                at = pl.ds(pl.multiple_of(k * 2 * block, 128), 2 * block)
                value = lax.dot_general(
                    left_v[:, at], right_v[i % 2], dims, preferred_element_type=f32
                )
                grad[i % n_grad, k] = value.astype(bf16).reshape(2, block, wide)
                return carry

            lax.fori_loop(0, 4, rows, 0)

        @pl.when(jnp.logical_and(i >= n_ffn, i < total))
        def _():
            a = i - n_ffn
            cols = pl.ds(pl.multiple_of(a * wide, 128), wide)

            def rows(k, carry):
                at = pl.ds(pl.multiple_of(k * 2 * block, 128), 2 * block)
                value = lax.dot_general(
                    lhs_ref[(a // 2) % 2, :, at], rhs_ref[:, cols], dims, preferred_element_type=f32
                )
                grad[i % n_grad, k] = value.astype(bf16).reshape(2, block, wide)
                return carry

            lax.fori_loop(0, 4, rows, 0)

        @pl.when(i < total)
        def _():
            mate_copy(i).start()

    def sum_cores(i):
        mate_copy(i).wait_recv()
        for k in range(4):
            core_sum[i % n_sum, k] = (
                grad[i % n_grad, k, core].astype(f32) + mate_land[i % n_mate, k].astype(f32)
            ).astype(bf16)
        for copy in one_copies(i):
            copy.start()

    def sum_near(i):
        for copy in one_copies(i):
            copy.wait_recv()
        s = core_sum.at[i % n_sum]
        second[i % 2, 0] = (s[at_y, :half].astype(f32) + x_land[i % ring, 1].astype(f32)).astype(bf16)
        second[i % 2, 1] = (s[at_x, half:].astype(f32) + y_land[i % ring, 1].astype(f32)).astype(bf16)
        for copy in two_copies(i):
            copy.start()

    def z_sends(a, what):
        for h in range(2):
            owner = (a % 2) * 2 + h
            hop = (owner - z + size) % size
            src = fin.at[a, :, pl.ds(h * part_w, part_w)]

            @pl.when(jnp.logical_and(a < 4, hop > 0))
            def _(src=src, owner=owner, hop=hop, h=h):
                copy = z_copy(
                    src, z_land.at[a // 2, hop - 1], z_send.at[a, h], z_recv.at[a // 2, hop - 1], owner
                )
                copy.start() if what == "start" else copy.wait_send()

        @pl.when(a == 4)
        def _():
            for hop in range(1, size):
                to = (z + hop) % size
                rows = pl.ds(pl.multiple_of(to * share, 16), share)
                copy = z_copy(
                    fin.at[4, rows, :], kv_land.at[hop - 1], kv_send.at[hop - 1], kv_recv.at[hop - 1], to
                )
                copy.start() if what == "start" else copy.wait_send()

    def finish(i):
        for copy in two_copies(i):
            copy.wait_recv()
        own = core_sum.at[i % n_sum, here]
        top = own[:half].astype(f32) + x_land[i % ring, 0].astype(f32) + y_last[i % n_last].astype(f32)
        low = own[half:].astype(f32) + y_land[i % ring, 0].astype(f32) + x_last[i % n_last].astype(f32)

        @pl.when(i < n_ffn)
        def _():
            @pl.when(i >= 2)
            def _():
                stage_copy(i - 2).wait()

            stage[i % 2, :half] = top
            stage[i % 2, half:] = low
            stage_copy(i).start()

        @pl.when(i >= n_ffn)
        def _():
            a = i - n_ffn
            fin[a, :half] = top.astype(bf16)
            fin[a, half:] = low.astype(bf16)
            z_sends(a, "start")

        for copy in one_copies(i) + two_copies(i):
            copy.wait_send()

    def back_norm(upstream, value, gain, base, col):
        inverse = lax.rsqrt(jnp.mean(value * value, axis=-1, keepdims=True) + EPSILON)
        unit = value * inverse
        scaled = upstream * gain
        term = jnp.sum(upstream * unit, axis=0, keepdims=True)
        small_ref[:, pl.ds(col, width)] += jnp.broadcast_to(term, (8, width))
        return base + inverse * (scaled - unit * jnp.mean(scaled * unit, axis=-1, keepdims=True))

    some_rows = max(16, chunk // 4)

    def by_rows(work):
        def some(r, carry):
            work(pl.ds(pl.multiple_of(r * some_rows, some_rows), some_rows))
            return carry

        lax.fori_loop(0, chunk // some_rows, some, 0)

    gain_one_at, gain_two_at = query_w + 2 * kv_w, query_w + 2 * kv_w + width

    def open_branch():
        for k in (0, 1, 2, 3):
            loads[k].wait()
        small_ref[...] = jnp.zeros_like(small_ref)

        def work(at):
            value = back_norm(
                up_v[at, :].astype(f32), mid_v[at, :], gain_v[1:2, :], own_v[at, :].astype(f32), gain_two_at
            )
            d_mid[at, :] = value
            lhs_ref[1, at, :] = value.astype(bf16)

        by_rows(work)

    def context_grads():
        loads[4].wait()
        tile = min(512, query_w)

        def some(n, carry):
            cols = pl.ds(pl.multiple_of(n * tile, tile), tile)
            d_ctx[:, cols] = jnp.dot(lhs_ref[1], w_v[:, cols], preferred_element_type=f32).astype(bf16)
            return carry

        lax.fori_loop(0, query_w // tile, some, 0)
        for copy in loads[-2:]:
            copy.start()
        for k in (5, 6, 7, 8, 9):
            loads[k].wait()
        d_win[...] = jnp.zeros_like(d_win)

    def turned_back(value):
        return value * turn_v[0] - pltpu.roll(value, HEAD_DIM // 2, 1) * turn_v[1]

    def attend_back(first, last):
        def head(h, carry):
            cols = pl.ds(pl.multiple_of(h * HEAD_DIM, 128), HEAD_DIM)
            group = h // (heads // KV_HEADS)
            key_cols = pl.ds(pl.multiple_of(group * HEAD_DIM, 128), HEAD_DIM)
            value_cols = pl.ds(pl.multiple_of(kv_w + group * HEAD_DIM, 128), HEAD_DIM)
            key = win_v[:, :, key_cols].reshape(3 * chunk, HEAD_DIM)
            value = win_v[:, :, value_cols].reshape(3 * chunk, HEAD_DIM)
            query, given = query_v[:, cols], d_ctx[:, cols]
            across, down = (((1,), (1,)), ((), ())), (((0,), (0,)), ((), ()))
            scores = lax.dot_general(query, key, across, preferred_element_type=f32)
            probs = jnp.exp(scores * scale + mask_v[...] - lse_v[h])
            d_probs = lax.dot_general(given, value, across, preferred_element_type=f32)
            delta = jnp.sum(probs * d_probs, axis=-1, keepdims=True)
            d_scores = (probs * (d_probs - delta)).astype(bf16)
            d_query = jnp.dot(d_scores, key, preferred_element_type=f32) * scale
            rhs_ref[:, cols] = turned_back(d_query).astype(bf16)
            d_key = lax.dot_general(d_scores, query, down, preferred_element_type=f32) * scale
            d_value = lax.dot_general(probs.astype(bf16), given, down, preferred_element_type=f32)
            d_win[:, :, key_cols] += d_key.reshape(3, chunk, HEAD_DIM)
            d_win[:, :, value_cols] += d_value.reshape(3, chunk, HEAD_DIM)
            return carry

        lax.fori_loop(first, last, head, 0)

    def give_copy(hop):
        return z_copy(
            kv_give.at[hop - 1], kv_take.at[hop - 1], give_send.at[hop - 1], give_recv.at[hop - 1], z - hop
        )

    def give():
        for hop in (1, 2):

            @pl.when(z >= hop)
            def _(hop=hop):
                kv_give[hop - 1] = d_win[2 - hop].astype(bf16)
                give_copy(hop).start()

    def take():
        for hop in (1, 2):

            @pl.when(z + hop < size)
            def _(hop=hop):
                pltpu.make_async_copy(kv_take.at[hop - 1], kv_take.at[hop - 1], give_recv.at[hop - 1]).wait()
                d_win[2] += kv_take[hop - 1].astype(f32)

        for g in range(KV_HEADS):
            cols = slice(g * HEAD_DIM, (g + 1) * HEAD_DIM)
            out_cols = slice(2 * query_w + g * HEAD_DIM, 2 * query_w + (g + 1) * HEAD_DIM)
            rhs_ref[:, out_cols] = turned_back(d_win[2, :, cols]).astype(bf16)
        rhs_ref[:, 2 * query_w + kv_w : 2 * query_w + 2 * kv_w] = d_win[2, :, kv_w:].astype(bf16)
        ones = jnp.ones((8, chunk), bf16)
        small_ref[:, :query_w] = jnp.dot(ones, rhs_ref[:, :query_w], preferred_element_type=f32)
        small_ref[:, query_w : query_w + 2 * kv_w] = jnp.dot(
            ones, rhs_ref[:, 2 * query_w : 2 * query_w + 2 * kv_w], preferred_element_type=f32
        )

    def one_grads():
        loads[-1].wait()
        tile = min(512, width)
        across = (((1,), (1,)), ((), ()))

        def some(n, carry):
            at_n = pl.ds(pl.multiple_of(n * tile, tile), tile)
            d_win[n] = lax.dot_general(
                rhs_ref[:, :query_w], w_v[at_n, 2 * kv_w :], across, preferred_element_type=f32
            ) + lax.dot_general(
                rhs_ref[:, 2 * query_w : 2 * query_w + 2 * kv_w], w_v[at_n, : 2 * kv_w], across,
                preferred_element_type=f32,
            )
            return carry

        lax.fori_loop(0, width // tile, some, 0)

    def close_branch():
        loads[-2].wait()

        def work(at):
            input_out[at, :] = back_norm(
                jnp.concatenate([d_win[n, at, :] for n in range(width // d_win.shape[2])], axis=1), up_v[at, :].astype(f32), gain_v[0:1, :], d_mid[at, :], gain_one_at
            ).astype(bf16)

        by_rows(work)
        for copy in small_copies:
            copy.start()

    def small_first():
        for copy in small_copies:
            copy.wait_recv()
        small_next[0] = small_ref[...] + small_z[0] + small_z[1] + small_z[2]
        hop_copy(0).start()

    def small_then(k):
        hop_copy(k).wait_recv()
        small_next[k + 1] = small_next[k] + small_hop[k]
        hop_copy(k + 1).start()

    def small_last():
        hop_copy(2).wait_recv()
        small_out[...] = small_next[2] + small_hop[2]

    span = n_ffn - 1
    quarter = heads // 4

    def at_turn(k):
        return min(k, span)

    steps = [
        (0, open_branch), (at_turn(1), context_grads),
        (at_turn(2), lambda: attend_back(0, quarter)),
        (at_turn(3), lambda: attend_back(quarter, 2 * quarter)),
        (at_turn(4), lambda: attend_back(2 * quarter, 3 * quarter)),
        (at_turn(5), lambda: attend_back(3 * quarter, heads)),
        (at_turn(5), give),
        (at_turn(3), lambda: fold(0)), (at_turn(5), lambda: fold(1)), (at_turn(8), lambda: fold(2)),
        (at_turn(7), take), (at_turn(7), lambda: [loads[k].wait() for k in (10, 11)]),
        (n_ffn + 1, one_grads), (n_ffn + 2, close_branch),
        (n_ffn + 4, small_first), (n_ffn + 5, lambda: small_then(0)), (n_ffn + 6, lambda: small_then(1)),
        (n_ffn + 7, small_last),
    ]

    def small_step(i):
        for when, step in steps:

            @pl.when(i == when)
            def _(step=step):
                step()

    def turn(i, carry):
        multiply(i)
        for lag, work in ((1, sum_cores), (2, sum_near), (3, finish)):

            @pl.when(jnp.logical_and(i >= lag, i - lag < total))
            def _(lag=lag, work=work):
                work(i - lag)

        small_step(i)
        return carry

    lax.fori_loop(0, total + 3, turn, 0)
    for i in range(total - n_grad, total):
        mate_copy(i).wait_send()
    for i in (n_ffn - 2, n_ffn - 1):
        stage_copy(i).wait()
    fold_load(z).wait()
    mid_v[...] += fold_own[...].astype(f32)

    @pl.when(middle)
    def _():
        pltpu.make_async_copy(fold_last.at[0], fold_last.at[0], last_recv.at[0]).wait()
        mid_v[...] += fold_last[0].astype(f32)

    pltpu.make_async_copy(fold_last.at[1], fold_last.at[1], last_recv.at[1]).wait()
    mixed_out[...] = (mid_v[...] + fold_last[1].astype(f32)).astype(bf16)
    for k in range(3):
        pltpu.make_async_copy(fold_land.at[k], fold_land.at[k], fold_send.at[k]).wait()
    for of, dst in ((0, query_out), (1, out_out)):
        for k in range(size - 1):
            ref = z_land.at[of, k]
            pltpu.make_async_copy(ref, ref, z_recv.at[of, k]).wait()
        for h in range(4):

            @pl.when(z == h)
            def _(of=of, dst=dst, h=h):
                acc = fin[2 * of + h // 2, :, (h % 2) * part_w : (h % 2 + 1) * part_w].astype(f32)
                for k in range(size - 1):
                    acc += z_land[of, k].astype(f32)
                dst[...] = acc

    for k in range(size - 1):
        pltpu.make_async_copy(kv_land.at[k], kv_land.at[k], kv_recv.at[k]).wait()
    rows = pl.ds(pl.multiple_of(z * share, 16), share)
    acc = fin[4, rows, :].astype(f32)
    for k in range(size - 1):
        acc += kv_land[k].astype(f32)
    kv_out[...] = acc
    for a in range(n_att):
        z_sends(a, "wait")
    for copy in small_copies:
        copy.wait_send()
    for k in range(3):
        hop_copy(k).wait_send()
    for hop in (1, 2):

        @pl.when(z >= hop)
        def _(hop=hop):
            give_copy(hop).wait_send()


def back(
    two, cot_rows, hid, dg, du, ffn_part, up, tokens, middle, gains, att_w, query_rot, kv_win, lse, context,
    normed_one, mask, turn, wide=768, collective_id=3, limit=67_000_000,
):
    length, width = two.shape
    size, chunk, block = 4, tokens.shape[0], width // 8
    units, query_w, kv_w = hid.shape[1], context.shape[1], kv_win.shape[2]
    n_f, n_att = units // wide, (2 * query_w + wide) // wide
    total = 3 * n_f + n_att
    half, part_w, share = block // 2, wide // 2, block // size
    heads = lse.shape[0]
    bf16, f32 = jnp.bfloat16, jnp.float32
    small = (8, query_w + kv_w + 2 * width)
    ring = 5
    hbm = pl.BlockSpec(memory_space=pl.ANY)
    vmem = pl.BlockSpec(memory_space=pltpu.VMEM)
    vm = pltpu.VMEM
    dma = pltpu.SemaphoreType.DMA
    shape = jax.ShapeDtypeStruct
    return pl.pallas_call(
        functools.partial(back_body, n_f=n_f, wide=wide),
        out_shape=(
            shape((block, 3 * units), f32), shape((block, part_w), f32), shape((block, part_w), f32),
            shape((share, wide), f32), shape((chunk, width), bf16), shape((chunk, width), bf16),
            shape(small, f32),
        ),
        in_specs=[hbm] * 18,
        out_specs=(hbm,) + (vmem,) * 6,
        scratch_shapes=[
            vm((chunk, width), bf16), vm((chunk, width), bf16),
            vm((chunk, width), f32), vm(gains.shape, f32), vm((width, kv_w + query_w), bf16),
            vm((chunk, query_w), bf16), vm(kv_win.shape, bf16), vm((heads, chunk, 1), f32),
            vm(mask.shape, f32), vm(turn.shape, f32), vm((2, chunk, width), bf16),
            vm((chunk, 2 * query_w + wide), bf16), vm((chunk, width), f32), vm((chunk, query_w), bf16),
            vm(kv_win.shape, f32), vm((2, chunk, kv_w), bf16), vm((2, chunk, kv_w), bf16),
            vm(small, f32),
            vm((length, width), bf16), vm((2, length, wide), bf16), vm((2, 4, 2, block, wide), bf16),
            vm((4, 4, block, wide), bf16), vm((4, 4, block, wide), bf16),
            vm((ring, 2, half, wide), bf16), vm((ring, 2, half, wide), bf16),
            vm((2, 2, half, wide), bf16), vm((4, half, wide), bf16), vm((4, half, wide), bf16),
            vm((2, block, wide), f32), vm((n_att, block, wide), bf16),
            vm((2, size - 1, block, part_w), bf16), vm((size - 1, share, wide), bf16),
            vm((3, chunk, width), bf16), vm((2, chunk, width), bf16), vm((chunk, width), bf16), vm((3,) + small, f32), vm((3,) + small, f32),
            vm((3,) + small, f32), dma((14,)), dma((2,)), dma((2,)),
            dma((2,)), dma((2,)), dma((6,)), dma((6,)), dma((4, ring)), dma((4, ring)),
            dma((2, ring)), dma((2, ring)), dma((2,)),
            dma((4, 2)), dma((2, size - 1)), dma((size - 1,)), dma((size - 1,)), dma((3,)),
            dma((3,)), dma((2,)), dma((1,)), dma((size - 1,)), dma((size - 1,)), dma((3,)), dma((3,)),
        ],
        compiler_params=pltpu.CompilerParams(
            collective_id=collective_id, has_side_effects=True, vmem_limit_bytes=limit
        ),
        cost_estimate=pl.CostEstimate(
            flops=6 * length * width * units, bytes_accessed=8 * length * units, transcendentals=0
        ),
        name="back",
    )(
        two, cot_rows, hid, dg, du, ffn_part, up, tokens, middle, gains, att_w, query_rot, kv_win, lse, context,
        normed_one, mask, turn,
    )


def angle_tables(first, length, head_width):
    position = (first + jnp.arange(length)).astype(jnp.float32)
    exponent = jnp.arange(head_width // 2, dtype=jnp.float32) * (2.0 / head_width)
    frequency = ROPE_BASE ** (-exponent)
    angle = position[:, None] * frequency[None, :]
    return (jnp.cos(angle), jnp.sin(angle))


def rotate(values, cosine, sine):
    half_width = values.shape[-1] // 2
    first_half = values[..., :half_width]
    second_half = values[..., half_width:]
    return jnp.concatenate(
        [first_half * cosine - second_half * sine, second_half * cosine + first_half * sine],
        axis=-1,
    )


def rotate_back(grads, cosine, sine):
    return rotate(grads, cosine, -sine)


def dot_f32(left, right, dims):
    return lax.dot_general(left, right, (dims, ((), ())), preferred_element_type=jnp.float32)


def contract_rows(left, right):
    return dot_f32(left, right, ((0,), (0,)))


def contract_cols(left, right):
    return dot_f32(left, right, ((1,), (1,)))


def norm_back(upstream, unit, inverse, gain):
    scaled = upstream * gain
    gain_term = jnp.sum(upstream * unit, axis=0)
    input_term = inverse * (scaled - unit * jnp.mean(scaled * unit, axis=-1, keepdims=True))
    return (gain_term, input_term)


def joined_units(gate_w, up_w, down_w):
    units = gate_w.shape[1]
    gap = -(-units // 768) * 768 - units
    wide = lambda w: jnp.pad(w, ((0, 0), (0, gap)))
    return jnp.concatenate([wide(gate_w), wide(up_w), wide(down_w)], axis=1)


def attention_branch(tokens, cosine, sine, mask, gains_w, query_w, query_b, kv_w, kv_b, out_w, ffn_w, cotangent):
    f32, bf16 = jnp.float32, jnp.bfloat16
    rows = tokens.shape[0]
    size = lax.axis_size("tensor")
    fixed_w = jnp.concatenate([gains_w, kv_w], axis=1)
    if lax.axis_size("dp") == 8 and size == 4:
        tall_query = jnp.concatenate([query_w, jnp.pad(query_b[None, :], ((0, 15), (0, 0)))], axis=0)
        tall_out = jnp.pad(out_w, ((0, 16), (0, 0)))
        turn = jnp.stack(
            [jnp.concatenate([cosine, cosine], axis=1), jnp.concatenate([-sine, sine], axis=1)]
        )
        att_w, ffn_all, cot_rows, two, middle, one, query_rot, kv_win, lse, context, gains = front(
            tokens, turn, mask, kv_b[None, :], tall_query, tall_out, fixed_w, ffn_w, cotangent
        )
        kv_win = kv_win.reshape(3 * rows, kv_w.shape[1])
        return att_w, ffn_all, cot_rows, two, middle, one, query_rot, kv_win, lse, context, gains
    pair = lax.all_gather(jnp.stack([query_w, out_w]), "tensor", axis=2, tiled=True)
    att_w = jnp.concatenate([fixed_w, pair[0], pair[1]], axis=1)
    att_w = lax.all_gather(att_w, "dp", axis=0, tiled=True)
    ffn_all = lax.all_gather(ffn_w, "dp", axis=0, tiled=True)
    cot_rows = lax.all_gather(cotangent, "tensor", axis=0, tiled=True)
    full_query_b = lax.all_gather(query_b, "tensor", axis=0, tiled=True).astype(f32)
    ahead = gains_w.shape[1]
    kv_width = kv_w.shape[1] // 2
    qkv_width = 2 * kv_width + full_query_b.shape[0]
    heads = full_query_b.shape[0] // HEAD_DIM
    gains = att_w[:, :2].T.astype(f32)
    inputs = tokens.astype(f32)
    inverse = lax.rsqrt(jnp.mean(inputs * inputs, axis=-1, keepdims=True) + EPSILON)
    one = (inputs * inverse * gains[0]).astype(bf16)
    lin = jnp.dot(one, att_w[:, ahead : ahead + qkv_width], preferred_element_type=f32)
    lin = lin + jnp.concatenate([kv_b, full_query_b])
    cos_h, sin_h = cosine[:, None, :], sine[:, None, :]
    query_rot = rotate(lin[:, 2 * kv_width :].reshape(rows, heads, HEAD_DIM), cos_h, sin_h).astype(bf16)
    key_rot = rotate(lin[:, :kv_width].reshape(rows, KV_HEADS, HEAD_DIM), cos_h, sin_h).astype(bf16)
    kv_own = jnp.concatenate(
        [key_rot.reshape(rows, kv_width), lin[:, kv_width : 2 * kv_width].astype(bf16)], axis=1
    )
    back_chunks = mask.shape[1] // rows - 1
    kv_win = jnp.concatenate(
        [shift(kv_own, hops) for hops in range(back_chunks, 0, -1)] + [kv_own], axis=0
    )
    window = kv_win.shape[0]
    key_win = kv_win[:, :kv_width].reshape(window, KV_HEADS, HEAD_DIM)
    value_win = kv_win[:, kv_width:].reshape(window, KV_HEADS, HEAD_DIM)
    grouped = query_rot.reshape(rows, KV_HEADS, heads // KV_HEADS, HEAD_DIM)
    scores = jnp.einsum("tagd,sad->agts", grouped, key_win, preferred_element_type=f32)
    scores = scores * HEAD_DIM ** (-0.5) + mask
    largest = jnp.max(scores, axis=-1, keepdims=True)
    lse = largest + jnp.log(jnp.sum(jnp.exp(scores - largest), axis=-1, keepdims=True))
    probs = jnp.exp(scores - lse).astype(bf16)
    context = jnp.einsum("agts,sad->tagd", probs, value_win, preferred_element_type=f32)
    context = context.reshape(rows, heads * HEAD_DIM).astype(bf16)
    middle = inputs + contract_cols(context, att_w[:, ahead + qkv_width :])
    inverse = lax.rsqrt(jnp.mean(middle * middle, axis=-1, keepdims=True) + EPSILON)
    two = (middle * inverse * gains[1]).astype(bf16)
    two = lax.all_gather(two, "tensor", axis=0, tiled=True)
    query_rot = query_rot.reshape(rows, heads * HEAD_DIM)
    return att_w, ffn_all, cot_rows, two, middle, one, query_rot, kv_win, lse, context, gains


def shift(value, hops):
    size = lax.axis_size("tensor")
    pairs = [(i, i + hops) for i in range(size) if 0 <= i + hops < size]
    return lax.ppermute(value, "tensor", pairs)


def sum_grads(two, cot_rows, hid, dg, du, normed_one, d_attended, d_lin, context, ffn_part, small):
    f32, bf16 = jnp.float32, jnp.bfloat16
    fixed = d_lin.shape[1] - context.shape[1]
    d_query = d_lin[:, fixed:]
    def over_dp(left, right):
        return lax.psum_scatter(
            contract_rows(left, right).astype(bf16), "dp", scatter_dimension=0, tiled=True
        )

    def over_tensor(value, axis):
        return lax.psum_scatter(value, "tensor", scatter_dimension=axis, tiled=True).astype(f32)

    return (
        over_dp(cot_rows, hid).astype(f32),
        over_dp(two, dg).astype(f32),
        over_dp(two, du).astype(f32),
        over_tensor(over_dp(normed_one, d_query), 1),
        over_tensor(over_dp(d_attended, context), 1),
        over_tensor(over_dp(normed_one, d_lin[:, :fixed]), 0),
        over_tensor(ffn_part, 0),
        lax.psum(small, ("dp", "tensor")),
    )


def branch_back(
    tokens, cosine, sine, mask, att_w, cot_rows, rows_two, hidden_low, d_gate, d_upper, ffn_part,
    d_normed_two, cotangent, middle, normed_one, query_rot, kv_win, lse, context, gains,
):
    f32, bf16 = jnp.float32, jnp.bfloat16
    rows = tokens.shape[0]
    kv_width, query_width = kv_win.shape[1] // 2, query_rot.shape[1]
    qkv_width = 2 * kv_width + query_width
    ahead = att_w.shape[1] - qkv_width - query_width
    heads, padded = query_width // HEAD_DIM, hidden_low.shape[1]
    if lax.axis_size("dp") == 8 and lax.axis_size("tensor") == 4:
        turn = jnp.stack(
            [jnp.concatenate([cosine, cosine], axis=1), jnp.concatenate([-sine, sine], axis=1)]
        )
        flat, sum_query, sum_out, sum_kv, mixed, input_grad, small = back(
            rows_two, cot_rows, hidden_low, d_gate, d_upper, ffn_part, d_normed_two, tokens, middle, gains,
            att_w, query_rot, kv_win.reshape(-1, rows, 2 * kv_width), lse, context, normed_one, mask, turn,
        )
        flat = [flat[:, k * padded : (k + 1) * padded] for k in range(3)]
        return mixed, input_grad, *flat, sum_query, sum_out, sum_kv, small[0]
    group = heads // KV_HEADS
    window = kv_win.shape[0]
    back_chunks = window // rows - 1
    scale = HEAD_DIM ** (-0.5)
    cos_h, sin_h = cosine[:, None, :], sine[:, None, :]
    d_normed_two = d_normed_two.astype(f32)
    qkv_w = att_w[:, ahead : ahead + qkv_width]
    out_full = att_w[:, ahead + qkv_width :]
    inputs = tokens.astype(f32)
    inverse_one = lax.rsqrt(jnp.mean(inputs * inputs, axis=-1, keepdims=True) + EPSILON)
    unit_one = inputs * inverse_one
    inverse_two = lax.rsqrt(jnp.mean(middle * middle, axis=-1, keepdims=True) + EPSILON)
    unit_two = middle * inverse_two
    gain_two_term, d_from_two = norm_back(d_normed_two, unit_two, inverse_two, gains[1])
    d_middle = cotangent.astype(f32) + d_from_two
    d_attended = d_middle.astype(bf16)
    d_context = jnp.dot(d_attended, out_full, preferred_element_type=f32).astype(bf16)
    d_context = d_context.reshape(rows, KV_HEADS, group, HEAD_DIM)
    key_win = kv_win[:, :kv_width].reshape(window, KV_HEADS, HEAD_DIM)
    value_win = kv_win[:, kv_width:].reshape(window, KV_HEADS, HEAD_DIM)
    grouped = query_rot.reshape(rows, KV_HEADS, group, HEAD_DIM)
    scores = jnp.einsum("tagd,sad->agts", grouped, key_win, preferred_element_type=f32) * scale + mask
    probs = jnp.exp(scores - lse.reshape(KV_HEADS, group, rows, 1))
    probs_low = probs.astype(bf16)
    d_probs = jnp.einsum("tagd,sad->agts", d_context, value_win, preferred_element_type=f32)
    row_delta = jnp.sum(probs * d_probs, axis=-1, keepdims=True)
    d_scores = (probs * (d_probs - row_delta)).astype(bf16)
    d_query_rot = jnp.einsum("agts,sad->tagd", d_scores, key_win, preferred_element_type=f32) * scale
    d_key_win = jnp.einsum("agts,tagd->sad", d_scores, grouped, preferred_element_type=f32) * scale
    d_value_win = jnp.einsum("agts,tagd->sad", probs_low, d_context, preferred_element_type=f32)
    d_query_lin = (
        rotate_back(d_query_rot.reshape(rows, heads, HEAD_DIM), cos_h, sin_h)
        .reshape(rows, query_width).astype(bf16)
    )
    d_kv_win = jnp.concatenate(
        [d_key_win.reshape(window, kv_width), d_value_win.reshape(window, kv_width)], axis=1
    ).astype(bf16)
    d_kv = d_kv_win[back_chunks * rows :].astype(f32)
    for hops in range(1, back_chunks + 1):
        given = d_kv_win[(back_chunks - hops) * rows : (back_chunks - hops + 1) * rows]
        d_kv = d_kv + shift(given, -hops).astype(f32)
    d_key_lin = rotate_back(d_kv[:, :kv_width].reshape(rows, KV_HEADS, HEAD_DIM), cos_h, sin_h)
    d_lin = jnp.concatenate(
        [d_key_lin.reshape(rows, kv_width).astype(bf16), d_kv[:, kv_width:].astype(bf16), d_query_lin],
        axis=1,
    )
    d_normed_one = contract_cols(d_lin, qkv_w)
    bias_term = jnp.sum(d_lin.astype(f32), axis=0)
    gain_one_term, d_from_one = norm_back(d_normed_one, unit_one, inverse_one, gains[0])
    input_grad = (d_middle + d_from_one).astype(bf16)

    sums = sum_grads(
        rows_two, cot_rows, hidden_low, d_gate, d_upper, normed_one, d_attended, d_lin, context,
        ffn_part, jnp.concatenate([bias_term[2 * kv_width :], bias_term[: 2 * kv_width], gain_one_term, gain_two_term]),
    )
    sum_down, sum_gate, sum_up, sum_query, sum_out, sum_kv, ffn_sum, small = sums
    mixed = (middle + ffn_sum.astype(f32)).astype(bf16)
    return mixed, input_grad, sum_down, sum_gate, sum_up, sum_query, sum_out, sum_kv, small


def local(
    tokens, segments, gain_one, query_w, query_b, key_w, key_b, value_w, value_b,
    out_w, gain_two, gate_w, up_w, down_w, cotangent,
):
    bf16, f32 = jnp.bfloat16, jnp.float32
    rows, model_width = tokens.shape
    tensor_size = lax.axis_size("tensor")
    rank = lax.axis_index("tensor")
    kv_width = key_w.shape[1]
    fixed_width = 2 * kv_width
    query_width = query_w.shape[1] * tensor_size
    qkv_width = fixed_width + query_width
    units = gate_w.shape[1]
    back_chunks = min(tensor_size - 1, -(-DOC_MAX // rows))
    window = (back_chunks + 1) * rows
    cosine, sine = angle_tables(rank * rows, rows, HEAD_DIM)
    segment = segments[0]
    own_segment = lax.dynamic_slice_in_dim(segment, rank * rows, rows, 0)
    before = jnp.full((back_chunks * rows,), -1, segment.dtype)
    win_segment = lax.dynamic_slice_in_dim(jnp.concatenate([before, segment]), rank * rows, window, 0)
    own_pos = back_chunks * rows + jnp.arange(rows)
    win_pos = jnp.arange(window)
    allowed = (own_segment[:, None] == win_segment[None, :]) & (win_pos[None, :] <= own_pos[:, None])
    mask = jnp.where(allowed, 0.0, NEGATIVE).astype(f32)
    ahead = 128
    gains_w = jnp.pad(jnp.stack([gain_one, gain_two], axis=1), ((0, 0), (0, ahead - 2)))
    (
        att_w, ffn_w, cot_rows, normed_two, middle, normed_one, query_rot, kv_win, lse, context, gains,
    ) = attention_branch(
        tokens, cosine, sine, mask, gains_w, query_w, query_b, jnp.concatenate([key_w, value_w], axis=1),
        jnp.concatenate([key_b, value_b]).astype(f32), out_w, joined_units(gate_w, up_w, down_w), cotangent,
    )
    rows_two, hidden_low, d_gate, d_upper, ffn_part, d_normed_two = ffn(
        normed_two, cot_rows, ffn_w
    )
    mixed, input_grad, sum_down, sum_gate, sum_up, sum_query, sum_out, sum_kv, small = branch_back(
        tokens, cosine, sine, mask, att_w, cot_rows, rows_two, hidden_low, d_gate, d_upper, ffn_part,
        d_normed_two, cotangent, middle, normed_one, query_rot, kv_win, lse, context, gains,
    )
    place = lax.axis_index("dp") * tensor_size + rank
    devices = lax.axis_size("dp") * tensor_size

    def own(start, size):
        share = size // devices
        return lax.dynamic_slice_in_dim(small, start + place * share, share, 0)

    return (
        mixed,
        input_grad,
        own(qkv_width, model_width),
        sum_query,
        own(0, query_width),
        sum_kv[:, :kv_width],
        small[query_width : query_width + kv_width],
        sum_kv[:, kv_width : 2 * kv_width],
        small[query_width + kv_width : qkv_width],
        sum_out,
        own(qkv_width + model_width, model_width),
        sum_gate[:, :units],
        sum_up[:, :units],
        sum_down[:, :units],
    )


def solution(mesh):
    both = ("dp", "tensor")
    return jax.shard_map(
        local,
        mesh=mesh,
        in_specs=(
            P(both, None), P("dp", None), P("dp"), P("dp", "tensor"), P("tensor"), P("dp", None), P(),
            P("dp", None), P(), P("dp", "tensor"), P("dp"), P("dp", "tensor"), P("dp", "tensor"),
            P("dp", "tensor"), P(both, None),
        ),
        out_specs=(
            P(both, None), P(both, None), P(both), P("dp", "tensor"), P(both), P(both, None), P(),
            P(both, None), P(), P("dp", "tensor"), P(both), P("dp", "tensor"), P("dp", "tensor"),
            P("dp", "tensor"),
        ),
        check_vma=False,
    )
```

```python
import functools

import jax
import jax.numpy as jnp
from jax import lax
from jax.experimental import pallas as pl
from jax.experimental.pallas import tpu as pltpu
from jax.sharding import PartitionSpec as P

MESH = pl.DeviceIdType.MESH
KV_HEADS = 2
HEAD_DIM = 128
DOC_MAX = 512
EPSILON = 1e-06
ROPE_BASE = 1000000.0
NEGATIVE = -1e30


def square(d):
    core, x, y = d % 2, (d // 2) % 2, d // 4
    by_x, by_y = d + 2 - 4 * x, d + 4 - 8 * y
    return by_x, by_y, d + 1 - 2 * core, by_x + 4 - 8 * y


def front_body(
    x_ref, turn_ref, mask_ref, own_ref, ffn_ref, cot_ref,
    att_all, ffn_all, cot_all, two_all, mid_out, one_out, query_rot, kv_win, lse_out, ctx_out, gain_out,
    att_v, w_v, one_v, q_v, kv_v, ctx_v, mid_v, two_v,
    fill_sem, z_send, z_recv, cot_send, cot_recv, send, recv, keep_sem, w_sem, kv_send, kv_recv, save_sem,
    two_send, two_recv,
    *, pieces, order, lead,
):
    f32, bf16 = jnp.float32, jnp.bfloat16
    d, z = lax.axis_index("dp"), lax.axis_index("tensor")
    size = 4
    by_x, by_y, mate, across = square(d)
    rows = ffn_ref.shape[0]
    half = rows // 2
    part = (att_v.shape[1] - own_ref.shape[1]) // (2 * size - 2)
    fixed = own_ref.shape[1] - 2 * part
    chunk = cot_ref.shape[0]
    tall = own_ref.shape[0]
    query_ref, out_ref = own_ref.at[:, pl.ds(0, part)], own_ref.at[:, pl.ds(part, part)]
    fixed_ref = own_ref.at[pl.ds(0, rows), pl.ds(2 * part, fixed)]

    barrier = pltpu.get_barrier_semaphore()
    for peer in (by_x, by_y, mate):
        pl.semaphore_signal(barrier, inc=1, device_id={"dp": peer}, device_id_type=MESH)
    for hop in range(1, size):
        pl.semaphore_signal(
            barrier, inc=1, device_id={"tensor": (z + hop) % size}, device_id_type=MESH
        )

    def place(of, owner):
        return pl.ds(pl.multiple_of(fixed + of * size * part + owner * part, 128), part)

    fills = [pltpu.make_async_copy(fixed_ref, att_v.at[pl.ds(0, rows), pl.ds(0, fixed)], fill_sem.at[0])]
    for of, ref in enumerate((query_ref, out_ref)):
        fills.append(pltpu.make_async_copy(ref, att_v.at[:, place(of, z)], fill_sem.at[1 + of]))
    at = pl.ds(pl.multiple_of(z * chunk, chunk), chunk)
    fills.append(pltpu.make_async_copy(cot_ref, cot_all.at[at, :], fill_sem.at[3]))
    for copy in fills:
        copy.start()

    pl.semaphore_wait(barrier, 3 + size - 1)

    def z_copy(of, j, dz, own):
        ref = att_v.at[:, place(of, j)]
        return pltpu.make_async_remote_copy(
            src_ref=(query_ref, out_ref)[of] if own else ref, dst_ref=ref,
            send_sem=z_send.at[of, (dz + 1) // 2, j], recv_sem=z_recv.at[of, j],
            device_id={"tensor": z + dz}, device_id_type=MESH,
        )

    def z_start(of):
        for dz, there in ((-1, has_low), (1, has_high)):

            @pl.when(there)
            def _(dz=dz):
                z_copy(of, z, dz, True).start()

    def z_step(of, hop):
        for sign, onward in ((-1, has_high), (1, has_low)):
            j = z + sign * hop
            inside = (j >= 0) if sign == -1 else (j < size)

            @pl.when(inside)
            def _(j=j, sign=sign):
                z_copy(of, j, -sign, False).wait_recv()

            @pl.when(jnp.logical_and(inside, onward))
            def _(j=j, sign=sign):
                z_copy(of, j, -sign, False).start()

    has_low, has_high = z > 0, z < size - 1

    def cot_copy(j, dz):
        ref = cot_all.at[pl.ds(pl.multiple_of(j * chunk, chunk), chunk), :]
        return pltpu.make_async_remote_copy(
            src_ref=ref, dst_ref=ref, send_sem=cot_send.at[(dz + 1) // 2, j], recv_sem=cot_recv.at[j],
            device_id={"tensor": z + dz}, device_id_type=MESH,
        )

    def cot_start():
        fills[3].wait()
        for dz, there in ((-1, has_low), (1, has_high)):

            @pl.when(there)
            def _(dz=dz):
                cot_copy(z, dz).start()

    def cot_step(hop):
        for sign, onward in ((-1, has_high), (1, has_low)):
            j = z + sign * hop
            inside = (j >= 0) if sign == -1 else (j < size)

            @pl.when(inside)
            def _(j=j, sign=sign):
                cot_copy(j, -sign).wait_recv()

            @pl.when(jnp.logical_and(inside, onward))
            def _(j=j, sign=sign):
                cot_copy(j, -sign).start()

    def two_copy(j, dz, own):
        ref = two_all.at[pl.ds(pl.multiple_of(j * chunk, chunk), chunk), :]
        return pltpu.make_async_remote_copy(
            src_ref=two_v if own else ref, dst_ref=ref, send_sem=two_send.at[(dz + 1) // 2, j],
            recv_sem=two_recv.at[j], device_id={"tensor": z + dz}, device_id_type=MESH,
        )

    def two_start():
        for dz, there in ((-1, has_low), (1, has_high)):

            @pl.when(there)
            def _(dz=dz):
                two_copy(z, dz, True).start()

    def two_step(hop):
        for sign, onward in ((-1, has_high), (1, has_low)):
            j = z + sign * hop
            inside = (j >= 0) if sign == -1 else (j < size)

            @pl.when(inside)
            def _(j=j, sign=sign):
                two_copy(j, -sign, False).wait_recv()

            if hop == 1:

                @pl.when(jnp.logical_and(inside, onward))
                def _(j=j, sign=sign):
                    two_copy(j, -sign, False).start()

    for of in range(2):
        z_start(of)
    fills[0].wait()

    def views(kind, p):
        src, dst = ((att_v, att_all), (ffn_ref, ffn_all))[kind]
        return src, dst, pl.ds(*pieces[kind][p])

    def slot(kind, p):
        return p + kind * len(pieces[0])

    def block(dst, cols, owner, first=0, many=None):
        many = rows if many is None else many
        return dst.at[pl.ds(pl.multiple_of(owner * rows + first, 16), many), cols]

    def remote(src, dst, way, at_slot, peer):
        return pltpu.make_async_remote_copy(
            src_ref=src, dst_ref=dst, send_sem=send.at[way, at_slot], recv_sem=recv.at[way, at_slot],
            device_id={"dp": peer}, device_id_type=MESH,
        )

    def own(kind, p):
        src, dst, cols = views(kind, p)
        mine = src.at[pl.ds(0, rows), cols]
        there = block(dst, cols, d)
        s = slot(kind, p)
        return [
            remote(mine, there, 0, s, by_x), remote(mine, there, 1, s, by_y),
            remote(mine, there, 2, s, mate),
        ], pltpu.make_async_copy(mine, there, keep_sem.at[s])

    def relays(kind, p, group):
        _, dst, cols = views(kind, p)
        s = slot(kind, p)
        if group == 2:
            whole = block(dst, cols, across)
            return [remote(whole, whole, 7, s, mate)]
        owner, peer = ((by_x, by_y), (by_y, by_x))[group]
        piece, whole = block(dst, cols, owner, group * half, half), block(dst, cols, owner)
        way = 3 + 2 * group
        return [remote(piece, piece, way, s, peer), remote(whole, whole, way + 1, s, mate)]

    def arrived(kind, p, way):
        _, dst, cols = views(kind, p)
        many = half if way in (3, 5) else rows
        ref = block(dst, cols, d, 0, many)
        pltpu.make_async_copy(ref, ref, recv.at[way, slot(kind, p)]).wait()

    def begin(kind, p):
        copies, keep = own(kind, p)
        for copy in copies:
            copy.start()
        keep.start()

    def pass_on(kind, p):
        for group in range(2):
            arrived(kind, p, group)
            for copy in relays(kind, p, group):
                copy.start()

    def close(kind, p):
        arrived(kind, p, 3)
        arrived(kind, p, 5)
        relays(kind, p, 2)[0].start()

    def settle(kind, p):
        for way in (2, 4, 6, 7):
            arrived(kind, p, way)
        own(kind, p)[1].wait()

    def finish(kind, p):
        copies = own(kind, p)[0]
        for group in range(3):
            copies = copies + relays(kind, p, group)
        for copy in copies:
            copy.wait_send()

    state = {"begun": 0, "query": False, "out": False}

    def ready(kind, p):
        end = sum(pieces[kind][p])
        if kind == 1 or end <= fixed:
            return
        need = 1 if end <= fixed + size * part else 2
        for of in range(need):
            if not state[("query", "out")[of]]:
                state[("query", "out")[of]] = True
                fills[1 + of].wait()
                if of == 1:
                    cot_start()

    def weight_load(p):
        cols = pl.ds(*pieces[0][p])
        return pltpu.make_async_copy(att_all.at[:, cols], w_v.at[:, cols], w_sem.at[p])

    def take(first, last):
        for p in range(first, last):
            settle(0, p)
            weight_load(p).start()

    def held(first, last):
        for p in range(first, last):
            weight_load(p).wait()

    saves = []

    def save(src, dst):
        copy = pltpu.make_async_copy(src, dst, save_sem.at[len(saves)])
        copy.start()
        saves.append(copy)

    part_rows = max(16, chunk // 4)

    def norm(value_of, row, dst):
        gain = gain_out[row : row + 1, :]

        def some(r, carry):
            at_r = pl.ds(pl.multiple_of(r * part_rows, part_rows), part_rows)
            value = value_of(at_r)
            inverse = lax.rsqrt(jnp.mean(value * value, axis=-1, keepdims=True) + EPSILON)
            dst[at_r, :] = (value * inverse * gain).astype(bf16)
            return carry

        lax.fori_loop(0, chunk // part_rows, some, 0)

    def turned(value):
        return value * turn_ref[0] + pltpu.roll(value, HEAD_DIM // 2, 1) * turn_ref[1]

    lead_w = fixed - 2 * KV_HEADS * HEAD_DIM
    kv_w = KV_HEADS * HEAD_DIM
    heads = size * part // HEAD_DIM
    scale = HEAD_DIM ** (-0.5)

    def kv_copy(hop):
        return pltpu.make_async_remote_copy(
            src_ref=kv_v.at[2], dst_ref=kv_v.at[2 - hop], send_sem=kv_send.at[hop - 1],
            recv_sem=kv_recv.at[hop - 1], device_id={"tensor": z + hop}, device_id_type=MESH,
        )

    def keys():
        pick = (
            lax.broadcasted_iota(jnp.int32, (8, lead_w), 0)
            == lax.broadcasted_iota(jnp.int32, (8, lead_w), 1)
        ).astype(bf16)
        gain_out[...] = lax.dot_general(
            pick, w_v[:, :lead_w], (((1,), (1,)), ((), ())), preferred_element_type=f32
        )
        norm(lambda at_r: x_ref[at_r, :].astype(f32), 0, one_v)
        save(one_v, one_out)
        lin = jnp.dot(one_v[...], w_v[:, lead_w:fixed], preferred_element_type=f32)
        lin += own_ref[rows:, 2 * part + lead_w :][0:1, :].astype(f32)
        for g in range(KV_HEADS):
            cols = slice(g * HEAD_DIM, (g + 1) * HEAD_DIM)
            kv_v[2, :, cols] = turned(lin[:, cols]).astype(bf16)
        kv_v[2, :, kv_w:] = lin[:, kv_w:].astype(bf16)
        for hop in (1, 2):

            @pl.when(z + hop < size)
            def _(hop=hop):
                kv_copy(hop).start()

            @pl.when(z < hop)
            def _(hop=hop):
                kv_v[2 - hop] = jnp.zeros(kv_v.shape[1:], bf16)

    per = pieces[0][1][1] // HEAD_DIM

    def queries(first):
        def pair(k, carry):
            h = first + 2 * k
            cols = pl.ds(pl.multiple_of(h * HEAD_DIM, 128), 2 * HEAD_DIM)
            from_w = pl.ds(pl.multiple_of(fixed + h * HEAD_DIM, 128), 2 * HEAD_DIM)
            lin = jnp.dot(one_v[...], w_v[:, from_w], preferred_element_type=f32)
            lin += att_v[pl.ds(rows, 16), from_w][0:1, :].astype(f32)
            q_v[:, cols] = jnp.concatenate(
                [turned(lin[:, :HEAD_DIM]), turned(lin[:, HEAD_DIM:])], axis=1
            ).astype(bf16)
            return carry

        lax.fori_loop(0, per // 2, pair, 0)

    def kv_wait():
        for hop in (1, 2):

            @pl.when(z >= hop)
            def _(hop=hop):
                pltpu.make_async_copy(kv_v.at[2 - hop], kv_v.at[2 - hop], kv_recv.at[hop - 1]).wait()

        save(kv_v, kv_win)

    def attend(first, last):
        def head(h, carry):
            cols = pl.ds(pl.multiple_of(h * HEAD_DIM, 128), HEAD_DIM)
            group = h // (heads // KV_HEADS)
            key_cols = pl.ds(pl.multiple_of(group * HEAD_DIM, 128), HEAD_DIM)
            value_cols = pl.ds(pl.multiple_of(kv_w + group * HEAD_DIM, 128), HEAD_DIM)
            key = kv_v[:, :, key_cols].reshape(3 * chunk, HEAD_DIM)
            value = kv_v[:, :, value_cols].reshape(3 * chunk, HEAD_DIM)
            scores = lax.dot_general(
                q_v[:, cols], key, (((1,), (1,)), ((), ())), preferred_element_type=f32
            )
            scores = scores * scale + mask_ref[...]
            largest = jnp.max(scores, axis=-1, keepdims=True)
            powers = jnp.exp(scores - largest)
            mass = jnp.sum(powers, axis=-1, keepdims=True)
            lse_out[h] = largest + jnp.log(mass)
            probs = (powers * (1.0 / mass)).astype(bf16)
            ctx_v[:, cols] = jnp.dot(probs, value, preferred_element_type=f32).astype(bf16)
            return carry

        lax.fori_loop(first, last, head, 0)

    def project(k):
        tile = min(512, w_v.shape[0])
        wide = per * HEAD_DIM

        def some(n, carry):
            at_n = pl.ds(pl.multiple_of(n * tile, tile), tile)
            added = lax.dot_general(
                ctx_v[:, k * wide : (k + 1) * wide],
                w_v[at_n, fixed + size * part + k * wide : fixed + size * part + (k + 1) * wide],
                (((1,), (1,)), ((), ())), preferred_element_type=f32,
            )
            so_far = mid_v[:, at_n] if k else x_ref[:, at_n].astype(f32)
            mid_v[:, at_n] = so_far + added
            return carry

        lax.fori_loop(0, w_v.shape[0] // tile, some, 0)

    def second_norm():
        norm(lambda at_r: mid_v[at_r, :], 1, two_v)
        save(two_v, two_all.at[at, :])
        two_start()
        save(mid_v, mid_out)
        save(q_v, query_rot)
        save(ctx_v, ctx_out)

    n_att = len(pieces[0])
    n_q = (n_att - 1) // 2
    when_q, when_out = [[order.index((0, 1 + of * n_q + k)) for k in range(n_q)] for of in range(2)]
    last_q, last_out = when_q[-1], when_out[-1]
    work = [(2, lambda: take(0, 1)), (2, lambda: held(0, 1)), (2, keys)]
    work += [(last_q + 1, lambda: cot_step(1)), (last_q + 4, lambda: cot_step(2)), (last_q + 6, lambda: cot_step(3))]
    work += [(when_q[0] + 2, kv_wait)]
    for k in range(n_q):
        work += [
            (when_q[k] + 2, lambda k=k: take(1 + k, 2 + k)), (when_q[k] + 3, lambda k=k: held(1 + k, 2 + k)),
            (when_q[k] + 3, lambda k=k: queries(k * per)),
            (when_q[k] + 3, lambda k=k: attend(k * per, (k + 1) * per)),
        ]
        late = 3 if k < n_q - 1 else 2
        work += [
            (when_out[k] + 2, lambda k=k: take(1 + n_q + k, 2 + n_q + k)),
            (when_out[k] + late, lambda k=k: held(1 + n_q + k, 2 + n_q + k)),
            (when_out[k] + late, lambda k=k: project(k)),
        ]
    work += [
        (last_out + 2, second_norm), (last_out + 5, lambda: two_step(1)), (last_out + 20, lambda: two_step(2)),
    ]
    work.sort(key=lambda step: step[0])
    total = len(order)
    for i in range(total + 1):
        while state["begun"] < min(total, i + lead):
            ready(*order[state["begun"]])
            begin(*order[state["begun"]])
            state["begun"] += 1
        if i == 0:
            for hop in range(1, size):
                for of in range(2):
                    z_step(of, hop)
                if hop < size - 1:
                    pass_on(*order[hop - 1])
        if size - 2 <= i < total:
            pass_on(*order[i])
        if i > 0:
            close(*order[i - 1])
        while work and (work[0][0] <= i or i == total):
            work.pop(0)[1]()
    for kind, p in order:
        if kind == 1:
            settle(kind, p)
    for kind, p in order:
        finish(kind, p)
    for copy in saves:
        copy.wait()
    for hop in (1, 2):

        @pl.when(z + hop < size)
        def _(hop=hop):
            kv_copy(hop).wait_send()

    for j in range(size):
        for dz, there in ((-1, has_low), (1, has_high)):
            came = jnp.logical_and((z <= j) if dz == -1 else (z >= j), there)

            @pl.when(came)
            def _(j=j, dz=dz):
                cot_copy(j, dz).wait_send()
                for of in range(2):
                    z_copy(of, j, dz, False).wait_send()

            near = jnp.logical_and(came, (j - z <= 1) if dz == -1 else (z - j <= 1))

            @pl.when(near)
            def _(j=j, dz=dz):
                two_copy(j, dz, False).wait_send()


def front(
    tokens, turn, mask, own, ffn_w, cot, fixed_w, att_tile=512, ffn_tile=768,
    collective_id=2, limit=60_000_000,
):
    tall, rows, size, ways = own.shape[0], ffn_w.shape[0], 4, 8
    part = (own.shape[1] - fixed_w) // 2
    chunk, width = tokens.shape
    query_w = size * part
    att_cols = fixed_w + 2 * query_w
    pieces = (
        [(0, fixed_w)] + [(fixed_w + p * att_tile, att_tile) for p in range(2 * query_w // att_tile)],
        [(p * ffn_tile, ffn_tile) for p in range(ffn_w.shape[1] // ffn_tile)],
    )
    n_att, n_ffn = len(pieces[0]), len(pieces[1])
    early = min(2, n_ffn)
    order = [(0, 0)] + [(1, p) for p in range(early)] + [(0, p) for p in range(1, n_att)]
    order += [(1, p) for p in range(early, n_ffn)]
    bf16, f32 = jnp.bfloat16, jnp.float32
    hbm = pl.BlockSpec(memory_space=pl.ANY)
    vmem = pl.BlockSpec(memory_space=pltpu.VMEM)
    vm = pltpu.VMEM
    dma = pltpu.SemaphoreType.DMA
    shape = lambda *s: jax.ShapeDtypeStruct(s, bf16)
    wide = lambda *s: jax.ShapeDtypeStruct(s, f32)
    slots = n_att + n_ffn
    kv_w = 2 * KV_HEADS * HEAD_DIM
    heads = query_w // HEAD_DIM
    return pl.pallas_call(
        functools.partial(front_body, pieces=pieces, order=order, lead=3),
        out_shape=(
            shape(8 * rows, att_cols), shape(8 * rows, ffn_w.shape[1]),
            shape(size * cot.shape[0], cot.shape[1]),
            shape(size * chunk, width), wide(chunk, width), shape(chunk, width), shape(chunk, query_w),
            shape(3, chunk, kv_w), wide(heads, chunk, 1), shape(chunk, query_w), wide(8, width),
        ),
        in_specs=[vmem] * 6,
        out_specs=(hbm,) * 8 + (vmem, hbm, vmem),
        scratch_shapes=[
            vm((tall, att_cols), bf16), vm((8 * rows, att_cols), bf16), vm((chunk, width), bf16),
            vm((chunk, query_w), bf16), vm((3, chunk, kv_w), bf16), vm((chunk, query_w), bf16),
            vm((chunk, width), f32), vm((chunk, width), bf16),
            dma((4,)), dma((2, 2, size)), dma((2, size)),
            dma((2, size)), dma((size,)), dma((ways, slots)), dma((ways, slots)), dma((slots,)),
            dma((n_att,)), dma((2,)), dma((2,)), dma((6,)), dma((2, size)), dma((size,)),
        ],
        compiler_params=pltpu.CompilerParams(
            collective_id=collective_id, has_side_effects=True, vmem_limit_bytes=limit
        ),
        cost_estimate=pl.CostEstimate(
            flops=2 * chunk * width * att_cols, bytes_accessed=20 * rows * (att_cols + ffn_w.shape[1]),
            transcendentals=0,
        ),
        name="front",
    )(tokens, turn, mask, own, ffn_w, cot)


def line_order(z, s):
    upper = z // 2
    near = z * (1 - upper) + (3 - z) * upper
    late = s // 2
    at = (1 - late) * (2 + s) + late * ((3 - s) * (1 - near) + (s - 2) * near)
    return at * (1 - upper) + (3 - at) * upper


def ffn_body(
    two_ref, cot_ref, weights_ref,
    rows_out, hid_out, dg_out, du_out, sum_out, dn_out,
    rows_v, cot_v, gate_v, up_v, down_v, hid_v, dg_v, du_v, part, land, below, above, res_v,
    tile_sem, load_sem, row_sem, ag_send, ag_recv, rs_send, rs_recv, own_recv, out_sem,
    *, axis, ft, nt,
):
    f32, bf16 = jnp.float32, jnp.bfloat16
    size = 4
    rows, width = two_ref.shape[0] // size, two_ref.shape[1]
    units = weights_ref.shape[1] // 3
    n_f, n_n = units // ft, width // nt
    z = lax.axis_index(axis)
    has_low, has_high = z > 0, z < size - 1

    def to(dz):
        return {axis: z + dz}

    barrier = pltpu.get_barrier_semaphore()

    @pl.when(has_low)
    def _():
        pl.semaphore_signal(barrier, inc=1, device_id=to(-1), device_id_type=MESH)

    @pl.when(has_high)
    def _():
        pl.semaphore_signal(barrier, inc=1, device_id=to(1), device_id_type=MESH)

    def chunk_rows(j):
        return two_ref.at[pl.ds(pl.multiple_of(j * rows, rows), rows), :]

    def far(j):
        return jnp.logical_or(j - z == 3, z - j == 3)

    def row_load(j):
        return pltpu.make_async_copy(chunk_rows(j), rows_v.at[j], row_sem.at[j])

    def load_rows(s):
        j = line_order(z, s)

        @pl.when(jnp.logical_not(far(j)))
        def _():
            row_load(j).start()

    load_rows(0)

    def tile_loads(f):
        cols = pl.ds(pl.multiple_of(f * ft, 128), ft)
        return [
            pltpu.make_async_copy(
                weights_ref.at[:, pl.ds(pl.multiple_of(k * units + f * ft, 128), ft)],
                dst.at[:, cols], tile_sem.at[k, f],
            )
            for k, dst in enumerate((gate_v, up_v, down_v))
        ]

    cot_load = pltpu.make_async_copy(cot_ref, cot_v, load_sem.at[1])
    for f in range(n_f):
        for copy in tile_loads(f):
            copy.start()
        if f == 0:
            cot_load.start()
            for s in range(1, size):
                load_rows(s)

    pl.semaphore_wait(barrier, (z + size - 1) // size + (2 * size - 2 - z) // size)

    def far_copy():
        j = 3 - 3 * (z // 2)
        return pltpu.make_async_remote_copy(
            src_ref=chunk_rows(j), dst_ref=rows_v.at[j], send_sem=ag_send.at[0], recv_sem=ag_recv.at[0],
            device_id=to(2 * (z // 2) - 1), device_id_type=MESH,
        )

    middle = jnp.logical_and(has_low, has_high)

    @pl.when(middle)
    def _():
        far_copy().start()

    def rs_copy(j, n, dz, own):
        way = (dz + 1) // 2
        if own:
            dst = below.at[n] if dz == 1 else above.at[n]
            sem = own_recv.at[1 - way, n]
        else:
            dst, sem = land.at[j, n], rs_recv.at[j, n]
        return pltpu.make_async_remote_copy(
            src_ref=part.at[j, n], dst_ref=dst, send_sem=rs_send.at[j, n],
            recv_sem=sem, device_id=to(dz), device_id_type=MESH,
        )

    def pass_on(j, n, what):
        for dz in (1, -1):
            for own in (True, False):
                hop = j == z + dz
                going = (j > z) if dz == 1 else (j < z)
                near = hop if own else jnp.logical_not(hop)

                @pl.when(jnp.logical_and(going, near))
                def _(dz=dz, own=own):
                    copy = rs_copy(j, n, dz, own)
                    copy.start() if what == "start" else copy.wait_send()

    def out_copies(j):
        at = pl.ds(pl.multiple_of(j * rows, rows), rows)
        return [
            pltpu.make_async_copy(src.at[j], dst.at[at, :], out_sem.at[k, j])
            for k, (src, dst) in enumerate(
                ((rows_v, rows_out), (hid_v, hid_out), (dg_v, dg_out), (du_v, du_out))
            )
        ]

    def forward(j, n):
        pltpu.make_async_copy(land.at[j, n], land.at[j, n], rs_recv.at[j, n]).wait()
        part[j, n] = (part[j, n].astype(f32) + land[j, n].astype(f32)).astype(bf16)
        pass_on(j, n, "start")

    def forward_all(j):
        def some(n, carry):
            forward(j, n)
            return carry

        lax.fori_loop(0, n_n, some, 0)

    def step(s, carry):
        j = line_order(z, s)

        @pl.when(far(j))
        def _():
            pltpu.make_async_copy(rows_v.at[j], rows_v.at[j], ag_recv.at[0]).wait()

        @pl.when(jnp.logical_not(far(j)))
        def _():
            row_load(j).wait()

        at = pl.ds(pl.multiple_of(j * rows, rows), rows)

        @pl.when(s == 0)
        def _():
            cot_load.wait()

        def units_tile(f, carry):
            @pl.when(s == 0)
            def _():
                for copy in tile_loads(f):
                    copy.wait()

            cols = pl.ds(pl.multiple_of(f * ft, 128), ft)
            mine = rows_v[j]
            gate = jnp.dot(mine, gate_v[:, cols], preferred_element_type=f32)
            upper = jnp.dot(mine, up_v[:, cols], preferred_element_type=f32)
            d_hidden = jnp.dot(cot_v[at, :], down_v[:, cols], preferred_element_type=f32)
            sig = 1.0 / (1.0 + jnp.exp(-gate))
            act = gate * sig
            hid_v[j, :, cols] = (act * upper).astype(bf16)
            du_v[j, :, cols] = (d_hidden * act).astype(bf16)
            dg_v[j, :, cols] = (d_hidden * upper * (sig + act * (1.0 - sig))).astype(bf16)
            return carry

        lax.fori_loop(0, n_f, units_tile, 0)
        for copy in out_copies(j):
            copy.start()
        ends = jnp.logical_and(s < 3, jnp.logical_not(middle))

        @pl.when(jnp.logical_and(middle, s == 3))
        def _():
            forward_all(3 - z)
            forward_all(3 - 3 * (z // 2))


        def width_tile(n, carry):
            at_n = pl.ds(pl.multiple_of(n * nt, nt), nt)
            dims = (((1,), (1,)), ((), ()))
            total = lax.dot_general(dg_v[j], gate_v[at_n, :], dims, preferred_element_type=f32)
            total += lax.dot_general(du_v[j], up_v[at_n, :], dims, preferred_element_type=f32)
            part[j, n] = total.astype(bf16)

            @pl.when(ends)
            def _():
                pass_on(j, n, "start")

            return carry

        lax.fori_loop(0, n_n, width_tile, 0)
        return carry

    lax.fori_loop(0, size, step, 0)

    def down_tile(i, carry):
        j, n = i // n_n, i % n_n
        at_n = pl.ds(pl.multiple_of(n * nt, nt), nt)
        total = lax.dot_general(
            hid_v[j], down_v[at_n, :], (((1,), (1,)), ((), ())), preferred_element_type=f32
        )
        res_v[j, :, at_n] = total.astype(bf16)
        return carry

    tiles = size * n_n
    done = tiles // 3
    lax.fori_loop(0, done, down_tile, 0)
    for n in range(n_n):
        until = tiles if n == n_n - 1 else done + (n + 1) * (tiles - done) // n_n

        @pl.when(middle)
        def _(n=n):
            forward(3 * (z // 2), n)

        lax.fori_loop(done + n * (tiles - done) // n_n, until, down_tile, 0)
    sum_copies = [
        pltpu.make_async_copy(
            res_v.at[j], sum_out.at[pl.ds(j * rows, rows), :], load_sem.at[2 + j]
        )
        for j in range(size)
    ]
    for copy in sum_copies:
        copy.start()

    def last(n, carry):
        @pl.when(has_low)
        def _():
            pltpu.make_async_copy(below.at[n], below.at[n], own_recv.at[0, n]).wait()
            part[z, n] = (part[z, n].astype(f32) + below[n].astype(f32)).astype(bf16)

        @pl.when(has_high)
        def _():
            pltpu.make_async_copy(above.at[n], above.at[n], own_recv.at[1, n]).wait()
            part[z, n] = (part[z, n].astype(f32) + above[n].astype(f32)).astype(bf16)

        dn_out[:, pl.ds(pl.multiple_of(n * nt, nt), nt)] = part[z, n]
        return carry

    lax.fori_loop(0, n_n, last, 0)

    def drain(j, carry):
        for copy in out_copies(j):
            copy.wait()
        def sent(n, carry):
            @pl.when(j != z)
            def _():
                pltpu.make_async_copy(part.at[j, n], part.at[j, n], rs_send.at[j, n]).wait()

            return carry

        lax.fori_loop(0, n_n, sent, 0)
        return carry

    lax.fori_loop(0, size, drain, 0)

    @pl.when(middle)
    def _():
        far_copy().wait_send()

    for copy in sum_copies:
        copy.wait()


def ffn(two, cot_rows, weights, axis="tensor", ft=768, nt=512, collective_id=1, limit=66_000_000):
    size = 4
    length, width = two.shape
    rows = length // size
    units = weights.shape[1] // 3
    n_f, n_n = units // ft, width // nt
    bf16 = jnp.bfloat16
    hbm = pl.BlockSpec(memory_space=pl.ANY)
    vm = pltpu.VMEM
    dma = pltpu.SemaphoreType.DMA
    shape = lambda *s: jax.ShapeDtypeStruct(s, bf16)
    return pl.pallas_call(
        functools.partial(ffn_body, axis=axis, ft=ft, nt=nt),
        out_shape=(
            shape(length, width), shape(length, units), shape(length, units), shape(length, units),
            shape(length, width), shape(rows, width),
        ),
        in_specs=[hbm] * 3,
        out_specs=(hbm,) * 5 + (pl.BlockSpec(memory_space=pltpu.VMEM),),
        scratch_shapes=[
            vm((size, rows, width), bf16), vm((length, width), bf16),
            vm((width, units), bf16), vm((width, units), bf16), vm((width, units), bf16),
            vm((size, rows, units), bf16), vm((size, rows, units), bf16), vm((size, rows, units), bf16),
            vm((size, n_n, rows, nt), bf16), vm((size, n_n, rows, nt), bf16),
            vm((n_n, rows, nt), bf16), vm((n_n, rows, nt), bf16),
            vm((size, rows, width), bf16),
            dma((3, n_f)), dma((2 + size,)), dma((size,)), dma((1,)), dma((1,)), dma((size, n_n)), dma((size, n_n)),
            dma((2, n_n)), dma((4, size)),
        ],
        compiler_params=pltpu.CompilerParams(
            collective_id=collective_id, has_side_effects=True, vmem_limit_bytes=limit
        ),
        cost_estimate=pl.CostEstimate(
            flops=12 * length * width * units, bytes_accessed=8 * width * units + 8 * length * units,
            transcendentals=length * units,
        ),
        name="ffn",
    )(two, cot_rows, weights)


def back_body(
    two_ref, cot_ref, hid_ref, dg_ref, du_ref, part_ref, up_ref, x_ref, mid_ref, gain_ref, att_ref,
    query_ref, win_ref, lse_ref, ctx_ref, one_ref, mask_ref, turn_ref,
    ffn_out, query_out, out_out, kv_out, mixed_out, input_out, small_out,
    up_v, own_v, mid_v, gain_v, w_v, query_v, win_v, lse_v, mask_v, turn_v, lhs_ref, rhs_ref,
    d_mid, d_ctx, d_win, kv_give, kv_take, small_ref,
    left_v, right_v, grad, mate_land, core_sum, x_land, y_land, second, x_last, y_last, stage, fin,
    z_land, kv_land, fold_land, fold_last, fold_own, small_z, small_hop, small_next, in_sem, give_send, give_recv,
    left_sem, right_sem, mate_send, mate_recv, one_send, one_recv, two_send, two_recv, stage_sem,
    z_send, z_recv, kv_send, kv_recv, fold_send, fold_recv, last_recv, own_sem, small_send, small_recv,
    hop_send, hop_recv, *, n_f, wide,
):
    f32, bf16 = jnp.float32, jnp.bfloat16
    d, z = lax.axis_index("dp"), lax.axis_index("tensor")
    size = 4
    core, x, y = d % 2, (d // 2) % 2, d // 4
    by_x, by_y, mate, _ = square(d)
    here, at_x, at_y = 2 * y + x, 2 * y + 1 - x, 2 * (1 - y) + x
    cross = 3 - here
    block, half = core_sum.shape[2], core_sum.shape[2] // 2
    n_ffn, n_att = 3 * n_f, rhs_ref.shape[1] // wide
    ring, n_sum, n_last = x_land.shape[0], core_sum.shape[0], x_last.shape[0]
    n_grad, n_mate = grad.shape[0], mate_land.shape[0]
    total = n_ffn + n_att
    cut = n_ffn - 1
    chunk, width = mixed_out.shape
    share = block // size
    part_w = wide // 2

    barrier = pltpu.get_barrier_semaphore()
    for peer in (by_x, by_y, mate):
        pl.semaphore_signal(barrier, inc=1, device_id={"dp": peer}, device_id_type=MESH)
    for hop in range(1, size):
        pl.semaphore_signal(
            barrier, inc=1, device_id={"tensor": (z + hop) % size}, device_id_type=MESH
        )

    lefts = [
        pltpu.make_async_copy(ref, left_v, left_sem.at[k]) for k, ref in enumerate((cot_ref, two_ref))
    ]
    query_w = query_ref.shape[1]
    kv_w = KV_HEADS * HEAD_DIM
    heads = query_w // HEAD_DIM
    scale = HEAD_DIM ** (-0.5)
    ahead = att_ref.shape[1] - 2 * query_w - 2 * kv_w
    own_rows = pl.ds(pl.multiple_of(z * chunk, chunk), chunk)
    ctx_cols = pl.ds(query_w, query_w)
    plan = (
        (up_ref, up_v), (cot_ref.at[own_rows, :], own_v), (mid_ref, mid_v), (gain_ref, gain_v),
        (att_ref.at[:, pl.ds(ahead + 2 * kv_w + query_w, query_w)], w_v.at[:, pl.ds(0, query_w)]),
        (query_ref, query_v), (win_ref, win_v), (lse_ref, lse_v), (mask_ref, mask_v), (turn_ref, turn_v),
        (ctx_ref, rhs_ref.at[:, ctx_cols]), (one_ref, lhs_ref.at[0]), (x_ref, up_v),
        (att_ref.at[:, pl.ds(ahead, 2 * kv_w + query_w)], w_v),
    )
    loads = [pltpu.make_async_copy(src, dst, in_sem.at[k]) for k, (src, dst) in enumerate(plan)]

    def is_ffn(i):
        return jnp.logical_or(i < cut, i == total - 1)

    def ffn_piece(i):
        return i - (i // (total - 1)) * n_att

    def right_load(i, what):
        cols = pl.ds(pl.multiple_of((i % n_f) * wide, 128), wide)
        for m, ref in enumerate((hid_ref, dg_ref, du_ref)):
            copy = pltpu.make_async_copy(ref.at[:, cols], right_v.at[i % 2], right_sem.at[i % 2])

            @pl.when(i // n_f == m)
            def _(copy=copy):
                copy.start() if what == "start" else copy.wait()

    lefts[0].start()
    right_load(jnp.int32(0), "start")
    for copy in loads[:-2]:
        copy.start()

    def chunk_rows(j):
        return part_ref.at[pl.ds(pl.multiple_of(j * chunk, chunk), chunk), :]

    upper = z // 2
    inward = 1 - 2 * upper
    middle = jnp.logical_and(z > 0, z < size - 1)

    def fold_load(j):
        return pltpu.make_async_copy(chunk_rows(j), fold_own, own_sem.at[0])

    def fold_copy(k, first):
        if first:
            j = (3 - 3 * upper, 2 - upper, z + inward)[k]
            src, to = chunk_rows(j), z + inward
            dst = (fold_land.at[0], fold_land.at[1], fold_last.at[0])[k]
            sem = (fold_recv.at[0], fold_recv.at[1], last_recv.at[0])[k]
        else:
            src, to = fold_land.at[k], z + (inward, inward, -inward)[k]
            dst = (fold_land.at[2], fold_last.at[1], fold_last.at[1])[k]
            sem = (fold_recv.at[2], last_recv.at[1], last_recv.at[1])[k]
        return pltpu.make_async_remote_copy(
            src_ref=src, dst_ref=dst, send_sem=fold_send.at[k], recv_sem=sem,
            device_id={"tensor": to}, device_id_type=MESH,
        )

    def fold(k):
        @pl.when(middle)
        def _():
            pltpu.make_async_copy(fold_land.at[k], fold_land.at[k], fold_recv.at[k]).wait()
            fold_load(z).wait()
            fold_land[k] = (fold_land[k].astype(f32) + fold_own[...].astype(f32)).astype(bf16)
            fold_copy(k, False).start()
            fold_load((2 - upper, 3 * upper, z)[k]).start()
    pl.semaphore_wait(barrier, 3 + size - 1)

    def dp_copy(src, dst, send_sem, recv_sem, peer):
        return pltpu.make_async_remote_copy(
            src_ref=src, dst_ref=dst, send_sem=send_sem, recv_sem=recv_sem,
            device_id={"dp": peer}, device_id_type=MESH,
        )

    def z_copy(src, dst, send_sem, recv_sem, peer):
        return pltpu.make_async_remote_copy(
            src_ref=src, dst_ref=dst, send_sem=send_sem, recv_sem=recv_sem,
            device_id={"tensor": peer}, device_id_type=MESH,
        )

    small_copies = []
    for hop in range(1, size):
        to, k = (z + hop) % size, hop - 1
        small_copies.append(
            z_copy(small_ref, small_z.at[k], small_send.at[k], small_recv.at[k], to)
        )

    @pl.when(jnp.logical_not(middle))
    def _():
        for k in range(3):
            fold_copy(k, True).start()
        fold_load(z).start()

    @pl.when(middle)
    def _():
        fold_load(3 - 3 * upper).start()

    rhs_ref[:, 2 * query_w + 2 * kv_w :] = jnp.zeros((chunk, rhs_ref.shape[1] - 2 * query_w - 2 * kv_w), bf16)

    hops = (mate, by_x, by_y)

    def hop_copy(k):
        return dp_copy(small_next.at[k], small_hop.at[k], hop_send.at[k], hop_recv.at[k], hops[k])

    def mate_copy(i):
        return dp_copy(
            grad.at[i % n_grad, :, 1 - core], mate_land.at[i % n_mate], mate_send.at[i % n_mate],
            mate_recv.at[i % n_mate], mate,
        )

    def one_copies(i):
        s = core_sum.at[i % n_sum]
        first, last = pl.ds(0, half), pl.ds(half, half)
        plan = (
            (s.at[at_x, first, :], x_land.at[i % ring, 0], by_x), (s.at[cross, first, :], x_land.at[i % ring, 1], by_x),
            (s.at[at_y, last, :], y_land.at[i % ring, 0], by_y), (s.at[cross, last, :], y_land.at[i % ring, 1], by_y),
        )
        return [
            dp_copy(src, dst, one_send.at[k, i % ring], one_recv.at[k, i % ring], peer)
            for k, (src, dst, peer) in enumerate(plan)
        ]

    def two_copies(i):
        return [
            dp_copy(second.at[i % 2, 0], y_last.at[i % n_last], two_send.at[0, i % ring], two_recv.at[0, i % ring], by_y),
            dp_copy(second.at[i % 2, 1], x_last.at[i % n_last], two_send.at[1, i % ring], two_recv.at[1, i % ring], by_x),
        ]

    def stage_copy(i):
        cols = pl.ds(pl.multiple_of(i * wide, 128), wide)
        return pltpu.make_async_copy(stage.at[i % 2], ffn_out.at[:, cols], stage_sem.at[i % 2])

    def multiply(i):
        @pl.when(jnp.logical_and(i >= n_grad, i < total))
        def _():
            mate_copy(i - n_grad).wait_send()

        @pl.when(is_ffn(i + 1))
        def _():
            right_load(ffn_piece(i + 1), "start")

        dims = (((0,), (0,)), ((), ()))

        @pl.when(is_ffn(i))
        def _():
            f = ffn_piece(i)

            @pl.when(i == 0)
            def _():
                lefts[0].wait()

            @pl.when(i == n_f)
            def _():
                lefts[1].start()
                lefts[1].wait()

            right_load(f, "wait")

            def rows(k, carry):
                at = pl.ds(pl.multiple_of(k * 2 * block, 128), 2 * block)
                value = lax.dot_general(
                    left_v[:, at], right_v[f % 2], dims, preferred_element_type=f32
                )
                grad[i % n_grad, k] = value.astype(bf16).reshape(2, block, wide)
                return carry

            lax.fori_loop(0, 4, rows, 0)

        @pl.when(jnp.logical_and(i >= cut, i < total - 1))
        def _():
            a = i - cut
            cols = pl.ds(pl.multiple_of(a * wide, 128), wide)

            def rows(k, carry):
                at = pl.ds(pl.multiple_of(k * 2 * block, 128), 2 * block)
                value = lax.dot_general(
                    lhs_ref[(a // 2) % 2, :, at], rhs_ref[:, cols], dims, preferred_element_type=f32
                )
                grad[i % n_grad, k] = value.astype(bf16).reshape(2, block, wide)
                return carry

            lax.fori_loop(0, 4, rows, 0)

        @pl.when(i < total)
        def _():
            mate_copy(i).start()

    def sum_cores(i):
        mate_copy(i).wait_recv()
        for k in range(4):
            core_sum[i % n_sum, k] = (
                grad[i % n_grad, k, core].astype(f32) + mate_land[i % n_mate, k].astype(f32)
            ).astype(bf16)
        for copy in one_copies(i):
            copy.start()

    def sum_near(i):
        for copy in one_copies(i):
            copy.wait_recv()
        s = core_sum.at[i % n_sum]
        second[i % 2, 0] = (s[at_y, :half].astype(f32) + x_land[i % ring, 1].astype(f32)).astype(bf16)
        second[i % 2, 1] = (s[at_x, half:].astype(f32) + y_land[i % ring, 1].astype(f32)).astype(bf16)
        for copy in two_copies(i):
            copy.start()

    def z_sends(a, what):
        for h in range(2):
            owner = (a % 2) * 2 + h
            hop = (owner - z + size) % size
            src = fin.at[a, :, pl.ds(h * part_w, part_w)]

            @pl.when(jnp.logical_and(a < 4, hop > 0))
            def _(src=src, owner=owner, hop=hop, h=h):
                copy = z_copy(
                    src, z_land.at[a // 2, hop - 1], z_send.at[a, h], z_recv.at[a // 2, hop - 1], owner
                )
                copy.start() if what == "start" else copy.wait_send()

        @pl.when(a == 4)
        def _():
            for hop in range(1, size):
                to = (z + hop) % size
                rows = pl.ds(pl.multiple_of(to * share, 16), share)
                copy = z_copy(
                    fin.at[4, rows, :], kv_land.at[hop - 1], kv_send.at[hop - 1], kv_recv.at[hop - 1], to
                )
                copy.start() if what == "start" else copy.wait_send()

    def finish(i):
        for copy in two_copies(i):
            copy.wait_recv()
        own = core_sum.at[i % n_sum, here]
        top = own[:half].astype(f32) + x_land[i % ring, 0].astype(f32) + y_last[i % n_last].astype(f32)
        low = own[half:].astype(f32) + y_land[i % ring, 0].astype(f32) + x_last[i % n_last].astype(f32)

        @pl.when(is_ffn(i))
        def _():
            f = ffn_piece(i)

            @pl.when(f >= 2)
            def _():
                stage_copy(f - 2).wait()

            stage[f % 2, :half] = top
            stage[f % 2, half:] = low
            stage_copy(f).start()

        @pl.when(jnp.logical_not(is_ffn(i)))
        def _():
            a = i - cut
            fin[a, :half] = top.astype(bf16)
            fin[a, half:] = low.astype(bf16)
            z_sends(a, "start")

        for copy in one_copies(i) + two_copies(i):
            copy.wait_send()

    def back_norm(upstream, value, gain, base, col):
        inverse = lax.rsqrt(jnp.mean(value * value, axis=-1, keepdims=True) + EPSILON)
        unit = value * inverse
        scaled = upstream * gain
        term = jnp.sum(upstream * unit, axis=0, keepdims=True)
        small_ref[:, pl.ds(col, width)] += jnp.broadcast_to(term, (8, width))
        return base + inverse * (scaled - unit * jnp.mean(scaled * unit, axis=-1, keepdims=True))

    some_rows = max(16, chunk // 4)

    def by_rows(work):
        def some(r, carry):
            work(pl.ds(pl.multiple_of(r * some_rows, some_rows), some_rows))
            return carry

        lax.fori_loop(0, chunk // some_rows, some, 0)

    gain_one_at, gain_two_at = query_w + 2 * kv_w, query_w + 2 * kv_w + width

    def open_branch():
        for k in (0, 1, 2, 3):
            loads[k].wait()
        small_ref[...] = jnp.zeros_like(small_ref)

        def work(at):
            value = back_norm(
                up_v[at, :].astype(f32), mid_v[at, :], gain_v[1:2, :], own_v[at, :].astype(f32), gain_two_at
            )
            d_mid[at, :] = value
            lhs_ref[1, at, :] = value.astype(bf16)

        by_rows(work)

    def context_grads():
        loads[4].wait()
        tile = min(512, query_w)

        def some(n, carry):
            cols = pl.ds(pl.multiple_of(n * tile, tile), tile)
            d_ctx[:, cols] = jnp.dot(lhs_ref[1], w_v[:, cols], preferred_element_type=f32).astype(bf16)
            return carry

        lax.fori_loop(0, query_w // tile, some, 0)
        for copy in loads[-2:]:
            copy.start()
        for k in (5, 6, 7, 8, 9):
            loads[k].wait()
        d_win[...] = jnp.zeros_like(d_win)

    def turned_back(value):
        return value * turn_v[0] - pltpu.roll(value, HEAD_DIM // 2, 1) * turn_v[1]

    def attend_back(first, last):
        def head(h, carry):
            cols = pl.ds(pl.multiple_of(h * HEAD_DIM, 128), HEAD_DIM)
            group = h // (heads // KV_HEADS)
            key_cols = pl.ds(pl.multiple_of(group * HEAD_DIM, 128), HEAD_DIM)
            value_cols = pl.ds(pl.multiple_of(kv_w + group * HEAD_DIM, 128), HEAD_DIM)
            key = win_v[:, :, key_cols].reshape(3 * chunk, HEAD_DIM)
            value = win_v[:, :, value_cols].reshape(3 * chunk, HEAD_DIM)
            query, given = query_v[:, cols], d_ctx[:, cols]
            across, down = (((1,), (1,)), ((), ())), (((0,), (0,)), ((), ()))
            scores = lax.dot_general(query, key, across, preferred_element_type=f32)
            probs = jnp.exp(scores * scale + mask_v[...] - lse_v[h])
            d_probs = lax.dot_general(given, value, across, preferred_element_type=f32)
            delta = jnp.sum(probs * d_probs, axis=-1, keepdims=True)
            d_scores = (probs * (d_probs - delta)).astype(bf16)
            d_query = jnp.dot(d_scores, key, preferred_element_type=f32) * scale
            rhs_ref[:, cols] = turned_back(d_query).astype(bf16)
            d_key = lax.dot_general(d_scores, query, down, preferred_element_type=f32) * scale
            d_value = lax.dot_general(probs.astype(bf16), given, down, preferred_element_type=f32)
            d_win[:, :, key_cols] += d_key.reshape(3, chunk, HEAD_DIM)
            d_win[:, :, value_cols] += d_value.reshape(3, chunk, HEAD_DIM)
            return carry

        lax.fori_loop(first, last, head, 0)

    def give_copy(hop):
        return z_copy(
            kv_give.at[hop - 1], kv_take.at[hop - 1], give_send.at[hop - 1], give_recv.at[hop - 1], z - hop
        )

    def give():
        for hop in (1, 2):

            @pl.when(z >= hop)
            def _(hop=hop):
                kv_give[hop - 1] = d_win[2 - hop].astype(bf16)
                give_copy(hop).start()

    def take():
        for hop in (1, 2):

            @pl.when(z + hop < size)
            def _(hop=hop):
                pltpu.make_async_copy(kv_take.at[hop - 1], kv_take.at[hop - 1], give_recv.at[hop - 1]).wait()
                d_win[2] += kv_take[hop - 1].astype(f32)

        for g in range(KV_HEADS):
            cols = slice(g * HEAD_DIM, (g + 1) * HEAD_DIM)
            out_cols = slice(2 * query_w + g * HEAD_DIM, 2 * query_w + (g + 1) * HEAD_DIM)
            rhs_ref[:, out_cols] = turned_back(d_win[2, :, cols]).astype(bf16)
        rhs_ref[:, 2 * query_w + kv_w : 2 * query_w + 2 * kv_w] = d_win[2, :, kv_w:].astype(bf16)
        ones = jnp.ones((8, chunk), bf16)
        small_ref[:, :query_w] = jnp.dot(ones, rhs_ref[:, :query_w], preferred_element_type=f32)
        small_ref[:, query_w : query_w + 2 * kv_w] = jnp.dot(
            ones, rhs_ref[:, 2 * query_w : 2 * query_w + 2 * kv_w], preferred_element_type=f32
        )

    def one_grads():
        loads[-1].wait()
        tile = min(512, width)
        across = (((1,), (1,)), ((), ()))

        def some(n, carry):
            at_n = pl.ds(pl.multiple_of(n * tile, tile), tile)
            d_win[n] = lax.dot_general(
                rhs_ref[:, :query_w], w_v[at_n, 2 * kv_w :], across, preferred_element_type=f32
            ) + lax.dot_general(
                rhs_ref[:, 2 * query_w : 2 * query_w + 2 * kv_w], w_v[at_n, : 2 * kv_w], across,
                preferred_element_type=f32,
            )
            return carry

        lax.fori_loop(0, width // tile, some, 0)

    def close_branch():
        loads[-2].wait()

        def work(at):
            input_out[at, :] = back_norm(
                jnp.concatenate([d_win[n, at, :] for n in range(width // d_win.shape[2])], axis=1), up_v[at, :].astype(f32), gain_v[0:1, :], d_mid[at, :], gain_one_at
            ).astype(bf16)

        by_rows(work)
        for copy in small_copies:
            copy.start()

    def small_first():
        for copy in small_copies:
            copy.wait_recv()
        small_next[0] = small_ref[...] + small_z[0] + small_z[1] + small_z[2]
        hop_copy(0).start()

    def small_then(k):
        hop_copy(k).wait_recv()
        small_next[k + 1] = small_next[k] + small_hop[k]
        hop_copy(k + 1).start()

    def small_last():
        hop_copy(2).wait_recv()
        small_out[...] = small_next[2] + small_hop[2]

    span = cut - 1
    quarter = heads // 4

    def at_turn(k):
        return min(k, span)

    steps = [
        (0, open_branch), (at_turn(1), context_grads),
        (at_turn(2), lambda: attend_back(0, quarter)),
        (at_turn(3), lambda: attend_back(quarter, 2 * quarter)),
        (at_turn(4), lambda: attend_back(2 * quarter, 3 * quarter)),
        (at_turn(5), lambda: attend_back(3 * quarter, heads)),
        (at_turn(5), give),
        (at_turn(3), lambda: fold(0)), (at_turn(5), lambda: fold(1)), (at_turn(8), lambda: fold(2)),
        (at_turn(7), take), (at_turn(7), lambda: [loads[k].wait() for k in (10, 11)]),
        (n_ffn + 1, one_grads), (n_ffn + 2, close_branch),
        (n_ffn + 4, small_first), (n_ffn + 5, lambda: small_then(0)), (n_ffn + 6, lambda: small_then(1)),
        (n_ffn + 7, small_last),
    ]

    def small_step(i):
        for when, step in steps:

            @pl.when(i == when)
            def _(step=step):
                step()

    def turn(i, carry):
        multiply(i)
        for lag, work in ((1, sum_cores), (2, sum_near), (3, finish)):

            @pl.when(jnp.logical_and(i >= lag, i - lag < total))
            def _(lag=lag, work=work):
                work(i - lag)

        small_step(i)
        return carry

    lax.fori_loop(0, total + 3, turn, 0)
    for i in range(total - n_grad, total):
        mate_copy(i).wait_send()
    for i in (n_ffn - 2, n_ffn - 1):
        stage_copy(i).wait()
    fold_load(z).wait()
    mid_v[...] += fold_own[...].astype(f32)

    @pl.when(middle)
    def _():
        pltpu.make_async_copy(fold_last.at[0], fold_last.at[0], last_recv.at[0]).wait()
        mid_v[...] += fold_last[0].astype(f32)

    pltpu.make_async_copy(fold_last.at[1], fold_last.at[1], last_recv.at[1]).wait()
    mixed_out[...] = (mid_v[...] + fold_last[1].astype(f32)).astype(bf16)
    for k in range(3):
        pltpu.make_async_copy(fold_land.at[k], fold_land.at[k], fold_send.at[k]).wait()
    for of, dst in ((0, query_out), (1, out_out)):
        for k in range(size - 1):
            ref = z_land.at[of, k]
            pltpu.make_async_copy(ref, ref, z_recv.at[of, k]).wait()
        for h in range(4):

            @pl.when(z == h)
            def _(of=of, dst=dst, h=h):
                acc = fin[2 * of + h // 2, :, (h % 2) * part_w : (h % 2 + 1) * part_w].astype(f32)
                for k in range(size - 1):
                    acc += z_land[of, k].astype(f32)
                dst[...] = acc

    for k in range(size - 1):
        pltpu.make_async_copy(kv_land.at[k], kv_land.at[k], kv_recv.at[k]).wait()
    rows = pl.ds(pl.multiple_of(z * share, 16), share)
    acc = fin[4, rows, :].astype(f32)
    for k in range(size - 1):
        acc += kv_land[k].astype(f32)
    kv_out[...] = acc
    for a in range(n_att):
        z_sends(a, "wait")
    for copy in small_copies:
        copy.wait_send()
    for k in range(3):
        hop_copy(k).wait_send()
    for hop in (1, 2):

        @pl.when(z >= hop)
        def _(hop=hop):
            give_copy(hop).wait_send()


def back(
    two, cot_rows, hid, dg, du, ffn_part, up, tokens, middle, gains, att_w, query_rot, kv_win, lse, context,
    normed_one, mask, turn, wide=768, collective_id=3, limit=67_000_000,
):
    length, width = two.shape
    size, chunk, block = 4, tokens.shape[0], width // 8
    units, query_w, kv_w = hid.shape[1], context.shape[1], kv_win.shape[2]
    n_f, n_att = units // wide, (2 * query_w + wide) // wide
    total = 3 * n_f + n_att
    half, part_w, share = block // 2, wide // 2, block // size
    heads = lse.shape[0]
    bf16, f32 = jnp.bfloat16, jnp.float32
    small = (8, query_w + kv_w + 2 * width)
    ring = 5
    hbm = pl.BlockSpec(memory_space=pl.ANY)
    vmem = pl.BlockSpec(memory_space=pltpu.VMEM)
    vm = pltpu.VMEM
    dma = pltpu.SemaphoreType.DMA
    shape = jax.ShapeDtypeStruct
    return pl.pallas_call(
        functools.partial(back_body, n_f=n_f, wide=wide),
        out_shape=(
            shape((block, 3 * units), f32), shape((block, part_w), f32), shape((block, part_w), f32),
            shape((share, wide), f32), shape((chunk, width), bf16), shape((chunk, width), bf16),
            shape(small, f32),
        ),
        in_specs=[hbm] * 18,
        out_specs=(hbm,) + (vmem,) * 6,
        scratch_shapes=[
            vm((chunk, width), bf16), vm((chunk, width), bf16),
            vm((chunk, width), f32), vm(gains.shape, f32), vm((width, kv_w + query_w), bf16),
            vm((chunk, query_w), bf16), vm(kv_win.shape, bf16), vm((heads, chunk, 1), f32),
            vm(mask.shape, f32), vm(turn.shape, f32), vm((2, chunk, width), bf16),
            vm((chunk, 2 * query_w + wide), bf16), vm((chunk, width), f32), vm((chunk, query_w), bf16),
            vm(kv_win.shape, f32), vm((2, chunk, kv_w), bf16), vm((2, chunk, kv_w), bf16),
            vm(small, f32),
            vm((length, width), bf16), vm((2, length, wide), bf16), vm((2, 4, 2, block, wide), bf16),
            vm((4, 4, block, wide), bf16), vm((4, 4, block, wide), bf16),
            vm((ring, 2, half, wide), bf16), vm((ring, 2, half, wide), bf16),
            vm((2, 2, half, wide), bf16), vm((4, half, wide), bf16), vm((4, half, wide), bf16),
            vm((2, block, wide), f32), vm((n_att, block, wide), bf16),
            vm((2, size - 1, block, part_w), bf16), vm((size - 1, share, wide), bf16),
            vm((3, chunk, width), bf16), vm((2, chunk, width), bf16), vm((chunk, width), bf16), vm((3,) + small, f32), vm((3,) + small, f32),
            vm((3,) + small, f32), dma((14,)), dma((2,)), dma((2,)),
            dma((2,)), dma((2,)), dma((6,)), dma((6,)), dma((4, ring)), dma((4, ring)),
            dma((2, ring)), dma((2, ring)), dma((2,)),
            dma((4, 2)), dma((2, size - 1)), dma((size - 1,)), dma((size - 1,)), dma((3,)),
            dma((3,)), dma((2,)), dma((1,)), dma((size - 1,)), dma((size - 1,)), dma((3,)), dma((3,)),
        ],
        compiler_params=pltpu.CompilerParams(
            collective_id=collective_id, has_side_effects=True, vmem_limit_bytes=limit
        ),
        cost_estimate=pl.CostEstimate(
            flops=6 * length * width * units, bytes_accessed=8 * length * units, transcendentals=0
        ),
        name="back",
    )(
        two, cot_rows, hid, dg, du, ffn_part, up, tokens, middle, gains, att_w, query_rot, kv_win, lse, context,
        normed_one, mask, turn,
    )


def angle_tables(first, length, head_width):
    position = (first + jnp.arange(length)).astype(jnp.float32)
    exponent = jnp.arange(head_width // 2, dtype=jnp.float32) * (2.0 / head_width)
    frequency = ROPE_BASE ** (-exponent)
    angle = position[:, None] * frequency[None, :]
    return (jnp.cos(angle), jnp.sin(angle))


def rotate(values, cosine, sine):
    half_width = values.shape[-1] // 2
    first_half = values[..., :half_width]
    second_half = values[..., half_width:]
    return jnp.concatenate(
        [first_half * cosine - second_half * sine, second_half * cosine + first_half * sine],
        axis=-1,
    )


def rotate_back(grads, cosine, sine):
    return rotate(grads, cosine, -sine)


def dot_f32(left, right, dims):
    return lax.dot_general(left, right, (dims, ((), ())), preferred_element_type=jnp.float32)


def contract_rows(left, right):
    return dot_f32(left, right, ((0,), (0,)))


def contract_cols(left, right):
    return dot_f32(left, right, ((1,), (1,)))


def norm_back(upstream, unit, inverse, gain):
    scaled = upstream * gain
    gain_term = jnp.sum(upstream * unit, axis=0)
    input_term = inverse * (scaled - unit * jnp.mean(scaled * unit, axis=-1, keepdims=True))
    return (gain_term, input_term)


def joined_units(gate_w, up_w, down_w):
    units = gate_w.shape[1]
    gap = -(-units // 768) * 768 - units
    wide = lambda w: jnp.pad(w, ((0, 0), (0, gap)))
    return jnp.concatenate([wide(gate_w), wide(up_w), wide(down_w)], axis=1)


def attention_branch(tokens, cosine, sine, mask, gains_w, query_w, query_b, kv_w, kv_b, out_w, ffn_w, cotangent):
    f32, bf16 = jnp.float32, jnp.bfloat16
    rows = tokens.shape[0]
    size = lax.axis_size("tensor")
    fixed_w = jnp.concatenate([gains_w, kv_w], axis=1)
    if lax.axis_size("dp") == 8 and size == 4:
        last = jnp.concatenate([query_b, jnp.zeros((query_b.shape[0] + gains_w.shape[1],), bf16), kv_b])
        own = jnp.concatenate(
            [jnp.concatenate([query_w, out_w, fixed_w], axis=1), jnp.pad(last[None, :], ((0, 15), (0, 0)))], axis=0
        )
        turn = jnp.stack(
            [jnp.concatenate([cosine, cosine], axis=1), jnp.concatenate([-sine, sine], axis=1)]
        )
        att_w, ffn_all, cot_rows, two, middle, one, query_rot, kv_win, lse, context, gains = front(
            tokens, turn, mask, own, ffn_w, cotangent, fixed_w.shape[1]
        )
        kv_win = kv_win.reshape(3 * rows, kv_w.shape[1])
        return att_w, ffn_all, cot_rows, two, middle, one, query_rot, kv_win, lse, context, gains
    pair = lax.all_gather(jnp.stack([query_w, out_w]), "tensor", axis=2, tiled=True)
    att_w = jnp.concatenate([fixed_w, pair[0], pair[1]], axis=1)
    att_w = lax.all_gather(att_w, "dp", axis=0, tiled=True)
    ffn_all = lax.all_gather(ffn_w, "dp", axis=0, tiled=True)
    cot_rows = lax.all_gather(cotangent, "tensor", axis=0, tiled=True)
    full_query_b = lax.all_gather(query_b, "tensor", axis=0, tiled=True).astype(f32)
    ahead = gains_w.shape[1]
    kv_width = kv_w.shape[1] // 2
    qkv_width = 2 * kv_width + full_query_b.shape[0]
    heads = full_query_b.shape[0] // HEAD_DIM
    gains = att_w[:, :2].T.astype(f32)
    inputs = tokens.astype(f32)
    inverse = lax.rsqrt(jnp.mean(inputs * inputs, axis=-1, keepdims=True) + EPSILON)
    one = (inputs * inverse * gains[0]).astype(bf16)
    lin = jnp.dot(one, att_w[:, ahead : ahead + qkv_width], preferred_element_type=f32)
    lin = lin + jnp.concatenate([kv_b.astype(f32), full_query_b])
    cos_h, sin_h = cosine[:, None, :], sine[:, None, :]
    query_rot = rotate(lin[:, 2 * kv_width :].reshape(rows, heads, HEAD_DIM), cos_h, sin_h).astype(bf16)
    key_rot = rotate(lin[:, :kv_width].reshape(rows, KV_HEADS, HEAD_DIM), cos_h, sin_h).astype(bf16)
    kv_own = jnp.concatenate(
        [key_rot.reshape(rows, kv_width), lin[:, kv_width : 2 * kv_width].astype(bf16)], axis=1
    )
    back_chunks = mask.shape[1] // rows - 1
    kv_win = jnp.concatenate(
        [shift(kv_own, hops) for hops in range(back_chunks, 0, -1)] + [kv_own], axis=0
    )
    window = kv_win.shape[0]
    key_win = kv_win[:, :kv_width].reshape(window, KV_HEADS, HEAD_DIM)
    value_win = kv_win[:, kv_width:].reshape(window, KV_HEADS, HEAD_DIM)
    grouped = query_rot.reshape(rows, KV_HEADS, heads // KV_HEADS, HEAD_DIM)
    scores = jnp.einsum("tagd,sad->agts", grouped, key_win, preferred_element_type=f32)
    scores = scores * HEAD_DIM ** (-0.5) + mask
    largest = jnp.max(scores, axis=-1, keepdims=True)
    lse = largest + jnp.log(jnp.sum(jnp.exp(scores - largest), axis=-1, keepdims=True))
    probs = jnp.exp(scores - lse).astype(bf16)
    context = jnp.einsum("agts,sad->tagd", probs, value_win, preferred_element_type=f32)
    context = context.reshape(rows, heads * HEAD_DIM).astype(bf16)
    middle = inputs + contract_cols(context, att_w[:, ahead + qkv_width :])
    inverse = lax.rsqrt(jnp.mean(middle * middle, axis=-1, keepdims=True) + EPSILON)
    two = (middle * inverse * gains[1]).astype(bf16)
    two = lax.all_gather(two, "tensor", axis=0, tiled=True)
    query_rot = query_rot.reshape(rows, heads * HEAD_DIM)
    return att_w, ffn_all, cot_rows, two, middle, one, query_rot, kv_win, lse, context, gains


def shift(value, hops):
    size = lax.axis_size("tensor")
    pairs = [(i, i + hops) for i in range(size) if 0 <= i + hops < size]
    return lax.ppermute(value, "tensor", pairs)


def sum_grads(two, cot_rows, hid, dg, du, normed_one, d_attended, d_lin, context, ffn_part, small):
    f32, bf16 = jnp.float32, jnp.bfloat16
    fixed = d_lin.shape[1] - context.shape[1]
    d_query = d_lin[:, fixed:]
    def over_dp(left, right):
        return lax.psum_scatter(
            contract_rows(left, right).astype(bf16), "dp", scatter_dimension=0, tiled=True
        )

    def over_tensor(value, axis):
        return lax.psum_scatter(value, "tensor", scatter_dimension=axis, tiled=True).astype(f32)

    return (
        over_dp(cot_rows, hid).astype(f32),
        over_dp(two, dg).astype(f32),
        over_dp(two, du).astype(f32),
        over_tensor(over_dp(normed_one, d_query), 1),
        over_tensor(over_dp(d_attended, context), 1),
        over_tensor(over_dp(normed_one, d_lin[:, :fixed]), 0),
        over_tensor(ffn_part, 0),
        lax.psum(small, ("dp", "tensor")),
    )


def branch_back(
    tokens, cosine, sine, mask, att_w, cot_rows, rows_two, hidden_low, d_gate, d_upper, ffn_part,
    d_normed_two, cotangent, middle, normed_one, query_rot, kv_win, lse, context, gains,
):
    f32, bf16 = jnp.float32, jnp.bfloat16
    rows = tokens.shape[0]
    kv_width, query_width = kv_win.shape[1] // 2, query_rot.shape[1]
    qkv_width = 2 * kv_width + query_width
    ahead = att_w.shape[1] - qkv_width - query_width
    heads, padded = query_width // HEAD_DIM, hidden_low.shape[1]
    if lax.axis_size("dp") == 8 and lax.axis_size("tensor") == 4:
        turn = jnp.stack(
            [jnp.concatenate([cosine, cosine], axis=1), jnp.concatenate([-sine, sine], axis=1)]
        )
        flat, sum_query, sum_out, sum_kv, mixed, input_grad, small = back(
            rows_two, cot_rows, hidden_low, d_gate, d_upper, ffn_part, d_normed_two, tokens, middle, gains,
            att_w, query_rot, kv_win.reshape(-1, rows, 2 * kv_width), lse, context, normed_one, mask, turn,
        )
        flat = [flat[:, k * padded : (k + 1) * padded] for k in range(3)]
        return mixed, input_grad, *flat, sum_query, sum_out, sum_kv, small[0]
    group = heads // KV_HEADS
    window = kv_win.shape[0]
    back_chunks = window // rows - 1
    scale = HEAD_DIM ** (-0.5)
    cos_h, sin_h = cosine[:, None, :], sine[:, None, :]
    d_normed_two = d_normed_two.astype(f32)
    qkv_w = att_w[:, ahead : ahead + qkv_width]
    out_full = att_w[:, ahead + qkv_width :]
    inputs = tokens.astype(f32)
    inverse_one = lax.rsqrt(jnp.mean(inputs * inputs, axis=-1, keepdims=True) + EPSILON)
    unit_one = inputs * inverse_one
    inverse_two = lax.rsqrt(jnp.mean(middle * middle, axis=-1, keepdims=True) + EPSILON)
    unit_two = middle * inverse_two
    gain_two_term, d_from_two = norm_back(d_normed_two, unit_two, inverse_two, gains[1])
    d_middle = cotangent.astype(f32) + d_from_two
    d_attended = d_middle.astype(bf16)
    d_context = jnp.dot(d_attended, out_full, preferred_element_type=f32).astype(bf16)
    d_context = d_context.reshape(rows, KV_HEADS, group, HEAD_DIM)
    key_win = kv_win[:, :kv_width].reshape(window, KV_HEADS, HEAD_DIM)
    value_win = kv_win[:, kv_width:].reshape(window, KV_HEADS, HEAD_DIM)
    grouped = query_rot.reshape(rows, KV_HEADS, group, HEAD_DIM)
    scores = jnp.einsum("tagd,sad->agts", grouped, key_win, preferred_element_type=f32) * scale + mask
    probs = jnp.exp(scores - lse.reshape(KV_HEADS, group, rows, 1))
    probs_low = probs.astype(bf16)
    d_probs = jnp.einsum("tagd,sad->agts", d_context, value_win, preferred_element_type=f32)
    row_delta = jnp.sum(probs * d_probs, axis=-1, keepdims=True)
    d_scores = (probs * (d_probs - row_delta)).astype(bf16)
    d_query_rot = jnp.einsum("agts,sad->tagd", d_scores, key_win, preferred_element_type=f32) * scale
    d_key_win = jnp.einsum("agts,tagd->sad", d_scores, grouped, preferred_element_type=f32) * scale
    d_value_win = jnp.einsum("agts,tagd->sad", probs_low, d_context, preferred_element_type=f32)
    d_query_lin = (
        rotate_back(d_query_rot.reshape(rows, heads, HEAD_DIM), cos_h, sin_h)
        .reshape(rows, query_width).astype(bf16)
    )
    d_kv_win = jnp.concatenate(
        [d_key_win.reshape(window, kv_width), d_value_win.reshape(window, kv_width)], axis=1
    ).astype(bf16)
    d_kv = d_kv_win[back_chunks * rows :].astype(f32)
    for hops in range(1, back_chunks + 1):
        given = d_kv_win[(back_chunks - hops) * rows : (back_chunks - hops + 1) * rows]
        d_kv = d_kv + shift(given, -hops).astype(f32)
    d_key_lin = rotate_back(d_kv[:, :kv_width].reshape(rows, KV_HEADS, HEAD_DIM), cos_h, sin_h)
    d_lin = jnp.concatenate(
        [d_key_lin.reshape(rows, kv_width).astype(bf16), d_kv[:, kv_width:].astype(bf16), d_query_lin],
        axis=1,
    )
    d_normed_one = contract_cols(d_lin, qkv_w)
    bias_term = jnp.sum(d_lin.astype(f32), axis=0)
    gain_one_term, d_from_one = norm_back(d_normed_one, unit_one, inverse_one, gains[0])
    input_grad = (d_middle + d_from_one).astype(bf16)

    sums = sum_grads(
        rows_two, cot_rows, hidden_low, d_gate, d_upper, normed_one, d_attended, d_lin, context,
        ffn_part, jnp.concatenate([bias_term[2 * kv_width :], bias_term[: 2 * kv_width], gain_one_term, gain_two_term]),
    )
    sum_down, sum_gate, sum_up, sum_query, sum_out, sum_kv, ffn_sum, small = sums
    mixed = (middle + ffn_sum.astype(f32)).astype(bf16)
    return mixed, input_grad, sum_down, sum_gate, sum_up, sum_query, sum_out, sum_kv, small


def local(
    tokens, segments, gain_one, query_w, query_b, key_w, key_b, value_w, value_b,
    out_w, gain_two, gate_w, up_w, down_w, cotangent,
):
    bf16, f32 = jnp.bfloat16, jnp.float32
    rows, model_width = tokens.shape
    tensor_size = lax.axis_size("tensor")
    rank = lax.axis_index("tensor")
    kv_width = key_w.shape[1]
    fixed_width = 2 * kv_width
    query_width = query_w.shape[1] * tensor_size
    qkv_width = fixed_width + query_width
    units = gate_w.shape[1]
    back_chunks = min(tensor_size - 1, -(-DOC_MAX // rows))
    window = (back_chunks + 1) * rows
    cosine, sine = angle_tables(rank * rows, rows, HEAD_DIM)
    segment = segments[0]
    own_segment = lax.dynamic_slice_in_dim(segment, rank * rows, rows, 0)
    before = jnp.full((back_chunks * rows,), -1, segment.dtype)
    win_segment = lax.dynamic_slice_in_dim(jnp.concatenate([before, segment]), rank * rows, window, 0)
    own_pos = back_chunks * rows + jnp.arange(rows)
    win_pos = jnp.arange(window)
    allowed = (own_segment[:, None] == win_segment[None, :]) & (win_pos[None, :] <= own_pos[:, None])
    mask = jnp.where(allowed, 0.0, NEGATIVE).astype(f32)
    ahead = 128
    gains_w = jnp.pad(jnp.stack([gain_one, gain_two], axis=1), ((0, 0), (0, ahead - 2)))
    (
        att_w, ffn_w, cot_rows, normed_two, middle, normed_one, query_rot, kv_win, lse, context, gains,
    ) = attention_branch(
        tokens, cosine, sine, mask, gains_w, query_w, query_b, jnp.concatenate([key_w, value_w], axis=1),
        jnp.concatenate([key_b, value_b]), out_w, joined_units(gate_w, up_w, down_w), cotangent,
    )
    rows_two, hidden_low, d_gate, d_upper, ffn_part, d_normed_two = ffn(
        normed_two, cot_rows, ffn_w
    )
    mixed, input_grad, sum_down, sum_gate, sum_up, sum_query, sum_out, sum_kv, small = branch_back(
        tokens, cosine, sine, mask, att_w, cot_rows, rows_two, hidden_low, d_gate, d_upper, ffn_part,
        d_normed_two, cotangent, middle, normed_one, query_rot, kv_win, lse, context, gains,
    )
    place = lax.axis_index("dp") * tensor_size + rank
    devices = lax.axis_size("dp") * tensor_size

    def own(start, size):
        share = size // devices
        return lax.dynamic_slice_in_dim(small, start + place * share, share, 0)

    return (
        mixed,
        input_grad,
        own(qkv_width, model_width),
        sum_query,
        own(0, query_width),
        sum_kv[:, :kv_width],
        small[query_width : query_width + kv_width],
        sum_kv[:, kv_width : 2 * kv_width],
        small[query_width + kv_width : qkv_width],
        sum_out,
        own(qkv_width + model_width, model_width),
        sum_gate[:, :units],
        sum_up[:, :units],
        sum_down[:, :units],
    )


def solution(mesh):
    both = ("dp", "tensor")
    return jax.shard_map(
        local,
        mesh=mesh,
        in_specs=(
            P(both, None), P("dp", None), P("dp"), P("dp", "tensor"), P("tensor"), P("dp", None), P(),
            P("dp", None), P(), P("dp", "tensor"), P("dp"), P("dp", "tensor"), P("dp", "tensor"),
            P("dp", "tensor"), P(both, None),
        ),
        out_specs=(
            P(both, None), P(both, None), P(both), P("dp", "tensor"), P(both), P(both, None), P(),
            P(both, None), P(), P("dp", "tensor"), P(both), P("dp", "tensor"), P("dp", "tensor"),
            P("dp", "tensor"),
        ),
        check_vma=False,
    )
```
